32 devices in a mesh: dp: 1 (over z), tp: 4 (over y), ep: 8 (over x, core).
Axes of the slice: x: 4, y: 4, z: 1, core: 2. Of those that a mesh axis runs over, the one named last changes fastest.
The devices are a block of a 4x4x8 slice.
Arguments:
- x: bfloat16 [64, 1024, 768], P(('dp', 'ep'))
- src_len: int32 [64], P(('dp', 'ep'))
- expert_idx: int32 [64, 1024, 2], P(('dp', 'ep'))
- ln_gain: float32 [4, 768], replicated
- ln_bias: float32 [4, 768], replicated
- w_query: bfloat16 [2, 768, 12, 64], P(None, None, 'tp')
- b_query: float32 [2, 12, 64], P(None, 'tp')
- w_key: bfloat16 [2, 768, 12, 64], P(None, None, 'tp')
- w_value: bfloat16 [2, 768, 12, 64], P(None, None, 'tp')
- b_value: float32 [2, 12, 64], P(None, 'tp')
- w_attn_out: bfloat16 [2, 12, 64, 768], P(None, 'tp')
- b_attn_out: float32 [2, 768], replicated
- w_fc1: bfloat16 [768, 3072], P(None, 'tp')
- b_fc1: float32 [3072], P('tp')
- w_fc2: bfloat16 [3072, 768], P('tp')
- b_fc2: float32 [768], replicated
- w_router: float32 [768, 128], replicated
- w_exp_in: bfloat16 [128, 768, 3072], P('ep', None, 'tp')
- b_exp_in: float32 [128, 3072], P('ep', 'tp')
- w_exp_out: bfloat16 [128, 3072, 768], P('ep', 'tp')
- b_exp_out: float32 [128, 768], P('ep')
Outputs:
- output: bfloat16 [64, 1024, 768], P(('dp', 'ep'))
All inputs are finite; a program needn't handle non-finite values.
Results may differ from the reference program's by a relative error of at most 0.0144607.
Values are sent between devices in bfloat16 or wider.
A program may use at most 768 MiB of HBM per device.

```python
import jax
import jax.numpy as jnp
from jax import lax

GROUPS = 8
ROWS_DEV = 8
SEQ_LEN = 1024
D_MODEL = 768
NUM_HEADS = 12
HEAD_DIM = 64
FF_DENSE = 3072
EXPERTS = 128
EXPERT_FF = 3072

BATCH = GROUPS * ROWS_DEV
TOKENS_GROUP = ROWS_DEV * SEQ_LEN
CAPACITY = 2 * ((TOKENS_GROUP + EXPERTS - 1) // EXPERTS)
DUMP_SLOT = EXPERTS * CAPACITY
INNER_DIM = NUM_HEADS * HEAD_DIM
LN_EPS = 1e-5


def layer_norm(hidden, gain, shift):
    hidden = hidden.astype(jnp.float32)
    centered = hidden - jnp.mean(hidden, axis=-1, keepdims=True)
    variance = jnp.mean(centered * centered, axis=-1, keepdims=True)
    return centered * lax.rsqrt(variance + LN_EPS) * gain + shift


def draw_routing(route_key):
    len_key, hot_key, pick_key, first_key, second_key = jax.random.split(route_key, 5)
    row_ids = jnp.arange(BATCH)
    lengths = jax.random.randint(len_key, (BATCH,), SEQ_LEN // 4, SEQ_LEN + 1)
    lengths = jnp.where(row_ids == 0, SEQ_LEN, lengths)
    lengths = jnp.where(row_ids == BATCH - 1, SEQ_LEN // 4, lengths)
    hot_count = max(EXPERTS // 16, 1)
    hot_start = jax.random.randint(hot_key, (), 0, EXPERTS)
    grid = (BATCH, SEQ_LEN)
    pick_hot = jax.random.randint(pick_key, grid, 0, 4) == 0
    uniform_first = jax.random.randint(first_key, grid, 0, EXPERTS)
    hot_first = (hot_start + uniform_first % hot_count) % EXPERTS
    first = jnp.where(pick_hot, hot_first, uniform_first)
    second = (first + jax.random.randint(second_key, grid, 1, EXPERTS)) % EXPERTS
    expert_idx = jnp.stack([first, second], axis=-1).astype(jnp.int32)
    return lengths.astype(jnp.int32), expert_idx


def scaled_normal(key, extent, scale):
    return jax.random.normal(key, extent, jnp.float32) * scale


def setup_inputs(seed: int = 0, part: int = 0) -> dict:
    part_key = jax.random.fold_in(jax.random.key(seed), part)
    x_key, route_key = jax.random.split(part_key, 2)
    keys = jax.random.split(jax.random.key(seed + 1), 18)
    src_len, expert_idx = draw_routing(route_key)
    attn_shape = (2, D_MODEL, NUM_HEADS, HEAD_DIM)
    model_scale = D_MODEL ** -0.5
    inner_scale = INNER_DIM ** -0.5
    return {
        'x': scaled_normal(x_key, (BATCH, SEQ_LEN, D_MODEL), 1.0).astype(jnp.bfloat16),
        'src_len': src_len,
        'expert_idx': expert_idx,
        'ln_gain': 1.0 + scaled_normal(keys[0], (4, D_MODEL), 0.2),
        'ln_bias': scaled_normal(keys[1], (4, D_MODEL), 0.2),
        'w_query': scaled_normal(keys[2], attn_shape, model_scale).astype(jnp.bfloat16),
        'b_query': scaled_normal(keys[3], (2, NUM_HEADS, HEAD_DIM), 0.5),
        'w_key': scaled_normal(keys[4], attn_shape, model_scale).astype(jnp.bfloat16),
        'w_value': scaled_normal(keys[5], attn_shape, model_scale).astype(jnp.bfloat16),
        'b_value': scaled_normal(keys[6], (2, NUM_HEADS, HEAD_DIM), 0.5),
        'w_attn_out': scaled_normal(keys[7], (2, NUM_HEADS, HEAD_DIM, D_MODEL), inner_scale).astype(jnp.bfloat16),
        'b_attn_out': scaled_normal(keys[8], (2, D_MODEL), 0.3),
        'w_fc1': scaled_normal(keys[9], (D_MODEL, FF_DENSE), model_scale).astype(jnp.bfloat16),
        'b_fc1': scaled_normal(keys[10], (FF_DENSE,), 0.5),
        'w_fc2': scaled_normal(keys[11], (FF_DENSE, D_MODEL), FF_DENSE ** -0.5).astype(jnp.bfloat16),
        'b_fc2': scaled_normal(keys[12], (D_MODEL,), 0.3),
        'w_router': scaled_normal(keys[13], (D_MODEL, EXPERTS), model_scale),
        'w_exp_in': scaled_normal(keys[14], (EXPERTS, D_MODEL, EXPERT_FF), model_scale).astype(jnp.bfloat16),
        'b_exp_in': scaled_normal(keys[15], (EXPERTS, EXPERT_FF), 0.5),
        'w_exp_out': scaled_normal(keys[16], (EXPERTS, EXPERT_FF, D_MODEL), EXPERT_FF ** -0.5).astype(jnp.bfloat16),
        'b_exp_out': scaled_normal(keys[17], (EXPERTS, D_MODEL), 0.5),
    }


def attention_row(residual, key_ok, gain, shift, w_q, b_q, w_k, w_v, b_v, w_o, b_o):
    normed = layer_norm(residual, gain, shift).astype(jnp.bfloat16)

    def project(weight):
        flat = jnp.dot(normed, weight.reshape(D_MODEL, INNER_DIM), preferred_element_type=jnp.float32)
        return flat.reshape(SEQ_LEN, NUM_HEADS, HEAD_DIM)

    query = (project(w_q) + b_q).astype(jnp.bfloat16)
    keys = project(w_k).astype(jnp.bfloat16)
    values = (project(w_v) + b_v).astype(jnp.bfloat16)
    scores = jnp.einsum('qhk,shk->hqs', query.astype(jnp.float32), keys.astype(jnp.float32)) * (HEAD_DIM ** -0.5)
    scores = jnp.where(key_ok[None, None, :], scores, -1e30)
    attn_probs = jax.nn.softmax(scores, axis=-1).astype(jnp.bfloat16)
    context = jnp.einsum('hqs,shk->qhk', attn_probs.astype(jnp.float32), values.astype(jnp.float32)).astype(jnp.bfloat16)
    projected = jnp.dot(context.reshape(SEQ_LEN, INNER_DIM), w_o.reshape(INNER_DIM, D_MODEL), preferred_element_type=jnp.float32)
    return (residual.astype(jnp.float32) + projected + b_o).astype(jnp.bfloat16)


def dense_ffn(residual, gain, shift, w_in, b_in, w_out, b_out):
    normed = layer_norm(residual, gain, shift).astype(jnp.bfloat16)
    inner = jax.nn.relu(jnp.dot(normed, w_in, preferred_element_type=jnp.float32) + b_in).astype(jnp.bfloat16)
    projected = jnp.dot(inner, w_out, preferred_element_type=jnp.float32)
    return (residual.astype(jnp.float32) + projected + b_out).astype(jnp.bfloat16)


def take_rows(rows, index):
    return rows[index]


def fill_table(dest_first, dest_second):
    token_ids = jnp.arange(TOKENS_GROUP, dtype=jnp.int32)
    table = jnp.full((DUMP_SLOT + 1,), TOKENS_GROUP, jnp.int32)
    table = table.at[dest_first].set(token_ids).at[dest_second].set(token_ids)
    return table[:DUMP_SLOT]


def run_expert(operands):
    rows_in, w_in, b_in, w_out, b_out = operands
    inner = jax.nn.relu(jnp.dot(rows_in, w_in, preferred_element_type=jnp.float32) + b_in).astype(jnp.bfloat16)
    return (jnp.dot(inner, w_out, preferred_element_type=jnp.float32) + b_out).astype(jnp.bfloat16)


def reference(x, src_len, expert_idx, ln_gain, ln_bias, w_query, b_query, w_key, w_value, b_value, w_attn_out, b_attn_out, w_fc1, b_fc1, w_fc2, b_fc2, w_router, w_exp_in, b_exp_in, w_exp_out, b_exp_out):
    positions = jnp.arange(SEQ_LEN)

    def row_layers(row_pair):
        row, length = row_pair
        key_ok = positions < length
        hidden = attention_row(row, key_ok, ln_gain[0], ln_bias[0], w_query[0], b_query[0], w_key[0], w_value[0], b_value[0], w_attn_out[0], b_attn_out[0])
        hidden = dense_ffn(hidden, ln_gain[1], ln_bias[1], w_fc1, b_fc1, w_fc2, b_fc2)
        hidden = attention_row(hidden, key_ok, ln_gain[2], ln_bias[2], w_query[1], b_query[1], w_key[1], w_value[1], b_value[1], w_attn_out[1], b_attn_out[1])
        normed = layer_norm(hidden, ln_gain[3], ln_bias[3])
        logits = jnp.dot(normed, w_router, preferred_element_type=jnp.float32)
        return hidden, normed.astype(jnp.bfloat16), logits

    residual, normed, logits = lax.map(row_layers, (x, src_len))
    grouped = (GROUPS, TOKENS_GROUP)
    valid = (positions[None, :] < src_len[:, None]).reshape(grouped)
    first = expert_idx[..., 0].reshape(grouped)
    second = expert_idx[..., 1].reshape(grouped)
    router_probs = jax.nn.softmax(logits, axis=-1).reshape(GROUPS, TOKENS_GROUP, EXPERTS)
    prob_first = jnp.take_along_axis(router_probs, first[..., None], axis=-1)[..., 0]
    prob_second = jnp.take_along_axis(router_probs, second[..., None], axis=-1)[..., 0]
    gate_first = prob_first / (prob_first + prob_second)
    gate_second = prob_second / (prob_first + prob_second)
    expert_ids = jnp.arange(EXPERTS)
    hot_first = ((first[..., None] == expert_ids) & valid[..., None]).astype(jnp.int32)
    hot_second = ((second[..., None] == expert_ids) & valid[..., None]).astype(jnp.int32)
    rank_first = jnp.cumsum(hot_first, axis=1) - 1
    rank_second = jnp.cumsum(hot_second, axis=1) - 1 + jnp.sum(hot_first, axis=1, keepdims=True)
    slot_first = jnp.sum(rank_first * hot_first, axis=-1)
    slot_second = jnp.sum(rank_second * hot_second, axis=-1)
    dest_first = jnp.where(valid & (slot_first < CAPACITY), first * CAPACITY + slot_first, DUMP_SLOT)
    dest_second = jnp.where(valid & (slot_second < CAPACITY), second * CAPACITY + slot_second, DUMP_SLOT)
    tables = jax.vmap(fill_table)(dest_first, dest_second)
    zero_row = jnp.zeros((GROUPS, 1, D_MODEL), jnp.bfloat16)
    padded = jnp.concatenate([normed.reshape(GROUPS, TOKENS_GROUP, D_MODEL), zero_row], axis=1)
    dispatched = jax.vmap(take_rows)(padded, tables)
    per_expert = dispatched.reshape(GROUPS, EXPERTS, CAPACITY, D_MODEL).transpose(1, 0, 2, 3).reshape(EXPERTS, GROUPS * CAPACITY, D_MODEL)
    expert_out = lax.map(run_expert, (per_expert, w_exp_in, b_exp_in, w_exp_out, b_exp_out))
    returned = expert_out.reshape(EXPERTS, GROUPS, CAPACITY, D_MODEL).transpose(1, 0, 2, 3).reshape(GROUPS, DUMP_SLOT, D_MODEL)
    returned = jnp.concatenate([returned, zero_row], axis=1)
    out_first = jax.vmap(take_rows)(returned, dest_first).astype(jnp.float32)
    out_second = jax.vmap(take_rows)(returned, dest_second).astype(jnp.float32)
    combined = gate_first[..., None] * out_first + gate_second[..., None] * out_second
    result = residual.reshape(GROUPS, TOKENS_GROUP, D_MODEL).astype(jnp.float32) + combined
    return result.astype(jnp.bfloat16).reshape(BATCH, SEQ_LEN, D_MODEL)
```

```python
import functools

import jax
import jax.numpy as jnp
from jax import lax
from jax.experimental import pallas as pl
from jax.experimental.pallas import tpu as pltpu
from jax.sharding import PartitionSpec as P

LN_EPS = 1e-5
BF16 = jnp.bfloat16
F32 = jnp.float32
LOG2E = 1.4426950408889634


def dot_t(lhs, rhs_t):
    return lax.dot_general(lhs, rhs_t, (((1,), (1,)), ((), ())), preferred_element_type=F32)


HBM = pltpu.HBM


def norm_rows(value, gain, shift):
    centered = value - jnp.mean(value, axis=-1, keepdims=True)
    variance = jnp.mean(centered * centered, axis=-1, keepdims=True)
    return centered * lax.rsqrt(variance + LN_EPS) * gain + shift


def away(axis, size, distance):
    return lax.rem(lax.axis_index(axis) + distance, size)


def enter(groups):
    barrier = pltpu.get_barrier_semaphore()
    count = 0
    for axis, size in groups:
        for distance in range(1, size):
            pl.semaphore_signal(barrier, inc=1, device_id={axis: away(axis, size, distance)}, device_id_type=pl.DeviceIdType.MESH)
            count += 1
    pl.semaphore_wait(barrier, count)


def exchange(tp_size, weight_ref, chunk, landing_ref, send_sem, recv_sem):
    return [pltpu.make_async_remote_copy(
        src_ref=weight_ref.at[chunk * tp_size + away('tp', tp_size, distance)], dst_ref=landing_ref.at[distance - 1],
        send_sem=send_sem.at[distance - 1], recv_sem=recv_sem.at[distance - 1],
        device_id={'tp': away('tp', tp_size, distance)}, device_id_type=pl.DeviceIdType.MESH)
        for distance in sorted(range(1, tp_size), key=lambda d: (min(d, tp_size - d), d))]


def attention_body(tp_size, chunk, head_dim, block_q, lens_ref, x_ref, gain_ref, shift_ref, w_qkv_ref, b_qkv_ref, w_out_ref, b_out_ref, gain2_ref, shift2_ref, w_move_ref,
                   hidden_ref, normed_ref, moved_ref, qkv_ref, context_ref, send_sem, recv_sem):
    row = pl.program_id(0)
    block = pl.program_id(1)
    seq, width = x_ref.shape
    copies = exchange(tp_size, w_move_ref, chunk, moved_ref, send_sem, recv_sem)

    @pl.when((row == 0) & (block == 0))
    def _():
        enter([('tp', tp_size)])
        for copy in copies:
            copy.start()

    @pl.when(block == 0)
    def _():
        def project(index, carry):
            rows = pl.ds(pl.multiple_of(index * block_q, block_q), block_q)
            normed = norm_rows(x_ref[rows, :].astype(F32), gain_ref[...], shift_ref[...]).astype(BF16)
            qkv_ref[rows, :] = (dot_t(normed, w_qkv_ref[...]) + b_qkv_ref[...]).astype(BF16)
            return carry
        lax.fori_loop(0, seq // block_q, project, 0)

    length = lens_ref[row]
    pair = 2 * head_dim
    key_ok = lax.broadcasted_iota(jnp.int32, (1, seq), 1) < length
    lane_head = lax.broadcasted_iota(jnp.int32, (1, pair), 1) // head_dim
    factor = (head_dim ** -0.5) * LOG2E
    rows = pl.ds(pl.multiple_of(block * block_q, block_q), block_q)

    def heads(index, carry):
        lanes = pl.multiple_of(index * pair, pair)
        query = qkv_ref[rows, pl.ds(lanes, pair)]
        keys = qkv_ref[:, pl.ds(pl.multiple_of(lanes + width, pair), pair)]
        values = qkv_ref[:, pl.ds(pl.multiple_of(lanes + 2 * width, pair), pair)]
        result = None
        for head in range(2):
            scores = dot_t(jnp.where(lane_head == head, query, jnp.zeros_like(query)), keys)
            scores = jnp.where(key_ok, scores, -1e30)
            top = jnp.max(scores, axis=-1, keepdims=True)
            weights = jnp.exp2((scores - top) * factor)
            scale = 1.0 / jnp.sum(weights, axis=-1, keepdims=True)
            part = jnp.dot((weights * scale).astype(BF16), values, preferred_element_type=F32)
            result = part if result is None else jnp.where(lane_head == head, part, result)
        context_ref[:, pl.ds(lanes, pair)] = result.astype(BF16)
        return carry

    lax.fori_loop(0, width // pair, heads, 0)
    projected = jnp.dot(context_ref[...], w_out_ref[...], preferred_element_type=F32)
    hidden = (x_ref[rows, :].astype(F32) + projected + b_out_ref[...]).astype(BF16)
    hidden_ref[...] = hidden
    normed_ref[...] = norm_rows(hidden.astype(F32), gain2_ref[...], shift2_ref[...]).astype(BF16)

    @pl.when((row == pl.num_programs(0) - 1) & (block == pl.num_programs(1) - 1))
    def _():
        for copy in copies:
            copy.wait()


def attention_layer(x, lens, seq, head_dim, norm, w_qkv, b_qkv, w_out, b_out, norm2, w_move, tp_size, chunk, call_id):
    tokens, width = x.shape
    block_q = min(256, seq)
    blocks = seq // block_q
    fixed = lambda shape: pl.BlockSpec(shape, lambda r, q: (0,) * len(shape), pipeline_mode=pl.Buffered(1))
    moved = (tp_size - 1,) + w_move.shape[1:]
    return pl.pallas_call(
        functools.partial(attention_body, tp_size, chunk, head_dim, block_q),
        out_shape=(jax.ShapeDtypeStruct((tokens, width), BF16), jax.ShapeDtypeStruct((tokens, width), BF16), jax.ShapeDtypeStruct(moved, BF16)),
        grid=(tokens // seq, blocks),
        in_specs=[pl.BlockSpec(memory_space=pltpu.SMEM), pl.BlockSpec((seq, width), lambda r, q: (r, 0)), fixed((1, width)), fixed((1, width)),
                  fixed(w_qkv.shape), fixed((1, 3 * width)), fixed(w_out.shape), fixed((1, width)), fixed((1, width)), fixed((1, width)), pl.BlockSpec(memory_space=HBM)],
        out_specs=(pl.BlockSpec((block_q, width), lambda r, q: (r * blocks + q, 0)), pl.BlockSpec((block_q, width), lambda r, q: (r * blocks + q, 0)), pl.BlockSpec(memory_space=HBM)),
        scratch_shapes=[pltpu.VMEM((seq, 3 * width), BF16), pltpu.VMEM((block_q, width), BF16), pltpu.SemaphoreType.DMA((tp_size - 1,)), pltpu.SemaphoreType.DMA((tp_size - 1,))],
        compiler_params=pltpu.CompilerParams(dimension_semantics=('arbitrary', 'arbitrary'), collective_id=call_id, has_side_effects=True, vmem_limit_bytes=52 * 1024 * 1024),
        cost_estimate=pl.CostEstimate(flops=30_000_000_000, transcendentals=0, bytes_accessed=40_000_000),
        name='attention_layer')(lens, x, *norm, w_qkv, b_qkv, w_out, b_out, *norm2, w_move)


def dense_body(tp_size, chunk, parts, x_ref, normed_ref, w_in_ref, b_in_ref, w_out_ref, b_out_ref, w_move_ref, o_ref, moved_ref, send_sem, recv_sem):
    block = pl.program_id(0)
    copies = exchange(tp_size, w_move_ref, chunk, moved_ref, send_sem, recv_sem)

    @pl.when(block == 0)
    def _():
        enter([('tp', tp_size)])
        for copy in copies:
            copy.start()

    size = w_in_ref.shape[0] // parts
    total = x_ref[...].astype(F32) + b_out_ref[...]
    for part in range(parts):
        cols = pl.ds(part * size, size)
        inner = jnp.maximum(dot_t(normed_ref[...], w_in_ref[cols, :]) + b_in_ref[:, cols], 0.0).astype(BF16)
        total += jnp.dot(inner, w_out_ref[cols, :], preferred_element_type=F32)
    o_ref[...] = total.astype(BF16)

    @pl.when(block == pl.num_programs(0) - 1)
    def _():
        for copy in copies:
            copy.wait()


def dense_layer(x, normed, w_in, b_in, w_out, b_out, w_move, tp_size, chunk, call_id):
    tokens, width = x.shape
    block_n = min(256, tokens)
    fixed = lambda shape: pl.BlockSpec(shape, lambda i: (0,) * len(shape), pipeline_mode=pl.Buffered(1))
    moved = (tp_size - 1,) + w_move.shape[1:]
    return pl.pallas_call(
        functools.partial(dense_body, tp_size, chunk, 4),
        out_shape=(jax.ShapeDtypeStruct((tokens, width), BF16), jax.ShapeDtypeStruct(moved, BF16)), grid=(tokens // block_n,),
        in_specs=[pl.BlockSpec((block_n, width), lambda i: (i, 0)), pl.BlockSpec((block_n, width), lambda i: (i, 0)), fixed(w_in.shape), fixed(b_in.shape), fixed(w_out.shape), fixed((1, width)), pl.BlockSpec(memory_space=HBM)],
        out_specs=(pl.BlockSpec((block_n, width), lambda i: (i, 0)), pl.BlockSpec(memory_space=HBM)),
        scratch_shapes=[pltpu.SemaphoreType.DMA((tp_size - 1,)), pltpu.SemaphoreType.DMA((tp_size - 1,))],
        compiler_params=pltpu.CompilerParams(dimension_semantics=('arbitrary',), collective_id=call_id, has_side_effects=True, vmem_limit_bytes=52 * 1024 * 1024),
        cost_estimate=pl.CostEstimate(flops=20_000_000_000, transcendentals=0, bytes_accessed=30_000_000),
        name='dense_layer')(x, normed, w_in, b_in, w_out, b_out, w_move)


def experts_body(tp_size, ep_size, early, dispatch_ref, early_refs, w_in_ref, w_out_ref, b_in_ref, b_out_ref, returned_ref,
                 arrived_ref, late_ref, early_buf, own_buf, out_buf, local_sem, send_sem, recv_sem, back_send, back_recv, move_send, move_recv):
    chunks, _, slots, width = arrived_ref.shape
    me = lax.axis_index('ep')
    mine = lax.axis_index('tp')
    weights = (w_in_ref, w_out_ref)
    units = [(chunk, which) for chunk in range(chunks) for which in range(2)]
    late = units[early:]

    sends = {}
    for chunk in range(chunks):
        for distance in range(1, ep_size):
            peer = away('ep', ep_size, distance)
            sends[chunk, distance] = pltpu.make_async_remote_copy(
                src_ref=dispatch_ref.at[chunk, peer], dst_ref=arrived_ref.at[chunk, me], send_sem=send_sem.at[chunk, distance], recv_sem=recv_sem.at[chunk, distance],
                device_id={'ep': peer}, device_id_type=pl.DeviceIdType.MESH)
    moves = {unit: exchange(tp_size, weights[unit[1]], unit[0], late_ref.at[index], move_send.at[index], move_recv.at[index]) for index, unit in enumerate(late)}
    kept = [pltpu.make_async_copy(dispatch_ref.at[chunk, me], arrived_ref.at[chunk, me], local_sem.at[0, chunk]) for chunk in range(chunks)]
    owns = {unit: pltpu.make_async_copy(weights[unit[1]].at[unit[0] * tp_size + mine], own_buf.at[unit[0], unit[1]], local_sem.at[1 + unit[1], unit[0]]) for unit in units}
    earlies = {unit: pltpu.make_async_copy(early_refs[index], early_buf.at[index], local_sem.at[3, index]) for index, unit in enumerate(units[:early])}

    enter([('tp', tp_size), ('ep', ep_size)])
    for unit in late:
        for copy in moves[unit]:
            copy.start()
    for chunk in range(chunks):
        for distance in range(1, ep_size):
            sends[chunk, distance].start()
        kept[chunk].start()
    for unit in units:
        owns[unit].start()
        if unit in earlies:
            earlies[unit].start()

    def part_ref(unit, part):
        if part == 0:
            return own_buf.at[unit[0], unit[1]]
        index = units.index(unit)
        return early_buf.at[index, part - 1] if index < early else late_ref.at[index - early, part - 1]

    backs = {}
    for chunk in range(chunks):
        slot = chunk % out_buf.shape[0]
        for distance in range(1, ep_size):
            sends[chunk, distance].wait_recv()
        kept[chunk].wait()
        for which in range(2):
            unit = (chunk, which)
            owns[unit].wait()
            if unit in earlies:
                earlies[unit].wait()
            else:
                for copy in moves[unit]:
                    copy.wait_recv()
        before = chunk - out_buf.shape[0]
        if before >= 0:
            for copy in backs[before][:-1]:
                copy.wait_send()
            backs[before][-1].wait()

        def rows(index, carry):
            tokens = arrived_ref[chunk, pl.ds(2 * index, 2)].reshape(2 * slots, width)
            total = jnp.zeros((2 * slots, width), F32)
            for part in range(tp_size):
                inner = jnp.dot(tokens, part_ref((chunk, 0), part)[...], preferred_element_type=F32) + b_in_ref[chunk, pl.ds(part, 1), :]
                total += jnp.dot(jnp.maximum(inner, 0.0).astype(BF16), part_ref((chunk, 1), part)[...], preferred_element_type=F32)
            out_buf[slot, pl.ds(2 * index, 2)] = (total + b_out_ref[pl.ds(chunk, 1), :]).astype(BF16).reshape(2, slots, width)
            return carry

        lax.fori_loop(0, ep_size // 2, rows, 0)
        backs[chunk] = []
        for distance in range(1, ep_size):
            peer = away('ep', ep_size, distance)
            backs[chunk].append(pltpu.make_async_remote_copy(
                src_ref=out_buf.at[slot, peer], dst_ref=returned_ref.at[chunk, me], send_sem=back_send.at[chunk, distance], recv_sem=back_recv.at[chunk, distance],
                device_id={'ep': peer}, device_id_type=pl.DeviceIdType.MESH))
        backs[chunk].append(pltpu.make_async_copy(out_buf.at[slot, me], returned_ref.at[chunk, me], local_sem.at[4, chunk]))
        for copy in backs[chunk]:
            copy.start()

    for chunk in range(chunks):
        for distance in range(1, ep_size):
            sends[chunk, distance].wait_send()
        for copy in backs[chunk][:-1]:
            copy.wait_recv()
            if chunk + out_buf.shape[0] >= chunks:
                copy.wait_send()
        if chunk + out_buf.shape[0] >= chunks:
            backs[chunk][-1].wait()
    for unit in late:
        for copy in moves[unit]:
            copy.wait_send()


def experts(dispatch, early_weights, w_in, w_out, b_in, b_out, tp_size, ep_size, call_id):
    chunks, _, slots, width = dispatch.shape
    hidden = w_in.shape[2]
    early = len(early_weights)
    late = 2 * chunks - early
    hbm = pl.BlockSpec(memory_space=HBM)
    vmem = pl.BlockSpec(memory_space=pltpu.VMEM)

    def body(dispatch_ref, *refs):
        experts_body(tp_size, ep_size, early, dispatch_ref, refs[:early], *refs[early:])

    dma = pltpu.SemaphoreType.DMA
    return pl.pallas_call(
        body, out_shape=jax.ShapeDtypeStruct(dispatch.shape, BF16),
        in_specs=[hbm] * (3 + early) + [vmem, vmem], out_specs=hbm,
        scratch_shapes=[pltpu.VMEM(dispatch.shape, BF16), pltpu.VMEM((late, tp_size - 1, width, hidden), BF16), pltpu.VMEM((early, tp_size - 1, width, hidden), BF16),
                        pltpu.VMEM((chunks, 2, width, hidden), BF16), pltpu.VMEM((2, ep_size, slots, width), BF16),
                        dma((5, max(chunks, early))), dma((chunks, ep_size)), dma((chunks, ep_size)), dma((chunks, ep_size)), dma((chunks, ep_size)),
                        dma((late, tp_size - 1)), dma((late, tp_size - 1))],
        compiler_params=pltpu.CompilerParams(collective_id=call_id, has_side_effects=True, vmem_limit_bytes=62 * 1024 * 1024),
        cost_estimate=pl.CostEstimate(flops=4 * chunks * ep_size * slots * width * hidden * tp_size, transcendentals=0, bytes_accessed=60_000_000),
        name='experts')(dispatch, *early_weights, w_in, w_out, b_in, b_out)


def combine_body(block_t, token_ref, gate_at_ref, gates_ref, slots_ref, o_ref, acc_ref, wide_ref):
    block = pl.program_id(0)
    slots, width = wide_ref.shape
    tokens = o_ref.shape[0]

    @pl.when(block == 0)
    def _():
        def clear(index, carry):
            rows = pl.ds(pl.multiple_of(index * block_t, block_t), block_t)
            acc_ref[rows, :] = jnp.zeros((block_t, width), F32)
            return carry
        lax.fori_loop(0, tokens // block_t, clear, 0)
        acc_ref[pl.ds(tokens, 8), :] = jnp.zeros((8, width), F32)

    wide_ref[...] = slots_ref[...].astype(F32)
    base = block * slots

    def step(index, carry):
        first = index * 8
        places = [token_ref[base + first + u] for u in range(8)]
        gates = [gates_ref[gate_at_ref[base + first + u]] for u in range(8)]
        old = [acc_ref[pl.ds(places[u], 1), :] for u in range(8)]
        new = [wide_ref[pl.ds(first + u, 1), :] for u in range(8)]
        for u in range(8):
            acc_ref[pl.ds(places[u], 1), :] = old[u] + gates[u] * new[u]
        return carry

    lax.fori_loop(0, slots // 8, step, 0)

    @pl.when(block == pl.num_programs(0) - 1)
    def _():
        def write(index, carry):
            rows = pl.ds(pl.multiple_of(index * block_t, block_t), block_t)
            o_ref[rows, :] = acc_ref[rows, :].astype(BF16)
            return carry
        lax.fori_loop(0, tokens // block_t, write, 0)


def combine(token_of, gate_at, gates, outputs, tokens):
    blocks, slots, width = outputs.shape
    block_t = min(256, tokens)
    grid_spec = pltpu.PrefetchScalarGridSpec(
        num_scalar_prefetch=3, grid=(blocks,),
        in_specs=[pl.BlockSpec((None, slots, width), lambda b, *_: (b, 0, 0))],
        out_specs=pl.BlockSpec((tokens, width), lambda b, *_: (0, 0)),
        scratch_shapes=[pltpu.VMEM((tokens + 8, width), F32), pltpu.VMEM((slots, width), F32)])
    return pl.pallas_call(
        functools.partial(combine_body, block_t),
        out_shape=jax.ShapeDtypeStruct((tokens, width), BF16), grid_spec=grid_spec,
        compiler_params=pltpu.CompilerParams(dimension_semantics=('arbitrary',), vmem_limit_bytes=56 * 1024 * 1024),
        cost_estimate=pl.CostEstimate(flops=30_000_000_000, transcendentals=0, bytes_accessed=2 * tokens * width + 2 * blocks * slots * width),
        name='combine')(token_of, gate_at, gates, outputs)


def route(key_ok, expert_idx, num_experts, capacity):
    tokens = key_ok.size
    valid = key_ok.reshape(tokens)
    first = expert_idx[..., 0].reshape(tokens)
    second = expert_idx[..., 1].reshape(tokens)
    expert_ids = jnp.arange(num_experts, dtype=jnp.int32)
    hot_first = ((first[:, None] == expert_ids) & valid[:, None]).astype(jnp.int32)
    hot_second = ((second[:, None] == expert_ids) & valid[:, None]).astype(jnp.int32)
    rank_first = jnp.cumsum(hot_first, axis=0) - 1
    rank_second = jnp.cumsum(hot_second, axis=0) - 1 + jnp.sum(hot_first, axis=0)
    slot_first = jnp.sum(rank_first * hot_first, axis=1)
    slot_second = jnp.sum(rank_second * hot_second, axis=1)
    dump = num_experts * capacity
    dest_first = jnp.where(valid & (slot_first < capacity), first * capacity + slot_first, dump)
    dest_second = jnp.where(valid & (slot_second < capacity), second * capacity + slot_second, dump)
    choice = jnp.full((dump + 1,), 2 * tokens, jnp.int32)
    ids = jnp.arange(tokens, dtype=jnp.int32)
    choice = choice.at[dest_first].set(ids).at[dest_second].set(ids + tokens)
    return choice[:dump].reshape(num_experts, capacity)


def solution(mesh):
    tp_size = mesh.shape['tp']
    ep_size = mesh.shape['ep']

    def gather_tp(value, axis=0, tiled=False):
        return lax.all_gather(value, 'tp', axis=axis, tiled=tiled)

    def local_fn(x, src_len, expert_idx, ln_gain, ln_bias, w_query, b_query, w_key, w_value, b_value, w_attn_out, b_attn_out, w_fc1, b_fc1, w_fc2, b_fc2, w_router, w_exp_in, b_exp_in, w_exp_out, b_exp_out):
        rows, seq, width = x.shape
        tokens = rows * seq
        num_experts = w_router.shape[1]
        capacity = 2 * (-(-tokens // num_experts))
        local_experts = w_exp_in.shape[0]
        own_experts = local_experts // tp_size
        _, _, local_heads, head_dim = w_query.shape
        heads = local_heads * tp_size
        head_cols = local_heads * head_dim
        hidden_cols = w_fc1.shape[1]
        tp_index = lax.axis_index('tp')
        ep_index = lax.axis_index('ep')
        own_rows = rows // tp_size
        own_tokens = own_rows * seq
        x_own = lax.dynamic_slice_in_dim(x, tp_index * own_rows, own_rows, 0).reshape(own_tokens, width)
        len_own = lax.dynamic_slice_in_dim(src_len, tp_index * own_rows, own_rows, 0)

        def pack_attention(j):
            columns = [w[j].reshape(width, head_cols).T for w in (w_query, w_key, w_value)]
            return jnp.concatenate(columns + [w_attn_out[j].reshape(head_cols, width)], axis=0)

        def unpack_attention(gathered):
            by_kind = gathered.reshape(tp_size, 4, head_cols, width).transpose(1, 0, 2, 3)
            return by_kind[:3].reshape(3 * heads * head_dim, width), by_kind[3].reshape(heads * head_dim, width)

        small = jnp.concatenate([b_query.reshape(-1), b_value.reshape(-1), b_fc1.reshape(-1), b_exp_in.reshape(-1)])
        small = gather_tp(small)
        attn_bias_size = 2 * head_cols
        b_query_all = small[:, :attn_bias_size].reshape(tp_size, 2, head_cols).transpose(1, 0, 2).reshape(2, -1)
        b_value_all = small[:, attn_bias_size:2 * attn_bias_size].reshape(tp_size, 2, head_cols).transpose(1, 0, 2).reshape(2, -1)
        b_fc1_all = small[:, 2 * attn_bias_size:2 * attn_bias_size + hidden_cols]
        b_exp_in_all = small[:, 2 * attn_bias_size + hidden_cols:].reshape(tp_size, local_experts, -1)
        b_qkv = jnp.concatenate([b_query_all, jnp.zeros_like(b_query_all), b_value_all], axis=1)

        first_pack = gather_tp(pack_attention(0))

        cut = hidden_cols // ep_size

        def own_slice(value):
            size = value.shape[0] // ep_size
            return lax.dynamic_slice_in_dim(value, ep_index * size, size, 0)

        later = jnp.concatenate([own_slice(w_fc1.T), own_slice(w_fc2), own_slice(pack_attention(1))], axis=0)
        later, first_pack = lax.optimization_barrier((later, first_pack))
        later = gather_tp(later)
        fc1_all = lax.all_gather(later[:, :cut], 'ep').reshape(-1, width)
        fc2_all = lax.all_gather(later[:, cut:2 * cut], 'ep').reshape(-1, width)
        second_pack = lax.all_gather(later[:, 2 * cut:], 'ep').transpose(1, 0, 2, 3).reshape(tp_size, -1, width)
        b_fc1_all = b_fc1_all.reshape(tp_size, ep_size, cut).transpose(1, 0, 2).reshape(-1)

        key_ok = jnp.arange(seq)[None, :] < src_len[:, None]
        choice_all = route(key_ok, expert_idx, num_experts, capacity)
        choice = choice_all.reshape(ep_size, own_experts, tp_size, capacity)
        choice = lax.dynamic_index_in_dim(choice, tp_index, 2, keepdims=False)
        source = jnp.where(choice < tokens, choice, choice - tokens)
        dispatch_at = jnp.where(choice == 2 * tokens, 0, source)

        def norm(i):
            return ln_gain[i].reshape(1, width), ln_bias[i].reshape(1, width)

        def row(value):
            return value.reshape(1, -1)

        w_qkv, w_out = unpack_attention(first_pack)
        hidden, normed, moved_0 = attention_layer(x_own, len_own, seq, head_dim, norm(0), w_qkv, row(b_qkv[0]), w_out, row(b_attn_out[0]), norm(1), w_exp_in, tp_size, 0, 0)
        hidden, moved_1 = dense_layer(hidden, normed, fc1_all, row(b_fc1_all), fc2_all, row(b_fc2), w_exp_out, tp_size, 0, 1)
        w_qkv, w_out = unpack_attention(second_pack)
        hidden, normed, moved_2 = attention_layer(hidden, len_own, seq, head_dim, norm(2), w_qkv, row(b_qkv[1]), w_out, row(b_attn_out[1]), norm(3), w_exp_in, tp_size, 1, 2)
        normed_all = gather_tp(normed, tiled=True)

        logits = jnp.dot(normed_all, w_router.astype(BF16), preferred_element_type=F32)
        expert_ids = jnp.arange(num_experts, dtype=jnp.int32)
        flat_idx = expert_idx.reshape(tokens, 2)
        picked = [jnp.sum(jnp.where(flat_idx[:, k:k + 1] == expert_ids, logits, 0.0), axis=1) for k in range(2)]
        gates = jnp.concatenate([jax.nn.sigmoid(picked[0] - picked[1]), jax.nn.sigmoid(picked[1] - picked[0]), jnp.zeros((128,), F32)])

        b_in_own = lax.dynamic_index_in_dim(b_exp_in_all.reshape(tp_size, own_experts, tp_size, -1), tp_index, 2, keepdims=False)
        part_order = lax.rem(tp_index - jnp.arange(tp_size) + tp_size, tp_size)
        b_in_own = b_in_own[part_order].transpose(1, 0, 2)
        b_out_own = lax.dynamic_index_in_dim(b_exp_out.reshape(own_experts, tp_size, width), tp_index, 1, keepdims=False)
        dispatch = normed_all[dispatch_at.transpose(1, 0, 2).reshape(-1)].reshape(own_experts, ep_size, capacity, width)
        outputs = experts(dispatch, [moved_0, moved_1, moved_2], w_exp_in, w_exp_out, b_in_own, b_out_own, tp_size, ep_size, 3)
        outputs = outputs.reshape(own_experts * ep_size, capacity, width)
        choice = choice.transpose(1, 0, 2).reshape(-1)
        token_of = jnp.where(choice == 2 * tokens, tokens, source.transpose(1, 0, 2).reshape(-1))
        partial = combine(token_of, choice, gates, outputs, tokens)
        summed = lax.psum_scatter(partial, 'tp', scatter_dimension=0, tiled=True)
        result = (hidden.astype(F32) + summed.astype(F32)).astype(BF16)
        return gather_tp(result, tiled=True).reshape(rows, seq, width)

    in_specs = (P(('dp', 'ep'), None, None), P(('dp', 'ep')), P(('dp', 'ep'), None, None), P(), P(), P(None, None, 'tp', None), P(None, 'tp', None), P(None, None, 'tp', None), P(None, None, 'tp', None), P(None, 'tp', None), P(None, 'tp', None, None), P(), P(None, 'tp'), P('tp'), P('tp', None), P(), P(), P('ep', None, 'tp'), P('ep', 'tp'), P('ep', 'tp', None), P('ep', None))
    return jax.shard_map(local_fn, mesh=mesh, in_specs=in_specs, out_specs=P(('dp', 'ep'), None, None), check_vma=False)
```

```python
import functools

import jax
import jax.numpy as jnp
from jax import lax
from jax.experimental import pallas as pl
from jax.experimental.pallas import tpu as pltpu
from jax.sharding import PartitionSpec as P

LN_EPS = 1e-5
BF16 = jnp.bfloat16
F32 = jnp.float32
LOG2E = 1.4426950408889634


def dot_t(lhs, rhs_t):
    return lax.dot_general(lhs, rhs_t, (((1,), (1,)), ((), ())), preferred_element_type=F32)


HBM = pltpu.HBM


def norm_rows(value, gain, shift):
    centered = value - jnp.mean(value, axis=-1, keepdims=True)
    variance = jnp.mean(centered * centered, axis=-1, keepdims=True)
    return centered * lax.rsqrt(variance + LN_EPS) * gain + shift


def away(axis, size, distance):
    return lax.rem(lax.axis_index(axis) + distance, size)


def enter(groups):
    barrier = pltpu.get_barrier_semaphore()
    count = 0
    for axis, size in groups:
        for distance in range(1, size):
            pl.semaphore_signal(barrier, inc=1, device_id={axis: away(axis, size, distance)}, device_id_type=pl.DeviceIdType.MESH)
            count += 1
    pl.semaphore_wait(barrier, count)


def exchange(tp_size, weights, piece, landing_ref, send_sem, recv_sem):
    chunk, which, start, rows = piece
    return [pltpu.make_async_remote_copy(
        src_ref=weights[which].at[chunk * tp_size + away('tp', tp_size, distance), pl.ds(start, rows)], dst_ref=landing_ref.at[distance - 1],
        send_sem=send_sem.at[distance - 1], recv_sem=recv_sem.at[distance - 1],
        device_id={'tp': away('tp', tp_size, distance)}, device_id_type=pl.DeviceIdType.MESH)
        for distance in sorted(range(1, tp_size), key=lambda d: (min(d, tp_size - d), d))]


def exchange_all(tp_size, weights, pieces, landing_refs, send_sem, recv_sem):
    copies = []
    for index, piece in enumerate(pieces):
        copies += exchange(tp_size, weights, piece, landing_refs[index], send_sem.at[index], recv_sem.at[index])
    return copies


def landings(tp_size, weight, pieces):
    return [jax.ShapeDtypeStruct((tp_size - 1, rows, weight.shape[2]), BF16) for _, _, _, rows in pieces]


def move_body(tp_size, pieces, w_in_ref, w_out_ref, after_ref, *rest):
    copies = exchange_all(tp_size, (w_in_ref, w_out_ref), pieces, rest[:len(pieces)], *rest[len(pieces):])
    enter([('tp', tp_size)])
    for copy in copies:
        copy.start()
    for copy in copies:
        copy.wait()


def move(w_in, w_out, after, tp_size, pieces, call_id):
    hbm = pl.BlockSpec(memory_space=HBM)
    dma = pltpu.SemaphoreType.DMA((len(pieces), tp_size - 1))
    return pl.pallas_call(
        functools.partial(move_body, tp_size, pieces), out_shape=landings(tp_size, w_in, pieces),
        in_specs=[hbm, hbm, hbm], out_specs=[hbm for _ in pieces], scratch_shapes=[dma, dma],
        compiler_params=pltpu.CompilerParams(collective_id=call_id, has_side_effects=True, vmem_limit_bytes=56 * 1024 * 1024),
        cost_estimate=pl.CostEstimate(flops=20_000_000_000, transcendentals=0, bytes_accessed=10_000_000),
        name='move')(w_in, w_out, after)


def attention_body(tp_size, pieces, head_dim, block_q, lens_ref, x_ref, gain_ref, shift_ref, w_qkv_ref, b_qkv_ref, w_out_ref, b_out_ref, gain2_ref, shift2_ref, w_in_ref, w_exp_out_ref, after_ref,
                   hidden_ref, normed_ref, *rest):
    row = pl.program_id(0)
    block = pl.program_id(1)
    seq, width = x_ref.shape
    moved_refs = rest[:len(pieces)]
    qkv_ref, context_ref, send_sem, recv_sem = rest[len(pieces):]
    copies = exchange_all(tp_size, (w_in_ref, w_exp_out_ref), pieces, moved_refs, send_sem, recv_sem)

    @pl.when((row == 0) & (block == 0))
    def _():
        enter([('tp', tp_size)])
        for copy in copies:
            copy.start()

    @pl.when(block == 0)
    def _():
        def project(index, carry):
            rows = pl.ds(pl.multiple_of(index * block_q, block_q), block_q)
            normed = norm_rows(x_ref[rows, :].astype(F32), gain_ref[...], shift_ref[...]).astype(BF16)
            qkv_ref[rows, :] = (dot_t(normed, w_qkv_ref[...]) + b_qkv_ref[...]).astype(BF16)
            return carry
        lax.fori_loop(0, seq // block_q, project, 0)

    length = lens_ref[row]
    pair = 2 * head_dim
    key_ok = lax.broadcasted_iota(jnp.int32, (1, seq), 1) < length
    lane_head = lax.broadcasted_iota(jnp.int32, (1, pair), 1) // head_dim
    factor = (head_dim ** -0.5) * LOG2E
    rows = pl.ds(pl.multiple_of(block * block_q, block_q), block_q)

    def heads(index, carry):
        lanes = pl.multiple_of(index * pair, pair)
        query = qkv_ref[rows, pl.ds(lanes, pair)]
        keys = qkv_ref[:, pl.ds(pl.multiple_of(lanes + width, pair), pair)]
        values = qkv_ref[:, pl.ds(pl.multiple_of(lanes + 2 * width, pair), pair)]
        result = None
        for head in range(2):
            scores = dot_t(jnp.where(lane_head == head, query, jnp.zeros_like(query)), keys)
            scores = jnp.where(key_ok, scores, -1e30)
            top = jnp.max(scores, axis=-1, keepdims=True)
            weights = jnp.exp2((scores - top) * factor)
            scale = 1.0 / jnp.sum(weights, axis=-1, keepdims=True)
            part = jnp.dot((weights * scale).astype(BF16), values, preferred_element_type=F32)
            result = part if result is None else jnp.where(lane_head == head, part, result)
        context_ref[:, pl.ds(lanes, pair)] = result.astype(BF16)
        return carry

    lax.fori_loop(0, width // pair, heads, 0)
    projected = jnp.dot(context_ref[...], w_out_ref[...], preferred_element_type=F32)
    hidden = (x_ref[rows, :].astype(F32) + projected + b_out_ref[...]).astype(BF16)
    hidden_ref[...] = hidden
    normed_ref[...] = norm_rows(hidden.astype(F32), gain2_ref[...], shift2_ref[...]).astype(BF16)

    @pl.when((row == pl.num_programs(0) - 1) & (block == pl.num_programs(1) - 1))
    def _():
        for copy in copies:
            copy.wait()


def attention_layer(x, lens, seq, head_dim, norm, w_qkv, b_qkv, w_out, b_out, norm2, w_exp_in, w_exp_out, after, tp_size, pieces, call_id):
    tokens, width = x.shape
    block_q = min(256, seq)
    blocks = seq // block_q
    fixed = lambda shape: pl.BlockSpec(shape, lambda r, q: (0,) * len(shape), pipeline_mode=pl.Buffered(1))
    moved = landings(tp_size, w_exp_in, pieces)
    hbm = pl.BlockSpec(memory_space=HBM)
    return pl.pallas_call(
        functools.partial(attention_body, tp_size, pieces, head_dim, block_q),
        out_shape=(jax.ShapeDtypeStruct((tokens, width), BF16), jax.ShapeDtypeStruct((tokens, width), BF16), *moved),
        grid=(tokens // seq, blocks),
        in_specs=[pl.BlockSpec(memory_space=pltpu.SMEM), pl.BlockSpec((seq, width), lambda r, q: (r, 0)), fixed((1, width)), fixed((1, width)),
                  fixed(w_qkv.shape), fixed((1, 3 * width)), fixed(w_out.shape), fixed((1, width)), fixed((1, width)), fixed((1, width)), hbm, hbm, hbm],
        out_specs=(pl.BlockSpec((block_q, width), lambda r, q: (r * blocks + q, 0)), pl.BlockSpec((block_q, width), lambda r, q: (r * blocks + q, 0)), *[hbm for _ in pieces]),
        scratch_shapes=[pltpu.VMEM((seq, 3 * width), BF16), pltpu.VMEM((block_q, width), BF16), pltpu.SemaphoreType.DMA((len(pieces), tp_size - 1)), pltpu.SemaphoreType.DMA((len(pieces), tp_size - 1))],
        compiler_params=pltpu.CompilerParams(dimension_semantics=('arbitrary', 'arbitrary'), collective_id=call_id, has_side_effects=True, vmem_limit_bytes=52 * 1024 * 1024),
        cost_estimate=pl.CostEstimate(flops=30_000_000_000, transcendentals=0, bytes_accessed=40_000_000),
        name='attention_layer')(lens, x, *norm, w_qkv, b_qkv, w_out, b_out, *norm2, w_exp_in, w_exp_out, after)


def dense_body(tp_size, pieces, parts, x_ref, normed_ref, w_in_ref, b_in_ref, w_out_ref, b_out_ref, w_exp_in_ref, w_exp_out_ref, o_ref, *rest):
    block = pl.program_id(0)
    copies = exchange_all(tp_size, (w_exp_in_ref, w_exp_out_ref), pieces, rest[:len(pieces)], *rest[len(pieces):])

    @pl.when(block == 0)
    def _():
        enter([('tp', tp_size)])
        for copy in copies:
            copy.start()

    size = w_in_ref.shape[0] // parts
    total = x_ref[...].astype(F32) + b_out_ref[...]
    for part in range(parts):
        cols = pl.ds(part * size, size)
        inner = jnp.maximum(dot_t(normed_ref[...], w_in_ref[cols, :]) + b_in_ref[:, cols], 0.0).astype(BF16)
        total += jnp.dot(inner, w_out_ref[cols, :], preferred_element_type=F32)
    o_ref[...] = total.astype(BF16)

    @pl.when(block == pl.num_programs(0) - 1)
    def _():
        for copy in copies:
            copy.wait()


def dense_layer(x, normed, w_in, b_in, w_out, b_out, w_exp_in, w_exp_out, tp_size, pieces, call_id):
    tokens, width = x.shape
    block_n = min(256, tokens)
    fixed = lambda shape: pl.BlockSpec(shape, lambda i: (0,) * len(shape), pipeline_mode=pl.Buffered(1))
    hbm = pl.BlockSpec(memory_space=HBM)
    dma = pltpu.SemaphoreType.DMA((len(pieces), tp_size - 1))
    return pl.pallas_call(
        functools.partial(dense_body, tp_size, pieces, 4),
        out_shape=(jax.ShapeDtypeStruct((tokens, width), BF16), *landings(tp_size, w_exp_in, pieces)), grid=(tokens // block_n,),
        in_specs=[pl.BlockSpec((block_n, width), lambda i: (i, 0)), pl.BlockSpec((block_n, width), lambda i: (i, 0)), fixed(w_in.shape), fixed(b_in.shape), fixed(w_out.shape), fixed((1, width)), hbm, hbm],
        out_specs=(pl.BlockSpec((block_n, width), lambda i: (i, 0)), *[hbm for _ in pieces]),
        scratch_shapes=[dma, dma],
        compiler_params=pltpu.CompilerParams(dimension_semantics=('arbitrary',), collective_id=call_id, has_side_effects=True, vmem_limit_bytes=52 * 1024 * 1024),
        cost_estimate=pl.CostEstimate(flops=20_000_000_000, transcendentals=0, bytes_accessed=30_000_000),
        name='dense_layer')(x, normed, w_in, b_in, w_out, b_out, w_exp_in, w_exp_out)


def experts_body(tp_size, ep_size, early, late, dispatch_ref, early_refs, w_in_ref, w_out_ref, normed_ref, b_in_ref, b_out_ref, w_router_ref, index_ref, returned_ref, gates_ref,
                 normed_buf, arrived_ref, parts_buf, own_buf, out_buf, local_sem, send_sem, recv_sem, back_send, back_recv, move_send, move_recv):
    chunks, _, slots, width = arrived_ref.shape
    me = lax.axis_index('ep')
    mine = lax.axis_index('tp')
    weights = (w_in_ref, w_out_ref)
    units = [(chunk, which) for chunk in range(chunks) for which in range(2)]

    sends = {}
    for chunk in range(chunks):
        for distance in range(1, ep_size):
            peer = away('ep', ep_size, distance)
            sends[chunk, distance] = pltpu.make_async_remote_copy(
                src_ref=dispatch_ref.at[chunk, peer], dst_ref=arrived_ref.at[chunk, me], send_sem=send_sem.at[chunk, distance], recv_sem=recv_sem.at[chunk, distance],
                device_id={'ep': peer}, device_id_type=pl.DeviceIdType.MESH)
    def landing(piece):
        chunk, which, start, rows = piece
        return parts_buf.at[units.index((chunk, which)), :, pl.ds(start, rows)]

    moves = {piece: exchange(tp_size, weights, piece, landing(piece), move_send.at[index], move_recv.at[index]) for index, piece in enumerate(late)}
    kept = [pltpu.make_async_copy(dispatch_ref.at[chunk, me], arrived_ref.at[chunk, me], local_sem.at[0, chunk]) for chunk in range(chunks)]
    owns = {unit: pltpu.make_async_copy(weights[unit[1]].at[unit[0] * tp_size + mine], own_buf.at[unit[0], unit[1]], local_sem.at[1 + unit[1], unit[0]]) for unit in units}
    earlies = {piece: pltpu.make_async_copy(early_refs[index], landing(piece), local_sem.at[3, index]) for index, piece in enumerate(early)}

    enter([('tp', tp_size), ('ep', ep_size)])
    for piece in late:
        for copy in moves[piece]:
            copy.start()
    for chunk in range(chunks):
        for distance in range(1, ep_size):
            sends[chunk, distance].start()
        kept[chunk].start()
    for unit in units:
        owns[unit].start()
        for piece in early:
            if piece[:2] == unit:
                earlies[piece].start()

    step = normed_buf.shape[1]
    blocks = normed_ref.shape[0] // step
    num_experts = w_router_ref.shape[0]
    expert_ids = lax.broadcasted_iota(jnp.int32, (num_experts, step), 0)

    def load(block):
        return pltpu.make_async_copy(normed_ref.at[pl.ds(block * step, step)], normed_buf.at[block % 2], local_sem.at[5, block % 2])

    load(0).start()
    for block in range(blocks):
        if block + 1 < blocks:
            load(block + 1).start()
        load(block).wait()
        logits = dot_t(w_router_ref[...], normed_buf[block % 2])
        cols = pl.ds(block * step, step)
        picked = [jnp.sum(jnp.where(expert_ids == index_ref[pl.ds(k, 1), cols], logits, 0.0), axis=0, keepdims=True) for k in range(2)]
        gates_ref[pl.ds(0, 1), cols] = jax.nn.sigmoid(picked[0] - picked[1])
        gates_ref[pl.ds(1, 1), cols] = jax.nn.sigmoid(picked[1] - picked[0])

    def part_ref(unit, part):
        if part == 0:
            return own_buf.at[unit[0], unit[1]]
        return parts_buf.at[units.index(unit), part - 1]

    backs = {}
    for chunk in range(chunks):
        slot = chunk % out_buf.shape[0]
        for distance in range(1, ep_size):
            sends[chunk, distance].wait_recv()
        kept[chunk].wait()
        for which in range(2):
            unit = (chunk, which)
            owns[unit].wait()
            for piece in early:
                if piece[:2] == unit:
                    earlies[piece].wait()
            for piece in late:
                if piece[:2] == unit:
                    for copy in moves[piece]:
                        copy.wait_recv()
        before = chunk - out_buf.shape[0]
        if before >= 0:
            for copy in backs[before][:-1]:
                copy.wait_send()
            backs[before][-1].wait()

        def rows(index, carry):
            tokens = arrived_ref[chunk, pl.ds(2 * index, 2)].reshape(2 * slots, width)
            total = jnp.zeros((2 * slots, width), F32)
            for part in range(tp_size):
                inner = jnp.dot(tokens, part_ref((chunk, 0), part)[...], preferred_element_type=F32) + b_in_ref[chunk, pl.ds(part, 1), :]
                total += jnp.dot(jnp.maximum(inner, 0.0).astype(BF16), part_ref((chunk, 1), part)[...], preferred_element_type=F32)
            out_buf[slot, pl.ds(2 * index, 2)] = (total + b_out_ref[pl.ds(chunk, 1), :]).astype(BF16).reshape(2, slots, width)
            return carry

        lax.fori_loop(0, ep_size // 2, rows, 0)
        backs[chunk] = []
        for distance in range(1, ep_size):
            peer = away('ep', ep_size, distance)
            backs[chunk].append(pltpu.make_async_remote_copy(
                src_ref=out_buf.at[slot, peer], dst_ref=returned_ref.at[chunk, me], send_sem=back_send.at[chunk, distance], recv_sem=back_recv.at[chunk, distance],
                device_id={'ep': peer}, device_id_type=pl.DeviceIdType.MESH))
        backs[chunk].append(pltpu.make_async_copy(out_buf.at[slot, me], returned_ref.at[chunk, me], local_sem.at[4, chunk]))
        for copy in backs[chunk]:
            copy.start()

    for chunk in range(chunks):
        for distance in range(1, ep_size):
            sends[chunk, distance].wait_send()
        for copy in backs[chunk][:-1]:
            copy.wait_recv()
            if chunk + out_buf.shape[0] >= chunks:
                copy.wait_send()
        if chunk + out_buf.shape[0] >= chunks:
            backs[chunk][-1].wait()
    for piece in late:
        for copy in moves[piece]:
            copy.wait_send()


def experts(dispatch, early_weights, w_in, w_out, normed, b_in, b_out, w_router, index, tp_size, ep_size, early, late, call_id):
    chunks, _, slots, width = dispatch.shape
    hidden = w_in.shape[2]
    hbm = pl.BlockSpec(memory_space=HBM)
    vmem = pl.BlockSpec(memory_space=pltpu.VMEM)

    def body(dispatch_ref, *refs):
        experts_body(tp_size, ep_size, early, late, dispatch_ref, refs[:len(early)], *refs[len(early):])

    dma = pltpu.SemaphoreType.DMA
    return pl.pallas_call(
        body, out_shape=(jax.ShapeDtypeStruct(dispatch.shape, BF16), jax.ShapeDtypeStruct(index.shape, F32)),
        in_specs=[hbm] * (4 + len(early)) + [vmem] * 4, out_specs=(hbm, vmem),
        scratch_shapes=[pltpu.VMEM((2, min(1024, normed.shape[0]), width), BF16), pltpu.VMEM(dispatch.shape, BF16), pltpu.VMEM((2 * chunks, tp_size - 1, width, hidden), BF16),
                        pltpu.VMEM((chunks, 2, width, hidden), BF16), pltpu.VMEM((2, ep_size, slots, width), BF16),
                        dma((6, max(chunks, len(early)))), dma((chunks, ep_size)), dma((chunks, ep_size)), dma((chunks, ep_size)), dma((chunks, ep_size)),
                        dma((len(late), tp_size - 1)), dma((len(late), tp_size - 1))],
        compiler_params=pltpu.CompilerParams(collective_id=call_id, has_side_effects=True, vmem_limit_bytes=62 * 1024 * 1024),
        cost_estimate=pl.CostEstimate(flops=4 * chunks * ep_size * slots * width * hidden * tp_size, transcendentals=0, bytes_accessed=60_000_000),
        name='experts')(dispatch, *early_weights, w_in, w_out, normed, b_in, b_out, w_router, index)


def combine_body(blocks, token_ref, gate_at_ref, gates_ref, slots_ref, o_ref, acc_ref, wide_ref):
    block = pl.program_id(0)
    slots, width = slots_ref.shape
    step = o_ref.shape[0]
    lanes = 128

    @pl.when(block == 0)
    def _():
        def clear(index, carry):
            acc_ref[pl.ds(pl.multiple_of(index * 256, 256), 256), :] = jnp.zeros((256, lanes), F32)
            return carry
        lax.fori_loop(0, acc_ref.shape[0] // 256, clear, 0)

    @pl.when(block < blocks)
    def _():
        for col in range(width // lanes):
            wide_ref[pl.ds(col, slots, stride=8), :] = slots_ref[:, col * lanes:(col + 1) * lanes].astype(F32)
        base = block * slots

        def add(index, carry):
            first = index * 16
            places = [pl.ds(pl.multiple_of(token_ref[base + first + u], 8), 8) for u in range(16)]
            gates = [gates_ref[gate_at_ref[base + first + u]] for u in range(16)]
            start = pl.multiple_of(index * 128, 128)
            new = [acc_ref[places[u], :] + gates[u] * wide_ref[pl.ds(start + u * 8, 8), :] for u in range(16)]
            for u in range(16):
                acc_ref[places[u], :] = new[u]
            return carry

        lax.fori_loop(0, slots // 16, add, 0)

    @pl.when(block >= blocks)
    def _():
        first = pl.multiple_of((block - blocks) * (step * 8), step * 8)
        for col in range(width // lanes):
            o_ref[:, col * lanes:(col + 1) * lanes] = acc_ref[pl.ds(first + col, step, stride=8), :].astype(BF16)


def combine(place, gate_at, gates, outputs, tokens):
    blocks, slots, width = outputs.shape
    step = min(512, tokens)
    grid_spec = pltpu.PrefetchScalarGridSpec(
        num_scalar_prefetch=3, grid=(blocks + tokens // step,),
        in_specs=[pl.BlockSpec((None, slots, width), lambda b, *_: (jnp.minimum(b, blocks - 1), 0, 0))],
        out_specs=pl.BlockSpec((step, width), lambda b, *_: (jnp.maximum(b - blocks, 0), 0)),
        scratch_shapes=[pltpu.VMEM(((tokens + 32) * 8, 128), F32), pltpu.VMEM((slots * 8, 128), F32)])
    return pl.pallas_call(
        functools.partial(combine_body, blocks),
        out_shape=jax.ShapeDtypeStruct((tokens, width), BF16), grid_spec=grid_spec,
        compiler_params=pltpu.CompilerParams(dimension_semantics=('arbitrary',), vmem_limit_bytes=56 * 1024 * 1024),
        cost_estimate=pl.CostEstimate(flops=15_000_000_000, transcendentals=0, bytes_accessed=2 * tokens * width + 2 * blocks * slots * width),
        name='combine')(place, gate_at, gates, outputs)


def route(key_ok, expert_idx, num_experts, capacity):
    tokens = key_ok.size
    valid = key_ok.reshape(tokens)
    first = expert_idx[..., 0].reshape(tokens)
    second = expert_idx[..., 1].reshape(tokens)
    expert_ids = jnp.arange(num_experts, dtype=jnp.int32)
    hot_first = ((first[:, None] == expert_ids) & valid[:, None]).astype(jnp.int32)
    hot_second = ((second[:, None] == expert_ids) & valid[:, None]).astype(jnp.int32)
    rank_first = jnp.cumsum(hot_first, axis=0) - 1
    rank_second = jnp.cumsum(hot_second, axis=0) - 1 + jnp.sum(hot_first, axis=0)
    slot_first = jnp.sum(rank_first * hot_first, axis=1)
    slot_second = jnp.sum(rank_second * hot_second, axis=1)
    dump = num_experts * capacity
    dest_first = jnp.where(valid & (slot_first < capacity), first * capacity + slot_first, dump)
    dest_second = jnp.where(valid & (slot_second < capacity), second * capacity + slot_second, dump)
    choice = jnp.full((dump + 1,), 2 * tokens, jnp.int32)
    ids = jnp.arange(tokens, dtype=jnp.int32)
    choice = choice.at[dest_first].set(ids).at[dest_second].set(ids + tokens)
    return choice[:dump].reshape(num_experts, capacity)


def solution(mesh):
    tp_size = mesh.shape['tp']
    ep_size = mesh.shape['ep']

    def gather_tp(value, axis=0, tiled=False):
        return lax.all_gather(value, 'tp', axis=axis, tiled=tiled)

    def local_fn(x, src_len, expert_idx, ln_gain, ln_bias, w_query, b_query, w_key, w_value, b_value, w_attn_out, b_attn_out, w_fc1, b_fc1, w_fc2, b_fc2, w_router, w_exp_in, b_exp_in, w_exp_out, b_exp_out):
        rows, seq, width = x.shape
        tokens = rows * seq
        num_experts = w_router.shape[1]
        capacity = 2 * (-(-tokens // num_experts))
        local_experts = w_exp_in.shape[0]
        own_experts = local_experts // tp_size
        _, _, local_heads, head_dim = w_query.shape
        heads = local_heads * tp_size
        head_cols = local_heads * head_dim
        hidden_cols = w_fc1.shape[1]
        tp_index = lax.axis_index('tp')
        ep_index = lax.axis_index('ep')
        own_rows = rows // tp_size
        own_tokens = own_rows * seq
        x_own = lax.dynamic_slice_in_dim(x, tp_index * own_rows, own_rows, 0).reshape(own_tokens, width)
        len_own = lax.dynamic_slice_in_dim(src_len, tp_index * own_rows, own_rows, 0)

        def pack_attention(j):
            columns = [w[j].reshape(width, head_cols).T for w in (w_query, w_key, w_value)]
            return jnp.concatenate(columns + [w_attn_out[j].reshape(head_cols, width)], axis=0)

        def unpack_attention(gathered):
            by_kind = gathered.reshape(4, ep_size // 4, tp_size, -1, width).transpose(0, 2, 1, 3, 4)
            return by_kind[:3].reshape(3 * heads * head_dim, width), by_kind[3].reshape(heads * head_dim, width)

        def own_slice(value):
            size = value.shape[0] // ep_size
            return lax.dynamic_slice_in_dim(value, ep_index * size, size, 0)

        slices = [own_slice(value) for value in (pack_attention(0), w_fc1.T, w_fc2, pack_attention(1))]
        cuts = [value.shape[0] for value in slices]
        slices = gather_tp(jnp.concatenate(slices, axis=0))
        small = jnp.concatenate([b_query.reshape(-1), b_value.reshape(-1), b_fc1.reshape(-1), b_exp_in.reshape(-1)])
        small = gather_tp(small)
        slices, small = lax.optimization_barrier((slices, small))
        starts = [sum(cuts[:i]) for i in range(5)]
        first_pack = lax.all_gather(slices[:, :starts[1]], 'ep')
        fc1_all, fc2_all, second_pack = [lax.all_gather(slices[:, starts[i]:starts[i + 1]], 'ep') for i in range(1, 4)]
        fc1_all, fc2_all = fc1_all.reshape(-1, width), fc2_all.reshape(-1, width)
        cut = cuts[1]
        attn_bias_size = 2 * head_cols
        b_query_all = small[:, :attn_bias_size].reshape(tp_size, 2, head_cols).transpose(1, 0, 2).reshape(2, -1)
        b_value_all = small[:, attn_bias_size:2 * attn_bias_size].reshape(tp_size, 2, head_cols).transpose(1, 0, 2).reshape(2, -1)
        b_fc1_all = small[:, 2 * attn_bias_size:2 * attn_bias_size + hidden_cols]
        b_exp_in_all = small[:, 2 * attn_bias_size + hidden_cols:].reshape(tp_size, local_experts, -1)
        b_qkv = jnp.concatenate([b_query_all, jnp.zeros_like(b_query_all), b_value_all], axis=1)
        b_fc1_all = b_fc1_all.reshape(tp_size, ep_size, cut).transpose(1, 0, 2).reshape(-1)

        key_ok = jnp.arange(seq)[None, :] < src_len[:, None]
        choice_all = route(key_ok, expert_idx, num_experts, capacity)
        choice = choice_all.reshape(ep_size, own_experts, tp_size, capacity)
        choice = lax.dynamic_index_in_dim(choice, tp_index, 2, keepdims=False)
        source = jnp.where(choice < tokens, choice, choice - tokens)
        dispatch_at = jnp.where(choice == 2 * tokens, 0, source)

        def norm(i):
            return ln_gain[i].reshape(1, width), ln_bias[i].reshape(1, width)

        def row(value):
            return value.reshape(1, -1)

        half = width // 2
        pieces = [(2, 1, 0, half)], [(0, 0, 0, width), (0, 1, 0, width)], [(1, 0, 0, width)], [(1, 1, 0, width), (2, 0, 0, width)], [(2, 1, half, half), (3, 0, 0, width), (3, 1, 0, width)]
        moved = []
        moved += move(w_exp_in, w_exp_out, slices[0, :8], tp_size, pieces[0], 4)
        w_qkv, w_out = unpack_attention(first_pack)
        hidden, normed, *landed = attention_layer(x_own, len_own, seq, head_dim, norm(0), w_qkv, row(b_qkv[0]), w_out, row(b_attn_out[0]), norm(1), w_exp_in, w_exp_out, moved[0], tp_size, pieces[1], 0)
        moved += landed
        second_pack, hidden = lax.optimization_barrier((second_pack, hidden))
        hidden, *landed = dense_layer(hidden, normed, fc1_all, row(b_fc1_all), fc2_all, row(b_fc2), w_exp_in, w_exp_out, tp_size, pieces[2], 1)
        moved += landed
        w_qkv, w_out = unpack_attention(second_pack)
        hidden, normed, *landed = attention_layer(hidden, len_own, seq, head_dim, norm(2), w_qkv, row(b_qkv[1]), w_out, row(b_attn_out[1]), norm(3), w_exp_in, w_exp_out, moved[0], tp_size, pieces[3], 2)
        moved += landed
        normed_all = gather_tp(normed, tiled=True)

        b_in_own = lax.dynamic_index_in_dim(b_exp_in_all.reshape(tp_size, own_experts, tp_size, -1), tp_index, 2, keepdims=False)
        part_order = lax.rem(tp_index - jnp.arange(tp_size) + tp_size, tp_size)
        b_in_own = b_in_own[part_order].transpose(1, 0, 2)
        b_out_own = lax.dynamic_index_in_dim(b_exp_out.reshape(own_experts, tp_size, width), tp_index, 1, keepdims=False)
        dispatch = normed_all[dispatch_at.transpose(1, 0, 2).reshape(-1)].reshape(own_experts, ep_size, capacity, width)
        outputs, gates = experts(dispatch, moved, w_exp_in, w_exp_out, normed_all, b_in_own, b_out_own,
                                 w_router.T.astype(BF16), expert_idx.reshape(tokens, 2).T, tp_size, ep_size, sum(pieces[:4], []), pieces[4], 3)
        outputs = outputs.reshape(own_experts * ep_size, capacity, width)
        choice = choice.transpose(1, 0, 2).reshape(-1)
        token_of = jnp.where(choice == 2 * tokens, tokens, source.transpose(1, 0, 2).reshape(-1))
        gate_at = jnp.where(choice == 2 * tokens, 0, choice)
        gates = gates.reshape(-1)
        partial = combine(8 * token_of, gate_at, gates, outputs, tokens)
        summed = lax.psum_scatter(partial, 'tp', scatter_dimension=0, tiled=True)
        result = (hidden.astype(F32) + summed.astype(F32)).astype(BF16)
        return gather_tp(result, tiled=True).reshape(rows, seq, width)

    in_specs = (P(('dp', 'ep'), None, None), P(('dp', 'ep')), P(('dp', 'ep'), None, None), P(), P(), P(None, None, 'tp', None), P(None, 'tp', None), P(None, None, 'tp', None), P(None, None, 'tp', None), P(None, 'tp', None), P(None, 'tp', None, None), P(), P(None, 'tp'), P('tp'), P('tp', None), P(), P(), P('ep', None, 'tp'), P('ep', 'tp'), P('ep', 'tp', None), P('ep', None))
    return jax.shard_map(local_fn, mesh=mesh, in_specs=in_specs, out_specs=P(('dp', 'ep'), None, None), check_vma=False)
```

```python
import functools

import jax
import jax.numpy as jnp
from jax import lax
from jax.experimental import pallas as pl
from jax.experimental.pallas import tpu as pltpu
from jax.sharding import PartitionSpec as P

LN_EPS = 1e-5
BF16 = jnp.bfloat16
F32 = jnp.float32
LOG2E = 1.4426950408889634


def dot_t(lhs, rhs_t):
    return lax.dot_general(lhs, rhs_t, (((1,), (1,)), ((), ())), preferred_element_type=F32)


HBM = pltpu.HBM


def norm_rows(value, gain, shift):
    centered = value - jnp.mean(value, axis=-1, keepdims=True)
    variance = jnp.mean(centered * centered, axis=-1, keepdims=True)
    return centered * lax.rsqrt(variance + LN_EPS) * gain + shift


def away(axis, size, distance):
    return lax.rem(lax.axis_index(axis) + distance, size)


def enter(groups):
    barrier = pltpu.get_barrier_semaphore()
    count = 0
    for axis, size in groups:
        for distance in range(1, size):
            pl.semaphore_signal(barrier, inc=1, device_id={axis: away(axis, size, distance)}, device_id_type=pl.DeviceIdType.MESH)
            count += 1
    pl.semaphore_wait(barrier, count)


def exchange(tp_size, weights, piece, landing_ref, send_sem, recv_sem):
    chunk, which, start, rows = piece
    return [pltpu.make_async_remote_copy(
        src_ref=weights[which].at[chunk * tp_size + away('tp', tp_size, distance), pl.ds(start, rows)], dst_ref=landing_ref.at[distance - 1],
        send_sem=send_sem.at[distance - 1], recv_sem=recv_sem.at[distance - 1],
        device_id={'tp': away('tp', tp_size, distance)}, device_id_type=pl.DeviceIdType.MESH)
        for distance in sorted(range(1, tp_size), key=lambda d: (min(d, tp_size - d), d))]


def exchange_all(tp_size, weights, pieces, landing_refs, send_sem, recv_sem):
    copies = []
    for index, piece in enumerate(pieces):
        copies += exchange(tp_size, weights, piece, landing_refs[index], send_sem.at[index], recv_sem.at[index])
    return copies


def landings(tp_size, weight, pieces):
    return [jax.ShapeDtypeStruct((tp_size - 1, rows, weight.shape[2]), BF16) for _, _, _, rows in pieces]


def move_body(tp_size, pieces, w_in_ref, w_out_ref, after_ref, *rest):
    copies = exchange_all(tp_size, (w_in_ref, w_out_ref), pieces, rest[:len(pieces)], *rest[len(pieces):])
    enter([('tp', tp_size)])
    for copy in copies:
        copy.start()
    for copy in copies:
        copy.wait()


def move(w_in, w_out, after, tp_size, pieces, call_id):
    hbm = pl.BlockSpec(memory_space=HBM)
    dma = pltpu.SemaphoreType.DMA((len(pieces), tp_size - 1))
    return pl.pallas_call(
        functools.partial(move_body, tp_size, pieces), out_shape=landings(tp_size, w_in, pieces),
        in_specs=[hbm, hbm, hbm], out_specs=[hbm for _ in pieces], scratch_shapes=[dma, dma],
        compiler_params=pltpu.CompilerParams(collective_id=call_id, has_side_effects=True, vmem_limit_bytes=56 * 1024 * 1024),
        cost_estimate=pl.CostEstimate(flops=20_000_000_000, transcendentals=0, bytes_accessed=10_000_000),
        name='move')(w_in, w_out, after)


def attention_body(tp_size, pieces, head_dim, block_q, lens_ref, x_ref, gain_ref, shift_ref, w_qkv_ref, b_qkv_ref, w_out_ref, b_out_ref, gain2_ref, shift2_ref, w_in_ref, w_exp_out_ref, after_ref,
                   hidden_ref, normed_ref, *rest):
    row = pl.program_id(0)
    block = pl.program_id(1)
    seq, width = x_ref.shape
    moved_refs = rest[:len(pieces)]
    qkv_ref, context_ref, send_sem, recv_sem = rest[len(pieces):]
    copies = exchange_all(tp_size, (w_in_ref, w_exp_out_ref), pieces, moved_refs, send_sem, recv_sem)

    @pl.when((row == 0) & (block == 0))
    def _():
        enter([('tp', tp_size)])
        for copy in copies:
            copy.start()

    @pl.when(block == 0)
    def _():
        def project(index, carry):
            rows = pl.ds(pl.multiple_of(index * block_q, block_q), block_q)
            normed = norm_rows(x_ref[rows, :].astype(F32), gain_ref[...], shift_ref[...]).astype(BF16)
            qkv_ref[rows, :] = (dot_t(normed, w_qkv_ref[...]) + b_qkv_ref[...]).astype(BF16)
            return carry
        lax.fori_loop(0, seq // block_q, project, 0)

    length = lens_ref[row]
    pair = 2 * head_dim
    key_ok = lax.broadcasted_iota(jnp.int32, (1, seq), 1) < length
    lane_head = lax.broadcasted_iota(jnp.int32, (1, pair), 1) // head_dim
    factor = (head_dim ** -0.5) * LOG2E
    rows = pl.ds(pl.multiple_of(block * block_q, block_q), block_q)

    def heads(index, carry):
        lanes = pl.multiple_of(index * pair, pair)
        query = qkv_ref[rows, pl.ds(lanes, pair)]
        keys = qkv_ref[:, pl.ds(pl.multiple_of(lanes + width, pair), pair)]
        values = qkv_ref[:, pl.ds(pl.multiple_of(lanes + 2 * width, pair), pair)]
        result = None
        for head in range(2):
            scores = dot_t(jnp.where(lane_head == head, query, jnp.zeros_like(query)), keys)
            scores = jnp.where(key_ok, scores, -1e30)
            top = jnp.max(scores, axis=-1, keepdims=True)
            weights = jnp.exp2((scores - top) * factor)
            scale = 1.0 / jnp.sum(weights, axis=-1, keepdims=True)
            part = jnp.dot((weights * scale).astype(BF16), values, preferred_element_type=F32)
            result = part if result is None else jnp.where(lane_head == head, part, result)
        context_ref[:, pl.ds(lanes, pair)] = result.astype(BF16)
        return carry

    lax.fori_loop(0, width // pair, heads, 0)
    projected = jnp.dot(context_ref[...], w_out_ref[...], preferred_element_type=F32)
    hidden = (x_ref[rows, :].astype(F32) + projected + b_out_ref[...]).astype(BF16)
    hidden_ref[...] = hidden
    normed_ref[...] = norm_rows(hidden.astype(F32), gain2_ref[...], shift2_ref[...]).astype(BF16)

    @pl.when((row == pl.num_programs(0) - 1) & (block == pl.num_programs(1) - 1))
    def _():
        for copy in copies:
            copy.wait()


def attention_layer(x, lens, seq, head_dim, norm, w_qkv, b_qkv, w_out, b_out, norm2, w_exp_in, w_exp_out, after, tp_size, pieces, call_id):
    tokens, width = x.shape
    block_q = min(256, seq)
    blocks = seq // block_q
    fixed = lambda shape: pl.BlockSpec(shape, lambda r, q: (0,) * len(shape), pipeline_mode=pl.Buffered(1))
    moved = landings(tp_size, w_exp_in, pieces)
    hbm = pl.BlockSpec(memory_space=HBM)
    return pl.pallas_call(
        functools.partial(attention_body, tp_size, pieces, head_dim, block_q),
        out_shape=(jax.ShapeDtypeStruct((tokens, width), BF16), jax.ShapeDtypeStruct((tokens, width), BF16), *moved),
        grid=(tokens // seq, blocks),
        in_specs=[pl.BlockSpec(memory_space=pltpu.SMEM), pl.BlockSpec((seq, width), lambda r, q: (r, 0)), fixed((1, width)), fixed((1, width)),
                  fixed(w_qkv.shape), fixed((1, 3 * width)), fixed(w_out.shape), fixed((1, width)), fixed((1, width)), fixed((1, width)), hbm, hbm, hbm],
        out_specs=(pl.BlockSpec((block_q, width), lambda r, q: (r * blocks + q, 0)), pl.BlockSpec((block_q, width), lambda r, q: (r * blocks + q, 0)), *[hbm for _ in pieces]),
        scratch_shapes=[pltpu.VMEM((seq, 3 * width), BF16), pltpu.VMEM((block_q, width), BF16), pltpu.SemaphoreType.DMA((len(pieces), tp_size - 1)), pltpu.SemaphoreType.DMA((len(pieces), tp_size - 1))],
        compiler_params=pltpu.CompilerParams(dimension_semantics=('arbitrary', 'arbitrary'), collective_id=call_id, has_side_effects=True, vmem_limit_bytes=52 * 1024 * 1024),
        cost_estimate=pl.CostEstimate(flops=30_000_000_000, transcendentals=0, bytes_accessed=40_000_000),
        name='attention_layer')(lens, x, *norm, w_qkv, b_qkv, w_out, b_out, *norm2, w_exp_in, w_exp_out, after)


def dense_body(tp_size, pieces, parts, x_ref, normed_ref, w_in_ref, b_in_ref, w_out_ref, b_out_ref, w_exp_in_ref, w_exp_out_ref, o_ref, *rest):
    block = pl.program_id(0)
    copies = exchange_all(tp_size, (w_exp_in_ref, w_exp_out_ref), pieces, rest[:len(pieces)], *rest[len(pieces):])

    @pl.when(block == 0)
    def _():
        enter([('tp', tp_size)])
        for copy in copies:
            copy.start()

    size = w_in_ref.shape[0] // parts
    total = x_ref[...].astype(F32) + b_out_ref[...]
    for part in range(parts):
        cols = pl.ds(part * size, size)
        inner = jnp.maximum(dot_t(normed_ref[...], w_in_ref[cols, :]) + b_in_ref[:, cols], 0.0).astype(BF16)
        total += jnp.dot(inner, w_out_ref[cols, :], preferred_element_type=F32)
    o_ref[...] = total.astype(BF16)

    @pl.when(block == pl.num_programs(0) - 1)
    def _():
        for copy in copies:
            copy.wait()


def dense_layer(x, normed, w_in, b_in, w_out, b_out, w_exp_in, w_exp_out, tp_size, pieces, call_id):
    tokens, width = x.shape
    block_n = min(256, tokens)
    fixed = lambda shape: pl.BlockSpec(shape, lambda i: (0,) * len(shape), pipeline_mode=pl.Buffered(1))
    hbm = pl.BlockSpec(memory_space=HBM)
    dma = pltpu.SemaphoreType.DMA((len(pieces), tp_size - 1))
    return pl.pallas_call(
        functools.partial(dense_body, tp_size, pieces, 4),
        out_shape=(jax.ShapeDtypeStruct((tokens, width), BF16), *landings(tp_size, w_exp_in, pieces)), grid=(tokens // block_n,),
        in_specs=[pl.BlockSpec((block_n, width), lambda i: (i, 0)), pl.BlockSpec((block_n, width), lambda i: (i, 0)), fixed(w_in.shape), fixed(b_in.shape), fixed(w_out.shape), fixed((1, width)), hbm, hbm],
        out_specs=(pl.BlockSpec((block_n, width), lambda i: (i, 0)), *[hbm for _ in pieces]),
        scratch_shapes=[dma, dma],
        compiler_params=pltpu.CompilerParams(dimension_semantics=('arbitrary',), collective_id=call_id, has_side_effects=True, vmem_limit_bytes=52 * 1024 * 1024),
        cost_estimate=pl.CostEstimate(flops=20_000_000_000, transcendentals=0, bytes_accessed=30_000_000),
        name='dense_layer')(x, normed, w_in, b_in, w_out, b_out, w_exp_in, w_exp_out)


def experts_body(tp_size, ep_size, early, late, dispatch_ref, early_refs, w_in_ref, w_out_ref, b_in_ref, b_out_ref, w_router_ref, other_ref, returned_ref, gates_ref,
                 sent_buf, arrived_ref, parts_buf, own_buf, out_buf, local_sem, send_sem, recv_sem, back_send, back_recv, move_send, move_recv):
    chunks, _, slots, width = arrived_ref.shape
    me = lax.axis_index('ep')
    mine = lax.axis_index('tp')
    weights = (w_in_ref, w_out_ref)
    units = [(chunk, which) for chunk in range(chunks) for which in range(2)]

    sends = {}
    for chunk in range(chunks):
        for distance in range(1, ep_size):
            peer = away('ep', ep_size, distance)
            sends[chunk, distance] = pltpu.make_async_remote_copy(
                src_ref=dispatch_ref.at[chunk, peer], dst_ref=arrived_ref.at[chunk, me], send_sem=send_sem.at[chunk, distance], recv_sem=recv_sem.at[chunk, distance],
                device_id={'ep': peer}, device_id_type=pl.DeviceIdType.MESH)
    def landing(piece):
        chunk, which, start, rows = piece
        return parts_buf.at[units.index((chunk, which)), :, pl.ds(start, rows)]

    moves = {piece: exchange(tp_size, weights, piece, landing(piece), move_send.at[index], move_recv.at[index]) for index, piece in enumerate(late)}
    kept = [pltpu.make_async_copy(dispatch_ref.at[chunk, me], arrived_ref.at[chunk, me], local_sem.at[0, chunk]) for chunk in range(chunks)]
    owns = {unit: pltpu.make_async_copy(weights[unit[1]].at[unit[0] * tp_size + mine], own_buf.at[unit[0], unit[1]], local_sem.at[1 + unit[1], unit[0]]) for unit in units}
    earlies = {piece: pltpu.make_async_copy(early_refs[index], landing(piece), local_sem.at[3, index]) for index, piece in enumerate(early)}

    enter([('tp', tp_size), ('ep', ep_size)])
    for piece in late:
        for copy in moves[piece]:
            copy.start()
    for chunk in range(chunks):
        for distance in range(1, ep_size):
            sends[chunk, distance].start()
        kept[chunk].start()
    for unit in units:
        owns[unit].start()
        for piece in early:
            if piece[:2] == unit:
                earlies[piece].start()

    lane = lax.broadcasted_iota(jnp.int32, (1, w_router_ref.shape[1]), 1)
    group = lax.broadcasted_iota(jnp.int32, (ep_size * slots, 1), 0) // slots

    def load(chunk):
        return pltpu.make_async_copy(dispatch_ref.at[chunk], sent_buf.at[chunk % 2], local_sem.at[5, chunk % 2])

    load(0).start()
    for chunk in range(chunks):
        if chunk + 1 < chunks:
            load(chunk + 1).start()
        load(chunk).wait()
        logits = jnp.dot(sent_buf[chunk % 2].reshape(ep_size * slots, width), w_router_ref[...], preferred_element_type=F32)
        rows = pl.ds(chunk * ep_size * slots, ep_size * slots)
        own = jnp.sum(jnp.where(lane == group * (chunks * tp_size) + (chunk * tp_size + mine), logits, 0.0), axis=1, keepdims=True)
        other = jnp.sum(jnp.where(lane == other_ref[rows, :], logits, 0.0), axis=1, keepdims=True)
        gates_ref[rows, :] = jax.nn.sigmoid(own - other)

    def part_ref(unit, part):
        if part == 0:
            return own_buf.at[unit[0], unit[1]]
        return parts_buf.at[units.index(unit), part - 1]

    def give_back(chunk, slot, index):
        for half in range(2):
            peer = 2 * index + half
            distance = lax.rem(peer - me + ep_size, ep_size)

            @pl.when(distance == 0)
            def _():
                pltpu.make_async_copy(out_buf.at[slot, peer], returned_ref.at[chunk, me], local_sem.at[4, chunk]).start()

            @pl.when(distance != 0)
            def _():
                pltpu.make_async_remote_copy(
                    src_ref=out_buf.at[slot, peer], dst_ref=returned_ref.at[chunk, me], send_sem=back_send.at[chunk, distance], recv_sem=back_recv.at[chunk, distance],
                    device_id={'ep': peer}, device_id_type=pl.DeviceIdType.MESH).start()

    backs = {}
    for chunk in range(chunks):
        slot = chunk % out_buf.shape[0]
        for distance in range(1, ep_size):
            sends[chunk, distance].wait_recv()
        kept[chunk].wait()
        for which in range(2):
            unit = (chunk, which)
            owns[unit].wait()
            for piece in early:
                if piece[:2] == unit:
                    earlies[piece].wait()
            for piece in late:
                if piece[:2] == unit:
                    for copy in moves[piece]:
                        copy.wait_recv()
        before = chunk - out_buf.shape[0]
        if before >= 0:
            for copy in backs[before][:-1]:
                copy.wait_send()
            backs[before][-1].wait()

        def rows(index, carry):
            tokens = arrived_ref[chunk, pl.ds(2 * index, 2)].reshape(2 * slots, width)
            total = jnp.zeros((2 * slots, width), F32)
            for part in range(tp_size):
                inner = jnp.dot(tokens, part_ref((chunk, 0), part)[...], preferred_element_type=F32) + b_in_ref[chunk, pl.ds(part, 1), :]
                total += jnp.dot(jnp.maximum(inner, 0.0).astype(BF16), part_ref((chunk, 1), part)[...], preferred_element_type=F32)
            out_buf[slot, pl.ds(2 * index, 2)] = (total + b_out_ref[pl.ds(chunk, 1), :]).astype(BF16).reshape(2, slots, width)

            @pl.when(index > 0)
            def _():
                give_back(chunk, slot, index - 1)

            return carry

        lax.fori_loop(0, ep_size // 2, rows, 0)
        give_back(chunk, slot, ep_size // 2 - 1)
        backs[chunk] = []
        for distance in range(1, ep_size):
            peer = away('ep', ep_size, distance)
            backs[chunk].append(pltpu.make_async_remote_copy(
                src_ref=out_buf.at[slot, peer], dst_ref=returned_ref.at[chunk, me], send_sem=back_send.at[chunk, distance], recv_sem=back_recv.at[chunk, distance],
                device_id={'ep': peer}, device_id_type=pl.DeviceIdType.MESH))
        backs[chunk].append(pltpu.make_async_copy(out_buf.at[slot, me], returned_ref.at[chunk, me], local_sem.at[4, chunk]))
    for chunk in range(chunks):
        for distance in range(1, ep_size):
            sends[chunk, distance].wait_send()
        for copy in backs[chunk][:-1]:
            copy.wait_recv()
            if chunk + out_buf.shape[0] >= chunks:
                copy.wait_send()
        if chunk + out_buf.shape[0] >= chunks:
            backs[chunk][-1].wait()
    for piece in late:
        for copy in moves[piece]:
            copy.wait_send()


def experts(dispatch, early_weights, w_in, w_out, b_in, b_out, w_router, other, tp_size, ep_size, early, late, call_id):
    chunks, _, slots, width = dispatch.shape
    hidden = w_in.shape[2]
    hbm = pl.BlockSpec(memory_space=HBM)
    vmem = pl.BlockSpec(memory_space=pltpu.VMEM)

    def body(dispatch_ref, *refs):
        experts_body(tp_size, ep_size, early, late, dispatch_ref, refs[:len(early)], *refs[len(early):])

    dma = pltpu.SemaphoreType.DMA
    return pl.pallas_call(
        body, out_shape=(jax.ShapeDtypeStruct(dispatch.shape, BF16), jax.ShapeDtypeStruct(other.shape, F32)),
        in_specs=[hbm] * (3 + len(early)) + [vmem] * 4, out_specs=(hbm, vmem),
        scratch_shapes=[pltpu.VMEM((2,) + dispatch.shape[1:], BF16), pltpu.VMEM(dispatch.shape, BF16), pltpu.VMEM((2 * chunks, tp_size - 1, width, hidden), BF16),
                        pltpu.VMEM((chunks, 2, width, hidden), BF16), pltpu.VMEM((2, ep_size, slots, width), BF16),
                        dma((6, max(chunks, len(early)))), dma((chunks, ep_size)), dma((chunks, ep_size)), dma((chunks, ep_size)), dma((chunks, ep_size)),
                        dma((len(late), tp_size - 1)), dma((len(late), tp_size - 1))],
        compiler_params=pltpu.CompilerParams(collective_id=call_id, has_side_effects=True, vmem_limit_bytes=62 * 1024 * 1024),
        cost_estimate=pl.CostEstimate(flops=4 * chunks * ep_size * slots * width * hidden * tp_size, transcendentals=0, bytes_accessed=60_000_000),
        name='experts')(dispatch, *early_weights, w_in, w_out, b_in, b_out, w_router, other)


def combine_body(blocks, token_ref, slots_ref, gates_ref, o_ref, acc_ref, wide_ref):
    block = pl.program_id(0)
    slots, width = slots_ref.shape
    step = o_ref.shape[0]
    lanes = 128

    @pl.when(block == 0)
    def _():
        def clear(index, carry):
            acc_ref[pl.ds(pl.multiple_of(index * 256, 256), 256), :] = jnp.zeros((256, lanes), F32)
            return carry
        lax.fori_loop(0, acc_ref.shape[0] // 256, clear, 0)

    @pl.when(block < blocks)
    def _():
        for col in range(width // lanes):
            wide_ref[pl.ds(col, slots, stride=8), :] = slots_ref[:, col * lanes:(col + 1) * lanes].astype(F32) * gates_ref[...]
        base = block * slots

        def add(index, carry):
            first = index * 16
            places = [pl.ds(pl.multiple_of(token_ref[base + first + u], 8), 8) for u in range(16)]
            start = pl.multiple_of(index * 128, 128)
            new = [acc_ref[places[u], :] + wide_ref[pl.ds(start + u * 8, 8), :] for u in range(16)]
            for u in range(16):
                acc_ref[places[u], :] = new[u]
            return carry

        lax.fori_loop(0, slots // 16, add, 0)

    @pl.when(block >= blocks)
    def _():
        first = pl.multiple_of((block - blocks) * (step * 8), step * 8)
        for col in range(width // lanes):
            o_ref[:, col * lanes:(col + 1) * lanes] = acc_ref[pl.ds(first + col, step, stride=8), :].astype(BF16)


def combine(place, gates, outputs, tokens):
    blocks, slots, width = outputs.shape
    step = min(512, tokens)
    grid_spec = pltpu.PrefetchScalarGridSpec(
        num_scalar_prefetch=1, grid=(blocks + tokens // step,),
        in_specs=[pl.BlockSpec((None, slots, width), lambda b, *_: (jnp.minimum(b, blocks - 1), 0, 0)), pl.BlockSpec((slots, 1), lambda b, *_: (jnp.minimum(b, blocks - 1), 0))],
        out_specs=pl.BlockSpec((step, width), lambda b, *_: (jnp.maximum(b - blocks, 0), 0)),
        scratch_shapes=[pltpu.VMEM(((tokens + 32) * 8, 128), F32), pltpu.VMEM((slots * 8, 128), F32)])
    return pl.pallas_call(
        functools.partial(combine_body, blocks),
        out_shape=jax.ShapeDtypeStruct((tokens, width), BF16), grid_spec=grid_spec,
        compiler_params=pltpu.CompilerParams(dimension_semantics=('arbitrary',), vmem_limit_bytes=56 * 1024 * 1024),
        cost_estimate=pl.CostEstimate(flops=15_000_000_000, transcendentals=0, bytes_accessed=2 * tokens * width + 2 * blocks * slots * width),
        name='combine')(place, outputs, gates)


def finish_body(tp_size, count, partial_ref, hidden_ref, o_ref, partial_buf, hidden_buf, sum_buf, own_buf, load_sem, sum_send, sum_recv, out_send, out_recv):
    me = lax.axis_index('tp')
    own_tokens, _ = hidden_ref.shape
    size = own_tokens // (2 * count)
    hops = tp_size - 1
    step_to = (1, tp_size - 1)

    def rows(way, chunk, index):
        return pl.ds(pl.multiple_of(chunk * own_tokens + (way * count + index) * size, size), size)

    def behind(way, distance):
        return away('tp', tp_size, (tp_size - distance) % tp_size if way == 0 else distance % tp_size)

    def send_sum(way, hop, index, src_ref):
        return pltpu.make_async_remote_copy(
            src_ref=src_ref, dst_ref=sum_buf.at[way, hop, index], send_sem=sum_send.at[way, hop, index], recv_sem=sum_recv.at[way, hop, index],
            device_id={'tp': away('tp', tp_size, step_to[way])}, device_id_type=pl.DeviceIdType.MESH)

    def send_out(way, hop, index, src_ref, chunk):
        return pltpu.make_async_remote_copy(
            src_ref=src_ref, dst_ref=o_ref.at[rows(way, chunk, index)], send_sem=out_send.at[way, hop, index], recv_sem=out_recv.at[way, hop, index],
            device_id={'tp': away('tp', tp_size, step_to[way])}, device_id_type=pl.DeviceIdType.MESH)

    loads = [pltpu.make_async_copy(partial_ref, partial_buf, load_sem.at[0]), pltpu.make_async_copy(hidden_ref, hidden_buf, load_sem.at[1])]
    for load in loads:
        load.start()
    barrier = pltpu.get_barrier_semaphore()
    for distance in step_to:
        pl.semaphore_signal(barrier, inc=1, device_id={'tp': away('tp', tp_size, distance)}, device_id_type=pl.DeviceIdType.MESH)
    pl.semaphore_wait(barrier, 2)

    def first(index, carry):
        for way in range(2):
            send_sum(way, 0, index, partial_ref.at[rows(way, behind(way, 1), index)]).start()
        return carry

    lax.fori_loop(0, count, first, 0)
    for load in loads:
        load.wait()

    def keep(way, index):
        own = own_buf.at[way, index]
        return pltpu.make_async_copy(own, o_ref.at[rows(way, me, index)], load_sem.at[2 + way])

    for hop in range(1, tp_size):
        def add(index, carry):
            for way in range(2):
                send_sum(way, hop - 1, index, sum_buf.at[way, hop - 1, index]).wait_recv()
                total = sum_buf[way, hop - 1, index].astype(F32) + partial_buf[rows(way, behind(way, hop + 1), index), :].astype(F32)
                if hop < hops:
                    sum_buf[way, hop - 1, index] = total.astype(BF16)
                else:
                    own_rows = pl.ds(pl.multiple_of((way * count + index) * size, size), size)
                    own_buf[way, index] = (total.astype(BF16).astype(F32) + hidden_buf[own_rows, :].astype(F32)).astype(BF16)
            for way in range(2):
                if hop < hops:
                    send_sum(way, hop, index, sum_buf.at[way, hop - 1, index]).start()
                else:
                    send_out(way, 0, index, own_buf.at[way, index], me).start()
                    keep(way, index).start()
                    keep(way, index).wait()
            return carry

        lax.fori_loop(0, count, add, 0)

    for hop in range(1, tp_size):
        def forward(index, carry):
            for way in range(2):
                chunk = behind(way, hop)
                arrived = o_ref.at[rows(way, chunk, index)]
                send_out(way, hop - 1, index, arrived, chunk).wait_recv()
                if hop < hops:
                    send_out(way, hop, index, arrived, chunk).start()
            return carry

        lax.fori_loop(0, count, forward, 0)

    def drain(index, carry):
        for way in range(2):
            for hop in range(hops):
                send_sum(way, hop, index, sum_buf.at[way, hop, index]).wait_send()
                send_out(way, hop, index, own_buf.at[way, index], me).wait_send()
        return carry

    lax.fori_loop(0, count, drain, 0)


def finish(partial, hidden, tp_size, call_id):
    tokens, width = partial.shape
    own_tokens = hidden.shape[0]
    size = min(256, own_tokens // 2)
    count = own_tokens // (2 * size)
    hops = tp_size - 1
    hbm = pl.BlockSpec(memory_space=HBM)
    dma = pltpu.SemaphoreType.DMA
    return pl.pallas_call(
        functools.partial(finish_body, tp_size, count), out_shape=jax.ShapeDtypeStruct(partial.shape, BF16), in_specs=[hbm, hbm], out_specs=hbm,
        scratch_shapes=[pltpu.VMEM(partial.shape, BF16), pltpu.VMEM(hidden.shape, BF16), pltpu.VMEM((2, hops, count, size, width), BF16), pltpu.VMEM((2, count, size, width), BF16),
                        dma((4,)), dma((2, hops, count)), dma((2, hops, count)), dma((2, hops, count)), dma((2, hops, count))],
        compiler_params=pltpu.CompilerParams(collective_id=call_id, has_side_effects=True, vmem_limit_bytes=56 * 1024 * 1024),
        cost_estimate=pl.CostEstimate(flops=100_000_000_000, transcendentals=0, bytes_accessed=60_000_000),
        name='finish')(partial, hidden)


def route(key_ok, expert_idx, num_experts, capacity):
    tokens = key_ok.size
    valid = key_ok.reshape(tokens)
    first = expert_idx[..., 0].reshape(tokens)
    second = expert_idx[..., 1].reshape(tokens)
    expert_ids = jnp.arange(num_experts, dtype=jnp.int32)
    hot_first = ((first[:, None] == expert_ids) & valid[:, None]).astype(jnp.int32)
    hot_second = ((second[:, None] == expert_ids) & valid[:, None]).astype(jnp.int32)
    rank_first = jnp.cumsum(hot_first, axis=0) - 1
    rank_second = jnp.cumsum(hot_second, axis=0) - 1 + jnp.sum(hot_first, axis=0)
    slot_first = jnp.sum(rank_first * hot_first, axis=1)
    slot_second = jnp.sum(rank_second * hot_second, axis=1)
    dump = num_experts * capacity
    dest_first = jnp.where(valid & (slot_first < capacity), first * capacity + slot_first, dump)
    dest_second = jnp.where(valid & (slot_second < capacity), second * capacity + slot_second, dump)
    choice = jnp.full((dump + 1,), -1, jnp.int32)
    ids = jnp.arange(tokens, dtype=jnp.int32)
    choice = choice.at[dest_first].set(ids + tokens * second).at[dest_second].set(ids + tokens * first)
    return choice[:dump].reshape(num_experts, capacity)


def solution(mesh):
    tp_size = mesh.shape['tp']
    ep_size = mesh.shape['ep']

    def gather_tp(value, axis=0, tiled=False):
        return lax.all_gather(value, 'tp', axis=axis, tiled=tiled)

    def local_fn(x, src_len, expert_idx, ln_gain, ln_bias, w_query, b_query, w_key, w_value, b_value, w_attn_out, b_attn_out, w_fc1, b_fc1, w_fc2, b_fc2, w_router, w_exp_in, b_exp_in, w_exp_out, b_exp_out):
        rows, seq, width = x.shape
        tokens = rows * seq
        num_experts = w_router.shape[1]
        capacity = 2 * (-(-tokens // num_experts))
        local_experts = w_exp_in.shape[0]
        own_experts = local_experts // tp_size
        _, _, local_heads, head_dim = w_query.shape
        heads = local_heads * tp_size
        head_cols = local_heads * head_dim
        hidden_cols = w_fc1.shape[1]
        tp_index = lax.axis_index('tp')
        ep_index = lax.axis_index('ep')
        own_rows = rows // tp_size
        own_tokens = own_rows * seq
        x_own = lax.dynamic_slice_in_dim(x, tp_index * own_rows, own_rows, 0).reshape(own_tokens, width)
        len_own = lax.dynamic_slice_in_dim(src_len, tp_index * own_rows, own_rows, 0)

        def pack_attention(j):
            columns = [w[j].reshape(width, head_cols).T for w in (w_query, w_key, w_value)]
            return jnp.concatenate(columns + [w_attn_out[j].reshape(head_cols, width)], axis=0)

        def unpack_attention(gathered):
            by_kind = gathered.reshape(4, ep_size // 4, tp_size, -1, width).transpose(0, 2, 1, 3, 4)
            return by_kind[:3].reshape(3 * heads * head_dim, width), by_kind[3].reshape(heads * head_dim, width)

        def own_slice(value):
            size = value.shape[0] // ep_size
            return lax.dynamic_slice_in_dim(value, ep_index * size, size, 0)

        slices = [own_slice(value) for value in (pack_attention(0), w_fc1.T, w_fc2, pack_attention(1))]
        cuts = [value.shape[0] for value in slices]
        slices = gather_tp(jnp.concatenate(slices, axis=0))
        small = jnp.concatenate([b_query.reshape(-1), b_value.reshape(-1), b_fc1.reshape(-1), b_exp_in.reshape(-1)])
        small = gather_tp(small)
        slices, small, x_own = lax.optimization_barrier((slices, small, x_own))
        starts = [sum(cuts[:i]) for i in range(5)]
        first_pack = lax.all_gather(slices[:, :starts[1]], 'ep')
        fc1_all, fc2_all, second_pack = [lax.all_gather(slices[:, starts[i]:starts[i + 1]], 'ep') for i in range(1, 4)]
        fc1_all, fc2_all = fc1_all.reshape(-1, width), fc2_all.reshape(-1, width)
        cut = cuts[1]
        attn_bias_size = 2 * head_cols
        b_query_all = small[:, :attn_bias_size].reshape(tp_size, 2, head_cols).transpose(1, 0, 2).reshape(2, -1)
        b_value_all = small[:, attn_bias_size:2 * attn_bias_size].reshape(tp_size, 2, head_cols).transpose(1, 0, 2).reshape(2, -1)
        b_fc1_all = small[:, 2 * attn_bias_size:2 * attn_bias_size + hidden_cols]
        b_exp_in_all = small[:, 2 * attn_bias_size + hidden_cols:].reshape(tp_size, local_experts, -1)
        b_qkv = jnp.concatenate([b_query_all, jnp.zeros_like(b_query_all), b_value_all], axis=1)
        b_fc1_all = b_fc1_all.reshape(tp_size, ep_size, cut).transpose(1, 0, 2).reshape(-1)

        key_ok = jnp.arange(seq)[None, :] < src_len[:, None]
        choice_all = route(key_ok, expert_idx, num_experts, capacity)
        choice = choice_all.reshape(ep_size, own_experts, tp_size, capacity)
        choice = lax.dynamic_index_in_dim(choice, tp_index, 2, keepdims=False)
        choice = choice.transpose(1, 0, 2).reshape(-1)
        filled = choice >= 0
        choice = jnp.where(filled, choice, 0)
        source = lax.rem(choice, tokens)
        other = lax.div(choice, tokens).reshape(-1, 1)
        place = 8 * jnp.where(filled, source, tokens)

        def norm(i):
            return ln_gain[i].reshape(1, width), ln_bias[i].reshape(1, width)

        def row(value):
            return value.reshape(1, -1)

        half = width // 2
        pieces = [(2, 1, 0, half)], [(0, 0, 0, width), (0, 1, 0, width)], [(1, 0, 0, width)], [(1, 1, 0, width), (2, 0, 0, width)], [(2, 1, half, half), (3, 0, 0, width), (3, 1, 0, width)]
        moved = []
        moved += move(w_exp_in, w_exp_out, slices[0, :8], tp_size, pieces[0], 4)
        w_qkv, w_out = unpack_attention(first_pack)
        hidden, normed, *landed = attention_layer(x_own, len_own, seq, head_dim, norm(0), w_qkv, row(b_qkv[0]), w_out, row(b_attn_out[0]), norm(1), w_exp_in, w_exp_out, moved[0], tp_size, pieces[1], 0)
        moved += landed
        second_pack, hidden = lax.optimization_barrier((second_pack, hidden))
        hidden, *landed = dense_layer(hidden, normed, fc1_all, row(b_fc1_all), fc2_all, row(b_fc2), w_exp_in, w_exp_out, tp_size, pieces[2], 1)
        moved += landed
        w_qkv, w_out = unpack_attention(second_pack)
        hidden, normed, *landed = attention_layer(hidden, len_own, seq, head_dim, norm(2), w_qkv, row(b_qkv[1]), w_out, row(b_attn_out[1]), norm(3), w_exp_in, w_exp_out, moved[0], tp_size, pieces[3], 2)
        moved += landed
        normed_all = gather_tp(normed, tiled=True)

        b_in_own = lax.dynamic_index_in_dim(b_exp_in_all.reshape(tp_size, own_experts, tp_size, -1), tp_index, 2, keepdims=False)
        part_order = lax.rem(tp_index - jnp.arange(tp_size) + tp_size, tp_size)
        b_in_own = b_in_own[part_order].transpose(1, 0, 2)
        b_out_own = lax.dynamic_index_in_dim(b_exp_out.reshape(own_experts, tp_size, width), tp_index, 1, keepdims=False)
        dispatch = normed_all[source].reshape(own_experts, ep_size, capacity, width)
        outputs, gates = experts(dispatch, moved, w_exp_in, w_exp_out, b_in_own, b_out_own,
                                 w_router.astype(BF16), other, tp_size, ep_size, sum(pieces[:4], []), pieces[4], 3)
        outputs = outputs.reshape(own_experts * ep_size, capacity, width)
        partial = combine(place, gates, outputs, tokens)
        return finish(partial, hidden, tp_size, 5).reshape(rows, seq, width)

    in_specs = (P(('dp', 'ep'), None, None), P(('dp', 'ep')), P(('dp', 'ep'), None, None), P(), P(), P(None, None, 'tp', None), P(None, 'tp', None), P(None, None, 'tp', None), P(None, None, 'tp', None), P(None, 'tp', None), P(None, 'tp', None, None), P(), P(None, 'tp'), P('tp'), P('tp', None), P(), P(), P('ep', None, 'tp'), P('ep', 'tp'), P('ep', 'tp', None), P('ep', None))
    return jax.shard_map(local_fn, mesh=mesh, in_specs=in_specs, out_specs=P(('dp', 'ep'), None, None), check_vma=False)
```

```python
import functools

import jax
import jax.numpy as jnp
from jax import lax
from jax.experimental import pallas as pl
from jax.experimental.pallas import tpu as pltpu
from jax.sharding import PartitionSpec as P

LN_EPS = 1e-5
BF16 = jnp.bfloat16
F32 = jnp.float32
LOG2E = 1.4426950408889634


MESH = pl.DeviceIdType.MESH
VMEM_SPEC = pl.BlockSpec(memory_space=pltpu.VMEM)
HBM_SPEC = pl.BlockSpec(memory_space=pltpu.HBM)
SMEM_SPEC = pl.BlockSpec(memory_space=pltpu.SMEM)
DMA = pltpu.SemaphoreType.DMA


def span(index, size):
    return pl.ds(pl.multiple_of(index * size, size), size)


def settings(call_id=None, mib=56, grid=None):
    return pltpu.CompilerParams(dimension_semantics=grid, collective_id=call_id, has_side_effects=call_id is not None, vmem_limit_bytes=mib << 20)


def cost(gflops):
    return pl.CostEstimate(flops=gflops * 10**9, transcendentals=0, bytes_accessed=10**7)


def dot_t(lhs, rhs_t):
    return lax.dot_general(lhs, rhs_t, (((1,), (1,)), ((), ())), preferred_element_type=F32)


def norm_rows(value, gain, shift):
    centered = value - jnp.mean(value, axis=-1, keepdims=True)
    variance = jnp.mean(centered * centered, axis=-1, keepdims=True)
    return centered * lax.rsqrt(variance + LN_EPS) * gain + shift


def away(axis, size, distance):
    return lax.rem(lax.axis_index(axis) + distance, size)


def enter(groups):
    barrier = pltpu.get_barrier_semaphore()
    count = 0
    for axis, size in groups:
        for distance in range(1, size):
            pl.semaphore_signal(barrier, device_id={axis: away(axis, size, distance)}, device_id_type=MESH)
            count += 1
    pl.semaphore_wait(barrier, count)


def exchange(tp_size, weights, piece, landing_ref, send_sem, recv_sem):
    chunk, which, start, rows = piece
    return [pltpu.make_async_remote_copy(
        src_ref=weights[which].at[chunk * tp_size + away('tp', tp_size, distance), pl.ds(start, rows)], dst_ref=landing_ref.at[distance - 1],
        send_sem=send_sem.at[distance - 1], recv_sem=recv_sem.at[distance - 1],
        device_id={'tp': away('tp', tp_size, distance)}, device_id_type=MESH)
        for distance in sorted(range(1, tp_size), key=lambda d: (min(d, tp_size - d), d))]


def exchange_all(tp_size, weights, pieces, landing_refs, send_sem, recv_sem):
    copies = []
    for index, piece in enumerate(pieces):
        copies += exchange(tp_size, weights, piece, landing_refs[index], send_sem.at[index], recv_sem.at[index])
    return copies


def landings(tp_size, weight, pieces):
    return [jax.ShapeDtypeStruct((tp_size - 1, rows, weight.shape[2]), BF16) for _, _, _, rows in pieces]


def route_tables(lens_ref, index_ref, total_ref, total_t_ref):
    rows, _, seq = index_ref.shape
    step = min(512, seq)
    per_row = seq // step
    experts_count, wide = total_ref.shape
    slots = wide // 3
    ids = lax.broadcasted_iota(jnp.int32, (experts_count, 1), 0)
    slot_ids = lax.broadcasted_iota(jnp.int32, (slots, 1), 0)
    before = (lax.broadcasted_iota(jnp.int32, (step, step), 0) < lax.broadcasted_iota(jnp.int32, (step, step), 1)).astype(BF16)
    total_ref[...] = jnp.zeros_like(total_ref)
    total_t_ref[...] = jnp.zeros_like(total_t_ref)
    count = jnp.zeros((experts_count, 1), F32)
    for choice in range(2):
        def block(index, count):
            row = index // per_row
            start = pl.multiple_of((index % per_row) * step, step)
            cols = pl.ds(start, step)
            position = lax.broadcasted_iota(jnp.int32, (1, step), 1) + start
            chosen = jnp.where(position < lens_ref[row], index_ref[row, pl.ds(choice, 1), cols], -1)
            other = index_ref[row, pl.ds(1 - choice, 1), cols]
            token = position + row * seq
            hot = jnp.where(ids == chosen, 1.0, 0.0)
            rank = jnp.dot(hot.astype(BF16), before, preferred_element_type=F32) + count
            slot = jnp.sum(rank * hot, axis=0, keepdims=True).astype(jnp.int32)
            at_slot = slot_ids == slot
            parts = [jnp.where(at_slot, value.astype(F32), 0.0).astype(BF16) for value in (token & 255, (token >> 8) + 1, other)]
            values = jnp.concatenate(parts, axis=0)
            hot16 = hot.astype(BF16)
            total_ref[...] += dot_t(hot16, values)
            total_t_ref[...] += dot_t(values, hot16)
            return count + jnp.sum(hot, axis=1, keepdims=True)

        count = lax.fori_loop(0, rows * per_row, block, count)


def move_body(tp_size, ep_size, pieces, own_experts, lens_ref, index_ref, w_in_ref, w_out_ref, after_ref, place_ref, source_ref, other_ref, *rest):
    moved_refs = rest[:len(pieces)]
    total_ref, total_t_ref, send_sem, recv_sem = rest[len(pieces):]
    copies = exchange_all(tp_size, (w_in_ref, w_out_ref), pieces, moved_refs, send_sem, recv_sem)
    enter([('tp', tp_size)])
    for copy in copies:
        copy.start()
    route_tables(lens_ref, index_ref, total_ref, total_t_ref)
    rows, _, seq = index_ref.shape
    experts_count, wide = total_ref.shape
    slots = wide // 3
    lane = lax.broadcasted_iota(jnp.int32, (1, experts_count), 1)

    def take(index, carry):
        chunk = index // ep_size
        expert = (index % ep_size) * (own_experts * tp_size) + chunk * tp_size + lax.axis_index('tp')
        line = total_ref[pl.ds(expert, 1), :].astype(jnp.int32)
        low, high = line[:, :slots], line[:, slots:2 * slots]
        place_ref[pl.ds(index, 1), :] = 8 * jnp.where(high > 0, 256 * (high - 1) + low, rows * seq)
        column = jnp.sum(jnp.where(lane == expert, total_t_ref[...], 0.0), axis=1, keepdims=True).astype(jnp.int32)
        low, high, other = column[:slots], column[slots:2 * slots], column[2 * slots:]
        at = span(index, slots)
        source_ref[at, :] = jnp.where(high > 0, 256 * (high - 1) + low, -1)
        other_ref[at, :] = other
        return carry

    lax.fori_loop(0, own_experts * ep_size, take, 0)
    for copy in copies:
        copy.wait()


def move(lens, index, w_in, w_out, after, num_experts, capacity, tp_size, ep_size, pieces, call_id):
    own_experts = w_in.shape[0] // tp_size
    blocks = own_experts * ep_size
    dma = DMA((len(pieces), tp_size - 1))
    column = jax.ShapeDtypeStruct((blocks * capacity, 1), jnp.int32)
    return pl.pallas_call(
        functools.partial(move_body, tp_size, ep_size, pieces, own_experts),
        out_shape=(jax.ShapeDtypeStruct((blocks, capacity), jnp.int32), column, column, *landings(tp_size, w_in, pieces)),
        in_specs=[SMEM_SPEC, VMEM_SPEC, HBM_SPEC, HBM_SPEC, HBM_SPEC], out_specs=(VMEM_SPEC, VMEM_SPEC, VMEM_SPEC, *[HBM_SPEC for _ in pieces]),
        scratch_shapes=[pltpu.VMEM((num_experts, 3 * capacity), F32), pltpu.VMEM((3 * capacity, num_experts), F32), dma, dma],
        compiler_params=settings(call_id),
        cost_estimate=cost(30),
        name='move')(lens, index, w_in, w_out, after)


def dispatch_body(tp_size, source_ref, normed_ref, o_ref, all_buf, acc_ref, load_sem, send_sem, recv_sem):
    me = lax.axis_index('tp')
    _, count, size, width = normed_ref.shape
    own_tokens = 2 * count * size
    slots = source_ref.shape[0]
    block = min(512, slots)
    hops = tp_size - 1
    step_to = (1, tp_size - 1)
    lane = lax.broadcasted_iota(jnp.int32, (1, size), 1)

    def behind(way, distance):
        return away('tp', tp_size, (tp_size - distance) % tp_size if way == 0 else distance % tp_size)

    def send(way, hop, index, src_ref, chunk):
        return pltpu.make_async_remote_copy(
            src_ref=src_ref, dst_ref=all_buf.at[chunk, way, index], send_sem=send_sem.at[way, hop, index], recv_sem=recv_sem.at[way, hop, index],
            device_id={'tp': away('tp', tp_size, step_to[way])}, device_id_type=MESH)

    load = pltpu.make_async_copy(normed_ref, all_buf.at[me], load_sem)
    load.start()
    enter([('tp', tp_size)])

    def first(index, carry):
        for way in range(2):
            send(way, 0, index, normed_ref.at[way, index], me).start()
        return carry

    lax.fori_loop(0, count, first, 0)
    load.wait()

    def place(index, chunks, fresh):
        def some(part, carry):
            at = span(part, block)
            total = None if fresh else acc_ref[at, :]
            for way in range(2):
                base = chunks[way] * own_tokens + (way * count + index) * size
                hot = jnp.where(source_ref[at, :] == lane + base, 1.0, 0.0).astype(BF16)
                part_sum = jnp.dot(hot, all_buf[chunks[way], way, index], preferred_element_type=F32)
                total = part_sum if total is None else total + part_sum
            acc_ref[at, :] = total
            return carry

        lax.fori_loop(0, slots // block, some, 0)

    place(0, (me, me), True)

    def own(index, carry):
        place(index, (me, me), False)
        return carry

    lax.fori_loop(1, count, own, 0)
    for hop in range(1, tp_size):
        def arrive(index, carry):
            chunks = [behind(way, hop) for way in range(2)]
            for way in range(2):
                arrived = all_buf.at[chunks[way], way, index]
                send(way, hop - 1, index, arrived, chunks[way]).wait_recv()
                if hop < hops:
                    send(way, hop, index, arrived, chunks[way]).start()
            place(index, chunks, False)
            return carry

        lax.fori_loop(0, count, arrive, 0)

    def finish_rows(part, carry):
        at = span(part, block)
        o_ref[at, :] = acc_ref[at, :].astype(BF16)
        return carry

    lax.fori_loop(0, slots // block, finish_rows, 0)

    def drain(index, carry):
        for way in range(2):
            for hop in range(hops):
                send(way, hop, index, normed_ref.at[way, index], me).wait_send()
        return carry

    lax.fori_loop(0, count, drain, 0)


def dispatch_rows(source, normed, tp_size, call_id):
    tokens, width = normed.shape
    size = min(256, tokens // 2)
    count = tokens // (2 * size)
    slots = source.shape[0]
    return pl.pallas_call(
        functools.partial(dispatch_body, tp_size), out_shape=jax.ShapeDtypeStruct((slots, width), BF16), in_specs=[VMEM_SPEC, HBM_SPEC], out_specs=VMEM_SPEC,
        scratch_shapes=[pltpu.VMEM((tp_size, 2, count, size, width), BF16), pltpu.VMEM((slots, width), F32), DMA, DMA((2, tp_size - 1, count)), DMA((2, tp_size - 1, count))],
        compiler_params=settings(call_id),
        cost_estimate=cost(30),
        name='dispatch_rows')(source, normed.reshape(2, count, size, width))


def attention_body(tp_size, pieces, head_dim, block_q, lens_ref, x_ref, gain_ref, shift_ref, w_qkv_ref, b_qkv_ref, w_out_ref, b_out_ref, gain2_ref, shift2_ref, w_in_ref, w_exp_out_ref, after_ref,
                   hidden_ref, normed_ref, *rest):
    row = pl.program_id(0)
    block = pl.program_id(1)
    seq, width = x_ref.shape
    moved_refs = rest[:len(pieces)]
    qkv_ref, context_ref, send_sem, recv_sem = rest[len(pieces):]
    copies = exchange_all(tp_size, (w_in_ref, w_exp_out_ref), pieces, moved_refs, send_sem, recv_sem)

    @pl.when((row == 0) & (block == 0))
    def _():
        enter([('tp', tp_size)])
        for copy in copies:
            copy.start()

    @pl.when(block == 0)
    def _():
        def project(index, carry):
            rows = span(index, block_q)
            normed = norm_rows(x_ref[rows, :].astype(F32), gain_ref[...], shift_ref[...]).astype(BF16)
            qkv_ref[rows, :] = (dot_t(normed, w_qkv_ref[...]) + b_qkv_ref[...]).astype(BF16)
            return carry
        lax.fori_loop(0, seq // block_q, project, 0)

    length = lens_ref[row]
    pair = 2 * head_dim
    key_ok = lax.broadcasted_iota(jnp.int32, (1, seq), 1) < length
    lane_head = lax.broadcasted_iota(jnp.int32, (1, pair), 1) // head_dim
    factor = (head_dim ** -0.5) * LOG2E
    rows = span(block, block_q)

    def heads(index, carry):
        lanes = pl.multiple_of(index * pair, pair)
        query = qkv_ref[rows, pl.ds(lanes, pair)]
        keys = qkv_ref[:, pl.ds(pl.multiple_of(lanes + width, pair), pair)]
        values = qkv_ref[:, pl.ds(pl.multiple_of(lanes + 2 * width, pair), pair)]
        result = None
        for head in range(2):
            scores = dot_t(jnp.where(lane_head == head, query, jnp.zeros_like(query)), keys)
            scores = jnp.where(key_ok, scores, -1e30)
            top = jnp.max(scores, axis=-1, keepdims=True)
            weights = jnp.exp2((scores - top) * factor)
            scale = 1.0 / jnp.sum(weights, axis=-1, keepdims=True)
            part = jnp.dot((weights * scale).astype(BF16), values, preferred_element_type=F32)
            result = part if result is None else jnp.where(lane_head == head, part, result)
        context_ref[:, pl.ds(lanes, pair)] = result.astype(BF16)
        return carry

    lax.fori_loop(0, width // pair, heads, 0)
    projected = jnp.dot(context_ref[...], w_out_ref[...], preferred_element_type=F32)
    hidden = (x_ref[rows, :].astype(F32) + projected + b_out_ref[...]).astype(BF16)
    hidden_ref[...] = hidden
    normed_ref[...] = norm_rows(hidden.astype(F32), gain2_ref[...], shift2_ref[...]).astype(BF16)

    @pl.when((row == pl.num_programs(0) - 1) & (block == pl.num_programs(1) - 1))
    def _():
        for copy in copies:
            copy.wait()


def attention_layer(x, lens, seq, head_dim, norm, w_qkv, b_qkv, w_out, b_out, norm2, w_exp_in, w_exp_out, after, tp_size, pieces, call_id):
    tokens, width = x.shape
    block_q = min(256, seq)
    blocks = seq // block_q
    fixed = lambda shape: pl.BlockSpec(shape, lambda r, q: (0,) * len(shape), pipeline_mode=pl.Buffered(1))
    moved = landings(tp_size, w_exp_in, pieces)
    return pl.pallas_call(
        functools.partial(attention_body, tp_size, pieces, head_dim, block_q),
        out_shape=(jax.ShapeDtypeStruct((tokens, width), BF16), jax.ShapeDtypeStruct((tokens, width), BF16), *moved),
        grid=(tokens // seq, blocks),
        in_specs=[SMEM_SPEC, pl.BlockSpec((seq, width), lambda r, q: (r, 0)), fixed((1, width)), fixed((1, width)),
                  fixed(w_qkv.shape), fixed((1, 3 * width)), fixed(w_out.shape), fixed((1, width)), fixed((1, width)), fixed((1, width)), HBM_SPEC, HBM_SPEC, HBM_SPEC],
        out_specs=(pl.BlockSpec((block_q, width), lambda r, q: (r * blocks + q, 0)), pl.BlockSpec((block_q, width), lambda r, q: (r * blocks + q, 0)), *[HBM_SPEC for _ in pieces]),
        scratch_shapes=[pltpu.VMEM((seq, 3 * width), BF16), pltpu.VMEM((block_q, width), BF16), DMA((len(pieces), tp_size - 1)), DMA((len(pieces), tp_size - 1))],
        compiler_params=settings(call_id, grid=('arbitrary', 'arbitrary')),
        cost_estimate=cost(30),
        name='attention_layer')(lens, x, *norm, w_qkv, b_qkv, w_out, b_out, *norm2, w_exp_in, w_exp_out, after)


def dense_body(tp_size, pieces, parts, x_ref, normed_ref, w_in_ref, b_in_ref, w_out_ref, b_out_ref, w_exp_in_ref, w_exp_out_ref, o_ref, *rest):
    block = pl.program_id(0)
    copies = exchange_all(tp_size, (w_exp_in_ref, w_exp_out_ref), pieces, rest[:len(pieces)], *rest[len(pieces):])

    @pl.when(block == 0)
    def _():
        enter([('tp', tp_size)])
        for copy in copies:
            copy.start()

    size = w_in_ref.shape[0] // parts
    total = x_ref[...].astype(F32) + b_out_ref[...]
    for part in range(parts):
        cols = pl.ds(part * size, size)
        inner = jnp.maximum(dot_t(normed_ref[...], w_in_ref[cols, :]) + b_in_ref[:, cols], 0.0).astype(BF16)
        total += jnp.dot(inner, w_out_ref[cols, :], preferred_element_type=F32)
    o_ref[...] = total.astype(BF16)

    @pl.when(block == pl.num_programs(0) - 1)
    def _():
        for copy in copies:
            copy.wait()


def dense_layer(x, normed, w_in, b_in, w_out, b_out, w_exp_in, w_exp_out, tp_size, pieces, call_id):
    tokens, width = x.shape
    block_n = min(256, tokens)
    fixed = lambda shape: pl.BlockSpec(shape, lambda i: (0,) * len(shape), pipeline_mode=pl.Buffered(1))
    dma = DMA((len(pieces), tp_size - 1))
    return pl.pallas_call(
        functools.partial(dense_body, tp_size, pieces, 4),
        out_shape=(jax.ShapeDtypeStruct((tokens, width), BF16), *landings(tp_size, w_exp_in, pieces)), grid=(tokens // block_n,),
        in_specs=[pl.BlockSpec((block_n, width), lambda i: (i, 0)), pl.BlockSpec((block_n, width), lambda i: (i, 0)), fixed(w_in.shape), fixed(b_in.shape), fixed(w_out.shape), fixed((1, width)), HBM_SPEC, HBM_SPEC],
        out_specs=(pl.BlockSpec((block_n, width), lambda i: (i, 0)), *[HBM_SPEC for _ in pieces]),
        scratch_shapes=[dma, dma],
        compiler_params=settings(call_id, grid=('arbitrary',)),
        cost_estimate=cost(30),
        name='dense_layer')(x, normed, w_in, b_in, w_out, b_out, w_exp_in, w_exp_out)


def experts_body(tp_size, ep_size, early, late, dispatch_ref, early_refs, w_in_ref, w_out_ref, b_in_ref, b_out_ref, w_router_ref, other_ref, returned_ref, gates_ref,
                 sent_buf, arrived_ref, parts_buf, own_buf, out_buf, local_sem, send_sem, recv_sem, back_send, back_recv, move_send, move_recv):
    chunks, _, slots, width = arrived_ref.shape
    me = lax.axis_index('ep')
    mine = lax.axis_index('tp')
    weights = (w_in_ref, w_out_ref)
    units = [(chunk, which) for chunk in range(chunks) for which in range(2)]

    sends = {}
    for chunk in range(chunks):
        for distance in range(1, ep_size):
            peer = away('ep', ep_size, distance)
            sends[chunk, distance] = pltpu.make_async_remote_copy(
                src_ref=dispatch_ref.at[chunk, peer], dst_ref=arrived_ref.at[chunk, me], send_sem=send_sem.at[chunk, distance], recv_sem=recv_sem.at[chunk, distance],
                device_id={'ep': peer}, device_id_type=MESH)

    def landing(piece):
        chunk, which, start, rows = piece
        return parts_buf.at[units.index((chunk, which)), :, pl.ds(start, rows)]

    moves = {piece: exchange(tp_size, weights, piece, landing(piece), move_send.at[index], move_recv.at[index]) for index, piece in enumerate(late)}
    kept = [pltpu.make_async_copy(dispatch_ref.at[chunk, me], arrived_ref.at[chunk, me], local_sem.at[0, chunk]) for chunk in range(chunks)]
    owns = {unit: pltpu.make_async_copy(weights[unit[1]].at[unit[0] * tp_size + mine], own_buf.at[unit[0], unit[1]], local_sem.at[1 + unit[1], unit[0]]) for unit in units}
    earlies = {piece: pltpu.make_async_copy(early_refs[index], landing(piece), local_sem.at[3, index]) for index, piece in enumerate(early)}

    enter([('tp', tp_size), ('ep', ep_size)])
    for piece in late:
        for copy in moves[piece]:
            copy.start()
    for chunk in range(chunks):
        for distance in range(1, ep_size):
            sends[chunk, distance].start()
        kept[chunk].start()
    for unit in units:
        owns[unit].start()
        for piece in early:
            if piece[:2] == unit:
                earlies[piece].start()

    lane = lax.broadcasted_iota(jnp.int32, (1, w_router_ref.shape[1]), 1)
    group = lax.broadcasted_iota(jnp.int32, (ep_size * slots, 1), 0) // slots

    def load(chunk):
        return pltpu.make_async_copy(dispatch_ref.at[chunk], sent_buf.at[chunk % 2], local_sem.at[5, chunk % 2])

    load(0).start()
    for chunk in range(chunks):
        if chunk + 1 < chunks:
            load(chunk + 1).start()
        load(chunk).wait()
        logits = jnp.dot(sent_buf[chunk % 2].reshape(ep_size * slots, width), w_router_ref[...], preferred_element_type=F32)
        rows = pl.ds(chunk * ep_size * slots, ep_size * slots)
        own = jnp.sum(jnp.where(lane == group * (chunks * tp_size) + (chunk * tp_size + mine), logits, 0.0), axis=1, keepdims=True)
        other = jnp.sum(jnp.where(lane == other_ref[rows, :], logits, 0.0), axis=1, keepdims=True)
        gates_ref[rows, :] = jax.nn.sigmoid(own - other)

    def part_ref(unit, part):
        if part == 0:
            return own_buf.at[unit[0], unit[1]]
        return parts_buf.at[units.index(unit), part - 1]

    def give_back(chunk, slot, index):
        for half in range(2):
            peer = 2 * index + half
            distance = lax.rem(peer - me + ep_size, ep_size)

            @pl.when(distance == 0)
            def _():
                pltpu.make_async_copy(out_buf.at[slot, peer], returned_ref.at[chunk, me], local_sem.at[4, chunk]).start()

            @pl.when(distance != 0)
            def _():
                pltpu.make_async_remote_copy(
                    src_ref=out_buf.at[slot, peer], dst_ref=returned_ref.at[chunk, me], send_sem=back_send.at[chunk, distance], recv_sem=back_recv.at[chunk, distance],
                    device_id={'ep': peer}, device_id_type=MESH).start()

    def weights_here(unit):
        owns[unit].wait()
        for piece in early:
            if piece[:2] == unit:
                earlies[piece].wait()
        for piece in late:
            if piece[:2] == unit:
                for copy in moves[piece]:
                    copy.wait_recv()

    def inner_part(chunk, index, part):
        tokens = arrived_ref[chunk, pl.ds(2 * index, 2)].reshape(2 * slots, width)
        inner = jnp.dot(tokens, part_ref((chunk, 0), part)[...], preferred_element_type=F32) + b_in_ref[chunk, pl.ds(part, 1), :]
        return jnp.maximum(inner, 0.0).astype(BF16)

    backs = {}
    for chunk in range(chunks):
        last = chunk == chunks - 1
        slot = chunk % out_buf.shape[0]
        for distance in range(1, ep_size):
            sends[chunk, distance].wait_recv()
        kept[chunk].wait()
        weights_here((chunk, 0))
        before = chunk - out_buf.shape[0]
        if before >= 0:
            for copy in backs[before][:-1]:
                copy.wait_send()
            backs[before][-1].wait()

        held = [sent_buf.at[0], sent_buf.at[1], arrived_ref.at[0], arrived_ref.at[1]]
        if last:
            def first_product(index, carry):
                for part in range(tp_size):
                    held[part][pl.ds(2 * index, 2)] = inner_part(chunk, index, part).reshape(2, slots, width)
                return carry

            lax.fori_loop(0, ep_size // 2, first_product, 0)
        weights_here((chunk, 1))

        def rows(index, carry):
            total = jnp.zeros((2 * slots, width), F32)
            for part in range(tp_size):
                inner = held[part][pl.ds(2 * index, 2)].reshape(2 * slots, width) if last else inner_part(chunk, index, part)
                total += jnp.dot(inner, part_ref((chunk, 1), part)[...], preferred_element_type=F32)
            out_buf[slot, pl.ds(2 * index, 2)] = (total + b_out_ref[pl.ds(chunk, 1), :]).astype(BF16).reshape(2, slots, width)

            @pl.when(index > 0)
            def _():
                give_back(chunk, slot, index - 1)

            return carry

        lax.fori_loop(0, ep_size // 2, rows, 0)
        give_back(chunk, slot, ep_size // 2 - 1)
        backs[chunk] = []
        for distance in range(1, ep_size):
            peer = away('ep', ep_size, distance)
            backs[chunk].append(pltpu.make_async_remote_copy(
                src_ref=out_buf.at[slot, peer], dst_ref=returned_ref.at[chunk, me], send_sem=back_send.at[chunk, distance], recv_sem=back_recv.at[chunk, distance],
                device_id={'ep': peer}, device_id_type=MESH))
        backs[chunk].append(pltpu.make_async_copy(out_buf.at[slot, me], returned_ref.at[chunk, me], local_sem.at[4, chunk]))

    for chunk in range(chunks):
        for distance in range(1, ep_size):
            sends[chunk, distance].wait_send()
        for copy in backs[chunk][:-1]:
            copy.wait_recv()
            if chunk + out_buf.shape[0] >= chunks:
                copy.wait_send()
        if chunk + out_buf.shape[0] >= chunks:
            backs[chunk][-1].wait()
    for piece in late:
        for copy in moves[piece]:
            copy.wait_send()


def experts(dispatch, early_weights, w_in, w_out, b_in, b_out, w_router, other, tp_size, ep_size, early, late, call_id):
    chunks, _, slots, width = dispatch.shape
    hidden = w_in.shape[2]

    def body(dispatch_ref, *refs):
        experts_body(tp_size, ep_size, early, late, dispatch_ref, refs[:len(early)], *refs[len(early):])

    return pl.pallas_call(
        body, out_shape=(jax.ShapeDtypeStruct(dispatch.shape, BF16), jax.ShapeDtypeStruct(other.shape, F32)),
        in_specs=[HBM_SPEC] * (3 + len(early)) + [VMEM_SPEC] * 4, out_specs=(HBM_SPEC, VMEM_SPEC),
        scratch_shapes=[pltpu.VMEM((2,) + dispatch.shape[1:], BF16), pltpu.VMEM(dispatch.shape, BF16), pltpu.VMEM((2 * chunks, tp_size - 1, width, hidden), BF16),
                        pltpu.VMEM((chunks, 2, width, hidden), BF16), pltpu.VMEM((2, ep_size, slots, width), BF16),
                        DMA((6, max(chunks, len(early)))), DMA((chunks, ep_size)), DMA((chunks, ep_size)), DMA((chunks, ep_size)), DMA((chunks, ep_size)),
                        DMA((len(late), tp_size - 1)), DMA((len(late), tp_size - 1))],
        compiler_params=settings(call_id, 62),
        cost_estimate=cost(30),
        name='experts')(dispatch, *early_weights, w_in, w_out, b_in, b_out, w_router, other)


def combine_body(blocks, token_ref, slots_ref, gates_ref, o_ref, acc_ref, wide_ref):
    block = pl.program_id(0)
    slots, width = slots_ref.shape
    step = o_ref.shape[0]
    lanes = 128
    piece = min(128, slots)

    @pl.when(block == 0)
    def _():
        def clear(index, carry):
            acc_ref[span(index, lanes), :] = jnp.zeros((lanes, lanes), F32)
            return carry
        lax.fori_loop(0, acc_ref.shape[0] // lanes, clear, 0)

    @pl.when(block < blocks)
    def _():
        def widen(index, carry):
            rows = span(index, piece)
            for col in range(width // lanes):
                wide_ref[pl.ds(index * (piece * 8) + col, piece, stride=8), :] = slots_ref[rows, col * lanes:(col + 1) * lanes].astype(F32) * gates_ref[rows, :]
            return carry
        lax.fori_loop(0, slots // piece, widen, 0)
        base = block * slots

        def add(index, carry):
            first = index * 16
            places = [pl.ds(pl.multiple_of(token_ref[base + first + u], 8), 8) for u in range(16)]
            start = pl.multiple_of(index * 128, 128)
            new = [acc_ref[places[u], :] + wide_ref[pl.ds(start + u * 8, 8), :] for u in range(16)]
            for u in range(16):
                acc_ref[places[u], :] = new[u]
            return carry

        lax.fori_loop(0, slots // 16, add, 0)

    @pl.when(block >= blocks)
    def _():
        first = (block - blocks) * (step * 8)
        some = min(256, step)

        def write(index, carry):
            rows = span(index, some)
            for col in range(width // lanes):
                o_ref[rows, col * lanes:(col + 1) * lanes] = acc_ref[pl.ds(first + index * (some * 8) + col, some, stride=8), :].astype(BF16)
            return carry
        lax.fori_loop(0, step // some, write, 0)


def combine(place, gates, outputs, tokens):
    count, slots, width = outputs.shape
    blocks = 4
    slots = count * slots // blocks
    outputs = outputs.reshape(blocks, slots, width)
    step = tokens // 4
    grid_spec = pltpu.PrefetchScalarGridSpec(
        num_scalar_prefetch=1, grid=(blocks + tokens // step,),
        in_specs=[pl.BlockSpec((None, slots, width), lambda b, *_: (jnp.minimum(b, blocks - 1), 0, 0)), pl.BlockSpec((slots, 1), lambda b, *_: (jnp.minimum(b, blocks - 1), 0))],
        out_specs=pl.BlockSpec((step, width), lambda b, *_: (jnp.maximum(b - blocks, 0), 0)),
        scratch_shapes=[pltpu.VMEM(((tokens + 32) * 8, 128), F32), pltpu.VMEM((slots * 8, 128), F32)])
    return pl.pallas_call(
        functools.partial(combine_body, blocks),
        out_shape=jax.ShapeDtypeStruct((tokens, width), BF16), grid_spec=grid_spec,
        compiler_params=settings(grid=('arbitrary',)),
        cost_estimate=cost(30),
        name='combine')(place, outputs, gates)


def finish_body(tp_size, count, partial_ref, hidden_ref, o_ref, partial_buf, hidden_buf, sum_buf, own_buf, load_sem, sum_send, sum_recv, out_send, out_recv):
    me = lax.axis_index('tp')
    own_tokens, _ = hidden_ref.shape
    size = own_tokens // (2 * count)
    hops = tp_size - 1
    step_to = (1, tp_size - 1)

    def rows(way, chunk, index):
        return pl.ds(pl.multiple_of(chunk * own_tokens + (way * count + index) * size, size), size)

    def behind(way, distance):
        return away('tp', tp_size, (tp_size - distance) % tp_size if way == 0 else distance % tp_size)

    def send_sum(way, hop, index, src_ref):
        return pltpu.make_async_remote_copy(
            src_ref=src_ref, dst_ref=sum_buf.at[way, hop, index], send_sem=sum_send.at[way, hop, index], recv_sem=sum_recv.at[way, hop, index],
            device_id={'tp': away('tp', tp_size, step_to[way])}, device_id_type=MESH)

    def send_out(way, hop, index, src_ref, chunk):
        return pltpu.make_async_remote_copy(
            src_ref=src_ref, dst_ref=o_ref.at[rows(way, chunk, index)], send_sem=out_send.at[way, hop, index], recv_sem=out_recv.at[way, hop, index],
            device_id={'tp': away('tp', tp_size, step_to[way])}, device_id_type=MESH)

    loads = [pltpu.make_async_copy(partial_ref, partial_buf, load_sem.at[0]), pltpu.make_async_copy(hidden_ref, hidden_buf, load_sem.at[1])]
    for load in loads:
        load.start()
    enter([('tp', tp_size)])

    def first(index, carry):
        for way in range(2):
            send_sum(way, 0, index, partial_ref.at[rows(way, behind(way, 1), index)]).start()
        return carry

    lax.fori_loop(0, count, first, 0)
    for load in loads:
        load.wait()

    def keep(way, index):
        own = own_buf.at[way, index]
        return pltpu.make_async_copy(own, o_ref.at[rows(way, me, index)], load_sem.at[2 + way])

    for hop in range(1, tp_size):
        def add(index, carry):
            for way in range(2):
                send_sum(way, hop - 1, index, sum_buf.at[way, hop - 1, index]).wait_recv()
                total = sum_buf[way, hop - 1, index].astype(F32) + partial_buf[rows(way, behind(way, hop + 1), index), :].astype(F32)
                if hop < hops:
                    sum_buf[way, hop - 1, index] = total.astype(BF16)
                else:
                    own_rows = pl.ds(pl.multiple_of((way * count + index) * size, size), size)
                    own_buf[way, index] = (total.astype(BF16).astype(F32) + hidden_buf[own_rows, :].astype(F32)).astype(BF16)
            for way in range(2):
                if hop < hops:
                    send_sum(way, hop, index, sum_buf.at[way, hop - 1, index]).start()
                else:
                    send_out(way, 0, index, own_buf.at[way, index], me).start()
                    keep(way, index).start()
                    keep(way, index).wait()
            return carry

        lax.fori_loop(0, count, add, 0)

    for hop in range(1, tp_size):
        def forward(index, carry):
            for way in range(2):
                chunk = behind(way, hop)
                arrived = o_ref.at[rows(way, chunk, index)]
                send_out(way, hop - 1, index, arrived, chunk).wait_recv()
                if hop < hops:
                    send_out(way, hop, index, arrived, chunk).start()
            return carry

        lax.fori_loop(0, count, forward, 0)

    def drain(index, carry):
        for way in range(2):
            for hop in range(hops):
                send_sum(way, hop, index, sum_buf.at[way, hop, index]).wait_send()
                send_out(way, hop, index, own_buf.at[way, index], me).wait_send()
        return carry

    lax.fori_loop(0, count, drain, 0)


def finish(partial, hidden, tp_size, call_id):
    tokens, width = partial.shape
    own_tokens = hidden.shape[0]
    size = min(256, own_tokens // 2)
    count = own_tokens // (2 * size)
    hops = tp_size - 1
    return pl.pallas_call(
        functools.partial(finish_body, tp_size, count), out_shape=jax.ShapeDtypeStruct(partial.shape, BF16), in_specs=[HBM_SPEC, HBM_SPEC], out_specs=HBM_SPEC,
        scratch_shapes=[pltpu.VMEM(partial.shape, BF16), pltpu.VMEM(hidden.shape, BF16), pltpu.VMEM((2, hops, count, size, width), BF16), pltpu.VMEM((2, count, size, width), BF16),
                        DMA((4,)), DMA((2, hops, count)), DMA((2, hops, count)), DMA((2, hops, count)), DMA((2, hops, count))],
        compiler_params=settings(call_id),
        cost_estimate=cost(30),
        name='finish')(partial, hidden)


def solution(mesh):
    tp_size = mesh.shape['tp']
    ep_size = mesh.shape['ep']

    def gather_tp(value):
        return lax.all_gather(value, 'tp')

    def local_fn(x, src_len, expert_idx, ln_gain, ln_bias, w_query, b_query, w_key, w_value, b_value, w_attn_out, b_attn_out, w_fc1, b_fc1, w_fc2, b_fc2, w_router, w_exp_in, b_exp_in, w_exp_out, b_exp_out):
        rows, seq, width = x.shape
        tokens = rows * seq
        num_experts = w_router.shape[1]
        capacity = 2 * (-(-tokens // num_experts))
        local_experts = w_exp_in.shape[0]
        own_experts = local_experts // tp_size
        _, _, local_heads, head_dim = w_query.shape
        heads = local_heads * tp_size
        head_cols = local_heads * head_dim
        hidden_cols = w_fc1.shape[1]
        tp_index = lax.axis_index('tp')
        ep_index = lax.axis_index('ep')
        own_rows = rows // tp_size
        own_tokens = own_rows * seq
        x_own = lax.dynamic_slice_in_dim(x, tp_index * own_rows, own_rows, 0).reshape(own_tokens, width)
        len_own = lax.dynamic_slice_in_dim(src_len, tp_index * own_rows, own_rows, 0)

        def pack_attention(j):
            columns = [w[j].reshape(width, head_cols).T for w in (w_query, w_key, w_value)]
            return jnp.concatenate(columns + [w_attn_out[j].reshape(head_cols, width)], axis=0)

        def unpack_attention(gathered):
            by_kind = gathered.reshape(4, ep_size // 4, tp_size, -1, width).transpose(0, 2, 1, 3, 4)
            return by_kind[:3].reshape(3 * heads * head_dim, width), by_kind[3].reshape(heads * head_dim, width)

        def own_slice(value):
            size = value.shape[0] // ep_size
            return lax.dynamic_slice_in_dim(value, ep_index * size, size, 0)

        slices = [own_slice(value) for value in (pack_attention(0), w_fc1.T, w_fc2, pack_attention(1))]
        cuts = [value.shape[0] for value in slices]
        slices = gather_tp(jnp.concatenate(slices, axis=0))
        small = jnp.concatenate([b_query.reshape(-1), b_value.reshape(-1), b_fc1.reshape(-1), b_exp_in.reshape(-1)])
        small = gather_tp(small)
        cut = cuts[1]
        pair = 2 * head_cols
        b_query_all, b_value_all, b_fc1_all, b_exp_in_all = jnp.split(small, [pair, 2 * pair, 2 * pair + hidden_cols], axis=1)
        b_query_all, b_value_all = [value.reshape(tp_size, 2, head_cols).transpose(1, 0, 2).reshape(2, -1) for value in (b_query_all, b_value_all)]
        b_qkv = jnp.concatenate([b_query_all, jnp.zeros_like(b_query_all), b_value_all], axis=1)
        b_fc1_all = b_fc1_all.reshape(tp_size, ep_size, cut).transpose(1, 0, 2).reshape(-1)
        b_in_own = lax.dynamic_index_in_dim(b_exp_in_all.reshape(tp_size, own_experts, tp_size, -1), tp_index, 2, keepdims=False)
        part_order = lax.rem(tp_index - jnp.arange(tp_size) + tp_size, tp_size)
        b_in_own = b_in_own[part_order].transpose(1, 0, 2)
        b_out_own = lax.dynamic_index_in_dim(b_exp_out.reshape(own_experts, tp_size, width), tp_index, 1, keepdims=False)
        router = w_router.astype(BF16)
        slices, x_own, b_qkv, b_fc1_all, b_in_own, b_out_own, router, len_own = lax.optimization_barrier((slices, x_own, b_qkv, b_fc1_all, b_in_own, b_out_own, router, len_own))
        starts = [sum(cuts[:i]) for i in range(5)]
        first_pack = lax.all_gather(slices[:, :starts[1]], 'ep')
        fc1_all, fc2_all, second_pack = [lax.all_gather(slices[:, starts[i]:starts[i + 1]], 'ep') for i in range(1, 4)]
        fc1_all, fc2_all = fc1_all.reshape(-1, width), fc2_all.reshape(-1, width)

        def row(value):
            return value.reshape(1, -1)

        def norm(i):
            return row(ln_gain[i]), row(ln_bias[i])

        def piece(code):
            chunk, which, *part = map(int, code)
            size = width // (1 + len(part))
            return chunk, which, sum(part) * size, size

        plan = ['210'], ['00', '01'], ['10'], ['11', '20'], ['211', '30', '31']
        at_start, in_first, in_dense, in_second, in_experts = [[piece(code) for code in codes] for codes in plan]
        place, source, other, *moved = move(src_len, expert_idx.transpose(0, 2, 1), w_exp_in, w_exp_out, slices[0, :8], num_experts, capacity, tp_size, ep_size, at_start, 4)
        w_qkv, w_out = unpack_attention(first_pack)
        hidden, normed, *landed = attention_layer(x_own, len_own, seq, head_dim, norm(0), w_qkv, row(b_qkv[0]), w_out, row(b_attn_out[0]), norm(1), w_exp_in, w_exp_out, moved[0], tp_size, in_first, 0)
        moved += landed
        second_pack, hidden = lax.optimization_barrier((second_pack, hidden))
        hidden, *landed = dense_layer(hidden, normed, fc1_all, row(b_fc1_all), fc2_all, row(b_fc2), w_exp_in, w_exp_out, tp_size, in_dense, 1)
        moved += landed
        w_qkv, w_out = unpack_attention(second_pack)
        hidden, normed, *landed = attention_layer(hidden, len_own, seq, head_dim, norm(2), w_qkv, row(b_qkv[1]), w_out, row(b_attn_out[1]), norm(3), w_exp_in, w_exp_out, moved[0], tp_size, in_second, 2)
        moved += landed
        dispatch = dispatch_rows(source, normed, tp_size, 6).reshape(own_experts, ep_size, capacity, width)

        outputs, gates = experts(dispatch, moved, w_exp_in, w_exp_out, b_in_own, b_out_own,
                                 router, other, tp_size, ep_size, at_start + in_first + in_dense + in_second, in_experts, 3)
        outputs = outputs.reshape(own_experts * ep_size, capacity, width)
        partial = combine(place.reshape(-1), gates, outputs, tokens)
        return finish(partial, hidden, tp_size, 5).reshape(rows, seq, width)

    axes = {'g': ('dp', 'ep'), 'e': 'ep', 't': 'tp', '.': None}

    def spec(code):
        return P(*[axes[letter] for letter in code])

    codes = ['g..', 'g', 'g..', '..', '..', '..t.', '.t.', '..t.', '..t.', '.t.', '.t..', '..', '.t', 't', 't.', '.', '..', 'e.t', 'et', 'et.', 'e.']
    in_specs = tuple(map(spec, codes))
    return jax.shard_map(local_fn, mesh=mesh, in_specs=in_specs, out_specs=spec('g..'), check_vma=False)
```

```python
import functools

import jax
import jax.numpy as jnp
from jax import lax
from jax.experimental import pallas as pl
from jax.experimental.pallas import tpu as pltpu
from jax.sharding import PartitionSpec as P

LN_EPS = 1e-5
BF16 = jnp.bfloat16
F32 = jnp.float32
LOG2E = 1.4426950408889634


MESH = pl.DeviceIdType.MESH
VMEM_SPEC = pl.BlockSpec(memory_space=pltpu.VMEM)
HBM_SPEC = pl.BlockSpec(memory_space=pltpu.HBM)
SMEM_SPEC = pl.BlockSpec(memory_space=pltpu.SMEM)
DMA = pltpu.SemaphoreType.DMA


def span(index, size):
    return pl.ds(pl.multiple_of(index * size, size), size)


def settings(call_id=None, mib=56, grid=None):
    return pltpu.CompilerParams(dimension_semantics=grid, collective_id=call_id, has_side_effects=call_id is not None, vmem_limit_bytes=mib << 20)


def cost(gflops):
    return pl.CostEstimate(flops=gflops * 10**9, transcendentals=0, bytes_accessed=10**7)


def dot_t(lhs, rhs_t):
    return lax.dot_general(lhs, rhs_t, (((1,), (1,)), ((), ())), preferred_element_type=F32)


def norm_rows(value, gain, shift):
    centered = value - jnp.mean(value, axis=-1, keepdims=True)
    variance = jnp.mean(centered * centered, axis=-1, keepdims=True)
    return centered * lax.rsqrt(variance + LN_EPS) * gain + shift


def away(axis, size, distance):
    return lax.rem(lax.axis_index(axis) + distance, size)


def enter(groups):
    barrier = pltpu.get_barrier_semaphore()
    count = 0
    for axis, size in groups:
        for distance in range(1, size):
            pl.semaphore_signal(barrier, device_id={axis: away(axis, size, distance)}, device_id_type=MESH)
            count += 1
    pl.semaphore_wait(barrier, count)


def exchange(tp_size, weights, piece, landing_ref, send_sem, recv_sem):
    chunk, which, start, rows = piece
    return [pltpu.make_async_remote_copy(
        src_ref=weights[which].at[chunk * tp_size + away('tp', tp_size, distance), pl.ds(start, rows)], dst_ref=landing_ref.at[distance - 1],
        send_sem=send_sem.at[distance - 1], recv_sem=recv_sem.at[distance - 1],
        device_id={'tp': away('tp', tp_size, distance)}, device_id_type=MESH)
        for distance in sorted(range(1, tp_size), key=lambda d: (min(d, tp_size - d), d))]


def exchange_all(tp_size, weights, pieces, landing_refs, send_sem, recv_sem):
    copies = []
    for index, piece in enumerate(pieces):
        copies += exchange(tp_size, weights, piece, landing_refs[index], send_sem.at[index], recv_sem.at[index])
    return copies


def landings(tp_size, weight, pieces):
    return [jax.ShapeDtypeStruct((tp_size - 1, rows, weight.shape[2]), BF16) for _, _, _, rows in pieces]


def route_tables(lens_ref, index_ref, total_ref, total_t_ref):
    rows, _, seq = index_ref.shape
    step = min(512, seq)
    per_row = seq // step
    experts_count, wide = total_ref.shape
    slots = wide // 3
    ids = lax.broadcasted_iota(jnp.int32, (experts_count, 1), 0)
    slot_ids = lax.broadcasted_iota(jnp.int32, (slots, 1), 0)
    before = (lax.broadcasted_iota(jnp.int32, (step, step), 0) < lax.broadcasted_iota(jnp.int32, (step, step), 1)).astype(BF16)
    total_ref[...] = jnp.zeros_like(total_ref)
    total_t_ref[...] = jnp.zeros_like(total_t_ref)
    count = jnp.zeros((experts_count, 1), F32)
    for choice in range(2):
        def block(index, count):
            row = index // per_row
            start = pl.multiple_of((index % per_row) * step, step)
            cols = pl.ds(start, step)
            position = lax.broadcasted_iota(jnp.int32, (1, step), 1) + start
            chosen = jnp.where(position < lens_ref[row], index_ref[row, pl.ds(choice, 1), cols], -1)
            other = index_ref[row, pl.ds(1 - choice, 1), cols]
            token = position + row * seq
            hot = jnp.where(ids == chosen, 1.0, 0.0)
            rank = jnp.dot(hot.astype(BF16), before, preferred_element_type=F32) + count
            slot = jnp.sum(rank * hot, axis=0, keepdims=True).astype(jnp.int32)
            at_slot = slot_ids == slot
            parts = [jnp.where(at_slot, value.astype(F32), 0.0).astype(BF16) for value in (token & 255, (token >> 8) + 1, other)]
            values = jnp.concatenate(parts, axis=0)
            hot16 = hot.astype(BF16)
            total_ref[...] += dot_t(hot16, values)
            total_t_ref[...] += dot_t(values, hot16)
            return count + jnp.sum(hot, axis=1, keepdims=True)

        count = lax.fori_loop(0, rows * per_row, block, count)


def spread(ep_size, src_ref, view, sems):
    me = lax.axis_index('ep')
    send_sem, recv_sem = sems
    copies = [pltpu.make_async_remote_copy(
        src_ref=src_ref, dst_ref=view(me), send_sem=send_sem.at[distance], recv_sem=recv_sem.at[distance],
        device_id={'ep': away('ep', ep_size, distance)}, device_id_type=MESH) for distance in range(1, ep_size)]
    return copies + [pltpu.make_async_copy(src_ref, view(me), send_sem.at[0])]


def by_kind(ref, ep_size):
    per = ep_size // ref.shape[0]
    return lambda index: ref.at[index // per, :, lax.rem(index, per)]


def start_body(tp_size, ep_size, pieces, own_experts, lens_ref, index_ref, w_in_ref, w_out_ref, own_ref, *refs):
    biases, refs = refs[:4], refs[4:]
    place_ref, source_ref, other_ref, first_ref, later_ref, *refs = refs
    biases_all, refs = refs[:4], refs[4:]
    moved_refs, refs = refs[:len(pieces)], refs[len(pieces):]
    total_ref, total_t_ref, move_send, move_recv, tp_send, tp_recv, row_send, row_recv, pair_send, pair_recv = refs
    mine = lax.axis_index('tp')
    me = lax.axis_index('ep')
    view = by_kind(first_ref, ep_size)
    moves = exchange_all(tp_size, (w_in_ref, w_out_ref), pieces, moved_refs, move_send, move_recv)
    pairs = [(own_ref.at[0], view(me).at[mine])]
    pairs += [(bias, whole.at[mine]) for bias, whole in zip(biases, biases_all)]
    pairs += [(own_ref.at[1 + index], later_ref.at[index, mine]) for index in range(later_ref.shape[0])]
    gathers = []
    for index, (src, dst) in enumerate(pairs):
        gathers.append([pltpu.make_async_copy(src, dst, tp_send.at[index, 0])] + [pltpu.make_async_remote_copy(
            src_ref=src, dst_ref=dst, send_sem=tp_send.at[index, distance], recv_sem=tp_recv.at[index, distance],
            device_id={'tp': away('tp', tp_size, distance)}, device_id_type=MESH) for distance in (1, tp_size - 1, *range(2, tp_size - 1))])
    enter([('tp', tp_size), ('ep', ep_size)])
    for copies in gathers:
        for copy in copies:
            copy.start()
    for copy in moves:
        copy.start()

    cores = 2
    steps = range(1, ep_size // cores)
    other_core = me + 1 - cores * lax.rem(me, cores)

    def along(step):
        return pltpu.make_async_remote_copy(
            src_ref=view(me), dst_ref=view(me), send_sem=row_send.at[step], recv_sem=row_recv.at[step],
            device_id={'ep': away('ep', ep_size, cores * step)}, device_id_type=MESH)

    def across(step):
        part = view(away('ep', ep_size, ep_size - cores * step))
        return pltpu.make_async_remote_copy(
            src_ref=part, dst_ref=part, send_sem=pair_send.at[step], recv_sem=pair_recv.at[step],
            device_id={'ep': other_core}, device_id_type=MESH)

    for copy in gathers[0]:
        copy.wait()
    for step in steps:
        along(step).start()
    across(0).start()

    route_tables(lens_ref, index_ref, total_ref, total_t_ref)
    rows, _, seq = index_ref.shape
    experts_count, wide = total_ref.shape
    slots = wide // 3
    lane = lax.broadcasted_iota(jnp.int32, (1, experts_count), 1)

    def take(index, carry):
        chunk = index // ep_size
        expert = (index % ep_size) * (own_experts * tp_size) + chunk * tp_size + mine
        line = total_ref[pl.ds(expert, 1), :].astype(jnp.int32)
        low, high = line[:, :slots], line[:, slots:2 * slots]
        place_ref[pl.ds(index, 1), :] = 8 * jnp.where(high > 0, 256 * (high - 1) + low, rows * seq)
        column = jnp.sum(jnp.where(lane == expert, total_t_ref[...], 0.0), axis=1, keepdims=True).astype(jnp.int32)
        low, high, other = column[:slots], column[slots:2 * slots], column[2 * slots:]
        at = span(index, slots)
        source_ref[at, :] = jnp.where(high > 0, 256 * (high - 1) + low, -1)
        other_ref[at, :] = other
        return carry

    for step in steps:
        along(step).wait()
        across(step).start()
    lax.fori_loop(0, own_experts * ep_size, take, 0)
    for step in range(ep_size // cores):
        across(step).wait()
    for copies in gathers[1:]:
        for copy in copies:
            copy.wait()
    for copy in moves:
        copy.wait()


def start(lens, index, w_in, w_out, own, biases, num_experts, capacity, tp_size, ep_size, pieces, call_id):
    own_experts = w_in.shape[0] // tp_size
    blocks = own_experts * ep_size
    packs, cut, width = own.shape
    column = jax.ShapeDtypeStruct((blocks * capacity, 1), jnp.int32)
    first = jax.ShapeDtypeStruct((packs, tp_size, ep_size // packs, cut, width), BF16)
    later = jax.ShapeDtypeStruct((packs - 1, tp_size, cut, width), BF16)
    biases_all = [jax.ShapeDtypeStruct((tp_size,) + bias.shape, F32) for bias in biases]
    moved = landings(tp_size, w_in, pieces)
    dma = [DMA((len(pieces), tp_size - 1))] * 2 + [DMA((packs + len(biases), tp_size))] * 2 + [DMA((ep_size,))] * 4
    return pl.pallas_call(
        functools.partial(start_body, tp_size, ep_size, pieces, own_experts),
        out_shape=(jax.ShapeDtypeStruct((blocks, capacity), jnp.int32), column, column, first, later, *biases_all, *moved),
        in_specs=[SMEM_SPEC, VMEM_SPEC] + [HBM_SPEC] * (3 + len(biases)), out_specs=[VMEM_SPEC] * 3 + [HBM_SPEC] * (2 + len(biases) + len(pieces)),
        scratch_shapes=[pltpu.VMEM((num_experts, 3 * capacity), F32), pltpu.VMEM((3 * capacity, num_experts), F32)] + dma,
        compiler_params=settings(call_id), cost_estimate=cost(30), name='start')(lens, index, w_in, w_out, own, *biases)


def dispatch_body(tp_size, source_ref, normed_ref, o_ref, all_buf, acc_ref, load_sem, send_sem, recv_sem):
    me = lax.axis_index('tp')
    _, count, size, width = normed_ref.shape
    own_tokens = 2 * count * size
    slots = source_ref.shape[0]
    block = min(512, slots)
    hops = tp_size - 1
    step_to = (1, tp_size - 1)
    lane = lax.broadcasted_iota(jnp.int32, (1, size), 1)

    def behind(way, distance):
        return away('tp', tp_size, (tp_size - distance) % tp_size if way == 0 else distance % tp_size)

    def send(way, hop, index, src_ref, chunk):
        return pltpu.make_async_remote_copy(
            src_ref=src_ref, dst_ref=all_buf.at[chunk, way, index], send_sem=send_sem.at[way, hop, index], recv_sem=recv_sem.at[way, hop, index],
            device_id={'tp': away('tp', tp_size, step_to[way])}, device_id_type=MESH)

    load = pltpu.make_async_copy(normed_ref, all_buf.at[me], load_sem)
    load.start()
    enter([('tp', tp_size)])

    def first(index, carry):
        for way in range(2):
            send(way, 0, index, normed_ref.at[way, index], me).start()
        return carry

    lax.fori_loop(0, count, first, 0)
    load.wait()

    def place(index, chunks, fresh):
        def some(part, carry):
            at = span(part, block)
            total = None if fresh else acc_ref[at, :]
            for way in range(2):
                base = chunks[way] * own_tokens + (way * count + index) * size
                hot = jnp.where(source_ref[at, :] == lane + base, 1.0, 0.0).astype(BF16)
                part_sum = jnp.dot(hot, all_buf[chunks[way], way, index], preferred_element_type=F32)
                total = part_sum if total is None else total + part_sum
            acc_ref[at, :] = total
            return carry

        lax.fori_loop(0, slots // block, some, 0)

    place(0, (me, me), True)

    def own(index, carry):
        place(index, (me, me), False)
        return carry

    lax.fori_loop(1, count, own, 0)
    for hop in range(1, tp_size):
        def arrive(index, carry):
            chunks = [behind(way, hop) for way in range(2)]
            for way in range(2):
                arrived = all_buf.at[chunks[way], way, index]
                send(way, hop - 1, index, arrived, chunks[way]).wait_recv()
                if hop < hops:
                    send(way, hop, index, arrived, chunks[way]).start()
            place(index, chunks, False)
            return carry

        lax.fori_loop(0, count, arrive, 0)

    def finish_rows(part, carry):
        at = span(part, block)
        o_ref[at, :] = acc_ref[at, :].astype(BF16)
        return carry

    lax.fori_loop(0, slots // block, finish_rows, 0)

    def drain(index, carry):
        for way in range(2):
            for hop in range(hops):
                send(way, hop, index, normed_ref.at[way, index], me).wait_send()
        return carry

    lax.fori_loop(0, count, drain, 0)


def dispatch_rows(source, normed, tp_size, call_id):
    tokens, width = normed.shape
    size = min(256, tokens // 2)
    count = tokens // (2 * size)
    slots = source.shape[0]
    return pl.pallas_call(
        functools.partial(dispatch_body, tp_size), out_shape=jax.ShapeDtypeStruct((slots, width), BF16), in_specs=[VMEM_SPEC, HBM_SPEC], out_specs=VMEM_SPEC,
        scratch_shapes=[pltpu.VMEM((tp_size, 2, count, size, width), BF16), pltpu.VMEM((slots, width), F32), DMA, DMA((2, tp_size - 1, count)), DMA((2, tp_size - 1, count))],
        compiler_params=settings(call_id),
        cost_estimate=cost(30),
        name='dispatch_rows')(source, normed.reshape(2, count, size, width))


def attention_body(tp_size, ep_size, layer, pieces, spreads, head_dim, block_q, lens_ref, x_ref, gain_ref, shift_ref, w_ref, b_query_ref, b_value_ref, b_out_ref, w_in_ref, w_exp_out_ref, later_ref,
                   hidden_ref, normed_ref, *refs):
    moved_refs, refs = refs[:len(pieces)], refs[len(pieces):]
    spread_refs, refs = refs[:spreads], refs[spreads:]
    x_buf, w_buf, bias_buf, qkv_ref, context_ref, load_sem, move_send, move_recv, spread_sem = refs
    row = pl.program_id(0)
    block = pl.program_id(1)
    own_rows, seq, width = x_buf.shape
    mine = lax.axis_index('tp')
    copies = exchange_all(tp_size, (w_in_ref, w_exp_out_ref), pieces, moved_refs, move_send, move_recv)
    for index, ref in enumerate(spread_refs):
        copies += spread(ep_size, later_ref.at[index], lambda part, ref=ref: ref.at[:, part], (spread_sem.at[0, index], spread_sem.at[1, index]))

    @pl.when((row == 0) & (block == 0))
    def _():
        base = mine * own_rows if layer == 0 else 0
        loads = [pltpu.make_async_copy(w_ref, w_buf, load_sem.at[0]), pltpu.make_async_copy(x_ref.at[pl.ds(base, own_rows)], x_buf, load_sem.at[1])]
        for load in loads:
            load.start()
        enter([('tp', tp_size), ('ep', ep_size)] if spreads else [('tp', tp_size)])
        for copy in copies:
            copy.start()
        bias_buf[...] = jnp.zeros_like(bias_buf)
        for ref, start in ((b_query_ref, 0), (b_value_ref, 2 * width)):
            parts = [ref[part, layer, pl.ds(head, 1), :] for part in range(tp_size) for head in range(ref.shape[2])]
            bias_buf[:, pl.ds(start, width)] = jnp.concatenate(parts, axis=1)
        for load in loads:
            load.wait()

    def norm(value, index):
        return norm_rows(value, gain_ref[pl.ds(index, 1), :], shift_ref[pl.ds(index, 1), :]).astype(BF16)

    @pl.when(block == 0)
    def _():
        def project(index, carry):
            rows = span(index, block_q)
            normed = norm(x_buf[row, rows, :].astype(F32), 2 * layer)
            qkv_ref[rows, :] = (dot_t(normed, w_buf[pl.ds(0, 3 * width), :]) + bias_buf[...]).astype(BF16)
            return carry
        lax.fori_loop(0, seq // block_q, project, 0)

    length = lens_ref[mine * own_rows + row]
    pair = 2 * head_dim
    key_ok = lax.broadcasted_iota(jnp.int32, (1, seq), 1) < length
    lane_head = lax.broadcasted_iota(jnp.int32, (1, pair), 1) // head_dim
    factor = (head_dim ** -0.5) * LOG2E
    rows = span(block, block_q)

    def heads(index, carry):
        lanes = pl.multiple_of(index * pair, pair)
        query = qkv_ref[rows, pl.ds(lanes, pair)]
        keys = qkv_ref[:, pl.ds(pl.multiple_of(lanes + width, pair), pair)]
        values = qkv_ref[:, pl.ds(pl.multiple_of(lanes + 2 * width, pair), pair)]
        result = None
        for head in range(2):
            scores = dot_t(jnp.where(lane_head == head, query, jnp.zeros_like(query)), keys)
            scores = jnp.where(key_ok, scores, -1e30)
            top = jnp.max(scores, axis=-1, keepdims=True)
            weights = jnp.exp2((scores - top) * factor)
            scale = 1.0 / jnp.sum(weights, axis=-1, keepdims=True)
            part = jnp.dot((weights * scale).astype(BF16), values, preferred_element_type=F32)
            result = part if result is None else jnp.where(lane_head == head, part, result)
        context_ref[:, pl.ds(lanes, pair)] = result.astype(BF16)
        return carry

    lax.fori_loop(0, width // pair, heads, 0)
    projected = jnp.dot(context_ref[...], w_buf[pl.ds(3 * width, width), :], preferred_element_type=F32)
    hidden = (x_buf[row, rows, :].astype(F32) + projected + b_out_ref[pl.ds(layer, 1), :]).astype(BF16)
    hidden_ref[...] = hidden
    normed_ref[...] = norm(hidden.astype(F32), 2 * layer + 1)

    @pl.when((row == pl.num_programs(0) - 1) & (block == pl.num_programs(1) - 1))
    def _():
        for copy in copies:
            copy.wait()


def attention_layer(layer, x, own_rows, lens, head_dim, gain, shift, w_pack, b_query, b_value, b_out, w_exp_in, w_exp_out, later, tp_size, ep_size, pieces, spreads, call_id):
    _, seq, width = x.shape
    block_q = min(256, seq)
    blocks = seq // block_q
    tokens = own_rows * seq
    _, _, cut, _ = later.shape
    moved = landings(tp_size, w_exp_in, pieces)
    spread_out = [jax.ShapeDtypeStruct((tp_size, ep_size, cut, width), BF16)] * spreads
    result = jax.ShapeDtypeStruct((tokens, width), BF16)
    result_spec = pl.BlockSpec((block_q, width), lambda r, q: (r * blocks + q, 0))
    dma = DMA((len(pieces), tp_size - 1))
    return pl.pallas_call(
        functools.partial(attention_body, tp_size, ep_size, layer, pieces, spreads, head_dim, block_q),
        out_shape=(result, result, *moved, *spread_out), grid=(own_rows, blocks),
        in_specs=[SMEM_SPEC, HBM_SPEC, VMEM_SPEC, VMEM_SPEC, HBM_SPEC, VMEM_SPEC, VMEM_SPEC, VMEM_SPEC, HBM_SPEC, HBM_SPEC, HBM_SPEC],
        out_specs=(result_spec, result_spec, *[HBM_SPEC for _ in moved + spread_out]),
        scratch_shapes=[pltpu.VMEM((own_rows, seq, width), BF16), pltpu.VMEM(w_pack.shape, BF16), pltpu.VMEM((1, 3 * width), F32), pltpu.VMEM((seq, 3 * width), BF16),
                        pltpu.VMEM((block_q, width), BF16), DMA((2,)), dma, dma, DMA((2, max(spreads, 1), ep_size))],
        compiler_params=settings(call_id, grid=('arbitrary', 'arbitrary')),
        cost_estimate=cost(30),
        name='attention_layer')(lens, x, gain, shift, w_pack, b_query, b_value, b_out, w_exp_in, w_exp_out, later)


def dense_body(tp_size, ep_size, pieces, x_ref, normed_ref, w_in_ref, b_in_ref, w_out_ref, b_out_ref, w_exp_in_ref, w_exp_out_ref, later_ref, o_ref, *refs):
    moved_refs, refs = refs[:len(pieces)], refs[len(pieces):]
    second_ref, w_in_buf, w_out_buf, load_sem, move_send, move_recv, spread_sem = refs
    block = pl.program_id(0)
    copies = exchange_all(tp_size, (w_exp_in_ref, w_exp_out_ref), pieces, moved_refs, move_send, move_recv)
    copies += spread(ep_size, later_ref.at[later_ref.shape[0] - 1], by_kind(second_ref, ep_size), (spread_sem.at[0], spread_sem.at[1]))

    @pl.when(block == 0)
    def _():
        loads = [pltpu.make_async_copy(w_in_ref, w_in_buf, load_sem.at[0]), pltpu.make_async_copy(w_out_ref, w_out_buf, load_sem.at[1])]
        for load in loads:
            load.start()
        enter([('tp', tp_size), ('ep', ep_size)])
        for copy in copies:
            copy.start()
        for load in loads:
            load.wait()

    parts, _, size = b_in_ref.shape
    total = x_ref[...].astype(F32) + b_out_ref[...]
    for part in range(parts):
        cols = pl.ds(part * size, size)
        inner = jnp.maximum(dot_t(normed_ref[...], w_in_buf[cols, :]) + b_in_ref[part], 0.0).astype(BF16)
        total += jnp.dot(inner, w_out_buf[cols, :], preferred_element_type=F32)
    o_ref[...] = total.astype(BF16)

    @pl.when(block == pl.num_programs(0) - 1)
    def _():
        for copy in copies:
            copy.wait()


def dense_layer(x, normed, w_in, b_in, w_out, b_out, w_exp_in, w_exp_out, later, tp_size, ep_size, pieces, call_id):
    tokens, width = x.shape
    block_n = min(256, tokens)
    _, _, cut, _ = later.shape
    kinds = 4
    second = jax.ShapeDtypeStruct((kinds, tp_size, ep_size // kinds, cut, width), BF16)
    dma = DMA((len(pieces), tp_size - 1))
    rows = pl.BlockSpec((block_n, width), lambda i: (i, 0))
    return pl.pallas_call(
        functools.partial(dense_body, tp_size, ep_size, pieces),
        out_shape=(jax.ShapeDtypeStruct((tokens, width), BF16), *landings(tp_size, w_exp_in, pieces), second), grid=(tokens // block_n,),
        in_specs=[rows, rows, HBM_SPEC, VMEM_SPEC, HBM_SPEC, VMEM_SPEC, HBM_SPEC, HBM_SPEC, HBM_SPEC],
        out_specs=(rows, *[HBM_SPEC for _ in pieces], HBM_SPEC),
        scratch_shapes=[pltpu.VMEM(w_in.shape, BF16), pltpu.VMEM(w_out.shape, BF16), DMA((2,)), dma, dma, DMA((2, ep_size))],
        compiler_params=settings(call_id, grid=('arbitrary',)),
        cost_estimate=cost(30),
        name='dense_layer')(x, normed, w_in, b_in, w_out, b_out, w_exp_in, w_exp_out, later)


def experts_body(tp_size, ep_size, early, late, dispatch_ref, early_refs, w_in_ref, w_out_ref, b_in_ref, b_out_ref, w_router_ref, other_ref, returned_ref, gates_ref,
                 sent_buf, arrived_ref, parts_buf, own_buf, out_buf, local_sem, send_sem, recv_sem, back_send, back_recv, move_send, move_recv):
    chunks, _, slots, width = arrived_ref.shape
    me = lax.axis_index('ep')
    mine = lax.axis_index('tp')
    weights = (w_in_ref, w_out_ref)
    units = [(chunk, which) for chunk in range(chunks) for which in range(2)]

    sends = {}
    for chunk in range(chunks):
        for distance in range(1, ep_size):
            peer = away('ep', ep_size, distance)
            sends[chunk, distance] = pltpu.make_async_remote_copy(
                src_ref=dispatch_ref.at[chunk, peer], dst_ref=arrived_ref.at[chunk, me], send_sem=send_sem.at[chunk, distance], recv_sem=recv_sem.at[chunk, distance],
                device_id={'ep': peer}, device_id_type=MESH)

    def landing(piece):
        chunk, which, start, rows = piece
        return parts_buf.at[units.index((chunk, which)), :, pl.ds(start, rows)]

    moves = {piece: exchange(tp_size, weights, piece, landing(piece), move_send.at[index], move_recv.at[index]) for index, piece in enumerate(late)}
    kept = [pltpu.make_async_copy(dispatch_ref.at[chunk, me], arrived_ref.at[chunk, me], local_sem.at[0, chunk]) for chunk in range(chunks)]
    owns = {unit: pltpu.make_async_copy(weights[unit[1]].at[unit[0] * tp_size + mine], own_buf.at[unit[0], unit[1]], local_sem.at[1 + unit[1], unit[0]]) for unit in units}
    earlies = {piece: pltpu.make_async_copy(early_refs[index], landing(piece), local_sem.at[3, index]) for index, piece in enumerate(early)}

    enter([('tp', tp_size), ('ep', ep_size)])
    for piece in late:
        for copy in moves[piece]:
            copy.start()
    for chunk in range(chunks):
        for distance in range(1, ep_size):
            sends[chunk, distance].start()
        kept[chunk].start()
    for unit in units:
        owns[unit].start()
        for piece in early:
            if piece[:2] == unit:
                earlies[piece].start()

    lane = lax.broadcasted_iota(jnp.int32, (1, w_router_ref.shape[1]), 1)
    group = lax.broadcasted_iota(jnp.int32, (ep_size * slots, 1), 0) // slots

    def load(chunk):
        return pltpu.make_async_copy(dispatch_ref.at[chunk], sent_buf.at[chunk % 2], local_sem.at[5, chunk % 2])

    load(0).start()
    for chunk in range(chunks):
        if chunk + 1 < chunks:
            load(chunk + 1).start()
        load(chunk).wait()
        logits = jnp.dot(sent_buf[chunk % 2].reshape(ep_size * slots, width), w_router_ref[...].astype(BF16), preferred_element_type=F32)
        rows = pl.ds(chunk * ep_size * slots, ep_size * slots)
        own = jnp.sum(jnp.where(lane == group * (chunks * tp_size) + (chunk * tp_size + mine), logits, 0.0), axis=1, keepdims=True)
        other = jnp.sum(jnp.where(lane == other_ref[rows, :], logits, 0.0), axis=1, keepdims=True)
        gates_ref[rows, :] = jax.nn.sigmoid(own - other)

    def part_ref(unit, part):
        if part == 0:
            return own_buf.at[unit[0], unit[1]]
        return parts_buf.at[units.index(unit), part - 1]

    def give_back(chunk, slot, index):
        for half in range(2):
            peer = 2 * index + half
            distance = lax.rem(peer - me + ep_size, ep_size)

            @pl.when(distance == 0)
            def _():
                pltpu.make_async_copy(out_buf.at[slot, peer], returned_ref.at[chunk, me], local_sem.at[4, chunk]).start()

            @pl.when(distance != 0)
            def _():
                pltpu.make_async_remote_copy(
                    src_ref=out_buf.at[slot, peer], dst_ref=returned_ref.at[chunk, me], send_sem=back_send.at[chunk, distance], recv_sem=back_recv.at[chunk, distance],
                    device_id={'ep': peer}, device_id_type=MESH).start()

    def weights_here(unit):
        owns[unit].wait()
        for piece in early:
            if piece[:2] == unit:
                earlies[piece].wait()
        for piece in late:
            if piece[:2] == unit:
                for copy in moves[piece]:
                    copy.wait_recv()

    def expert_row(chunk):
        return pl.ds(chunk * tp_size + mine, 1)

    def inner_part(chunk, index, part):
        tokens = arrived_ref[chunk, pl.ds(2 * index, 2)].reshape(2 * slots, width)
        inner = jnp.dot(tokens, part_ref((chunk, 0), part)[...], preferred_element_type=F32) + b_in_ref[away('tp', tp_size, tp_size - part), expert_row(chunk), :]
        return jnp.maximum(inner, 0.0).astype(BF16)

    backs = {}
    for chunk in range(chunks):
        last = chunk == chunks - 1
        slot = chunk % out_buf.shape[0]
        for distance in range(1, ep_size):
            sends[chunk, distance].wait_recv()
        kept[chunk].wait()
        weights_here((chunk, 0))
        before = chunk - out_buf.shape[0]
        if before >= 0:
            for copy in backs[before][:-1]:
                copy.wait_send()
            backs[before][-1].wait()

        held = [sent_buf.at[0], sent_buf.at[1], arrived_ref.at[0], arrived_ref.at[1]]
        if last:
            def first_product(index, carry):
                for part in range(tp_size):
                    held[part][pl.ds(2 * index, 2)] = inner_part(chunk, index, part).reshape(2, slots, width)
                return carry

            lax.fori_loop(0, ep_size // 2, first_product, 0)
        weights_here((chunk, 1))

        def rows(index, carry):
            total = jnp.zeros((2 * slots, width), F32)
            for part in range(tp_size):
                inner = held[part][pl.ds(2 * index, 2)].reshape(2 * slots, width) if last else inner_part(chunk, index, part)
                total += jnp.dot(inner, part_ref((chunk, 1), part)[...], preferred_element_type=F32)
            out_buf[slot, pl.ds(2 * index, 2)] = (total + b_out_ref[expert_row(chunk), :]).astype(BF16).reshape(2, slots, width)

            @pl.when(index > 0)
            def _():
                give_back(chunk, slot, index - 1)

            return carry

        lax.fori_loop(0, ep_size // 2, rows, 0)
        give_back(chunk, slot, ep_size // 2 - 1)
        backs[chunk] = []
        for distance in range(1, ep_size):
            peer = away('ep', ep_size, distance)
            backs[chunk].append(pltpu.make_async_remote_copy(
                src_ref=out_buf.at[slot, peer], dst_ref=returned_ref.at[chunk, me], send_sem=back_send.at[chunk, distance], recv_sem=back_recv.at[chunk, distance],
                device_id={'ep': peer}, device_id_type=MESH))
        backs[chunk].append(pltpu.make_async_copy(out_buf.at[slot, me], returned_ref.at[chunk, me], local_sem.at[4, chunk]))

    for chunk in range(chunks):
        for distance in range(1, ep_size):
            sends[chunk, distance].wait_send()
        for copy in backs[chunk][:-1]:
            copy.wait_recv()
            if chunk + out_buf.shape[0] >= chunks:
                copy.wait_send()
        if chunk + out_buf.shape[0] >= chunks:
            backs[chunk][-1].wait()
    for piece in late:
        for copy in moves[piece]:
            copy.wait_send()


def experts(dispatch, early_weights, w_in, w_out, b_in, b_out, w_router, other, tp_size, ep_size, early, late, call_id):
    chunks, _, slots, width = dispatch.shape
    hidden = w_in.shape[2]

    def body(dispatch_ref, *refs):
        experts_body(tp_size, ep_size, early, late, dispatch_ref, refs[:len(early)], *refs[len(early):])

    return pl.pallas_call(
        body, out_shape=(jax.ShapeDtypeStruct(dispatch.shape, BF16), jax.ShapeDtypeStruct(other.shape, F32)),
        in_specs=[HBM_SPEC] * (3 + len(early)) + [VMEM_SPEC] * 4, out_specs=(HBM_SPEC, VMEM_SPEC),
        scratch_shapes=[pltpu.VMEM((2,) + dispatch.shape[1:], BF16), pltpu.VMEM(dispatch.shape, BF16), pltpu.VMEM((2 * chunks, tp_size - 1, width, hidden), BF16),
                        pltpu.VMEM((chunks, 2, width, hidden), BF16), pltpu.VMEM((2, ep_size, slots, width), BF16),
                        DMA((6, max(chunks, len(early)))), DMA((chunks, ep_size)), DMA((chunks, ep_size)), DMA((chunks, ep_size)), DMA((chunks, ep_size)),
                        DMA((len(late), tp_size - 1)), DMA((len(late), tp_size - 1))],
        compiler_params=settings(call_id, 62),
        cost_estimate=cost(30),
        name='experts')(dispatch, *early_weights, w_in, w_out, b_in, b_out, w_router, other)


def combine_body(blocks, token_ref, slots_ref, gates_ref, o_ref, acc_ref, wide_ref):
    block = pl.program_id(0)
    slots, width = slots_ref.shape
    step = o_ref.shape[0]
    lanes = 128
    piece = min(128, slots)

    @pl.when(block == 0)
    def _():
        def clear(index, carry):
            acc_ref[span(index, lanes), :] = jnp.zeros((lanes, lanes), F32)
            return carry
        lax.fori_loop(0, acc_ref.shape[0] // lanes, clear, 0)

    @pl.when(block < blocks)
    def _():
        def widen(index, carry):
            rows = span(index, piece)
            for col in range(width // lanes):
                wide_ref[pl.ds(index * (piece * 8) + col, piece, stride=8), :] = slots_ref[rows, col * lanes:(col + 1) * lanes].astype(F32) * gates_ref[rows, :]
            return carry
        lax.fori_loop(0, slots // piece, widen, 0)
        base = block * slots

        def add(index, carry):
            first = index * 16
            places = [pl.ds(pl.multiple_of(token_ref[base + first + u], 8), 8) for u in range(16)]
            start = pl.multiple_of(index * 128, 128)
            new = [acc_ref[places[u], :] + wide_ref[pl.ds(start + u * 8, 8), :] for u in range(16)]
            for u in range(16):
                acc_ref[places[u], :] = new[u]
            return carry

        lax.fori_loop(0, slots // 16, add, 0)

    @pl.when(block >= blocks)
    def _():
        first = (block - blocks) * (step * 8)
        some = min(256, step)

        def write(index, carry):
            rows = span(index, some)
            for col in range(width // lanes):
                o_ref[rows, col * lanes:(col + 1) * lanes] = acc_ref[pl.ds(first + index * (some * 8) + col, some, stride=8), :].astype(BF16)
            return carry
        lax.fori_loop(0, step // some, write, 0)


def combine(place, gates, outputs, tokens):
    count, slots, width = outputs.shape
    blocks = 4
    slots = count * slots // blocks
    outputs = outputs.reshape(blocks, slots, width)
    step = tokens // 4
    grid_spec = pltpu.PrefetchScalarGridSpec(
        num_scalar_prefetch=1, grid=(blocks + tokens // step,),
        in_specs=[pl.BlockSpec((None, slots, width), lambda b, *_: (jnp.minimum(b, blocks - 1), 0, 0)), pl.BlockSpec((slots, 1), lambda b, *_: (jnp.minimum(b, blocks - 1), 0))],
        out_specs=pl.BlockSpec((step, width), lambda b, *_: (jnp.maximum(b - blocks, 0), 0)),
        scratch_shapes=[pltpu.VMEM(((tokens + 32) * 8, 128), F32), pltpu.VMEM((slots * 8, 128), F32)])
    return pl.pallas_call(
        functools.partial(combine_body, blocks),
        out_shape=jax.ShapeDtypeStruct((tokens, width), BF16), grid_spec=grid_spec,
        compiler_params=settings(grid=('arbitrary',)),
        cost_estimate=cost(30),
        name='combine')(place, outputs, gates)


def finish_body(tp_size, count, partial_ref, hidden_ref, o_ref, partial_buf, hidden_buf, sum_buf, own_buf, load_sem, sum_send, sum_recv, out_send, out_recv):
    me = lax.axis_index('tp')
    own_tokens, _ = hidden_ref.shape
    size = own_tokens // (2 * count)
    hops = tp_size - 1
    step_to = (1, tp_size - 1)

    def rows(way, chunk, index):
        return pl.ds(pl.multiple_of(chunk * own_tokens + (way * count + index) * size, size), size)

    def behind(way, distance):
        return away('tp', tp_size, (tp_size - distance) % tp_size if way == 0 else distance % tp_size)

    def send_sum(way, hop, index, src_ref):
        return pltpu.make_async_remote_copy(
            src_ref=src_ref, dst_ref=sum_buf.at[way, hop, index], send_sem=sum_send.at[way, hop, index], recv_sem=sum_recv.at[way, hop, index],
            device_id={'tp': away('tp', tp_size, step_to[way])}, device_id_type=MESH)

    def send_out(way, hop, index, src_ref, chunk):
        return pltpu.make_async_remote_copy(
            src_ref=src_ref, dst_ref=o_ref.at[rows(way, chunk, index)], send_sem=out_send.at[way, hop, index], recv_sem=out_recv.at[way, hop, index],
            device_id={'tp': away('tp', tp_size, step_to[way])}, device_id_type=MESH)

    loads = [pltpu.make_async_copy(partial_ref, partial_buf, load_sem.at[0]), pltpu.make_async_copy(hidden_ref, hidden_buf, load_sem.at[1])]
    for load in loads:
        load.start()
    enter([('tp', tp_size)])

    def first(index, carry):
        for way in range(2):
            send_sum(way, 0, index, partial_ref.at[rows(way, behind(way, 1), index)]).start()
        return carry

    lax.fori_loop(0, count, first, 0)
    for load in loads:
        load.wait()

    def keep(way, index):
        own = own_buf.at[way, index]
        return pltpu.make_async_copy(own, o_ref.at[rows(way, me, index)], load_sem.at[2 + way])

    for hop in range(1, tp_size):
        def add(index, carry):
            for way in range(2):
                send_sum(way, hop - 1, index, sum_buf.at[way, hop - 1, index]).wait_recv()
                total = sum_buf[way, hop - 1, index].astype(F32) + partial_buf[rows(way, behind(way, hop + 1), index), :].astype(F32)
                if hop < hops:
                    sum_buf[way, hop - 1, index] = total.astype(BF16)
                else:
                    own_rows = pl.ds(pl.multiple_of((way * count + index) * size, size), size)
                    own_buf[way, index] = (total.astype(BF16).astype(F32) + hidden_buf[own_rows, :].astype(F32)).astype(BF16)
            for way in range(2):
                if hop < hops:
                    send_sum(way, hop, index, sum_buf.at[way, hop - 1, index]).start()
                else:
                    send_out(way, 0, index, own_buf.at[way, index], me).start()
                    keep(way, index).start()
                    keep(way, index).wait()
            return carry

        lax.fori_loop(0, count, add, 0)

    for hop in range(1, tp_size):
        def forward(index, carry):
            for way in range(2):
                chunk = behind(way, hop)
                arrived = o_ref.at[rows(way, chunk, index)]
                send_out(way, hop - 1, index, arrived, chunk).wait_recv()
                if hop < hops:
                    send_out(way, hop, index, arrived, chunk).start()
            return carry

        lax.fori_loop(0, count, forward, 0)

    def drain(index, carry):
        for way in range(2):
            for hop in range(hops):
                send_sum(way, hop, index, sum_buf.at[way, hop, index]).wait_send()
                send_out(way, hop, index, own_buf.at[way, index], me).wait_send()
        return carry

    lax.fori_loop(0, count, drain, 0)


def finish(partial, hidden, tp_size, call_id):
    tokens, width = partial.shape
    own_tokens = hidden.shape[0]
    size = min(256, own_tokens // 2)
    count = own_tokens // (2 * size)
    hops = tp_size - 1
    return pl.pallas_call(
        functools.partial(finish_body, tp_size, count), out_shape=jax.ShapeDtypeStruct(partial.shape, BF16), in_specs=[HBM_SPEC, HBM_SPEC], out_specs=HBM_SPEC,
        scratch_shapes=[pltpu.VMEM(partial.shape, BF16), pltpu.VMEM(hidden.shape, BF16), pltpu.VMEM((2, hops, count, size, width), BF16), pltpu.VMEM((2, count, size, width), BF16),
                        DMA((4,)), DMA((2, hops, count)), DMA((2, hops, count)), DMA((2, hops, count)), DMA((2, hops, count))],
        compiler_params=settings(call_id),
        cost_estimate=cost(30),
        name='finish')(partial, hidden)


def solution(mesh):
    tp_size = mesh.shape['tp']
    ep_size = mesh.shape['ep']

    def local_fn(x, src_len, expert_idx, ln_gain, ln_bias, w_query, b_query, w_key, w_value, b_value, w_attn_out, b_attn_out, w_fc1, b_fc1, w_fc2, b_fc2, w_router, w_exp_in, b_exp_in, w_exp_out, b_exp_out):
        rows, seq, width = x.shape
        tokens = rows * seq
        num_experts = w_router.shape[1]
        capacity = 2 * (-(-tokens // num_experts))
        local_experts = w_exp_in.shape[0]
        own_experts = local_experts // tp_size
        _, _, local_heads, head_dim = w_query.shape
        head_cols = local_heads * head_dim
        own_rows = rows // tp_size

        def pack_attention(j):
            columns = [w[j].reshape(width, head_cols).T for w in (w_query, w_key, w_value)]
            return jnp.concatenate(columns + [w_attn_out[j].reshape(head_cols, width)], axis=0)

        def own_slice(value):
            size = value.shape[0] // ep_size
            return lax.dynamic_slice_in_dim(value, lax.axis_index('ep') * size, size, 0)

        own = jnp.stack([own_slice(value) for value in (pack_attention(0), w_fc1.T, w_fc2, pack_attention(1))])

        def piece(code):
            chunk, which, *part = map(int, code)
            size = width // (1 + len(part))
            return chunk, which, sum(part) * size, size

        plan = ['210'], ['00', '01'], ['10'], ['11', '20'], ['211', '30', '31']
        at_start, in_first, in_dense, in_second, in_experts = [[piece(code) for code in codes] for codes in plan]
        weights = w_exp_in, w_exp_out
        place, source, other, pack, later, b_query, b_value, b_fc1, b_exp_in, *moved = start(
            src_len, expert_idx.transpose(0, 2, 1), *weights, own, (b_query, b_value, b_fc1.reshape(1, -1), b_exp_in), num_experts, capacity, tp_size, ep_size, at_start, 4)

        def attention(layer, hidden, pack, pieces, spreads):
            return attention_layer(layer, hidden, own_rows, src_len, head_dim, ln_gain, ln_bias, pack.reshape(-1, width), b_query, b_value, b_attn_out, *weights, later,
                                   tp_size, ep_size, pieces, spreads, layer)

        hidden, normed, *landed, fc1_all, fc2_all = attention(0, x, pack, in_first, 2)
        moved += landed
        hidden, *landed, pack = dense_layer(hidden, normed, fc1_all.reshape(-1, width), b_fc1, fc2_all.reshape(-1, width), b_fc2.reshape(1, width), *weights, later, tp_size, ep_size, in_dense, 2)
        moved += landed
        hidden, normed, *landed = attention(1, hidden.reshape(own_rows, seq, width), pack, in_second, 0)
        moved += landed
        dispatch = dispatch_rows(source, normed, tp_size, 6).reshape(own_experts, ep_size, capacity, width)
        outputs, gates = experts(dispatch, moved, *weights, b_exp_in, b_exp_out, w_router, other, tp_size, ep_size, at_start + in_first + in_dense + in_second, in_experts, 3)
        partial = combine(place.reshape(-1), gates, outputs.reshape(-1, capacity, width), tokens)
        return finish(partial, hidden, tp_size, 5).reshape(rows, seq, width)

    axes = {'g': ('dp', 'ep'), 'e': 'ep', 't': 'tp', '.': None}

    def spec(code):
        return P(*[axes[letter] for letter in code])

    codes = ['g..', 'g', 'g..', '..', '..', '..t.', '.t.', '..t.', '..t.', '.t.', '.t..', '..', '.t', 't', 't.', '.', '..', 'e.t', 'et', 'et.', 'e.']
    in_specs = tuple(map(spec, codes))
    return jax.shard_map(local_fn, mesh=mesh, in_specs=in_specs, out_specs=spec('g..'), check_vma=False)
```

```python
import functools

import jax
import jax.numpy as jnp
from jax import lax
from jax.experimental import pallas as pl
from jax.experimental.pallas import tpu as pltpu
from jax.sharding import PartitionSpec as P

LN_EPS = 1e-5
BF16 = jnp.bfloat16
F32 = jnp.float32
LOG2E = 1.4426950408889634


MESH = pl.DeviceIdType.MESH
VMEM_SPEC = pl.BlockSpec(memory_space=pltpu.VMEM)
HBM_SPEC = pl.BlockSpec(memory_space=pltpu.HBM)
SMEM_SPEC = pl.BlockSpec(memory_space=pltpu.SMEM)
DMA = pltpu.SemaphoreType.DMA


def span(index, size):
    return pl.ds(pl.multiple_of(index * size, size), size)


def settings(call_id=None, mib=56, grid=None):
    return pltpu.CompilerParams(dimension_semantics=grid, collective_id=call_id, has_side_effects=call_id is not None, vmem_limit_bytes=mib << 20)


def cost(gflops):
    return pl.CostEstimate(flops=gflops * 10**9, transcendentals=0, bytes_accessed=10**7)


def dot_t(lhs, rhs_t):
    return lax.dot_general(lhs, rhs_t, (((1,), (1,)), ((), ())), preferred_element_type=F32)


def norm_rows(value, gain, shift):
    centered = value - jnp.mean(value, axis=-1, keepdims=True)
    variance = jnp.mean(centered * centered, axis=-1, keepdims=True)
    return centered * lax.rsqrt(variance + LN_EPS) * gain + shift


def away(axis, size, distance):
    return lax.rem(lax.axis_index(axis) + distance, size)


def enter(groups):
    barrier = pltpu.get_barrier_semaphore()
    count = 0
    for axis, size in groups:
        for distance in range(1, size):
            pl.semaphore_signal(barrier, device_id={axis: away(axis, size, distance)}, device_id_type=MESH)
            count += 1
    pl.semaphore_wait(barrier, count)


def exchange(tp_size, weights, piece, landing_ref, send_sem, recv_sem):
    chunk, which, start, cols = piece
    return [pltpu.make_async_remote_copy(
        src_ref=weights[which].at[chunk * tp_size + away('tp', tp_size, distance), :, pl.ds(start, cols)], dst_ref=landing_ref.at[distance - 1],
        send_sem=send_sem.at[distance - 1], recv_sem=recv_sem.at[distance - 1],
        device_id={'tp': away('tp', tp_size, distance)}, device_id_type=MESH)
        for distance in sorted(range(1, tp_size), key=lambda d: (min(d, tp_size - d), d))]


def exchange_all(tp_size, weights, pieces, landing_refs, send_sem, recv_sem):
    copies = []
    for index, piece in enumerate(pieces):
        copies += exchange(tp_size, weights, piece, landing_refs[index], send_sem.at[index], recv_sem.at[index])
    return copies


def landings(tp_size, weight, pieces):
    return [jax.ShapeDtypeStruct((tp_size - 1, weight.shape[1], cols), BF16) for _, _, _, cols in pieces]


def route_tables(lens_ref, index_ref, total_ref, total_t_ref):
    rows, _, seq = index_ref.shape
    step = min(512, seq)
    per_row = seq // step
    experts_count, wide = total_ref.shape
    slots = wide // 3
    ids = lax.broadcasted_iota(jnp.int32, (experts_count, 1), 0)
    slot_ids = lax.broadcasted_iota(jnp.int32, (slots, 1), 0)
    before = (lax.broadcasted_iota(jnp.int32, (step, step), 0) < lax.broadcasted_iota(jnp.int32, (step, step), 1)).astype(BF16)
    total_ref[...] = jnp.zeros_like(total_ref)
    total_t_ref[...] = jnp.zeros_like(total_t_ref)
    count = jnp.zeros((experts_count, 1), F32)
    for choice in range(2):
        def block(index, count):
            row = index // per_row
            start = pl.multiple_of((index % per_row) * step, step)
            cols = pl.ds(start, step)
            position = lax.broadcasted_iota(jnp.int32, (1, step), 1) + start
            chosen = jnp.where(position < lens_ref[row], index_ref[row, pl.ds(choice, 1), cols], -1)
            other = index_ref[row, pl.ds(1 - choice, 1), cols]
            token = position + row * seq
            hot = jnp.where(ids == chosen, 1.0, 0.0)
            rank = jnp.dot(hot.astype(BF16), before, preferred_element_type=F32) + count
            slot = jnp.sum(rank * hot, axis=0, keepdims=True).astype(jnp.int32)
            at_slot = slot_ids == slot
            parts = [jnp.where(at_slot, value.astype(F32), 0.0).astype(BF16) for value in (token & 255, (token >> 8) + 1, other)]
            values = jnp.concatenate(parts, axis=0)
            hot16 = hot.astype(BF16)
            total_ref[...] += dot_t(hot16, values)
            total_t_ref[...] += dot_t(values, hot16)
            return count + jnp.sum(hot, axis=1, keepdims=True)

        count = lax.fori_loop(0, rows * per_row, block, count)


def spread(ep_size, src_ref, view, sems):
    me = lax.axis_index('ep')
    send_sem, recv_sem = sems
    copies = [pltpu.make_async_remote_copy(
        src_ref=src_ref, dst_ref=view(me), send_sem=send_sem.at[distance], recv_sem=recv_sem.at[distance],
        device_id={'ep': away('ep', ep_size, distance)}, device_id_type=MESH) for distance in range(1, ep_size)]
    return copies + [pltpu.make_async_copy(src_ref, view(me), send_sem.at[0])]


def by_kind(ref, ep_size):
    per = ep_size // ref.shape[0]
    return lambda index: ref.at[index // per, :, lax.rem(index, per)]


def front_body(tp_size, ep_size, pieces, own_experts, head_dim, lens_ref, index_ref, gain_ref, shift_ref, b_out_ref, b_fc2_ref, x_ref, w_in_ref, w_out_ref, own_ref, *refs):
    biases, refs = refs[:4], refs[4:]
    place_ref, other_ref, hidden_ref, o_ref, b_exp_ref, *refs = refs
    moved_refs, refs = refs[:len(pieces)], refs[len(pieces):]
    (b_query_ref, b_value_ref, b_fc1_ref, first_ref, second_ref, later_ref, fc1_ref, fc2_ref, source_ref, total_ref, total_t_ref, bias_buf, qkv_ref, context_ref, all_buf,
     load_sem, move_send, move_recv, tp_send, tp_recv, row_send, row_recv, pair_send, pair_recv, spread_sem, ring_send, ring_recv) = refs
    mine = lax.axis_index('tp')
    me = lax.axis_index('ep')
    own_rows, seq, width = hidden_ref.shape
    _, ways, count, size, _ = all_buf.shape
    own_tokens = own_rows * seq

    view = by_kind(first_ref, ep_size)
    moves = exchange_all(tp_size, (w_in_ref, w_out_ref), pieces, moved_refs, move_send, move_recv)
    pairs = [(own_ref.at[0], view(me).at[mine])]
    pairs += [(bias, whole.at[mine]) for bias, whole in zip(biases, (b_query_ref, b_value_ref, b_fc1_ref, b_exp_ref))]
    pairs += [(own_ref.at[1 + index], later_ref.at[index, mine]) for index in range(later_ref.shape[0])]
    gathers = []
    for index, (src, dst) in enumerate(pairs):
        gathers.append([pltpu.make_async_copy(src, dst, tp_send.at[index, 0])] + [pltpu.make_async_remote_copy(
            src_ref=src, dst_ref=dst, send_sem=tp_send.at[index, distance], recv_sem=tp_recv.at[index, distance],
            device_id={'tp': away('tp', tp_size, distance)}, device_id_type=MESH) for distance in (1, tp_size - 1, *range(2, tp_size - 1))])
    load_x = pltpu.make_async_copy(x_ref.at[pl.ds(mine * own_rows, own_rows)], hidden_ref, load_sem)
    load_x.start()
    enter([('tp', tp_size), ('ep', ep_size)])
    for copies in gathers:
        for copy in copies:
            copy.start()
    for copy in moves:
        copy.start()

    cores = 2
    steps = range(1, ep_size // cores)
    other_core = me + 1 - cores * lax.rem(me, cores)

    def along(step):
        return pltpu.make_async_remote_copy(
            src_ref=view(me), dst_ref=view(me), send_sem=row_send.at[step], recv_sem=row_recv.at[step],
            device_id={'ep': away('ep', ep_size, cores * step)}, device_id_type=MESH)

    def across(step):
        part = view(away('ep', ep_size, ep_size - cores * step))
        return pltpu.make_async_remote_copy(
            src_ref=part, dst_ref=part, send_sem=pair_send.at[step], recv_sem=pair_recv.at[step],
            device_id={'ep': other_core}, device_id_type=MESH)

    for copy in gathers[0]:
        copy.wait()
    for step in steps:
        along(step).start()
    across(0).start()
    for copies in gathers[1:]:
        for copy in copies:
            copy.wait()
    views = [lambda part: fc1_ref.at[:, part], lambda part: fc2_ref.at[:, part], by_kind(second_ref, ep_size)]
    spreads = [spread(ep_size, later_ref.at[index], where, (spread_sem.at[0, index], spread_sem.at[1, index])) for index, where in enumerate(views)]
    for copies in spreads:
        for copy in copies:
            copy.start()

    route_tables(lens_ref, index_ref, total_ref, total_t_ref)
    rows, _, _ = index_ref.shape
    experts_count, wide = total_ref.shape
    slots = wide // 3
    lane = lax.broadcasted_iota(jnp.int32, (1, experts_count), 1)

    def take(index, carry):
        chunk = index // ep_size
        expert = (index % ep_size) * (own_experts * tp_size) + chunk * tp_size + mine
        line = total_ref[pl.ds(expert, 1), :].astype(jnp.int32)
        low, high = line[:, :slots], line[:, slots:2 * slots]
        place_ref[pl.ds(index, 1), :] = 8 * jnp.where(high > 0, 256 * (high - 1) + low, rows * seq)
        column = jnp.sum(jnp.where(lane == expert, total_t_ref[...], 0.0), axis=1, keepdims=True).astype(jnp.int32)
        low, high, other = column[:slots], column[slots:2 * slots], column[2 * slots:]
        at = span(index, slots)
        source_ref[at, :] = jnp.where(high > 0, 256 * (high - 1) + low, -1)
        other_ref[at, :] = other
        return carry

    for step in steps:
        along(step).wait()
        across(step).start()
    lax.fori_loop(0, own_experts * ep_size, take, 0)
    for step in range(ep_size // cores):
        across(step).wait()
    load_x.wait()

    hops = tp_size - 1

    def behind(way, distance):
        return away('tp', tp_size, (tp_size - distance) % tp_size if way == 0 else distance % tp_size)

    def ring(way, hop, index, chunk):
        piece = all_buf.at[chunk, way, index]
        return pltpu.make_async_remote_copy(
            src_ref=piece, dst_ref=piece, send_sem=ring_send.at[way, hop, index], recv_sem=ring_recv.at[way, hop, index],
            device_id={'tp': away('tp', tp_size, 1 + way * (tp_size - 2))}, device_id_type=MESH)

    def norm(value, index):
        return norm_rows(value, gain_ref[pl.ds(index, 1), :], shift_ref[pl.ds(index, 1), :]).astype(BF16)

    pair = 2 * head_dim
    lane_head = lax.broadcasted_iota(jnp.int32, (1, pair), 1) // head_dim
    factor = (head_dim ** -0.5) * LOG2E
    blocks = seq // size

    def attention(layer, pack_ref):
        def pack_rows(start, number):
            return pack_ref[pl.ds(start, number)].reshape(number * width, width)

        bias_buf[...] = jnp.zeros_like(bias_buf)
        for ref, start in ((b_query_ref, 0), (b_value_ref, 2 * width)):
            parts = [ref[part, head, pl.ds(layer, 1), :] for part in range(tp_size) for head in range(ref.shape[1])]
            bias_buf[:, pl.ds(start, width)] = jnp.concatenate(parts, axis=1)
        def one_row(row, carry):
            key_ok = lax.broadcasted_iota(jnp.int32, (1, seq), 1) < lens_ref[mine * own_rows + row]

            def project(index, carry):
                rows = span(index, size)
                normed = norm(hidden_ref[row, rows, :].astype(F32), 2 * layer)
                qkv_ref[rows, :] = (dot_t(normed, pack_rows(0, 3)) + bias_buf[...]).astype(BF16)
                return carry

            lax.fori_loop(0, blocks, project, 0)

            def attend(block, carry):
                rows = span(block, size)

                def heads(index, carry):
                    lanes = pl.multiple_of(index * pair, pair)
                    query = qkv_ref[rows, pl.ds(lanes, pair)]
                    keys = qkv_ref[:, pl.ds(pl.multiple_of(lanes + width, pair), pair)]
                    values = qkv_ref[:, pl.ds(pl.multiple_of(lanes + 2 * width, pair), pair)]
                    result = None
                    for head in range(2):
                        scores = dot_t(jnp.where(lane_head == head, query, jnp.zeros_like(query)), keys)
                        scores = jnp.where(key_ok, scores, -1e30)
                        top = jnp.max(scores, axis=-1, keepdims=True)
                        weights = jnp.exp2((scores - top) * factor)
                        scale = 1.0 / jnp.sum(weights, axis=-1, keepdims=True)
                        part = jnp.dot((weights * scale).astype(BF16), values, preferred_element_type=F32)
                        result = part if result is None else jnp.where(lane_head == head, part, result)
                    context_ref[:, pl.ds(lanes, pair)] = result.astype(BF16)
                    return carry

                lax.fori_loop(0, width // pair, heads, 0)
                projected = jnp.dot(context_ref[...], pack_rows(3, 1), preferred_element_type=F32)
                hidden = (hidden_ref[row, rows, :].astype(F32) + projected + b_out_ref[pl.ds(layer, 1), :]).astype(BF16)
                hidden_ref[row, rows, :] = hidden
                if layer:
                    all_buf[mine, row, block] = norm(hidden.astype(F32), 2 * layer + 1)
                    ring(row, 0, block, mine).start()
                return carry

            lax.fori_loop(0, blocks, attend, 0)
            return carry

        lax.fori_loop(0, own_rows, one_row, 0)

    attention(0, first_ref)

    for copies in spreads[:2]:
        for copy in copies:
            copy.wait()

    def dense(index, carry):
        row, rows = index // blocks, span(index % blocks, size)
        value = hidden_ref[row, rows, :].astype(F32)
        normed = norm(value, 1)
        total = value + b_fc2_ref[...]
        for part in range(tp_size):
            cols = fc1_ref[part].reshape(-1, width)
            inner = jnp.maximum(dot_t(normed, cols) + b_fc1_ref[part], 0.0).astype(BF16)
            total += jnp.dot(inner, fc2_ref[part].reshape(-1, width), preferred_element_type=F32)
        hidden_ref[row, rows, :] = total.astype(BF16)
        return carry

    lax.fori_loop(0, own_rows * blocks, dense, 0)
    for copy in spreads[2]:
        copy.wait()
    attention(1, second_ref)

    token = lax.broadcasted_iota(jnp.int32, (1, size), 1)
    slot_count, _ = o_ref.shape
    some = min(512, slot_count)

    def dispatch(index, chunks, fresh):
        def part(part, carry):
            at = span(part, some)
            total = None if fresh else o_ref[at, :].astype(F32)
            for way in range(ways):
                base = chunks[way] * own_tokens + (way * count + index) * size
                hot = jnp.where(source_ref[at, :] == token + base, 1.0, 0.0).astype(BF16)
                taken = jnp.dot(hot, all_buf[chunks[way], way, index], preferred_element_type=F32)
                total = taken if total is None else total + taken
            o_ref[at, :] = total.astype(BF16)
            return carry

        lax.fori_loop(0, slot_count // some, part, 0)

    dispatch(0, (mine, mine), True)

    def own(index, carry):
        dispatch(index, (mine, mine), False)
        return carry

    lax.fori_loop(1, count, own, 0)
    for hop in range(1, tp_size):
        def arrive(index, carry):
            chunks = [behind(way, hop) for way in range(ways)]
            for way in range(ways):
                ring(way, hop - 1, index, chunks[way]).wait_recv()
                if hop < hops:
                    ring(way, hop, index, chunks[way]).start()
            dispatch(index, chunks, False)
            return carry

        lax.fori_loop(0, count, arrive, 0)

    def drain(index, carry):
        for way in range(ways):
            for hop in range(hops):
                ring(way, hop, index, mine).wait_send()
        return carry

    lax.fori_loop(0, count, drain, 0)
    for copy in moves:
        copy.wait()


def front(lens, index, gain, shift, b_out, b_fc2, x, w_in, w_out, own, biases, num_experts, capacity, head_dim, tp_size, ep_size, pieces, call_id):
    own_experts = w_in.shape[0] // tp_size
    blocks = own_experts * ep_size
    packs, cut, width = own.shape
    rows, seq, _ = x.shape
    own_rows = rows // tp_size
    size = min(256, seq)
    count = seq // size
    slots = blocks * capacity
    per = ep_size // packs

    def vmem(*shape, dtype=BF16):
        return pltpu.VMEM(shape, dtype)

    moved = landings(tp_size, w_in, pieces)
    b_exp = jax.ShapeDtypeStruct((tp_size,) + biases[3].shape, F32)
    pack = vmem(packs, tp_size, per, cut, width)
    piece_dma, gather_dma, ring_dma = DMA((len(pieces), tp_size - 1)), DMA((packs + len(biases), tp_size)), DMA((own_rows, tp_size - 1, count))
    return pl.pallas_call(
        functools.partial(front_body, tp_size, ep_size, pieces, own_experts, head_dim),
        out_shape=(jax.ShapeDtypeStruct((blocks, capacity), jnp.int32), jax.ShapeDtypeStruct((slots, 1), jnp.int32), jax.ShapeDtypeStruct((own_rows, seq, width), BF16),
                   jax.ShapeDtypeStruct((slots, width), BF16), b_exp, *moved),
        in_specs=[SMEM_SPEC] + [VMEM_SPEC] * 5 + [HBM_SPEC] * (4 + len(biases)), out_specs=[VMEM_SPEC] * 4 + [HBM_SPEC] * (1 + len(pieces)),
        scratch_shapes=[vmem(tp_size, *biases[0].shape, dtype=F32), vmem(tp_size, *biases[1].shape, dtype=F32), vmem(tp_size, *biases[2].shape, dtype=F32), pack, pack,
                        vmem(packs - 1, tp_size, cut, width), vmem(tp_size, ep_size, cut, width), vmem(tp_size, ep_size, cut, width), vmem(slots, 1, dtype=jnp.int32),
                        vmem(num_experts, 3 * capacity, dtype=F32), vmem(3 * capacity, num_experts, dtype=F32), vmem(1, 3 * width, dtype=F32), vmem(seq, 3 * width), vmem(size, width),
                        vmem(tp_size, own_rows, count, size, width), DMA, piece_dma, piece_dma, gather_dma, gather_dma] + [DMA((ep_size,))] * 4
                       + [DMA((2, packs - 1, ep_size)), ring_dma, ring_dma],
        compiler_params=settings(call_id, 62), cost_estimate=cost(100), name='front')(lens, index, gain, shift, b_out, b_fc2, x, w_in, w_out, own, *biases)


def experts_body(tp_size, ep_size, early, late, dispatch_ref, early_refs, w_in_ref, w_out_ref, b_in_ref, b_out_ref, w_router_ref, other_ref, returned_ref, gates_ref,
                 sent_buf, arrived_ref, parts_buf, own_buf, out_buf, local_sem, send_sem, recv_sem, back_send, back_recv, move_send, move_recv):
    chunks, _, slots, width = arrived_ref.shape
    me = lax.axis_index('ep')
    mine = lax.axis_index('tp')
    weights = (w_in_ref, w_out_ref)
    units = [(chunk, which) for chunk in range(chunks) for which in range(2)]

    sends = {}
    for chunk in range(chunks):
        for distance in range(1, ep_size):
            peer = away('ep', ep_size, distance)
            sends[chunk, distance] = pltpu.make_async_remote_copy(
                src_ref=dispatch_ref.at[chunk, peer], dst_ref=arrived_ref.at[chunk, me], send_sem=send_sem.at[chunk, distance], recv_sem=recv_sem.at[chunk, distance],
                device_id={'ep': peer}, device_id_type=MESH)

    def landing(piece):
        chunk, which, start, cols = piece
        return parts_buf.at[units.index((chunk, which)), :, :, pl.ds(start, cols)]

    moves = {piece: exchange(tp_size, weights, piece, landing(piece), move_send.at[index], move_recv.at[index]) for index, piece in enumerate(late)}
    kept = [pltpu.make_async_copy(dispatch_ref.at[chunk, me], arrived_ref.at[chunk, me], local_sem.at[0, chunk]) for chunk in range(chunks)]
    owns = {unit: pltpu.make_async_copy(weights[unit[1]].at[unit[0] * tp_size + mine], own_buf.at[unit[0], unit[1]], local_sem.at[1 + unit[1], unit[0]]) for unit in units}
    earlies = {piece: pltpu.make_async_copy(early_refs[index], landing(piece), local_sem.at[3, index]) for index, piece in enumerate(early)}

    enter([('tp', tp_size), ('ep', ep_size)])
    for piece in late:
        for copy in moves[piece]:
            copy.start()
    for chunk in range(chunks):
        for distance in range(1, ep_size):
            sends[chunk, distance].start()
        kept[chunk].start()
    for unit in units:
        owns[unit].start()
        for piece in early:
            if piece[:2] == unit:
                earlies[piece].start()

    lane = lax.broadcasted_iota(jnp.int32, (1, w_router_ref.shape[1]), 1)
    group = lax.broadcasted_iota(jnp.int32, (ep_size * slots, 1), 0) // slots

    def load(chunk):
        return pltpu.make_async_copy(dispatch_ref.at[chunk], sent_buf.at[chunk % 2], local_sem.at[5, chunk % 2])

    load(0).start()
    for chunk in range(chunks):
        if chunk + 1 < chunks:
            load(chunk + 1).start()
        load(chunk).wait()
        logits = jnp.dot(sent_buf[chunk % 2].reshape(ep_size * slots, width), w_router_ref[...].astype(BF16), preferred_element_type=F32)
        rows = pl.ds(chunk * ep_size * slots, ep_size * slots)
        own = jnp.sum(jnp.where(lane == group * (chunks * tp_size) + (chunk * tp_size + mine), logits, 0.0), axis=1, keepdims=True)
        other = jnp.sum(jnp.where(lane == other_ref[rows, :], logits, 0.0), axis=1, keepdims=True)
        gates_ref[rows, :] = jax.nn.sigmoid(own - other)

    def part_ref(unit, part):
        if part == 0:
            return own_buf.at[unit[0], unit[1]]
        return parts_buf.at[units.index(unit), part - 1]

    def give_back(chunk, slot, index, cols):
        for half in range(2):
            peer = 2 * index + half
            distance = lax.rem(peer - me + ep_size, ep_size)

            @pl.when(distance == 0)
            def _():
                pltpu.make_async_copy(out_buf.at[slot, peer, :, cols], returned_ref.at[chunk, me, :, cols], local_sem.at[4, chunk]).start()

            @pl.when(distance != 0)
            def _():
                pltpu.make_async_remote_copy(
                    src_ref=out_buf.at[slot, peer, :, cols], dst_ref=returned_ref.at[chunk, me, :, cols], send_sem=back_send.at[chunk, distance], recv_sem=back_recv.at[chunk, distance],
                    device_id={'ep': peer}, device_id_type=MESH).start()

    def weights_here(chunk, which, cols=None):
        unit = (chunk, which)
        if cols is None or cols.start == 0:
            owns[unit].wait()
            for piece in early:
                if piece[:2] == unit:
                    earlies[piece].wait()
        for piece in late:
            if piece[:2] == unit and (cols is None or piece[2] == cols.start):
                for copy in moves[piece]:
                    copy.wait_recv()

    def expert_row(chunk):
        return pl.ds(chunk * tp_size + mine, 1)

    def inner_part(chunk, index, part):
        tokens = arrived_ref[chunk, pl.ds(2 * index, 2)].reshape(2 * slots, width)
        inner = jnp.dot(tokens, part_ref((chunk, 0), part)[...], preferred_element_type=F32) + b_in_ref[away('tp', tp_size, tp_size - part), expert_row(chunk), :]
        return jnp.maximum(inner, 0.0).astype(BF16)

    backs = {}
    for chunk in range(chunks):
        last = chunk == chunks - 1
        slot = chunk % out_buf.shape[0]
        for distance in range(1, ep_size):
            sends[chunk, distance].wait_recv()
        kept[chunk].wait()
        weights_here(chunk, 0)
        before = chunk - out_buf.shape[0]
        if before >= 0:
            for copy in backs[before][:-1]:
                copy.wait_send()
            backs[before][-1].wait()

        held = [sent_buf.at[0], sent_buf.at[1], arrived_ref.at[0], arrived_ref.at[1]]
        if last:
            def first_product(index, carry):
                for part in range(tp_size):
                    held[part][pl.ds(2 * index, 2)] = inner_part(chunk, index, part).reshape(2, slots, width)
                return carry

            lax.fori_loop(0, ep_size // 2, first_product, 0)
        for cols in ([pl.ds(0, width // 2), pl.ds(width // 2, width // 2)] if last else [pl.ds(0, width)]):
            weights_here(chunk, 1, cols if last else None)

            def rows(index, carry):
                total = jnp.zeros((2 * slots, cols.size), F32)
                for part in range(tp_size):
                    inner = held[part][pl.ds(2 * index, 2)].reshape(2 * slots, width) if last else inner_part(chunk, index, part)
                    total += jnp.dot(inner, part_ref((chunk, 1), part)[:, cols], preferred_element_type=F32)
                out_buf[slot, pl.ds(2 * index, 2), :, cols] = (total + b_out_ref[expert_row(chunk), cols]).astype(BF16).reshape(2, slots, cols.size)

                @pl.when(index > 0)
                def _():
                    give_back(chunk, slot, index - 1, cols)

                return carry

            lax.fori_loop(0, ep_size // 2, rows, 0)
            give_back(chunk, slot, ep_size // 2 - 1, cols)
        backs[chunk] = []
        for distance in range(1, ep_size):
            peer = away('ep', ep_size, distance)
            backs[chunk].append(pltpu.make_async_remote_copy(
                src_ref=out_buf.at[slot, peer], dst_ref=returned_ref.at[chunk, me], send_sem=back_send.at[chunk, distance], recv_sem=back_recv.at[chunk, distance],
                device_id={'ep': peer}, device_id_type=MESH))
        backs[chunk].append(pltpu.make_async_copy(out_buf.at[slot, me], returned_ref.at[chunk, me], local_sem.at[4, chunk]))

    for chunk in range(chunks):
        for distance in range(1, ep_size):
            sends[chunk, distance].wait_send()
        for copy in backs[chunk][:-1]:
            copy.wait_recv()
            if chunk + out_buf.shape[0] >= chunks:
                copy.wait_send()
        if chunk + out_buf.shape[0] >= chunks:
            backs[chunk][-1].wait()
    for piece in late:
        for copy in moves[piece]:
            copy.wait_send()


def experts(dispatch, early_weights, w_in, w_out, b_in, b_out, w_router, other, tp_size, ep_size, early, late, call_id):
    chunks, _, slots, width = dispatch.shape
    hidden = w_in.shape[2]

    def body(dispatch_ref, *refs):
        experts_body(tp_size, ep_size, early, late, dispatch_ref, refs[:len(early)], *refs[len(early):])

    return pl.pallas_call(
        body, out_shape=(jax.ShapeDtypeStruct(dispatch.shape, BF16), jax.ShapeDtypeStruct(other.shape, F32)),
        in_specs=[HBM_SPEC] * (3 + len(early)) + [VMEM_SPEC] * 4, out_specs=(HBM_SPEC, VMEM_SPEC),
        scratch_shapes=[pltpu.VMEM((2,) + dispatch.shape[1:], BF16), pltpu.VMEM(dispatch.shape, BF16), pltpu.VMEM((2 * chunks, tp_size - 1, width, hidden), BF16),
                        pltpu.VMEM((chunks, 2, width, hidden), BF16), pltpu.VMEM((2, ep_size, slots, width), BF16),
                        DMA((6, max(chunks, len(early)))), DMA((chunks, ep_size)), DMA((chunks, ep_size)), DMA((chunks, ep_size)), DMA((chunks, ep_size)),
                        DMA((len(late), tp_size - 1)), DMA((len(late), tp_size - 1))],
        compiler_params=settings(call_id, 62),
        cost_estimate=cost(30),
        name='experts')(dispatch, *early_weights, w_in, w_out, b_in, b_out, w_router, other)


def combine_body(blocks, batch, token_ref, slots_ref, gates_ref, o_ref, acc_ref, wide_ref):
    block = pl.program_id(0)
    slots, width = slots_ref.shape
    step = o_ref.shape[0]
    lanes = 128
    piece = min(128, slots)

    @pl.when(block == 0)
    def _():
        def clear(index, carry):
            acc_ref[span(index, lanes), :] = jnp.zeros((lanes, lanes), F32)
            return carry
        lax.fori_loop(0, acc_ref.shape[0] // lanes, clear, 0)

    @pl.when(block < blocks)
    def _():
        def widen(index, carry):
            rows = span(index, piece)
            for col in range(width // lanes):
                wide_ref[pl.ds(index * (piece * 8) + col, piece, stride=8), :] = slots_ref[rows, col * lanes:(col + 1) * lanes].astype(F32) * gates_ref[rows, :]
            return carry
        lax.fori_loop(0, slots // piece, widen, 0)
        base = block * slots

        def add(index, carry):
            first = index * batch
            places = [pl.ds(pl.multiple_of(token_ref[base + first + u], 8), 8) for u in range(batch)]
            start = pl.multiple_of(first * 8, batch * 8)
            new = [acc_ref[places[u], :] + wide_ref[pl.ds(start + u * 8, 8), :] for u in range(batch)]
            for u in range(batch):
                acc_ref[places[u], :] = new[u]
            return carry

        lax.fori_loop(0, slots // batch, add, 0)

    @pl.when(block >= blocks)
    def _():
        first = (block - blocks) * (step * 8)
        some = min(256, step)

        def write(index, carry):
            rows = span(index, some)
            for col in range(width // lanes):
                o_ref[rows, col * lanes:(col + 1) * lanes] = acc_ref[pl.ds(first + index * (some * 8) + col, some, stride=8), :].astype(BF16)
            return carry
        lax.fori_loop(0, step // some, write, 0)


def combine(place, gates, outputs, tokens):
    count, slots, width = outputs.shape
    blocks = 4
    batch = min(32, slots)
    slots = count * slots // blocks
    outputs = outputs.reshape(blocks, slots, width)
    step = tokens // 4
    grid_spec = pltpu.PrefetchScalarGridSpec(
        num_scalar_prefetch=1, grid=(blocks + tokens // step,),
        in_specs=[pl.BlockSpec((None, slots, width), lambda b, *_: (jnp.minimum(b, blocks - 1), 0, 0)), pl.BlockSpec((slots, 1), lambda b, *_: (jnp.minimum(b, blocks - 1), 0))],
        out_specs=pl.BlockSpec((step, width), lambda b, *_: (jnp.maximum(b - blocks, 0), 0)),
        scratch_shapes=[pltpu.VMEM(((tokens + 32) * 8, 128), F32), pltpu.VMEM((slots * 8, 128), F32)])
    return pl.pallas_call(
        functools.partial(combine_body, blocks, batch),
        out_shape=jax.ShapeDtypeStruct((tokens, width), BF16), grid_spec=grid_spec,
        compiler_params=settings(grid=('arbitrary',)),
        cost_estimate=cost(30),
        name='combine')(place, outputs, gates)


def finish_body(tp_size, count, partial_ref, hidden_ref, o_ref, partial_buf, hidden_buf, sum_buf, own_buf, load_sem, sum_send, sum_recv, out_send, out_recv):
    me = lax.axis_index('tp')
    own_tokens, _ = hidden_ref.shape
    size = own_tokens // (2 * count)
    hops = tp_size - 1
    step_to = (1, tp_size - 1)

    def rows(way, chunk, index):
        return pl.ds(pl.multiple_of(chunk * own_tokens + (way * count + index) * size, size), size)

    def behind(way, distance):
        return away('tp', tp_size, (tp_size - distance) % tp_size if way == 0 else distance % tp_size)

    def send_sum(way, hop, index, src_ref):
        return pltpu.make_async_remote_copy(
            src_ref=src_ref, dst_ref=sum_buf.at[way, hop, index], send_sem=sum_send.at[way, hop, index], recv_sem=sum_recv.at[way, hop, index],
            device_id={'tp': away('tp', tp_size, step_to[way])}, device_id_type=MESH)

    def send_out(way, hop, index, src_ref, chunk):
        return pltpu.make_async_remote_copy(
            src_ref=src_ref, dst_ref=o_ref.at[rows(way, chunk, index)], send_sem=out_send.at[way, hop, index], recv_sem=out_recv.at[way, hop, index],
            device_id={'tp': away('tp', tp_size, step_to[way])}, device_id_type=MESH)

    loads = [pltpu.make_async_copy(partial_ref, partial_buf, load_sem.at[0]), pltpu.make_async_copy(hidden_ref, hidden_buf, load_sem.at[1])]
    for load in loads:
        load.start()
    enter([('tp', tp_size)])

    def first(index, carry):
        for way in range(2):
            send_sum(way, 0, index, partial_ref.at[rows(way, behind(way, 1), index)]).start()
        return carry

    lax.fori_loop(0, count, first, 0)
    for load in loads:
        load.wait()

    def keep(way, index):
        own = own_buf.at[way, index]
        return pltpu.make_async_copy(own, o_ref.at[rows(way, me, index)], load_sem.at[2 + way])

    for hop in range(1, tp_size):
        def add(index, carry):
            for way in range(2):
                send_sum(way, hop - 1, index, sum_buf.at[way, hop - 1, index]).wait_recv()
                total = sum_buf[way, hop - 1, index].astype(F32) + partial_buf[rows(way, behind(way, hop + 1), index), :].astype(F32)
                if hop < hops:
                    sum_buf[way, hop - 1, index] = total.astype(BF16)
                else:
                    own_rows = pl.ds(pl.multiple_of((way * count + index) * size, size), size)
                    own_buf[way, index] = (total.astype(BF16).astype(F32) + hidden_buf[own_rows, :].astype(F32)).astype(BF16)
            for way in range(2):
                if hop < hops:
                    send_sum(way, hop, index, sum_buf.at[way, hop - 1, index]).start()
                else:
                    send_out(way, 0, index, own_buf.at[way, index], me).start()
                    keep(way, index).start()
                    keep(way, index).wait()
            return carry

        lax.fori_loop(0, count, add, 0)

    for hop in range(1, tp_size):
        def forward(index, carry):
            for way in range(2):
                chunk = behind(way, hop)
                arrived = o_ref.at[rows(way, chunk, index)]
                send_out(way, hop - 1, index, arrived, chunk).wait_recv()
                if hop < hops:
                    send_out(way, hop, index, arrived, chunk).start()
            return carry

        lax.fori_loop(0, count, forward, 0)

    def drain(index, carry):
        for way in range(2):
            for hop in range(hops):
                send_sum(way, hop, index, sum_buf.at[way, hop, index]).wait_send()
                send_out(way, hop, index, own_buf.at[way, index], me).wait_send()
        return carry

    lax.fori_loop(0, count, drain, 0)


def finish(partial, hidden, tp_size, call_id):
    tokens, width = partial.shape
    own_tokens = hidden.shape[0]
    size = min(256, own_tokens // 2)
    count = own_tokens // (2 * size)
    hops = tp_size - 1
    return pl.pallas_call(
        functools.partial(finish_body, tp_size, count), out_shape=jax.ShapeDtypeStruct(partial.shape, BF16), in_specs=[HBM_SPEC, HBM_SPEC], out_specs=HBM_SPEC,
        scratch_shapes=[pltpu.VMEM(partial.shape, BF16), pltpu.VMEM(hidden.shape, BF16), pltpu.VMEM((2, hops, count, size, width), BF16), pltpu.VMEM((2, count, size, width), BF16),
                        DMA((4,)), DMA((2, hops, count)), DMA((2, hops, count)), DMA((2, hops, count)), DMA((2, hops, count))],
        compiler_params=settings(call_id),
        cost_estimate=cost(30),
        name='finish')(partial, hidden)


def solution(mesh):
    tp_size = mesh.shape['tp']
    ep_size = mesh.shape['ep']

    def local_fn(x, src_len, expert_idx, ln_gain, ln_bias, w_query, b_query, w_key, w_value, b_value, w_attn_out, b_attn_out, w_fc1, b_fc1, w_fc2, b_fc2, w_router, w_exp_in, b_exp_in, w_exp_out, b_exp_out):
        rows, seq, width = x.shape
        tokens = rows * seq
        num_experts = w_router.shape[1]
        capacity = 2 * (-(-tokens // num_experts))
        local_experts = w_exp_in.shape[0]
        own_experts = local_experts // tp_size
        _, _, local_heads, head_dim = w_query.shape
        head_cols = local_heads * head_dim

        def pack_attention(j):
            columns = [w[j].reshape(width, head_cols).T for w in (w_query, w_key, w_value)]
            return jnp.concatenate(columns + [w_attn_out[j].reshape(head_cols, width)], axis=0)

        def own_slice(value):
            size = value.shape[0] // ep_size
            return lax.dynamic_slice_in_dim(value, lax.axis_index('ep') * size, size, 0)

        own = jnp.stack([own_slice(value) for value in (pack_attention(0), w_fc1.T, w_fc2, pack_attention(1))])

        def piece(code):
            chunk, which, *part = map(int, code)
            size = width // (1 + len(part))
            return chunk, which, sum(part) * size, size

        plan = ['00', '01', '10', '11', '20', '210'], ['211', '30', '310', '311']
        early, late = [[piece(code) for code in codes] for codes in plan]
        weights = w_exp_in, w_exp_out
        biases = b_query.transpose(1, 0, 2), b_value.transpose(1, 0, 2), b_fc1.reshape(1, -1), b_exp_in
        place, other, hidden, dispatch, b_exp_in, *moved = front(
            src_len, expert_idx.transpose(0, 2, 1), ln_gain, ln_bias, b_attn_out, b_fc2.reshape(1, -1), x, *weights, own, biases, num_experts, capacity, head_dim, tp_size, ep_size, early, 0)
        dispatch = dispatch.reshape(own_experts, ep_size, capacity, width)
        outputs, gates = experts(dispatch, moved, *weights, b_exp_in, b_exp_out, w_router, other, tp_size, ep_size, early, late, 1)
        partial = combine(place.reshape(-1), gates, outputs.reshape(-1, capacity, width), tokens)
        return finish(partial, hidden.reshape(-1, width), tp_size, 2).reshape(rows, seq, width)

    axes = {'g': ('dp', 'ep'), 'e': 'ep', 't': 'tp', '.': None}

    def spec(code):
        return P(*[axes[letter] for letter in code])

    codes = ['g..', 'g', 'g..', '..', '..', '..t.', '.t.', '..t.', '..t.', '.t.', '.t..', '..', '.t', 't', 't.', '.', '..', 'e.t', 'et', 'et.', 'e.']
    in_specs = tuple(map(spec, codes))
    return jax.shard_map(local_fn, mesh=mesh, in_specs=in_specs, out_specs=spec('g..'), check_vma=False)
```

```python
import functools

import jax
import jax.numpy as jnp
from jax import lax
from jax.experimental import pallas as pl
from jax.experimental.pallas import tpu as pltpu
from jax.sharding import PartitionSpec as P

LN_EPS = 1e-5
BF16 = jnp.bfloat16
F32 = jnp.float32
LOG2E = 1.4426950408889634


MESH = pl.DeviceIdType.MESH
VMEM_SPEC = pl.BlockSpec(memory_space=pltpu.VMEM)
HBM_SPEC = pl.BlockSpec(memory_space=pltpu.HBM)
SMEM_SPEC = pl.BlockSpec(memory_space=pltpu.SMEM)
DMA = pltpu.SemaphoreType.DMA


def span(index, size):
    return pl.ds(pl.multiple_of(index * size, size), size)


def settings(call_id=None, mib=56, grid=None):
    return pltpu.CompilerParams(dimension_semantics=grid, collective_id=call_id, has_side_effects=call_id is not None, vmem_limit_bytes=mib << 20)


def cost(gflops):
    return pl.CostEstimate(flops=gflops * 10**9, transcendentals=0, bytes_accessed=10**7)


def dot_t(lhs, rhs_t):
    return lax.dot_general(lhs, rhs_t, (((1,), (1,)), ((), ())), preferred_element_type=F32)


def norm_rows(value, gain, shift):
    centered = value - jnp.mean(value, axis=-1, keepdims=True)
    variance = jnp.mean(centered * centered, axis=-1, keepdims=True)
    return centered * lax.rsqrt(variance + LN_EPS) * gain + shift


def away(axis, size, distance):
    return lax.rem(lax.axis_index(axis) + distance, size)


def enter(groups):
    barrier = pltpu.get_barrier_semaphore()
    count = 0
    for axis, size in groups:
        for distance in range(1, size):
            pl.semaphore_signal(barrier, device_id={axis: away(axis, size, distance)}, device_id_type=MESH)
            count += 1
    pl.semaphore_wait(barrier, count)


def exchange(tp_size, weights, piece, landing_ref, send_sem, recv_sem):
    chunk, which, start, cols = piece
    return [pltpu.make_async_remote_copy(
        src_ref=weights[which].at[chunk * tp_size + away('tp', tp_size, distance), :, pl.ds(start, cols)], dst_ref=landing_ref.at[distance - 1],
        send_sem=send_sem.at[distance - 1], recv_sem=recv_sem.at[distance - 1],
        device_id={'tp': away('tp', tp_size, distance)}, device_id_type=MESH)
        for distance in sorted(range(1, tp_size), key=lambda d: (min(d, tp_size - d), d))]


def exchange_all(tp_size, weights, pieces, landing_refs, send_sem, recv_sem):
    copies = []
    for index, piece in enumerate(pieces):
        copies += exchange(tp_size, weights, piece, landing_refs[index], send_sem.at[index], recv_sem.at[index])
    return copies


def landings(tp_size, weight, pieces):
    return [jax.ShapeDtypeStruct((tp_size - 1, weight.shape[1], cols), BF16) for _, _, _, cols in pieces]


def route_tables(own_experts, tp_size, ep_size, lens_ref, index_ref, table_ref, total_ref):
    rows, _, seq = index_ref.shape
    step = min(512, seq)
    per_row = seq // step
    wide, experts_count = total_ref.shape
    slots = wide // 3
    lanes = table_ref.shape[1]
    mine = lax.axis_index('tp')
    ids = lax.broadcasted_iota(jnp.int32, (experts_count, 1), 0)
    slot_ids = lax.broadcasted_iota(jnp.int32, (slots, 1), 0)
    before = (lax.broadcasted_iota(jnp.int32, (step, step), 0) < lax.broadcasted_iota(jnp.int32, (step, step), 1)).astype(BF16)
    total_ref[...] = jnp.zeros_like(total_ref)
    count = jnp.zeros((experts_count, 1), F32)
    for choice in range(2):
        def block(index, count):
            row = index // per_row
            start = pl.multiple_of((index % per_row) * step, step)
            cols = pl.ds(start, step)
            position = lax.broadcasted_iota(jnp.int32, (1, step), 1) + start
            chosen = jnp.where(position < lens_ref[row], index_ref[row, pl.ds(choice, 1), cols], -1)
            other = index_ref[row, pl.ds(1 - choice, 1), cols]
            token = position + row * seq
            hot = jnp.where(ids == chosen, 1.0, 0.0)
            rank = jnp.dot(hot.astype(BF16), before, preferred_element_type=F32) + count
            slot = jnp.sum(rank * hot, axis=0, keepdims=True).astype(jnp.int32)
            at_slot = slot_ids == slot
            parts = [jnp.where(at_slot, value.astype(F32), 0.0).astype(BF16) for value in (token & 255, (token >> 8) + 1, other)]
            values = jnp.concatenate(parts, axis=0)
            hot16 = hot.astype(BF16)
            total_ref[...] += dot_t(values, hot16)
            local = own_experts * tp_size
            own = (lax.rem(chosen, tp_size) == mine) & (slot < slots)
            line = (lax.div(lax.rem(chosen, local), tp_size) * ep_size + lax.div(chosen, local)) * slots + slot
            line = jnp.where(own, line, own_experts * ep_size * slots)
            for part in range(step // lanes):
                at = (choice * rows * per_row + index) * (step // lanes) + part
                table_ref[pl.ds(at, 1), :] = line[:, part * lanes:(part + 1) * lanes]
            return count + jnp.sum(hot, axis=1, keepdims=True)

        count = lax.fori_loop(0, rows * per_row, block, count)


def spread(ep_size, src_ref, view, sems):
    me = lax.axis_index('ep')
    send_sem, recv_sem = sems
    copies = [pltpu.make_async_remote_copy(
        src_ref=src_ref, dst_ref=view(me), send_sem=send_sem.at[distance], recv_sem=recv_sem.at[distance],
        device_id={'ep': away('ep', ep_size, distance)}, device_id_type=MESH) for distance in range(1, ep_size)]
    return copies + [pltpu.make_async_copy(src_ref, view(me), send_sem.at[0])]


def by_kind(ref, ep_size):
    per = ep_size // ref.shape[0]
    return lambda index: ref.at[index // per, :, lax.rem(index, per)]


def front_body(tp_size, ep_size, pieces, own_experts, head_dim, lens_ref, index_ref, gain_ref, shift_ref, b_out_ref, b_fc2_ref, x_ref, w_in_ref, w_out_ref, own_ref, *refs):
    biases, refs = refs[:4], refs[4:]
    table_ref, other_ref, hidden_ref, o_ref, b_exp_ref, *refs = refs
    moved_refs, refs = refs[:len(pieces)], refs[len(pieces):]
    (b_query_ref, b_value_ref, b_fc1_ref, first_ref, second_ref, later_ref, fc1_ref, fc2_ref, source_ref, total_ref, bias_buf, qkv_ref, context_ref, all_buf,
     load_sem, move_send, move_recv, tp_send, tp_recv, row_send, row_recv, pair_send, pair_recv, spread_sem, ring_send, ring_recv) = refs
    mine = lax.axis_index('tp')
    me = lax.axis_index('ep')
    own_rows, seq, width = hidden_ref.shape
    _, ways, count, size, _ = all_buf.shape
    own_tokens = own_rows * seq

    view = by_kind(first_ref, ep_size)
    moves = exchange_all(tp_size, (w_in_ref, w_out_ref), pieces, moved_refs, move_send, move_recv)
    pairs = [(own_ref.at[0], view(me).at[mine])]
    pairs += [(bias, whole.at[mine]) for bias, whole in zip(biases, (b_query_ref, b_value_ref, b_fc1_ref, b_exp_ref))]
    pairs += [(own_ref.at[1 + index], later_ref.at[index, mine]) for index in range(later_ref.shape[0])]
    gathers = []
    for index, (src, dst) in enumerate(pairs):
        gathers.append([pltpu.make_async_copy(src, dst, tp_send.at[index, 0])] + [pltpu.make_async_remote_copy(
            src_ref=src, dst_ref=dst, send_sem=tp_send.at[index, distance], recv_sem=tp_recv.at[index, distance],
            device_id={'tp': away('tp', tp_size, distance)}, device_id_type=MESH) for distance in (1, tp_size - 1, *range(2, tp_size - 1))])
    load_x = pltpu.make_async_copy(x_ref.at[pl.ds(mine * own_rows, own_rows)], hidden_ref, load_sem)
    load_x.start()
    enter([('tp', tp_size), ('ep', ep_size)])
    for copies in gathers:
        for copy in copies:
            copy.start()
    for copy in moves:
        copy.start()

    cores = 2
    steps = range(1, ep_size // cores)
    other_core = me + 1 - cores * lax.rem(me, cores)

    def along(step):
        return pltpu.make_async_remote_copy(
            src_ref=view(me), dst_ref=view(me), send_sem=row_send.at[step], recv_sem=row_recv.at[step],
            device_id={'ep': away('ep', ep_size, cores * step)}, device_id_type=MESH)

    def across(step):
        part = view(away('ep', ep_size, ep_size - cores * step))
        return pltpu.make_async_remote_copy(
            src_ref=part, dst_ref=part, send_sem=pair_send.at[step], recv_sem=pair_recv.at[step],
            device_id={'ep': other_core}, device_id_type=MESH)

    for copy in gathers[0]:
        copy.wait()
    for step in steps:
        along(step).start()
    across(0).start()
    for copies in gathers[1:]:
        for copy in copies:
            copy.wait()
    views = [lambda part: fc1_ref.at[:, part], lambda part: fc2_ref.at[:, part], by_kind(second_ref, ep_size)]
    spreads = [spread(ep_size, later_ref.at[index], where, (spread_sem.at[0, index], spread_sem.at[1, index])) for index, where in enumerate(views)]
    for copies in spreads:
        for copy in copies:
            copy.start()

    route_tables(own_experts, tp_size, ep_size, lens_ref, index_ref, table_ref, total_ref)
    wide, experts_count = total_ref.shape
    slots = wide // 3
    lane = lax.broadcasted_iota(jnp.int32, (1, experts_count), 1)

    def take(index, carry):
        chunk = index // ep_size
        expert = (index % ep_size) * (own_experts * tp_size) + chunk * tp_size + mine
        column = jnp.sum(jnp.where(lane == expert, total_ref[...], 0.0), axis=1, keepdims=True).astype(jnp.int32)
        low, high, other = column[:slots], column[slots:2 * slots], column[2 * slots:]
        at = span(index, slots)
        source_ref[at, :] = jnp.where(high > 0, 256 * (high - 1) + low, -1)
        other_ref[at, :] = other
        return carry

    for step in steps:
        along(step).wait()
        across(step).start()
    lax.fori_loop(0, own_experts * ep_size, take, 0)
    for step in range(ep_size // cores):
        across(step).wait()
    load_x.wait()

    hops = tp_size - 1

    def behind(way, distance):
        return away('tp', tp_size, (tp_size - distance) % tp_size if way == 0 else distance % tp_size)

    def ring(way, hop, index, chunk):
        piece = all_buf.at[chunk, way, index]
        return pltpu.make_async_remote_copy(
            src_ref=piece, dst_ref=piece, send_sem=ring_send.at[way, hop, index], recv_sem=ring_recv.at[way, hop, index],
            device_id={'tp': away('tp', tp_size, 1 + way * (tp_size - 2))}, device_id_type=MESH)

    def norm(value, index):
        return norm_rows(value, gain_ref[pl.ds(index, 1), :], shift_ref[pl.ds(index, 1), :]).astype(BF16)

    pair = 2 * head_dim
    lane_head = lax.broadcasted_iota(jnp.int32, (1, pair), 1) // head_dim
    factor = (head_dim ** -0.5) * LOG2E
    blocks = seq // size

    def attention(layer, pack_ref):
        def pack_rows(start, number):
            return pack_ref[pl.ds(start, number)].reshape(number * width, width)

        bias_buf[...] = jnp.zeros_like(bias_buf)
        for ref, start in ((b_query_ref, 0), (b_value_ref, 2 * width)):
            parts = [ref[part, head, pl.ds(layer, 1), :] for part in range(tp_size) for head in range(ref.shape[1])]
            bias_buf[:, pl.ds(start, width)] = jnp.concatenate(parts, axis=1)
        def one_row(row, carry):
            key_ok = lax.broadcasted_iota(jnp.int32, (1, seq), 1) < lens_ref[mine * own_rows + row]

            def project(index, carry):
                rows = span(index, size)
                normed = norm(hidden_ref[row, rows, :].astype(F32), 2 * layer)
                qkv_ref[rows, :] = (dot_t(normed, pack_rows(0, 3)) + bias_buf[...]).astype(BF16)
                return carry

            lax.fori_loop(0, blocks, project, 0)

            def attend(block, carry):
                rows = span(block, size)

                def heads(index, carry):
                    lanes = pl.multiple_of(index * pair, pair)
                    query = qkv_ref[rows, pl.ds(lanes, pair)]
                    keys = qkv_ref[:, pl.ds(pl.multiple_of(lanes + width, pair), pair)]
                    values = qkv_ref[:, pl.ds(pl.multiple_of(lanes + 2 * width, pair), pair)]
                    result = None
                    for head in range(2):
                        scores = dot_t(jnp.where(lane_head == head, query, jnp.zeros_like(query)), keys)
                        scores = jnp.where(key_ok, scores, -1e30)
                        top = jnp.max(scores, axis=-1, keepdims=True)
                        weights = jnp.exp2((scores - top) * factor)
                        scale = 1.0 / jnp.sum(weights, axis=-1, keepdims=True)
                        part = jnp.dot((weights * scale).astype(BF16), values, preferred_element_type=F32)
                        result = part if result is None else jnp.where(lane_head == head, part, result)
                    context_ref[:, pl.ds(lanes, pair)] = result.astype(BF16)
                    return carry

                lax.fori_loop(0, width // pair, heads, 0)
                projected = jnp.dot(context_ref[...], pack_rows(3, 1), preferred_element_type=F32)
                hidden = (hidden_ref[row, rows, :].astype(F32) + projected + b_out_ref[pl.ds(layer, 1), :]).astype(BF16)
                hidden_ref[row, rows, :] = hidden
                if layer:
                    all_buf[mine, row, block] = norm(hidden.astype(F32), 2 * layer + 1)
                    ring(row, 0, block, mine).start()
                return carry

            lax.fori_loop(0, blocks, attend, 0)
            return carry

        lax.fori_loop(0, own_rows, one_row, 0)

    attention(0, first_ref)

    for copies in spreads[:2]:
        for copy in copies:
            copy.wait()

    def as_row(ref):
        return jnp.concatenate([ref[pl.ds(part, 1), :] for part in range(ref.shape[0])], axis=1)

    def dense(index, carry):
        row, rows = index // blocks, span(index % blocks, size)
        value = hidden_ref[row, rows, :].astype(F32)
        normed = norm(value, 1)
        total = value + as_row(b_fc2_ref)
        for part in range(tp_size):
            cols = fc1_ref[part].reshape(-1, width)
            inner = jnp.maximum(dot_t(normed, cols) + as_row(b_fc1_ref.at[part]), 0.0).astype(BF16)
            total += jnp.dot(inner, fc2_ref[part].reshape(-1, width), preferred_element_type=F32)
        hidden_ref[row, rows, :] = total.astype(BF16)
        return carry

    lax.fori_loop(0, own_rows * blocks, dense, 0)
    for copy in spreads[2]:
        copy.wait()
    attention(1, second_ref)

    token = lax.broadcasted_iota(jnp.int32, (1, size), 1)
    slot_count, _ = o_ref.shape
    some = min(512, slot_count)

    def dispatch(index, chunks, fresh):
        def part(part, carry):
            at = span(part, some)
            total = None if fresh else o_ref[at, :].astype(F32)
            for way in range(ways):
                base = chunks[way] * own_tokens + (way * count + index) * size
                hot = jnp.where(source_ref[at, :] == token + base, 1.0, 0.0).astype(BF16)
                taken = jnp.dot(hot, all_buf[chunks[way], way, index], preferred_element_type=F32)
                total = taken if total is None else total + taken
            o_ref[at, :] = total.astype(BF16)
            return carry

        lax.fori_loop(0, slot_count // some, part, 0)

    dispatch(0, (mine, mine), True)

    def own(index, carry):
        dispatch(index, (mine, mine), False)
        return carry

    lax.fori_loop(1, count, own, 0)
    for hop in range(1, tp_size):
        def arrive(index, carry):
            chunks = [behind(way, hop) for way in range(ways)]
            for way in range(ways):
                ring(way, hop - 1, index, chunks[way]).wait_recv()
                if hop < hops:
                    ring(way, hop, index, chunks[way]).start()
            dispatch(index, chunks, False)
            return carry

        lax.fori_loop(0, count, arrive, 0)

    def drain(index, carry):
        for way in range(ways):
            for hop in range(hops):
                ring(way, hop, index, mine).wait_send()
        return carry

    lax.fori_loop(0, count, drain, 0)
    for copy in moves:
        copy.wait()


def front(lens, index, gain, shift, b_out, b_fc2, x, w_in, w_out, own, biases, num_experts, capacity, head_dim, tp_size, ep_size, pieces, call_id):
    own_experts = w_in.shape[0] // tp_size
    blocks = own_experts * ep_size
    packs, cut, width = own.shape
    rows, seq, _ = x.shape
    own_rows = rows // tp_size
    size = min(256, seq)
    count = seq // size
    slots = blocks * capacity
    per = ep_size // packs

    def vmem(*shape, dtype=BF16):
        return pltpu.VMEM(shape, dtype)

    moved = landings(tp_size, w_in, pieces)
    b_exp = jax.ShapeDtypeStruct((tp_size,) + biases[3].shape, F32)
    pack = vmem(packs, tp_size, per, cut, width)
    piece_dma, gather_dma, ring_dma = DMA((len(pieces), tp_size - 1)), DMA((packs + len(biases), tp_size)), DMA((own_rows, tp_size - 1, count))
    return pl.pallas_call(
        functools.partial(front_body, tp_size, ep_size, pieces, own_experts, head_dim),
        out_shape=(jax.ShapeDtypeStruct((2 * rows * seq // 128, 128), jnp.int32), jax.ShapeDtypeStruct((slots, 1), jnp.int32), jax.ShapeDtypeStruct((own_rows, seq, width), BF16),
                   jax.ShapeDtypeStruct((slots, width), BF16), b_exp, *moved),
        in_specs=[SMEM_SPEC] + [VMEM_SPEC] * 5 + [HBM_SPEC] * (4 + len(biases)), out_specs=[VMEM_SPEC] * 4 + [HBM_SPEC] * (1 + len(pieces)),
        scratch_shapes=[vmem(tp_size, *biases[0].shape, dtype=F32), vmem(tp_size, *biases[1].shape, dtype=F32), vmem(tp_size, *biases[2].shape, dtype=F32), pack, pack,
                        vmem(packs - 1, tp_size, cut, width), vmem(tp_size, ep_size, cut, width), vmem(tp_size, ep_size, cut, width), vmem(slots, 1, dtype=jnp.int32),
                        vmem(3 * capacity, num_experts, dtype=F32), vmem(1, 3 * width, dtype=F32), vmem(seq, 3 * width), vmem(size, width),
                        vmem(tp_size, own_rows, count, size, width), DMA, piece_dma, piece_dma, gather_dma, gather_dma] + [DMA((ep_size,))] * 4
                       + [DMA((2, packs - 1, ep_size)), ring_dma, ring_dma],
        compiler_params=settings(call_id, 62), cost_estimate=cost(100), name='front')(lens, index, gain, shift, b_out, b_fc2, x, w_in, w_out, own, *biases)


def experts_body(tp_size, ep_size, early, late, dispatch_ref, early_refs, w_in_ref, w_out_ref, b_in_ref, b_out_ref, w_router_ref, other_ref, returned_ref, gates_ref,
                 sent_buf, arrived_ref, parts_buf, own_buf, out_buf, local_sem, send_sem, recv_sem, back_send, back_recv, move_send, move_recv):
    chunks, _, slots, width = arrived_ref.shape
    me = lax.axis_index('ep')
    mine = lax.axis_index('tp')
    weights = (w_in_ref, w_out_ref)
    units = [(chunk, which) for chunk in range(chunks) for which in range(2)]

    sends = {}
    for chunk in range(chunks):
        for distance in range(1, ep_size):
            peer = away('ep', ep_size, distance)
            sends[chunk, distance] = pltpu.make_async_remote_copy(
                src_ref=dispatch_ref.at[chunk, peer], dst_ref=arrived_ref.at[chunk, me], send_sem=send_sem.at[chunk, distance], recv_sem=recv_sem.at[chunk, distance],
                device_id={'ep': peer}, device_id_type=MESH)

    def landing(piece):
        chunk, which, start, cols = piece
        return parts_buf.at[units.index((chunk, which)), :, :, pl.ds(start, cols)]

    moves = {piece: exchange(tp_size, weights, piece, landing(piece), move_send.at[index], move_recv.at[index]) for index, piece in enumerate(late)}
    kept = [pltpu.make_async_copy(dispatch_ref.at[chunk, me], arrived_ref.at[chunk, me], local_sem.at[0, chunk]) for chunk in range(chunks)]
    owns = {unit: pltpu.make_async_copy(weights[unit[1]].at[unit[0] * tp_size + mine], own_buf.at[unit[0], unit[1]], local_sem.at[1 + unit[1], unit[0]]) for unit in units}
    earlies = {piece: pltpu.make_async_copy(early_refs[index], landing(piece), local_sem.at[3, index]) for index, piece in enumerate(early)}

    enter([('tp', tp_size), ('ep', ep_size)])
    for piece in late:
        for copy in moves[piece]:
            copy.start()
    for chunk in range(chunks):
        for distance in range(1, ep_size):
            sends[chunk, distance].start()
        kept[chunk].start()
    for unit in units:
        owns[unit].start()
        for piece in early:
            if piece[:2] == unit:
                earlies[piece].start()

    lane = lax.broadcasted_iota(jnp.int32, (1, w_router_ref.shape[1]), 1)
    group = lax.broadcasted_iota(jnp.int32, (ep_size * slots, 1), 0) // slots

    def load(chunk):
        return pltpu.make_async_copy(dispatch_ref.at[chunk], sent_buf.at[chunk % 2], local_sem.at[5, chunk % 2])

    load(0).start()
    for chunk in range(chunks):
        if chunk + 1 < chunks:
            load(chunk + 1).start()
        load(chunk).wait()
        logits = jnp.dot(sent_buf[chunk % 2].reshape(ep_size * slots, width), w_router_ref[...].astype(BF16), preferred_element_type=F32)
        rows = pl.ds(chunk * ep_size * slots, ep_size * slots)
        own = jnp.sum(jnp.where(lane == group * (chunks * tp_size) + (chunk * tp_size + mine), logits, 0.0), axis=1, keepdims=True)
        other = jnp.sum(jnp.where(lane == other_ref[rows, :], logits, 0.0), axis=1, keepdims=True)
        gates_ref[rows, :] = jax.nn.sigmoid(own - other)

    def part_ref(unit, part):
        if part == 0:
            return own_buf.at[unit[0], unit[1]]
        return parts_buf.at[units.index(unit), part - 1]

    def give_back(chunk, slot, index, cols):
        for half in range(2):
            peer = 2 * index + half
            distance = lax.rem(peer - me + ep_size, ep_size)

            @pl.when(distance == 0)
            def _():
                pltpu.make_async_copy(out_buf.at[slot, peer, :, cols], returned_ref.at[chunk, me, :, cols], local_sem.at[4, chunk]).start()

            @pl.when(distance != 0)
            def _():
                pltpu.make_async_remote_copy(
                    src_ref=out_buf.at[slot, peer, :, cols], dst_ref=returned_ref.at[chunk, me, :, cols], send_sem=back_send.at[chunk, distance], recv_sem=back_recv.at[chunk, distance],
                    device_id={'ep': peer}, device_id_type=MESH).start()

    def weights_here(chunk, which, cols=None):
        unit = (chunk, which)
        if cols is None or cols.start == 0:
            owns[unit].wait()
            for piece in early:
                if piece[:2] == unit:
                    earlies[piece].wait()
        for piece in late:
            if piece[:2] == unit and (cols is None or piece[2] == cols.start):
                for copy in moves[piece]:
                    copy.wait_recv()

    def expert_row(chunk):
        return pl.ds(chunk * tp_size + mine, 1)

    def inner_part(chunk, index, part):
        tokens = arrived_ref[chunk, pl.ds(2 * index, 2)].reshape(2 * slots, width)
        inner = jnp.dot(tokens, part_ref((chunk, 0), part)[...], preferred_element_type=F32) + b_in_ref[away('tp', tp_size, tp_size - part), expert_row(chunk), :]
        return jnp.maximum(inner, 0.0).astype(BF16)

    backs = {}
    for chunk in range(chunks):
        last = chunk == chunks - 1
        slot = chunk % out_buf.shape[0]
        for distance in range(1, ep_size):
            sends[chunk, distance].wait_recv()
        kept[chunk].wait()
        weights_here(chunk, 0)
        before = chunk - out_buf.shape[0]
        if before >= 0:
            for copy in backs[before][:-1]:
                copy.wait_send()
            backs[before][-1].wait()

        held = [sent_buf.at[0], sent_buf.at[1], arrived_ref.at[0], arrived_ref.at[1]]
        if last:
            def first_product(index, carry):
                for part in range(tp_size):
                    held[part][pl.ds(2 * index, 2)] = inner_part(chunk, index, part).reshape(2, slots, width)
                return carry

            lax.fori_loop(0, ep_size // 2, first_product, 0)
        for cols in ([pl.ds(piece[2], piece[3]) for piece in late if piece[:2] == (chunk, 1)] if last else [pl.ds(0, width)]):
            weights_here(chunk, 1, cols if last else None)

            def rows(index, carry):
                total = jnp.zeros((2 * slots, cols.size), F32)
                for part in range(tp_size):
                    inner = held[part][pl.ds(2 * index, 2)].reshape(2 * slots, width) if last else inner_part(chunk, index, part)
                    total += jnp.dot(inner, part_ref((chunk, 1), part)[:, cols], preferred_element_type=F32)
                out_buf[slot, pl.ds(2 * index, 2), :, cols] = (total + b_out_ref[expert_row(chunk), cols]).astype(BF16).reshape(2, slots, cols.size)

                @pl.when(index > 0)
                def _():
                    give_back(chunk, slot, index - 1, cols)

                return carry

            lax.fori_loop(0, ep_size // 2, rows, 0)
            give_back(chunk, slot, ep_size // 2 - 1, cols)
        backs[chunk] = []
        for distance in range(1, ep_size):
            peer = away('ep', ep_size, distance)
            backs[chunk].append(pltpu.make_async_remote_copy(
                src_ref=out_buf.at[slot, peer], dst_ref=returned_ref.at[chunk, me], send_sem=back_send.at[chunk, distance], recv_sem=back_recv.at[chunk, distance],
                device_id={'ep': peer}, device_id_type=MESH))
        backs[chunk].append(pltpu.make_async_copy(out_buf.at[slot, me], returned_ref.at[chunk, me], local_sem.at[4, chunk]))

    for chunk in range(chunks):
        for distance in range(1, ep_size):
            sends[chunk, distance].wait_send()
        for copy in backs[chunk][:-1]:
            copy.wait_recv()
            if chunk + out_buf.shape[0] >= chunks:
                copy.wait_send()
        if chunk + out_buf.shape[0] >= chunks:
            backs[chunk][-1].wait()
    for piece in late:
        for copy in moves[piece]:
            copy.wait_send()


def experts(dispatch, early_weights, w_in, w_out, b_in, b_out, w_router, other, tp_size, ep_size, early, late, call_id):
    chunks, _, slots, width = dispatch.shape
    hidden = w_in.shape[2]

    def body(dispatch_ref, *refs):
        experts_body(tp_size, ep_size, early, late, dispatch_ref, refs[:len(early)], *refs[len(early):])

    return pl.pallas_call(
        body, out_shape=(jax.ShapeDtypeStruct(dispatch.shape, BF16), jax.ShapeDtypeStruct(other.shape, F32)),
        in_specs=[HBM_SPEC] * (3 + len(early)) + [VMEM_SPEC] * 4, out_specs=(HBM_SPEC, VMEM_SPEC),
        scratch_shapes=[pltpu.VMEM((2,) + dispatch.shape[1:], BF16), pltpu.VMEM(dispatch.shape, BF16), pltpu.VMEM((2 * chunks, tp_size - 1, width, hidden), BF16),
                        pltpu.VMEM((chunks, 2, width, hidden), BF16), pltpu.VMEM((2, ep_size, slots, width), BF16),
                        DMA((6, max(chunks, len(early)))), DMA((chunks, ep_size)), DMA((chunks, ep_size)), DMA((chunks, ep_size)), DMA((chunks, ep_size)),
                        DMA((len(late), tp_size - 1)), DMA((len(late), tp_size - 1))],
        compiler_params=settings(call_id, 62),
        cost_estimate=cost(30),
        name='experts')(dispatch, *early_weights, w_in, w_out, b_in, b_out, w_router, other)


def finish_body(tp_size, count, table_ref, gates_ref, outputs_ref, hidden_ref, o_ref, slots_buf, wide_ref, stage_ref, first_buf, hidden_buf, sum_buf, own_buf,
                load_sem, slots_sem, sum_send, sum_recv, out_send, out_recv):
    me = lax.axis_index('tp')
    own_tokens, width = hidden_ref.shape
    tokens = tp_size * own_tokens
    size = own_tokens // (2 * count)
    hops = tp_size - 1
    lanes = 128
    columns = [slice(start, start + lanes) for start in range(0, width, lanes)]

    def rows(way, chunk, index):
        return pl.ds(pl.multiple_of(chunk * own_tokens + (way * count + index) * size, size), size)

    def behind(way, distance):
        return away('tp', tp_size, (tp_size - distance) % tp_size if way == 0 else distance % tp_size)

    def ahead(way):
        return {'tp': away('tp', tp_size, 1 if way == 0 else tp_size - 1)}

    def send_sum(way, hop, index, src_ref):
        return pltpu.make_async_remote_copy(
            src_ref=src_ref, dst_ref=sum_buf.at[way, hop, index], send_sem=sum_send.at[way, hop, index], recv_sem=sum_recv.at[way, hop, index],
            device_id=ahead(way), device_id_type=MESH)

    def send_out(way, hop, index, src_ref, chunk):
        return pltpu.make_async_remote_copy(
            src_ref=src_ref, dst_ref=o_ref.at[rows(way, chunk, index)], send_sem=out_send.at[way, hop, index], recv_sem=out_recv.at[way, hop, index],
            device_id=ahead(way), device_id_type=MESH)

    slots = outputs_ref.shape[0]
    parts = slots_sem.shape[0]
    part_slots = slots // parts
    piece = min(128, part_slots)
    loads = [pltpu.make_async_copy(outputs_ref.at[span(part, part_slots)], slots_buf.at[span(part, part_slots)], slots_sem.at[part]) for part in range(parts)]
    load_hidden = pltpu.make_async_copy(hidden_ref, hidden_buf, load_sem.at[2])
    for load in loads + [load_hidden]:
        load.start()
    enter([('tp', tp_size)])
    wide_ref[slots] = jnp.zeros(wide_ref.shape[1:], F32)

    def widen(index, carry):
        at = span(index, piece)
        for column, cols in enumerate(columns):
            wide_ref[at, column, :] = slots_buf[at, cols].astype(F32) * gates_ref[at, :]
        return carry

    for part, load in enumerate(loads):
        load.wait()
        lax.fori_loop(part * (part_slots // piece), (part + 1) * (part_slots // piece), widen, 0)

    def combine(way, chunk, index):
        base = chunk * own_tokens + (way * count + index) * size
        batch = 16

        def some(part, carry):
            first = part * batch
            for u in range(batch):
                slot_of = [table_ref[choice * tokens + base + first + u] for choice in range(2)]
                stage_ref[way, pl.ds(pl.multiple_of((first + u) * 8, 8), 8), :] = wide_ref[slot_of[0]] + wide_ref[slot_of[1]]
            return carry

        lax.fori_loop(0, size // batch, some, 0)

    def staged(way, column):
        return stage_ref[way, pl.ds(column, size, stride=8), :]

    def first(index, carry):
        for way in range(2):
            combine(way, behind(way, 1), index)
            for column, cols in enumerate(columns):
                first_buf[way, index, :, cols] = staged(way, column).astype(BF16)
        for way in range(2):
            send_sum(way, 0, index, first_buf.at[way, index]).start()
        return carry

    lax.fori_loop(0, count, first, 0)
    load_hidden.wait()

    def keep(way, index):
        return pltpu.make_async_copy(own_buf.at[way, index], o_ref.at[rows(way, me, index)], load_sem.at[way])

    for hop in range(1, tp_size):
        def add(index, carry):
            for way in range(2):
                combine(way, behind(way, hop + 1), index)
            for way in range(2):
                send_sum(way, hop - 1, index, sum_buf.at[way, hop - 1, index]).wait_recv()
                own_rows = pl.ds(pl.multiple_of((way * count + index) * size, size), size)
                for column, cols in enumerate(columns):
                    total = (sum_buf[way, hop - 1, index, :, cols].astype(F32) + staged(way, column)).astype(BF16)
                    if hop < hops:
                        sum_buf[way, hop - 1, index, :, cols] = total
                    else:
                        own_buf[way, index, :, cols] = (total.astype(F32) + hidden_buf[own_rows, cols].astype(F32)).astype(BF16)
            for way in range(2):
                if hop < hops:
                    send_sum(way, hop, index, sum_buf.at[way, hop - 1, index]).start()
                else:
                    send_out(way, 0, index, own_buf.at[way, index], me).start()
                    keep(way, index).start()
                    keep(way, index).wait()
            return carry

        lax.fori_loop(0, count, add, 0)

    for hop in range(1, tp_size):
        def forward(index, carry):
            for way in range(2):
                chunk = behind(way, hop)
                arrived = o_ref.at[rows(way, chunk, index)]
                send_out(way, hop - 1, index, arrived, chunk).wait_recv()
                if hop < hops:
                    send_out(way, hop, index, arrived, chunk).start()
            return carry

        lax.fori_loop(0, count, forward, 0)

    def drain(index, carry):
        for way in range(2):
            for hop in range(hops):
                send_sum(way, hop, index, sum_buf.at[way, hop, index]).wait_send()
                send_out(way, hop, index, own_buf.at[way, index], me).wait_send()
        return carry

    lax.fori_loop(0, count, drain, 0)


def finish(table, gates, outputs, hidden, tp_size, call_id):
    slots, width = outputs.shape
    own_tokens = hidden.shape[0]
    size = min(256, own_tokens // 2)
    count = own_tokens // (2 * size)
    hops = tp_size - 1
    pieces = (2, count, size, width)
    ring = DMA((2, hops, count))

    def vmem(*shape, dtype=BF16):
        return pltpu.VMEM(shape, dtype)

    return pl.pallas_call(
        functools.partial(finish_body, tp_size, count), out_shape=jax.ShapeDtypeStruct((tp_size * own_tokens, width), BF16),
        in_specs=[SMEM_SPEC, VMEM_SPEC, HBM_SPEC, HBM_SPEC], out_specs=HBM_SPEC,
        scratch_shapes=[vmem(slots, width), vmem(slots + 1, 8, 128, dtype=F32), vmem(2, size * 8, 128, dtype=F32), vmem(*pieces), vmem(own_tokens, width),
                        vmem(2, hops, *pieces[1:]), vmem(*pieces), DMA((3,)), DMA((4,)), ring, ring, ring, ring],
        compiler_params=settings(call_id), cost_estimate=cost(100), name='finish')(table, gates, outputs, hidden)


def solution(mesh):
    tp_size = mesh.shape['tp']
    ep_size = mesh.shape['ep']

    def local_fn(x, src_len, expert_idx, ln_gain, ln_bias, w_query, b_query, w_key, w_value, b_value, w_attn_out, b_attn_out, w_fc1, b_fc1, w_fc2, b_fc2, w_router, w_exp_in, b_exp_in, w_exp_out, b_exp_out):
        rows, seq, width = x.shape
        tokens = rows * seq
        num_experts = w_router.shape[1]
        capacity = 2 * (-(-tokens // num_experts))
        local_experts = w_exp_in.shape[0]
        own_experts = local_experts // tp_size
        _, _, local_heads, head_dim = w_query.shape
        head_cols = local_heads * head_dim

        def pack_attention(j):
            columns = [w[j].reshape(width, head_cols).T for w in (w_query, w_key, w_value)]
            return jnp.concatenate(columns + [w_attn_out[j].reshape(head_cols, width)], axis=0)

        def own_slice(value):
            size = value.shape[0] // ep_size
            return lax.dynamic_slice_in_dim(value, lax.axis_index('ep') * size, size, 0)

        own = jnp.stack([own_slice(value) for value in (pack_attention(0), w_fc1.T, w_fc2, pack_attention(1))])

        def piece(code):
            chunk, which, *part = map(int, code)
            size = width // 3 if part else width
            return chunk, which, sum(part) * size, size

        plan = ['00', '01', '10', '11', '20', '210'], ['211', '212', '30', '310', '311', '312']
        early, late = [[piece(code) for code in codes] for codes in plan]
        weights = w_exp_in, w_exp_out
        biases = b_query.transpose(1, 0, 2), b_value.transpose(1, 0, 2), b_fc1.reshape(-1, 128), b_exp_in
        table, other, hidden, dispatch, b_exp_in, *moved = front(
            src_len, expert_idx.transpose(0, 2, 1), ln_gain, ln_bias, b_attn_out, b_fc2.reshape(-1, 128), x, *weights, own, biases, num_experts, capacity, head_dim, tp_size, ep_size, early, 0)
        dispatch = dispatch.reshape(own_experts, ep_size, capacity, width)
        outputs, gates = experts(dispatch, moved, *weights, b_exp_in, b_exp_out, w_router, other, tp_size, ep_size, early, late, 1)
        return finish(table.reshape(-1), gates, outputs.reshape(-1, width), hidden.reshape(-1, width), tp_size, 2).reshape(rows, seq, width)

    axes = {'g': ('dp', 'ep'), 'e': 'ep', 't': 'tp', '.': None}

    def spec(code):
        return P(*[axes[letter] for letter in code])

    codes = ['g..', 'g', 'g..', '..', '..', '..t.', '.t.', '..t.', '..t.', '.t.', '.t..', '..', '.t', 't', 't.', '.', '..', 'e.t', 'et', 'et.', 'e.']
    in_specs = tuple(map(spec, codes))
    return jax.shard_map(local_fn, mesh=mesh, in_specs=in_specs, out_specs=spec('g..'), check_vma=False)
```

```python
import functools

import jax
import jax.numpy as jnp
from jax import lax
from jax.experimental import pallas as pl
from jax.experimental.pallas import tpu as pltpu
from jax.sharding import PartitionSpec as P

LN_EPS = 1e-5
BF16 = jnp.bfloat16
F32 = jnp.float32
LOG2E = 1.4426950408889634


MESH = pl.DeviceIdType.MESH
VMEM_SPEC = pl.BlockSpec(memory_space=pltpu.VMEM)
HBM_SPEC = pl.BlockSpec(memory_space=pltpu.HBM)
SMEM_SPEC = pl.BlockSpec(memory_space=pltpu.SMEM)
DMA = pltpu.SemaphoreType.DMA


def span(index, size):
    return pl.ds(pl.multiple_of(index * size, size), size)


def settings(call_id=None, mib=56, grid=None):
    return pltpu.CompilerParams(dimension_semantics=grid, collective_id=call_id, has_side_effects=call_id is not None, vmem_limit_bytes=mib << 20)


def cost(gflops):
    return pl.CostEstimate(flops=gflops * 10**9, transcendentals=0, bytes_accessed=10**7)


def dot_t(lhs, rhs_t):
    return lax.dot_general(lhs, rhs_t, (((1,), (1,)), ((), ())), preferred_element_type=F32)


def norm_rows(value, gain, shift):
    centered = value - jnp.mean(value, axis=-1, keepdims=True)
    variance = jnp.mean(centered * centered, axis=-1, keepdims=True)
    return centered * lax.rsqrt(variance + LN_EPS) * gain + shift


def away(axis, size, distance):
    return lax.rem(lax.axis_index(axis) + distance, size)


def enter(groups):
    barrier = pltpu.get_barrier_semaphore()
    count = 0
    for axis, size in groups:
        for distance in range(1, size):
            pl.semaphore_signal(barrier, device_id={axis: away(axis, size, distance)}, device_id_type=MESH)
            count += 1
    pl.semaphore_wait(barrier, count)


def exchange(tp_size, weights, piece, landing_ref, send_sem, recv_sem):
    chunk, which, start, cols = piece
    return [pltpu.make_async_remote_copy(
        src_ref=weights[which].at[chunk * tp_size + away('tp', tp_size, distance), :, pl.ds(start, cols)], dst_ref=landing_ref.at[distance - 1],
        send_sem=send_sem.at[distance - 1], recv_sem=recv_sem.at[distance - 1],
        device_id={'tp': away('tp', tp_size, distance)}, device_id_type=MESH)
        for distance in sorted(range(1, tp_size), key=lambda d: (min(d, tp_size - d), d))]


def exchange_all(tp_size, weights, pieces, landing_refs, send_sem, recv_sem):
    copies = []
    for index, piece in enumerate(pieces):
        copies += exchange(tp_size, weights, piece, landing_refs[index], send_sem.at[index], recv_sem.at[index])
    return copies


def landings(tp_size, weight, pieces):
    return [jax.ShapeDtypeStruct((tp_size - 1, weight.shape[1], cols), BF16) for _, _, _, cols in pieces]


def route_tables(own_experts, tp_size, ep_size, lens_ref, index_ref, table_ref, total_ref):
    rows, _, seq = index_ref.shape
    step = min(512, seq)
    per_row = seq // step
    wide, experts_count = total_ref.shape
    slots = wide // 3
    lanes = table_ref.shape[1]
    mine = lax.axis_index('tp')
    ids = lax.broadcasted_iota(jnp.int32, (experts_count, 1), 0)
    slot_ids = lax.broadcasted_iota(jnp.int32, (slots, 1), 0)
    before = (lax.broadcasted_iota(jnp.int32, (step, step), 0) < lax.broadcasted_iota(jnp.int32, (step, step), 1)).astype(BF16)
    total_ref[...] = jnp.zeros_like(total_ref)
    count = jnp.zeros((experts_count, 1), F32)
    for choice in range(2):
        def block(index, count):
            row = index // per_row
            start = pl.multiple_of((index % per_row) * step, step)
            cols = pl.ds(start, step)
            position = lax.broadcasted_iota(jnp.int32, (1, step), 1) + start
            chosen = jnp.where(position < lens_ref[row], index_ref[row, pl.ds(choice, 1), cols], -1)
            other = index_ref[row, pl.ds(1 - choice, 1), cols]
            token = position + row * seq
            hot = jnp.where(ids == chosen, 1.0, 0.0)
            rank = jnp.dot(hot.astype(BF16), before, preferred_element_type=F32) + count
            slot = jnp.sum(rank * hot, axis=0, keepdims=True).astype(jnp.int32)
            at_slot = slot_ids == slot
            parts = [jnp.where(at_slot, value.astype(F32), 0.0).astype(BF16) for value in (token & 255, (token >> 8) + 1, other)]
            values = jnp.concatenate(parts, axis=0)
            hot16 = hot.astype(BF16)
            total_ref[...] += dot_t(values, hot16)
            local = own_experts * tp_size
            own = (lax.rem(chosen, tp_size) == mine) & (slot < slots)
            line = (lax.div(lax.rem(chosen, local), tp_size) * ep_size + lax.div(chosen, local)) * slots + slot
            line = jnp.where(own, line, own_experts * ep_size * slots)
            for part in range(step // lanes):
                at = (choice * rows * per_row + index) * (step // lanes) + part
                table_ref[pl.ds(at, 1), :] = line[:, part * lanes:(part + 1) * lanes]
            return count + jnp.sum(hot, axis=1, keepdims=True)

        count = lax.fori_loop(0, rows * per_row, block, count)


def spread(ep_size, src_ref, view, sems):
    me = lax.axis_index('ep')
    send_sem, recv_sem = sems
    copies = [pltpu.make_async_remote_copy(
        src_ref=src_ref, dst_ref=view(me), send_sem=send_sem.at[distance], recv_sem=recv_sem.at[distance],
        device_id={'ep': away('ep', ep_size, distance)}, device_id_type=MESH) for distance in range(1, ep_size)]
    return copies + [pltpu.make_async_copy(src_ref, view(me), send_sem.at[0])]


def by_kind(ref, ep_size):
    per = ep_size // ref.shape[0]
    return lambda index: ref.at[index // per, :, lax.rem(index, per)]


def front_body(tp_size, ep_size, pieces, own_experts, head_dim, lens_ref, index_ref, gain_ref, shift_ref, b_out_ref, b_fc2_ref, x_ref, w_in_ref, w_out_ref, own_ref, *refs):
    biases, refs = refs[:4], refs[4:]
    table_ref, o_ref, other_out, hidden_out, b_exp_ref, *refs = refs
    moved_refs, refs = refs[:len(pieces)], refs[len(pieces):]
    (other_ref, hidden_ref, b_query_ref, b_value_ref, b_fc1_ref, first_ref, second_ref, later_ref, fc1_ref, fc2_ref, source_ref, total_ref, bias_buf, qkv_ref, context_ref, all_buf,
     load_sem, move_send, move_recv, tp_send, tp_recv, row_send, row_recv, pair_send, pair_recv, spread_sem, ring_send, ring_recv) = refs
    mine = lax.axis_index('tp')
    me = lax.axis_index('ep')
    own_rows, seq, width = hidden_ref.shape
    _, ways, count, size, _ = all_buf.shape
    own_tokens = own_rows * seq

    view = by_kind(first_ref, ep_size)
    moves = exchange_all(tp_size, (w_in_ref, w_out_ref), pieces, moved_refs, move_send, move_recv)
    pairs = [(own_ref.at[0], view(me).at[mine])]
    pairs += [(bias, whole.at[mine]) for bias, whole in zip(biases, (b_query_ref, b_value_ref, b_fc1_ref, b_exp_ref))]
    pairs += [(own_ref.at[1 + index], later_ref.at[index, mine]) for index in range(later_ref.shape[0])]
    near = (1, tp_size - 1)
    gathers = []
    for index, (src, dst) in enumerate(pairs):
        far = range(2, tp_size - 1) if 0 < index <= len(biases) else ()
        gathers.append([pltpu.make_async_copy(src, dst, tp_send.at[index, 0])] + [pltpu.make_async_remote_copy(
            src_ref=src, dst_ref=dst, send_sem=tp_send.at[index, distance], recv_sem=tp_recv.at[index, distance],
            device_id={'tp': away('tp', tp_size, distance)}, device_id_type=MESH) for distance in (*near, *far)])

    def relay(index, where):
        half = own_ref.shape[1] // 2
        copies = []
        for way, distance in enumerate(near):
            piece = where(away('tp', tp_size, tp_size - distance)).at[pl.ds(way * half, half)]
            copies.append(pltpu.make_async_remote_copy(
                src_ref=piece, dst_ref=piece, send_sem=tp_send.at[index, 2 + 2 * way], recv_sem=tp_recv.at[index, 2 + 2 * way],
                device_id={'tp': away('tp', tp_size, distance)}, device_id_type=MESH))
        return copies

    load_x = pltpu.make_async_copy(x_ref.at[pl.ds(mine * own_rows, own_rows)], hidden_ref, load_sem.at[0])
    keep_other = pltpu.make_async_copy(other_ref, other_out, load_sem.at[1])
    keep_hidden = pltpu.make_async_copy(hidden_ref, hidden_out, load_sem.at[2])
    load_x.start()
    enter([('tp', tp_size), ('ep', ep_size)])
    for copies in gathers:
        for copy in copies:
            copy.start()
    one = tp_size - 1
    for copy in moves[-one:]:
        copy.start()

    cores = 2
    steps = range(1, ep_size // cores)
    other_core = me + 1 - cores * lax.rem(me, cores)

    def along(step):
        return pltpu.make_async_remote_copy(
            src_ref=view(me), dst_ref=view(me), send_sem=row_send.at[step], recv_sem=row_recv.at[step],
            device_id={'ep': away('ep', ep_size, cores * step)}, device_id_type=MESH)

    def across(step):
        part = view(away('ep', ep_size, ep_size - cores * step))
        return pltpu.make_async_remote_copy(
            src_ref=part, dst_ref=part, send_sem=pair_send.at[step], recv_sem=pair_recv.at[step],
            device_id={'ep': other_core}, device_id_type=MESH)

    for copy in gathers[0]:
        copy.wait()
    first_relay = relay(0, lambda part: view(me).at[part])
    for copy in first_relay:
        copy.start()
    for copies in gathers[1:]:
        for copy in copies:
            copy.wait()
    later_relays = [relay(1 + len(biases) + index, lambda part, index=index: later_ref.at[index, part]) for index in range(later_ref.shape[0])]
    for copies in later_relays:
        for copy in copies:
            copy.start()
    for copy in moves[:-one]:
        copy.start()
    for copy in first_relay:
        copy.wait()
    for step in steps:
        along(step).start()
    across(0).start()
    for copies in later_relays:
        for copy in copies:
            copy.wait()
    views = [lambda part: fc1_ref.at[:, part], lambda part: fc2_ref.at[:, part], by_kind(second_ref, ep_size)]
    spreads = [spread(ep_size, later_ref.at[index], where, (spread_sem.at[0, index], spread_sem.at[1, index])) for index, where in enumerate(views)]
    for copies in spreads:
        for copy in copies:
            copy.start()

    route_tables(own_experts, tp_size, ep_size, lens_ref, index_ref, table_ref, total_ref)
    wide, experts_count = total_ref.shape
    slots = wide // 3
    lane = lax.broadcasted_iota(jnp.int32, (1, experts_count), 1)

    def take(index, carry):
        chunk = index // ep_size
        expert = (index % ep_size) * (own_experts * tp_size) + chunk * tp_size + mine
        column = jnp.sum(jnp.where(lane == expert, total_ref[...], 0.0), axis=1, keepdims=True).astype(jnp.int32)
        low, high, other = column[:slots], column[slots:2 * slots], column[2 * slots:]
        at = span(index, slots)
        source_ref[at, :] = jnp.where(high > 0, 256 * (high - 1) + low, -1)
        other_ref[at, :] = other
        return carry

    for step in steps:
        along(step).wait()
        across(step).start()
    lax.fori_loop(0, own_experts * ep_size, take, 0)
    for step in range(ep_size // cores):
        across(step).wait()
    load_x.wait()

    hops = tp_size - 1

    def behind(way, distance):
        return away('tp', tp_size, (tp_size - distance) % tp_size if way == 0 else distance % tp_size)

    def ring(way, hop, index, chunk):
        piece = all_buf.at[chunk, way, index]
        return pltpu.make_async_remote_copy(
            src_ref=piece, dst_ref=piece, send_sem=ring_send.at[way, hop, index], recv_sem=ring_recv.at[way, hop, index],
            device_id={'tp': away('tp', tp_size, 1 + way * (tp_size - 2))}, device_id_type=MESH)

    def norm(value, index):
        return norm_rows(value, gain_ref[pl.ds(index, 1), :], shift_ref[pl.ds(index, 1), :]).astype(BF16)

    pair = 2 * head_dim
    lane_head = lax.broadcasted_iota(jnp.int32, (1, pair), 1) // head_dim
    factor = (head_dim ** -0.5) * LOG2E
    blocks = seq // size

    def attention(layer, pack_ref):
        def pack_rows(start, number):
            return pack_ref[pl.ds(start, number)].reshape(number * width, width)

        bias_buf[...] = jnp.zeros_like(bias_buf)
        for ref, start in ((b_query_ref, 0), (b_value_ref, 2 * width)):
            parts = [ref[part, head, pl.ds(layer, 1), :] for part in range(tp_size) for head in range(ref.shape[1])]
            bias_buf[:, pl.ds(start, width)] = jnp.concatenate(parts, axis=1)
        def one_row(row, carry):
            key_ok = lax.broadcasted_iota(jnp.int32, (1, seq), 1) < lens_ref[mine * own_rows + row]

            def project(index, carry):
                rows = span(index, size)
                normed = norm(hidden_ref[row, rows, :].astype(F32), 2 * layer)
                qkv_ref[rows, :] = (dot_t(normed, pack_rows(0, 3)) + bias_buf[...]).astype(BF16)
                return carry

            lax.fori_loop(0, blocks, project, 0)

            def attend(block, carry):
                rows = span(block, size)

                def heads(index, carry):
                    lanes = pl.multiple_of(index * pair, pair)
                    query = qkv_ref[rows, pl.ds(lanes, pair)]
                    keys = qkv_ref[:, pl.ds(pl.multiple_of(lanes + width, pair), pair)]
                    values = qkv_ref[:, pl.ds(pl.multiple_of(lanes + 2 * width, pair), pair)]
                    result = None
                    for head in range(2):
                        scores = dot_t(jnp.where(lane_head == head, query, jnp.zeros_like(query)), keys)
                        scores = jnp.where(key_ok, scores, -1e30)
                        top = jnp.max(scores, axis=-1, keepdims=True)
                        weights = jnp.exp2((scores - top) * factor)
                        scale = 1.0 / jnp.sum(weights, axis=-1, keepdims=True)
                        part = jnp.dot((weights * scale).astype(BF16), values, preferred_element_type=F32)
                        result = part if result is None else jnp.where(lane_head == head, part, result)
                    context_ref[:, pl.ds(lanes, pair)] = result.astype(BF16)
                    return carry

                lax.fori_loop(0, width // pair, heads, 0)
                projected = jnp.dot(context_ref[...], pack_rows(3, 1), preferred_element_type=F32)
                hidden = (hidden_ref[row, rows, :].astype(F32) + projected + b_out_ref[pl.ds(layer, 1), :]).astype(BF16)
                hidden_ref[row, rows, :] = hidden
                if layer:
                    all_buf[mine, row, block] = norm(hidden.astype(F32), 2 * layer + 1)
                    ring(row, 0, block, mine).start()
                return carry

            lax.fori_loop(0, blocks, attend, 0)
            return carry

        lax.fori_loop(0, own_rows, one_row, 0)

    attention(0, first_ref)

    for copies in spreads[:2]:
        for copy in copies:
            copy.wait()

    def as_row(ref):
        return jnp.concatenate([ref[pl.ds(part, 1), :] for part in range(ref.shape[0])], axis=1)

    def dense(index, carry):
        row, rows = index // blocks, span(index % blocks, size)
        value = hidden_ref[row, rows, :].astype(F32)
        normed = norm(value, 1)
        total = value + as_row(b_fc2_ref)
        for part in range(tp_size):
            cols = fc1_ref[part].reshape(-1, width)
            inner = jnp.maximum(dot_t(normed, cols) + as_row(b_fc1_ref.at[part]), 0.0).astype(BF16)
            total += jnp.dot(inner, fc2_ref[part].reshape(-1, width), preferred_element_type=F32)
        hidden_ref[row, rows, :] = total.astype(BF16)
        return carry

    lax.fori_loop(0, own_rows * blocks, dense, 0)
    for copy in spreads[2]:
        copy.wait()
    attention(1, second_ref)
    keep_hidden.start()
    keep_other.start()

    token = lax.broadcasted_iota(jnp.int32, (1, size), 1)
    slot_count, _ = o_ref.shape
    some = min(512, slot_count)

    def dispatch(index, chunks, fresh):
        def part(part, carry):
            at = span(part, some)
            total = None if fresh else o_ref[at, :].astype(F32)
            for way in range(ways):
                base = chunks[way] * own_tokens + (way * count + index) * size
                hot = jnp.where(source_ref[at, :] == token + base, 1.0, 0.0).astype(BF16)
                taken = jnp.dot(hot, all_buf[chunks[way], way, index], preferred_element_type=F32)
                total = taken if total is None else total + taken
            o_ref[at, :] = total.astype(BF16)
            return carry

        lax.fori_loop(0, slot_count // some, part, 0)

    dispatch(0, (mine, mine), True)

    def own(index, carry):
        dispatch(index, (mine, mine), False)
        return carry

    lax.fori_loop(1, count, own, 0)
    for hop in range(1, tp_size):
        def arrive(index, carry):
            chunks = [behind(way, hop) for way in range(ways)]
            for way in range(ways):
                ring(way, hop - 1, index, chunks[way]).wait_recv()
                if hop < hops:
                    ring(way, hop, index, chunks[way]).start()
            dispatch(index, chunks, False)
            return carry

        lax.fori_loop(0, count, arrive, 0)

    def drain(index, carry):
        for way in range(ways):
            for hop in range(hops):
                ring(way, hop, index, mine).wait_send()
        return carry

    lax.fori_loop(0, count, drain, 0)
    for copy in [*moves, keep_hidden, keep_other]:
        copy.wait()


def front(lens, index, gain, shift, b_out, b_fc2, x, w_in, w_out, own, biases, num_experts, capacity, head_dim, tp_size, ep_size, pieces, call_id):
    own_experts = w_in.shape[0] // tp_size
    blocks = own_experts * ep_size
    packs, cut, width = own.shape
    rows, seq, _ = x.shape
    own_rows = rows // tp_size
    size = min(256, seq)
    count = seq // size
    slots = blocks * capacity
    per = ep_size // packs

    def vmem(*shape, dtype=BF16):
        return pltpu.VMEM(shape, dtype)

    moved = landings(tp_size, w_in, pieces)
    b_exp = jax.ShapeDtypeStruct((tp_size,) + biases[3].shape, F32)
    pack = vmem(packs, tp_size, per, cut, width)
    piece_dma, gather_dma, ring_dma = DMA((len(pieces), tp_size - 1)), DMA((packs + len(biases), tp_size + 1)), DMA((own_rows, tp_size - 1, count))
    return pl.pallas_call(
        functools.partial(front_body, tp_size, ep_size, pieces, own_experts, head_dim),
        out_shape=(jax.ShapeDtypeStruct((2 * rows * seq // 128, 128), jnp.int32), jax.ShapeDtypeStruct((slots, width), BF16), jax.ShapeDtypeStruct((slots, 1), jnp.int32),
                   jax.ShapeDtypeStruct((own_rows, seq, width), BF16), b_exp, *moved),
        in_specs=[SMEM_SPEC] + [VMEM_SPEC] * 5 + [HBM_SPEC] * (4 + len(biases)), out_specs=[VMEM_SPEC] * 2 + [HBM_SPEC] * (3 + len(pieces)),
        scratch_shapes=[vmem(slots, 1, dtype=jnp.int32), vmem(own_rows, seq, width), vmem(tp_size, *biases[0].shape, dtype=F32), vmem(tp_size, *biases[1].shape, dtype=F32), vmem(tp_size, *biases[2].shape, dtype=F32), pack, pack,
                        vmem(packs - 1, tp_size, cut, width), vmem(tp_size, ep_size, cut, width), vmem(tp_size, ep_size, cut, width), vmem(slots, 1, dtype=jnp.int32),
                        vmem(3 * capacity, num_experts, dtype=F32), vmem(1, 3 * width, dtype=F32), vmem(seq, 3 * width), vmem(size, width),
                        vmem(tp_size, own_rows, count, size, width), DMA((3,)), piece_dma, piece_dma, gather_dma, gather_dma] + [DMA((ep_size,))] * 4
                       + [DMA((2, packs - 1, ep_size)), ring_dma, ring_dma],
        compiler_params=settings(call_id, 62), cost_estimate=cost(100), name='front')(lens, index, gain, shift, b_out, b_fc2, x, w_in, w_out, own, *biases)


def experts_body(tp_size, ep_size, early, late, dispatch_ref, early_refs, w_in_ref, w_out_ref, b_in_ref, b_out_ref, w_router_ref, other_ref, returned_ref, gates_ref,
                 sent_buf, arrived_ref, parts_buf, own_buf, out_buf, local_sem, send_sem, recv_sem, back_send, back_recv, move_send, move_recv):
    chunks, _, slots, width = arrived_ref.shape
    me = lax.axis_index('ep')
    mine = lax.axis_index('tp')
    weights = (w_in_ref, w_out_ref)
    units = [(chunk, which) for chunk in range(chunks) for which in range(2)]

    sends = {}
    for chunk in range(chunks):
        for distance in range(1, ep_size):
            peer = away('ep', ep_size, distance)
            sends[chunk, distance] = pltpu.make_async_remote_copy(
                src_ref=dispatch_ref.at[chunk, peer], dst_ref=arrived_ref.at[chunk, me], send_sem=send_sem.at[chunk, distance], recv_sem=recv_sem.at[chunk, distance],
                device_id={'ep': peer}, device_id_type=MESH)

    def landing(piece):
        chunk, which, start, cols = piece
        return parts_buf.at[units.index((chunk, which)), :, :, pl.ds(start, cols)]

    moves = {piece: exchange(tp_size, weights, piece, landing(piece), move_send.at[index], move_recv.at[index]) for index, piece in enumerate(late)}
    kept = [pltpu.make_async_copy(dispatch_ref.at[chunk, me], arrived_ref.at[chunk, me], local_sem.at[0, chunk]) for chunk in range(chunks)]
    owns = {unit: pltpu.make_async_copy(weights[unit[1]].at[unit[0] * tp_size + mine], own_buf.at[unit[0], unit[1]], local_sem.at[1 + unit[1], unit[0]]) for unit in units}
    earlies = {piece: pltpu.make_async_copy(early_refs[index], landing(piece), local_sem.at[3, index]) for index, piece in enumerate(early)}

    enter([('tp', tp_size), ('ep', ep_size)])
    for piece in late:
        for copy in moves[piece]:
            copy.start()
    for chunk in range(chunks):
        for distance in range(1, ep_size):
            sends[chunk, distance].start()
        kept[chunk].start()
    for unit in units:
        owns[unit].start()
        for piece in early:
            if piece[:2] == unit:
                earlies[piece].start()

    lane = lax.broadcasted_iota(jnp.int32, (1, w_router_ref.shape[1]), 1)
    group = lax.broadcasted_iota(jnp.int32, (ep_size * slots, 1), 0) // slots

    def load(chunk):
        return pltpu.make_async_copy(dispatch_ref.at[chunk], sent_buf.at[chunk % 2], local_sem.at[5, chunk % 2])

    load(0).start()
    for chunk in range(chunks):
        if chunk + 1 < chunks:
            load(chunk + 1).start()
        load(chunk).wait()
        logits = jnp.dot(sent_buf[chunk % 2].reshape(ep_size * slots, width), w_router_ref[...].astype(BF16), preferred_element_type=F32)
        rows = pl.ds(chunk * ep_size * slots, ep_size * slots)
        own = jnp.sum(jnp.where(lane == group * (chunks * tp_size) + (chunk * tp_size + mine), logits, 0.0), axis=1, keepdims=True)
        other = jnp.sum(jnp.where(lane == other_ref[rows, :], logits, 0.0), axis=1, keepdims=True)
        gates_ref[rows, :] = jax.nn.sigmoid(own - other)

    def part_ref(unit, part):
        if part == 0:
            return own_buf.at[unit[0], unit[1]]
        return parts_buf.at[units.index(unit), part - 1]

    def give_back(chunk, slot, index, cols):
        for half in range(2):
            peer = 2 * index + half
            distance = lax.rem(peer - me + ep_size, ep_size)

            @pl.when(distance == 0)
            def _():
                pltpu.make_async_copy(out_buf.at[slot, peer, :, cols], returned_ref.at[chunk, me, :, cols], local_sem.at[4, chunk]).start()

            @pl.when(distance != 0)
            def _():
                pltpu.make_async_remote_copy(
                    src_ref=out_buf.at[slot, peer, :, cols], dst_ref=returned_ref.at[chunk, me, :, cols], send_sem=back_send.at[chunk, distance], recv_sem=back_recv.at[chunk, distance],
                    device_id={'ep': peer}, device_id_type=MESH).start()

    def weights_here(chunk, which, cols=None):
        unit = (chunk, which)
        if cols is None or cols.start == 0:
            owns[unit].wait()
            for piece in early:
                if piece[:2] == unit:
                    earlies[piece].wait()
        for piece in late:
            if piece[:2] == unit and (cols is None or piece[2] == cols.start):
                for copy in moves[piece]:
                    copy.wait_recv()

    def expert_row(chunk):
        return pl.ds(chunk * tp_size + mine, 1)

    def inner_part(chunk, index, part):
        tokens = arrived_ref[chunk, pl.ds(2 * index, 2)].reshape(2 * slots, width)
        inner = jnp.dot(tokens, part_ref((chunk, 0), part)[...], preferred_element_type=F32) + b_in_ref[away('tp', tp_size, tp_size - part), expert_row(chunk), :]
        return jnp.maximum(inner, 0.0).astype(BF16)

    backs = {}
    for chunk in range(chunks):
        last = chunk == chunks - 1
        slot = chunk % out_buf.shape[0]
        for distance in range(1, ep_size):
            sends[chunk, distance].wait_recv()
        kept[chunk].wait()
        weights_here(chunk, 0)
        before = chunk - out_buf.shape[0]
        if before >= 0:
            for copy in backs[before][:-1]:
                copy.wait_send()
            backs[before][-1].wait()

        held = [sent_buf.at[0], sent_buf.at[1], arrived_ref.at[0], arrived_ref.at[1]]
        if last:
            def first_product(index, carry):
                for part in range(tp_size):
                    held[part][pl.ds(2 * index, 2)] = inner_part(chunk, index, part).reshape(2, slots, width)
                return carry

            lax.fori_loop(0, ep_size // 2, first_product, 0)
        for cols in ([pl.ds(piece[2], piece[3]) for piece in late if piece[:2] == (chunk, 1)] if last else [pl.ds(0, width)]):
            weights_here(chunk, 1, cols if last else None)

            def rows(index, carry):
                total = jnp.zeros((2 * slots, cols.size), F32)
                for part in range(tp_size):
                    inner = held[part][pl.ds(2 * index, 2)].reshape(2 * slots, width) if last else inner_part(chunk, index, part)
                    total += jnp.dot(inner, part_ref((chunk, 1), part)[:, cols], preferred_element_type=F32)
                out_buf[slot, pl.ds(2 * index, 2), :, cols] = (total + b_out_ref[expert_row(chunk), cols]).astype(BF16).reshape(2, slots, cols.size)

                @pl.when(index > 0)
                def _():
                    give_back(chunk, slot, index - 1, cols)

                return carry

            lax.fori_loop(0, ep_size // 2, rows, 0)
            give_back(chunk, slot, ep_size // 2 - 1, cols)
        backs[chunk] = []
        for distance in range(1, ep_size):
            peer = away('ep', ep_size, distance)
            backs[chunk].append(pltpu.make_async_remote_copy(
                src_ref=out_buf.at[slot, peer], dst_ref=returned_ref.at[chunk, me], send_sem=back_send.at[chunk, distance], recv_sem=back_recv.at[chunk, distance],
                device_id={'ep': peer}, device_id_type=MESH))
        backs[chunk].append(pltpu.make_async_copy(out_buf.at[slot, me], returned_ref.at[chunk, me], local_sem.at[4, chunk]))

    for chunk in range(chunks):
        for distance in range(1, ep_size):
            sends[chunk, distance].wait_send()
        for copy in backs[chunk][:-1]:
            copy.wait_recv()
            if chunk + out_buf.shape[0] >= chunks:
                copy.wait_send()
        if chunk + out_buf.shape[0] >= chunks:
            backs[chunk][-1].wait()
    for piece in late:
        for copy in moves[piece]:
            copy.wait_send()


def experts(dispatch, early_weights, w_in, w_out, b_in, b_out, w_router, other, tp_size, ep_size, early, late, call_id):
    chunks, _, slots, width = dispatch.shape
    hidden = w_in.shape[2]

    def body(dispatch_ref, *refs):
        experts_body(tp_size, ep_size, early, late, dispatch_ref, refs[:len(early)], *refs[len(early):])

    return pl.pallas_call(
        body, out_shape=(jax.ShapeDtypeStruct(dispatch.shape, BF16), jax.ShapeDtypeStruct(other.shape, F32)),
        in_specs=[HBM_SPEC] * (3 + len(early)) + [VMEM_SPEC] * 4, out_specs=(HBM_SPEC, VMEM_SPEC),
        scratch_shapes=[pltpu.VMEM((2,) + dispatch.shape[1:], BF16), pltpu.VMEM(dispatch.shape, BF16), pltpu.VMEM((2 * chunks, tp_size - 1, width, hidden), BF16),
                        pltpu.VMEM((chunks, 2, width, hidden), BF16), pltpu.VMEM((2, ep_size, slots, width), BF16),
                        DMA((6, max(chunks, len(early)))), DMA((chunks, ep_size)), DMA((chunks, ep_size)), DMA((chunks, ep_size)), DMA((chunks, ep_size)),
                        DMA((len(late), tp_size - 1)), DMA((len(late), tp_size - 1))],
        compiler_params=settings(call_id, 62),
        cost_estimate=cost(30),
        name='experts')(dispatch, *early_weights, w_in, w_out, b_in, b_out, w_router, other)


def finish_body(tp_size, count, table_ref, gates_ref, outputs_ref, hidden_ref, o_ref, slots_buf, wide_ref, stage_ref, first_buf, hidden_buf, sum_buf, own_buf,
                load_sem, slots_sem, sum_send, sum_recv, out_send, out_recv):
    me = lax.axis_index('tp')
    own_tokens, width = hidden_ref.shape
    tokens = tp_size * own_tokens
    size = own_tokens // (2 * count)
    hops = tp_size - 1
    lanes = 128
    columns = [slice(start, start + lanes) for start in range(0, width, lanes)]

    def rows(way, chunk, index):
        return pl.ds(pl.multiple_of(chunk * own_tokens + (way * count + index) * size, size), size)

    def behind(way, distance):
        return away('tp', tp_size, (tp_size - distance) % tp_size if way == 0 else distance % tp_size)

    def ahead(way):
        return {'tp': away('tp', tp_size, 1 if way == 0 else tp_size - 1)}

    def send_sum(way, hop, index, src_ref):
        return pltpu.make_async_remote_copy(
            src_ref=src_ref, dst_ref=sum_buf.at[way, hop, index], send_sem=sum_send.at[way, hop, index], recv_sem=sum_recv.at[way, hop, index],
            device_id=ahead(way), device_id_type=MESH)

    def send_out(way, hop, index, src_ref, chunk):
        return pltpu.make_async_remote_copy(
            src_ref=src_ref, dst_ref=o_ref.at[rows(way, chunk, index)], send_sem=out_send.at[way, hop, index], recv_sem=out_recv.at[way, hop, index],
            device_id=ahead(way), device_id_type=MESH)

    slots = outputs_ref.shape[0]
    parts = slots_sem.shape[0]
    part_slots = slots // parts
    piece = min(128, part_slots)
    loads = [pltpu.make_async_copy(outputs_ref.at[span(part, part_slots)], slots_buf.at[span(part, part_slots)], slots_sem.at[part]) for part in range(parts)]
    load_hidden = pltpu.make_async_copy(hidden_ref, hidden_buf, load_sem.at[2])
    for load in loads + [load_hidden]:
        load.start()
    enter([('tp', tp_size)])
    wide_ref[slots] = jnp.zeros(wide_ref.shape[1:], F32)
    flat_ref = wide_ref.reshape((slots + 1) * 8, lanes)

    def widen(index, carry):
        at = span(index, piece)
        for column, cols in enumerate(columns):
            flat_ref[pl.ds(index * (piece * 8) + column, piece, stride=8), :] = slots_buf[at, cols].astype(F32) * gates_ref[at, :]
        return carry

    for part, load in enumerate(loads):
        load.wait()
        lax.fori_loop(part * (part_slots // piece), (part + 1) * (part_slots // piece), widen, 0)

    def combine(way, chunk, index):
        base = chunk * own_tokens + (way * count + index) * size
        batch = 16

        def some(part, carry):
            first = part * batch
            for u in range(batch):
                slot_of = [table_ref[choice * tokens + base + first + u] for choice in range(2)]
                stage_ref[way, pl.ds(pl.multiple_of((first + u) * 8, 8), 8), :] = wide_ref[slot_of[0]] + wide_ref[slot_of[1]]
            return carry

        lax.fori_loop(0, size // batch, some, 0)

    def staged(way, column):
        return stage_ref[way, pl.ds(column, size, stride=8), :]

    def first(index, carry):
        for way in range(2):
            combine(way, behind(way, 1), index)
            for column, cols in enumerate(columns):
                first_buf[way, index, :, cols] = staged(way, column).astype(BF16)
        for way in range(2):
            send_sum(way, 0, index, first_buf.at[way, index]).start()
        return carry

    lax.fori_loop(0, count, first, 0)
    load_hidden.wait()

    def keep(way, index):
        return pltpu.make_async_copy(own_buf.at[way, index], o_ref.at[rows(way, me, index)], load_sem.at[way])

    for hop in range(1, tp_size):
        def add(index, carry):
            for way in range(2):
                combine(way, behind(way, hop + 1), index)
            for way in range(2):
                send_sum(way, hop - 1, index, sum_buf.at[way, hop - 1, index]).wait_recv()
                own_rows = pl.ds(pl.multiple_of((way * count + index) * size, size), size)
                for column, cols in enumerate(columns):
                    total = (sum_buf[way, hop - 1, index, :, cols].astype(F32) + staged(way, column)).astype(BF16)
                    if hop < hops:
                        sum_buf[way, hop - 1, index, :, cols] = total
                    else:
                        own_buf[way, index, :, cols] = (total.astype(F32) + hidden_buf[own_rows, cols].astype(F32)).astype(BF16)
            for way in range(2):
                if hop < hops:
                    send_sum(way, hop, index, sum_buf.at[way, hop - 1, index]).start()
                else:
                    send_out(way, 0, index, own_buf.at[way, index], me).start()
                    keep(way, index).start()
                    keep(way, index).wait()
            return carry

        lax.fori_loop(0, count, add, 0)

    for hop in range(1, tp_size):
        def forward(index, carry):
            for way in range(2):
                chunk = behind(way, hop)
                arrived = o_ref.at[rows(way, chunk, index)]
                send_out(way, hop - 1, index, arrived, chunk).wait_recv()
                if hop < hops:
                    send_out(way, hop, index, arrived, chunk).start()
            return carry

        lax.fori_loop(0, count, forward, 0)

    def drain(index, carry):
        for way in range(2):
            for hop in range(hops):
                send_sum(way, hop, index, sum_buf.at[way, hop, index]).wait_send()
                send_out(way, hop, index, own_buf.at[way, index], me).wait_send()
        return carry

    lax.fori_loop(0, count, drain, 0)


def finish(table, gates, outputs, hidden, tp_size, call_id):
    slots, width = outputs.shape
    own_tokens = hidden.shape[0]
    size = min(256, own_tokens // 2)
    count = own_tokens // (2 * size)
    hops = tp_size - 1
    pieces = (2, count, size, width)
    ring = DMA((2, hops, count))

    def vmem(*shape, dtype=BF16):
        return pltpu.VMEM(shape, dtype)

    return pl.pallas_call(
        functools.partial(finish_body, tp_size, count), out_shape=jax.ShapeDtypeStruct((tp_size * own_tokens, width), BF16),
        in_specs=[SMEM_SPEC, VMEM_SPEC, HBM_SPEC, HBM_SPEC], out_specs=HBM_SPEC,
        scratch_shapes=[vmem(slots, width), vmem(slots + 1, 8, 128, dtype=F32), vmem(2, size * 8, 128, dtype=F32), vmem(*pieces), vmem(own_tokens, width),
                        vmem(2, hops, *pieces[1:]), vmem(*pieces), DMA((3,)), DMA((4,)), ring, ring, ring, ring],
        compiler_params=settings(call_id), cost_estimate=cost(100), name='finish')(table, gates, outputs, hidden)


def solution(mesh):
    tp_size = mesh.shape['tp']
    ep_size = mesh.shape['ep']

    def local_fn(x, src_len, expert_idx, ln_gain, ln_bias, w_query, b_query, w_key, w_value, b_value, w_attn_out, b_attn_out, w_fc1, b_fc1, w_fc2, b_fc2, w_router, w_exp_in, b_exp_in, w_exp_out, b_exp_out):
        rows, seq, width = x.shape
        tokens = rows * seq
        num_experts = w_router.shape[1]
        capacity = 2 * (-(-tokens // num_experts))
        local_experts = w_exp_in.shape[0]
        own_experts = local_experts // tp_size
        _, _, local_heads, head_dim = w_query.shape
        head_cols = local_heads * head_dim

        def pack_attention(j):
            columns = [w[j].reshape(width, head_cols).T for w in (w_query, w_key, w_value)]
            return jnp.concatenate(columns + [w_attn_out[j].reshape(head_cols, width)], axis=0)

        def own_slice(value):
            size = value.shape[0] // ep_size
            return lax.dynamic_slice_in_dim(value, lax.axis_index('ep') * size, size, 0)

        own = jnp.stack([own_slice(value) for value in (pack_attention(0), w_fc1.T, w_fc2, pack_attention(1))])

        def piece(code):
            chunk, which, *part = map(int, code)
            size = width // 3 if part else width
            return chunk, which, sum(part) * size, size

        plan = ['00', '01', '10', '11', '20', '210'], ['211', '212', '30', '310', '311', '312']
        early, late = [[piece(code) for code in codes] for codes in plan]
        weights = w_exp_in, w_exp_out
        biases = b_query.transpose(1, 0, 2), b_value.transpose(1, 0, 2), b_fc1.reshape(-1, 128), b_exp_in
        table, dispatch, other, hidden, b_exp_in, *moved = front(
            src_len, expert_idx.transpose(0, 2, 1), ln_gain, ln_bias, b_attn_out, b_fc2.reshape(-1, 128), x, *weights, own, biases, num_experts, capacity, head_dim, tp_size, ep_size, early, 0)
        dispatch = dispatch.reshape(own_experts, ep_size, capacity, width)
        outputs, gates = experts(dispatch, moved, *weights, b_exp_in, b_exp_out, w_router, other, tp_size, ep_size, early, late, 1)
        return finish(table.reshape(-1), gates, outputs.reshape(-1, width), hidden.reshape(-1, width), tp_size, 2).reshape(rows, seq, width)

    axes = {'g': ('dp', 'ep'), 'e': 'ep', 't': 'tp', '.': None}

    def spec(code):
        return P(*[axes[letter] for letter in code])

    codes = ['g..', 'g', 'g..', '..', '..', '..t.', '.t.', '..t.', '..t.', '.t.', '.t..', '..', '.t', 't', 't.', '.', '..', 'e.t', 'et', 'et.', 'e.']
    in_specs = tuple(map(spec, codes))
    return jax.shard_map(local_fn, mesh=mesh, in_specs=in_specs, out_specs=spec('g..'), check_vma=False)
```

```python
import functools

import jax
import jax.numpy as jnp
from jax import lax
from jax.experimental import pallas as pl
from jax.experimental.pallas import tpu as pltpu
from jax.sharding import PartitionSpec as P

LN_EPS = 1e-5
BF16 = jnp.bfloat16
F32 = jnp.float32
LOG2E = 1.4426950408889634


MESH = pl.DeviceIdType.MESH
VMEM_SPEC = pl.BlockSpec(memory_space=pltpu.VMEM)
HBM_SPEC = pl.BlockSpec(memory_space=pltpu.HBM)
SMEM_SPEC = pl.BlockSpec(memory_space=pltpu.SMEM)
DMA = pltpu.SemaphoreType.DMA


def span(index, size):
    return pl.ds(pl.multiple_of(index * size, size), size)


def settings(call_id=None, mib=56, grid=None):
    return pltpu.CompilerParams(dimension_semantics=grid, collective_id=call_id, has_side_effects=call_id is not None, vmem_limit_bytes=mib << 20)


def cost(gflops):
    return pl.CostEstimate(flops=gflops * 10**9, transcendentals=0, bytes_accessed=10**7)


def dot_t(lhs, rhs_t):
    return lax.dot_general(lhs, rhs_t, (((1,), (1,)), ((), ())), preferred_element_type=F32)


def norm_rows(value, gain, shift):
    centered = value - jnp.mean(value, axis=-1, keepdims=True)
    variance = jnp.mean(centered * centered, axis=-1, keepdims=True)
    return centered * lax.rsqrt(variance + LN_EPS) * gain + shift


def away(axis, size, distance):
    return lax.rem(lax.axis_index(axis) + distance, size)


def enter(groups):
    barrier = pltpu.get_barrier_semaphore()
    count = 0
    for axis, size in groups:
        for distance in range(1, size):
            pl.semaphore_signal(barrier, device_id={axis: away(axis, size, distance)}, device_id_type=MESH)
            count += 1
    pl.semaphore_wait(barrier, count)


def exchange(tp_size, weights, piece, landing_ref, send_sem, recv_sem):
    chunk, which, start, cols = piece
    return [pltpu.make_async_remote_copy(
        src_ref=weights[which].at[chunk * tp_size + away('tp', tp_size, distance), :, pl.ds(start, cols)], dst_ref=landing_ref.at[distance - 1],
        send_sem=send_sem.at[distance - 1], recv_sem=recv_sem.at[distance - 1],
        device_id={'tp': away('tp', tp_size, distance)}, device_id_type=MESH)
        for distance in sorted(range(1, tp_size), key=lambda d: (min(d, tp_size - d), d))]


def exchange_all(tp_size, weights, pieces, landing_refs, send_sem, recv_sem):
    copies = []
    for index, piece in enumerate(pieces):
        copies += exchange(tp_size, weights, piece, landing_refs[index], send_sem.at[index], recv_sem.at[index])
    return copies


def landings(tp_size, weight, pieces):
    return [jax.ShapeDtypeStruct((tp_size - 1, weight.shape[1], cols), BF16) for _, _, _, cols in pieces]


def route_tables(own_experts, tp_size, ep_size, lens_ref, index_ref, table_ref, total_ref):
    rows, _, seq = index_ref.shape
    step = min(512, seq)
    per_row = seq // step
    wide, experts_count = total_ref.shape
    slots = wide // 3
    lanes = table_ref.shape[1]
    mine = lax.axis_index('tp')
    ids = lax.broadcasted_iota(jnp.int32, (experts_count, 1), 0)
    slot_ids = lax.broadcasted_iota(jnp.int32, (slots, 1), 0)
    before = (lax.broadcasted_iota(jnp.int32, (step, step), 0) < lax.broadcasted_iota(jnp.int32, (step, step), 1)).astype(BF16)
    total_ref[...] = jnp.zeros_like(total_ref)
    count = jnp.zeros((experts_count, 1), F32)
    for choice in range(2):
        def block(index, count):
            row = index // per_row
            start = pl.multiple_of((index % per_row) * step, step)
            cols = pl.ds(start, step)
            position = lax.broadcasted_iota(jnp.int32, (1, step), 1) + start
            chosen = jnp.where(position < lens_ref[row], index_ref[row, pl.ds(choice, 1), cols], -1)
            other = index_ref[row, pl.ds(1 - choice, 1), cols]
            token = position + row * seq
            hot = jnp.where(ids == chosen, 1.0, 0.0)
            rank = jnp.dot(hot.astype(BF16), before, preferred_element_type=F32) + count
            slot = jnp.sum(rank * hot, axis=0, keepdims=True).astype(jnp.int32)
            at_slot = slot_ids == slot
            parts = [jnp.where(at_slot, value.astype(F32), 0.0).astype(BF16) for value in (token & 255, (token >> 8) + 1, other)]
            values = jnp.concatenate(parts, axis=0)
            hot16 = hot.astype(BF16)
            total_ref[...] += dot_t(values, hot16)
            local = own_experts * tp_size
            own = (lax.rem(chosen, tp_size) == mine) & (slot < slots)
            line = (lax.div(lax.rem(chosen, local), tp_size) * ep_size + lax.div(chosen, local)) * slots + slot
            line = jnp.where(own, line, own_experts * ep_size * slots)
            for part in range(step // lanes):
                at = (choice * rows * per_row + index) * (step // lanes) + part
                table_ref[pl.ds(at, 1), :] = line[:, part * lanes:(part + 1) * lanes]
            return count + jnp.sum(hot, axis=1, keepdims=True)

        count = lax.fori_loop(0, rows * per_row, block, count)


def spread(ep_size, src_ref, view, sems):
    me = lax.axis_index('ep')
    send_sem, recv_sem = sems
    copies = [pltpu.make_async_remote_copy(
        src_ref=src_ref, dst_ref=view(me), send_sem=send_sem.at[distance], recv_sem=recv_sem.at[distance],
        device_id={'ep': away('ep', ep_size, distance)}, device_id_type=MESH) for distance in range(1, ep_size)]
    return copies + [pltpu.make_async_copy(src_ref, view(me), send_sem.at[0])]


def by_kind(ref, ep_size):
    per = ep_size // ref.shape[0]
    return lambda index: ref.at[index // per, :, lax.rem(index, per)]


def front_body(tp_size, ep_size, pieces, own_experts, head_dim, lens_ref, index_ref, gain_ref, shift_ref, b_out_ref, b_fc2_ref, x_ref, w_in_ref, w_out_ref, own_ref, *refs):
    biases, refs = refs[:4], refs[4:]
    table_ref, o_ref, other_out, hidden_out, b_exp_ref, *refs = refs
    moved_refs, refs = refs[:len(pieces)], refs[len(pieces):]
    (other_ref, hidden_ref, b_query_ref, b_value_ref, b_fc1_ref, first_ref, second_ref, later_ref, fc1_ref, fc2_ref, source_ref, total_ref, bias_buf, qkv_ref, context_ref, all_buf,
     load_sem, move_send, move_recv, tp_send, tp_recv, row_send, row_recv, pair_send, pair_recv, spread_sem, ring_send, ring_recv) = refs
    mine = lax.axis_index('tp')
    me = lax.axis_index('ep')
    own_rows, seq, width = hidden_ref.shape
    _, ways, count, size, _ = all_buf.shape
    own_tokens = own_rows * seq

    view = by_kind(first_ref, ep_size)
    moves = exchange_all(tp_size, (w_in_ref, w_out_ref), pieces, moved_refs, move_send, move_recv)
    pairs = [(own_ref.at[0], view(me).at[mine])]
    pairs += [(bias, whole.at[mine]) for bias, whole in zip(biases, (b_query_ref, b_value_ref, b_fc1_ref, b_exp_ref))]
    pairs += [(own_ref.at[1 + index], later_ref.at[index, mine]) for index in range(later_ref.shape[0])]
    near = (1, tp_size - 1)
    gathers = []
    for index, (src, dst) in enumerate(pairs):
        far = range(2, tp_size - 1) if 0 < index <= len(biases) else ()
        gathers.append([pltpu.make_async_copy(src, dst, tp_send.at[index, 0])] + [pltpu.make_async_remote_copy(
            src_ref=src, dst_ref=dst, send_sem=tp_send.at[index, distance], recv_sem=tp_recv.at[index, distance],
            device_id={'tp': away('tp', tp_size, distance)}, device_id_type=MESH) for distance in (*near, *far)])

    def relay(index, where):
        half = own_ref.shape[1] // 2
        copies = []
        for way, distance in enumerate(near):
            piece = where(away('tp', tp_size, tp_size - distance)).at[pl.ds(way * half, half)]
            copies.append(pltpu.make_async_remote_copy(
                src_ref=piece, dst_ref=piece, send_sem=tp_send.at[index, 2 + 2 * way], recv_sem=tp_recv.at[index, 2 + 2 * way],
                device_id={'tp': away('tp', tp_size, distance)}, device_id_type=MESH))
        return copies

    load_x = pltpu.make_async_copy(x_ref.at[pl.ds(mine * own_rows, own_rows)], hidden_ref, load_sem.at[0])
    keep_other = pltpu.make_async_copy(other_ref, other_out, load_sem.at[1])
    keep_hidden = pltpu.make_async_copy(hidden_ref, hidden_out, load_sem.at[2])
    load_x.start()
    enter([('tp', tp_size), ('ep', ep_size)])
    for copies in gathers:
        for copy in copies:
            copy.start()
    one = tp_size - 1
    for copy in moves[:one]:
        copy.start()

    cores = 2
    steps = range(1, ep_size // cores)
    other_core = me + 1 - cores * lax.rem(me, cores)

    def along(step):
        return pltpu.make_async_remote_copy(
            src_ref=view(me), dst_ref=view(me), send_sem=row_send.at[step], recv_sem=row_recv.at[step],
            device_id={'ep': away('ep', ep_size, cores * step)}, device_id_type=MESH)

    def across(step):
        part = view(away('ep', ep_size, ep_size - cores * step))
        return pltpu.make_async_remote_copy(
            src_ref=part, dst_ref=part, send_sem=pair_send.at[step], recv_sem=pair_recv.at[step],
            device_id={'ep': other_core}, device_id_type=MESH)

    for copy in gathers[0]:
        copy.wait()
    first_relay = relay(0, lambda part: view(me).at[part])
    for copy in first_relay:
        copy.start()
    for copies in gathers[1:]:
        for copy in copies:
            copy.wait()
    later_relays = [relay(1 + len(biases) + index, lambda part, index=index: later_ref.at[index, part]) for index in range(later_ref.shape[0])]
    for copies in later_relays:
        for copy in copies:
            copy.start()
    for copy in moves[one:-one]:
        copy.start()
    for copy in first_relay:
        copy.wait()
    for step in steps:
        along(step).start()
    across(0).start()
    for copies in later_relays:
        for copy in copies:
            copy.wait()
    views = [lambda part: fc1_ref.at[:, part], lambda part: fc2_ref.at[:, part], by_kind(second_ref, ep_size)]
    spreads = [spread(ep_size, later_ref.at[index], where, (spread_sem.at[0, index], spread_sem.at[1, index])) for index, where in enumerate(views)]
    for copies in spreads:
        for copy in copies:
            copy.start()

    route_tables(own_experts, tp_size, ep_size, lens_ref, index_ref, table_ref, total_ref)
    wide, experts_count = total_ref.shape
    slots = wide // 3
    lane = lax.broadcasted_iota(jnp.int32, (1, experts_count), 1)

    def take(index, carry):
        chunk = index // ep_size
        expert = (index % ep_size) * (own_experts * tp_size) + chunk * tp_size + mine
        column = jnp.sum(jnp.where(lane == expert, total_ref[...], 0.0), axis=1, keepdims=True).astype(jnp.int32)
        low, high, other = column[:slots], column[slots:2 * slots], column[2 * slots:]
        at = span(index, slots)
        source_ref[at, :] = jnp.where(high > 0, 256 * (high - 1) + low, -1)
        other_ref[at, :] = other
        return carry

    for step in steps:
        along(step).wait()
        across(step).start()
    lax.fori_loop(0, own_experts * ep_size, take, 0)
    for step in range(ep_size // cores):
        across(step).wait()
    load_x.wait()

    hops = tp_size - 1

    def behind(way, distance):
        return away('tp', tp_size, (tp_size - distance) % tp_size if way == 0 else distance % tp_size)

    def ring(way, hop, index, chunk):
        piece = all_buf.at[chunk, way, index]
        return pltpu.make_async_remote_copy(
            src_ref=piece, dst_ref=piece, send_sem=ring_send.at[way, hop, index], recv_sem=ring_recv.at[way, hop, index],
            device_id={'tp': away('tp', tp_size, 1 + way * (tp_size - 2))}, device_id_type=MESH)

    def norm(value, index):
        return norm_rows(value, gain_ref[pl.ds(index, 1), :], shift_ref[pl.ds(index, 1), :]).astype(BF16)

    pair = 2 * head_dim
    lane_head = lax.broadcasted_iota(jnp.int32, (1, pair), 1) // head_dim
    factor = (head_dim ** -0.5) * LOG2E
    blocks = seq // size

    def attention(layer, pack_ref):
        def pack_rows(start, number):
            return pack_ref[pl.ds(start, number)].reshape(number * width, width)

        bias_buf[...] = jnp.zeros_like(bias_buf)
        for ref, start in ((b_query_ref, 0), (b_value_ref, 2 * width)):
            parts = [ref[part, head, pl.ds(layer, 1), :] for part in range(tp_size) for head in range(ref.shape[1])]
            bias_buf[:, pl.ds(start, width)] = jnp.concatenate(parts, axis=1)
        def one_row(row, carry):
            key_ok = lax.broadcasted_iota(jnp.int32, (1, seq), 1) < lens_ref[mine * own_rows + row]

            def project(index, carry):
                rows = span(index, size)
                normed = norm(hidden_ref[row, rows, :].astype(F32), 2 * layer)
                qkv_ref[rows, :] = (dot_t(normed, pack_rows(0, 3)) + bias_buf[...]).astype(BF16)
                return carry

            lax.fori_loop(0, blocks, project, 0)

            def attend(block, carry):
                rows = span(block, size)

                def heads(index, carry):
                    lanes = pl.multiple_of(index * pair, pair)
                    query = qkv_ref[rows, pl.ds(lanes, pair)]
                    keys = qkv_ref[:, pl.ds(pl.multiple_of(lanes + width, pair), pair)]
                    values = qkv_ref[:, pl.ds(pl.multiple_of(lanes + 2 * width, pair), pair)]
                    result = None
                    for head in range(2):
                        scores = dot_t(jnp.where(lane_head == head, query, jnp.zeros_like(query)), keys)
                        scores = jnp.where(key_ok, scores, -1e30)
                        top = jnp.max(scores, axis=-1, keepdims=True)
                        weights = jnp.exp2((scores - top) * factor)
                        scale = 1.0 / jnp.sum(weights, axis=-1, keepdims=True)
                        part = jnp.dot((weights * scale).astype(BF16), values, preferred_element_type=F32)
                        result = part if result is None else jnp.where(lane_head == head, part, result)
                    context_ref[:, pl.ds(lanes, pair)] = result.astype(BF16)
                    return carry

                lax.fori_loop(0, width // pair, heads, 0)
                projected = jnp.dot(context_ref[...], pack_rows(3, 1), preferred_element_type=F32)
                hidden = (hidden_ref[row, rows, :].astype(F32) + projected + b_out_ref[pl.ds(layer, 1), :]).astype(BF16)
                hidden_ref[row, rows, :] = hidden
                if layer:
                    all_buf[mine, row, block] = norm(hidden.astype(F32), 2 * layer + 1)
                    ring(row, 0, block, mine).start()
                return carry

            lax.fori_loop(0, blocks, attend, 0)
            return carry

        lax.fori_loop(0, own_rows, one_row, 0)

    attention(0, first_ref)

    for copies in spreads[:2]:
        for copy in copies:
            copy.wait()

    def as_row(ref):
        return jnp.concatenate([ref[pl.ds(part, 1), :] for part in range(ref.shape[0])], axis=1)

    def dense(index, carry):
        row, rows = index // blocks, span(index % blocks, size)
        value = hidden_ref[row, rows, :].astype(F32)
        normed = norm(value, 1)
        total = value + as_row(b_fc2_ref)
        for part in range(tp_size):
            cols = fc1_ref[part].reshape(-1, width)
            inner = jnp.maximum(dot_t(normed, cols) + as_row(b_fc1_ref.at[part]), 0.0).astype(BF16)
            total += jnp.dot(inner, fc2_ref[part].reshape(-1, width), preferred_element_type=F32)
        hidden_ref[row, rows, :] = total.astype(BF16)
        return carry

    lax.fori_loop(0, own_rows * blocks, dense, 0)
    for copy in spreads[2]:
        copy.wait()
    attention(1, second_ref)

    token = lax.broadcasted_iota(jnp.int32, (1, size), 1)
    slot_count, _ = o_ref.shape
    some = min(512, slot_count)

    def dispatch(index, chunks, fresh):
        def part(part, carry):
            at = span(part, some)
            total = None if fresh else o_ref[at, :].astype(F32)
            for way in range(ways):
                base = chunks[way] * own_tokens + (way * count + index) * size
                hot = jnp.where(source_ref[at, :] == token + base, 1.0, 0.0).astype(BF16)
                taken = jnp.dot(hot, all_buf[chunks[way], way, index], preferred_element_type=F32)
                total = taken if total is None else total + taken
            o_ref[at, :] = total.astype(BF16)
            return carry

        lax.fori_loop(0, slot_count // some, part, 0)

    dispatch(0, (mine, mine), True)

    def own(index, carry):
        dispatch(index, (mine, mine), False)
        return carry

    lax.fori_loop(1, count, own, 0)
    keep_hidden.start()
    keep_other.start()
    for hop in range(1, tp_size):
        def arrive(index, carry):
            chunks = [behind(way, hop) for way in range(ways)]
            for way in range(ways):
                ring(way, hop - 1, index, chunks[way]).wait_recv()
                if hop < hops:
                    ring(way, hop, index, chunks[way]).start()
            dispatch(index, chunks, False)
            return carry

        lax.fori_loop(0, count, arrive, 0)
        if hop == hops - 1:
            for copy in moves[-one:]:
                copy.start()

    def drain(index, carry):
        for way in range(ways):
            for hop in range(hops):
                ring(way, hop, index, mine).wait_send()
        return carry

    lax.fori_loop(0, count, drain, 0)
    for copy in [*moves, keep_hidden, keep_other]:
        copy.wait()


def front(lens, index, gain, shift, b_out, b_fc2, x, w_in, w_out, own, biases, num_experts, capacity, head_dim, tp_size, ep_size, pieces, call_id):
    own_experts = w_in.shape[0] // tp_size
    blocks = own_experts * ep_size
    packs, cut, width = own.shape
    rows, seq, _ = x.shape
    own_rows = rows // tp_size
    size = min(256, seq)
    count = seq // size
    slots = blocks * capacity
    per = ep_size // packs

    def vmem(*shape, dtype=BF16):
        return pltpu.VMEM(shape, dtype)

    moved = landings(tp_size, w_in, pieces)
    b_exp = jax.ShapeDtypeStruct((tp_size,) + biases[3].shape, F32)
    pack = vmem(packs, tp_size, per, cut, width)
    piece_dma, gather_dma, ring_dma = DMA((len(pieces), tp_size - 1)), DMA((packs + len(biases), tp_size + 1)), DMA((own_rows, tp_size - 1, count))
    return pl.pallas_call(
        functools.partial(front_body, tp_size, ep_size, pieces, own_experts, head_dim),
        out_shape=(jax.ShapeDtypeStruct((2 * rows * seq // 128, 128), jnp.int32), jax.ShapeDtypeStruct((slots, width), BF16), jax.ShapeDtypeStruct((slots, 1), jnp.int32),
                   jax.ShapeDtypeStruct((own_rows, seq, width), BF16), b_exp, *moved),
        in_specs=[SMEM_SPEC] + [VMEM_SPEC] * 5 + [HBM_SPEC] * (4 + len(biases)), out_specs=[VMEM_SPEC] * 2 + [HBM_SPEC] * (3 + len(pieces)),
        scratch_shapes=[vmem(slots, 1, dtype=jnp.int32), vmem(own_rows, seq, width), vmem(tp_size, *biases[0].shape, dtype=F32), vmem(tp_size, *biases[1].shape, dtype=F32), vmem(tp_size, *biases[2].shape, dtype=F32), pack, pack,
                        vmem(packs - 1, tp_size, cut, width), vmem(tp_size, ep_size, cut, width), vmem(tp_size, ep_size, cut, width), vmem(slots, 1, dtype=jnp.int32),
                        vmem(3 * capacity, num_experts, dtype=F32), vmem(1, 3 * width, dtype=F32), vmem(seq, 3 * width), vmem(size, width),
                        vmem(tp_size, own_rows, count, size, width), DMA((3,)), piece_dma, piece_dma, gather_dma, gather_dma] + [DMA((ep_size,))] * 4
                       + [DMA((2, packs - 1, ep_size)), ring_dma, ring_dma],
        compiler_params=settings(call_id, 62), cost_estimate=cost(100), name='front')(lens, index, gain, shift, b_out, b_fc2, x, w_in, w_out, own, *biases)


def experts_body(tp_size, ep_size, early, late, dispatch_ref, early_refs, w_in_ref, w_out_ref, b_in_ref, b_out_ref, w_router_ref, other_in, returned_ref, gates_out,
                 other_ref, gates_ref, sent_buf, arrived_ref, parts_buf, own_buf, out_buf, local_sem, send_sem, recv_sem, back_send, back_recv, move_send, move_recv):
    chunks, _, slots, width = arrived_ref.shape
    me = lax.axis_index('ep')
    mine = lax.axis_index('tp')
    weights = (w_in_ref, w_out_ref)
    units = [(chunk, which) for chunk in range(chunks) for which in range(2)]

    sends = {}
    for chunk in range(chunks):
        for distance in range(1, ep_size):
            peer = away('ep', ep_size, distance)
            sends[chunk, distance] = pltpu.make_async_remote_copy(
                src_ref=dispatch_ref.at[chunk, peer], dst_ref=arrived_ref.at[chunk, me], send_sem=send_sem.at[chunk, distance], recv_sem=recv_sem.at[chunk, distance],
                device_id={'ep': peer}, device_id_type=MESH)

    def landing(piece):
        chunk, which, start, cols = piece
        return parts_buf.at[units.index((chunk, which)), :, :, pl.ds(start, cols)]

    moves = {piece: exchange(tp_size, weights, piece, landing(piece), move_send.at[index], move_recv.at[index]) for index, piece in enumerate(late)}
    kept = [pltpu.make_async_copy(dispatch_ref.at[chunk, me], arrived_ref.at[chunk, me], local_sem.at[0, chunk]) for chunk in range(chunks)]
    owns = {unit: pltpu.make_async_copy(weights[unit[1]].at[unit[0] * tp_size + mine], own_buf.at[unit[0], unit[1]], local_sem.at[1 + unit[1], unit[0]]) for unit in units}
    earlies = {piece: pltpu.make_async_copy(early_refs[index], landing(piece), local_sem.at[3, index]) for index, piece in enumerate(early)}

    enter([('tp', tp_size), ('ep', ep_size)])
    for piece in late:
        for copy in moves[piece]:
            copy.start()
    for chunk in range(chunks):
        for distance in range(1, ep_size):
            sends[chunk, distance].start()
        kept[chunk].start()
    for unit in units:
        owns[unit].start()
        for piece in early:
            if piece[:2] == unit:
                earlies[piece].start()

    lane = lax.broadcasted_iota(jnp.int32, (1, w_router_ref.shape[1]), 1)
    group = lax.broadcasted_iota(jnp.int32, (ep_size * slots, 1), 0) // slots

    def load(chunk):
        return pltpu.make_async_copy(dispatch_ref.at[chunk], sent_buf.at[chunk % 2], local_sem.at[5, chunk % 2])

    load_other = pltpu.make_async_copy(other_in, other_ref, local_sem.at[5, 2])
    keep_gates = pltpu.make_async_copy(gates_ref, gates_out, local_sem.at[5, 3])
    load(0).start()
    load_other.start()
    load_other.wait()
    for chunk in range(chunks):
        if chunk + 1 < chunks:
            load(chunk + 1).start()
        load(chunk).wait()
        logits = jnp.dot(sent_buf[chunk % 2].reshape(ep_size * slots, width), w_router_ref[...].astype(BF16), preferred_element_type=F32)
        rows = pl.ds(chunk * ep_size * slots, ep_size * slots)
        own = jnp.sum(jnp.where(lane == group * (chunks * tp_size) + (chunk * tp_size + mine), logits, 0.0), axis=1, keepdims=True)
        other = jnp.sum(jnp.where(lane == other_ref[rows, :], logits, 0.0), axis=1, keepdims=True)
        gates_ref[rows, :] = jax.nn.sigmoid(own - other)

    def part_ref(unit, part):
        if part == 0:
            return own_buf.at[unit[0], unit[1]]
        return parts_buf.at[units.index(unit), part - 1]

    def give_back(chunk, slot, index, cols):
        for half in range(2):
            peer = 2 * index + half
            distance = lax.rem(peer - me + ep_size, ep_size)

            @pl.when(distance == 0)
            def _():
                pltpu.make_async_copy(out_buf.at[slot, peer, :, cols], returned_ref.at[chunk, me, :, cols], local_sem.at[4, chunk]).start()

            @pl.when(distance != 0)
            def _():
                pltpu.make_async_remote_copy(
                    src_ref=out_buf.at[slot, peer, :, cols], dst_ref=returned_ref.at[chunk, me, :, cols], send_sem=back_send.at[chunk, distance], recv_sem=back_recv.at[chunk, distance],
                    device_id={'ep': peer}, device_id_type=MESH).start()

    def weights_here(chunk, which, cols=None):
        unit = (chunk, which)
        if cols is None or cols.start == 0:
            owns[unit].wait()
            for piece in early:
                if piece[:2] == unit:
                    earlies[piece].wait()
        for piece in late:
            if piece[:2] == unit and (cols is None or piece[2] == cols.start):
                for copy in moves[piece]:
                    copy.wait_recv()

    def expert_row(chunk):
        return pl.ds(chunk * tp_size + mine, 1)

    def inner_part(chunk, index, part):
        tokens = arrived_ref[chunk, pl.ds(2 * index, 2)].reshape(2 * slots, width)
        inner = jnp.dot(tokens, part_ref((chunk, 0), part)[...], preferred_element_type=F32) + b_in_ref[away('tp', tp_size, tp_size - part), expert_row(chunk), :]
        return jnp.maximum(inner, 0.0).astype(BF16)

    backs = {}
    for chunk in range(chunks):
        last = chunk == chunks - 1
        slot = chunk % out_buf.shape[0]
        for distance in range(1, ep_size):
            sends[chunk, distance].wait_recv()
        kept[chunk].wait()
        weights_here(chunk, 0)
        before = chunk - out_buf.shape[0]
        if before >= 0:
            for copy in backs[before][:-1]:
                copy.wait_send()
            backs[before][-1].wait()

        held = [sent_buf.at[0], sent_buf.at[1], arrived_ref.at[0], arrived_ref.at[1]]
        if last:
            def first_product(index, carry):
                for part in range(tp_size):
                    held[part][pl.ds(2 * index, 2)] = inner_part(chunk, index, part).reshape(2, slots, width)
                return carry

            lax.fori_loop(0, ep_size // 2, first_product, 0)
        for cols in ([pl.ds(piece[2], piece[3]) for piece in late if piece[:2] == (chunk, 1)] if last else [pl.ds(0, width)]):
            weights_here(chunk, 1, cols if last else None)

            def rows(index, carry):
                total = jnp.zeros((2 * slots, cols.size), F32)
                for part in range(tp_size):
                    inner = held[part][pl.ds(2 * index, 2)].reshape(2 * slots, width) if last else inner_part(chunk, index, part)
                    total += jnp.dot(inner, part_ref((chunk, 1), part)[:, cols], preferred_element_type=F32)
                out_buf[slot, pl.ds(2 * index, 2), :, cols] = (total + b_out_ref[expert_row(chunk), cols]).astype(BF16).reshape(2, slots, cols.size)

                @pl.when(index > 0)
                def _():
                    give_back(chunk, slot, index - 1, cols)

                return carry

            lax.fori_loop(0, ep_size // 2, rows, 0)
            give_back(chunk, slot, ep_size // 2 - 1, cols)
        backs[chunk] = []
        for distance in range(1, ep_size):
            peer = away('ep', ep_size, distance)
            backs[chunk].append(pltpu.make_async_remote_copy(
                src_ref=out_buf.at[slot, peer], dst_ref=returned_ref.at[chunk, me], send_sem=back_send.at[chunk, distance], recv_sem=back_recv.at[chunk, distance],
                device_id={'ep': peer}, device_id_type=MESH))
        backs[chunk].append(pltpu.make_async_copy(out_buf.at[slot, me], returned_ref.at[chunk, me], local_sem.at[4, chunk]))

    keep_gates.start()
    for chunk in range(chunks):
        for distance in range(1, ep_size):
            sends[chunk, distance].wait_send()
        for copy in backs[chunk][:-1]:
            copy.wait_recv()
            if chunk + out_buf.shape[0] >= chunks:
                copy.wait_send()
        if chunk + out_buf.shape[0] >= chunks:
            backs[chunk][-1].wait()
    for piece in late:
        for copy in moves[piece]:
            copy.wait_send()
    keep_gates.wait()


def experts(dispatch, early_weights, w_in, w_out, b_in, b_out, w_router, other, tp_size, ep_size, early, late, call_id):
    chunks, _, slots, width = dispatch.shape
    hidden = w_in.shape[2]

    def body(dispatch_ref, *refs):
        experts_body(tp_size, ep_size, early, late, dispatch_ref, refs[:len(early)], *refs[len(early):])

    return pl.pallas_call(
        body, out_shape=(jax.ShapeDtypeStruct(dispatch.shape, BF16), jax.ShapeDtypeStruct(other.shape, F32)),
        in_specs=[HBM_SPEC] * (3 + len(early)) + [VMEM_SPEC] * 3 + [HBM_SPEC], out_specs=(HBM_SPEC, HBM_SPEC),
        scratch_shapes=[pltpu.VMEM(other.shape, jnp.int32), pltpu.VMEM(other.shape, F32), pltpu.VMEM((2,) + dispatch.shape[1:], BF16), pltpu.VMEM(dispatch.shape, BF16), pltpu.VMEM((2 * chunks, tp_size - 1, width, hidden), BF16),
                        pltpu.VMEM((chunks, 2, width, hidden), BF16), pltpu.VMEM((2, ep_size, slots, width), BF16),
                        DMA((6, max(chunks, len(early)))), DMA((chunks, ep_size)), DMA((chunks, ep_size)), DMA((chunks, ep_size)), DMA((chunks, ep_size)),
                        DMA((len(late), tp_size - 1)), DMA((len(late), tp_size - 1))],
        compiler_params=settings(call_id, 62),
        cost_estimate=cost(30),
        name='experts')(dispatch, *early_weights, w_in, w_out, b_in, b_out, w_router, other)


def finish_body(tp_size, count, table_in, gates_in, outputs_ref, hidden_ref, o_ref, table_ref, gates_ref, slots_buf, wide_ref, stage_ref, first_buf, hidden_buf, sum_buf, own_buf,
                load_sem, slots_sem, sum_send, sum_recv, out_send, out_recv):
    me = lax.axis_index('tp')
    own_tokens, width = hidden_ref.shape
    tokens = tp_size * own_tokens
    size = own_tokens // (2 * count)
    hops = tp_size - 1
    lanes = 128
    columns = [slice(start, start + lanes) for start in range(0, width, lanes)]

    def rows(way, chunk, index):
        return pl.ds(pl.multiple_of(chunk * own_tokens + (way * count + index) * size, size), size)

    def behind(way, distance):
        return away('tp', tp_size, (tp_size - distance) % tp_size if way == 0 else distance % tp_size)

    def ahead(way):
        return {'tp': away('tp', tp_size, 1 if way == 0 else tp_size - 1)}

    def send_sum(way, hop, index, src_ref):
        return pltpu.make_async_remote_copy(
            src_ref=src_ref, dst_ref=sum_buf.at[way, hop, index], send_sem=sum_send.at[way, hop, index], recv_sem=sum_recv.at[way, hop, index],
            device_id=ahead(way), device_id_type=MESH)

    def send_out(way, hop, index, src_ref, chunk):
        return pltpu.make_async_remote_copy(
            src_ref=src_ref, dst_ref=o_ref.at[rows(way, chunk, index)], send_sem=out_send.at[way, hop, index], recv_sem=out_recv.at[way, hop, index],
            device_id=ahead(way), device_id_type=MESH)

    slots = outputs_ref.shape[0]
    parts = slots_sem.shape[0]
    part_slots = slots // parts
    piece = min(128, part_slots)
    loads = [pltpu.make_async_copy(outputs_ref.at[span(part, part_slots)], slots_buf.at[span(part, part_slots)], slots_sem.at[part]) for part in range(parts)]
    load_hidden = pltpu.make_async_copy(hidden_ref, hidden_buf, load_sem.at[2])
    load_gates = pltpu.make_async_copy(gates_in, gates_ref, load_sem.at[3])
    load_table = pltpu.make_async_copy(table_in, table_ref, load_sem.at[4])
    for load in [load_gates, *loads, load_table, load_hidden]:
        load.start()
    enter([('tp', tp_size)])
    wide_ref[slots] = jnp.zeros(wide_ref.shape[1:], F32)
    flat_ref = wide_ref.reshape((slots + 1) * 8, lanes)

    def widen(index, carry):
        at = span(index, piece)
        for column, cols in enumerate(columns):
            flat_ref[pl.ds(index * (piece * 8) + column, piece, stride=8), :] = slots_buf[at, cols].astype(F32) * gates_ref[at, :]
        return carry

    load_gates.wait()
    for part, load in enumerate(loads):
        load.wait()
        lax.fori_loop(part * (part_slots // piece), (part + 1) * (part_slots // piece), widen, 0)

    def combine(way, chunk, index):
        base = chunk * own_tokens + (way * count + index) * size
        batch = 16

        def some(part, carry):
            first = part * batch
            for u in range(batch):
                slot_of = [table_ref[choice * tokens + base + first + u] for choice in range(2)]
                stage_ref[way, pl.ds(pl.multiple_of((first + u) * 8, 8), 8), :] = wide_ref[slot_of[0]] + wide_ref[slot_of[1]]
            return carry

        lax.fori_loop(0, size // batch, some, 0)

    def staged(way, column):
        return stage_ref[way, pl.ds(column, size, stride=8), :]

    def first(index, carry):
        for way in range(2):
            combine(way, behind(way, 1), index)
            for column, cols in enumerate(columns):
                first_buf[way, index, :, cols] = staged(way, column).astype(BF16)
            send_sum(way, 0, index, first_buf.at[way, index]).start()
        return carry

    load_table.wait()
    lax.fori_loop(0, count, first, 0)
    load_hidden.wait()

    def keep(way, index):
        return pltpu.make_async_copy(own_buf.at[way, index], o_ref.at[rows(way, me, index)], load_sem.at[way])

    for hop in range(1, tp_size):
        def add(index, carry):
            for way in range(2):
                combine(way, behind(way, hop + 1), index)
            for way in range(2):
                send_sum(way, hop - 1, index, sum_buf.at[way, hop - 1, index]).wait_recv()
                own_rows = pl.ds(pl.multiple_of((way * count + index) * size, size), size)
                for column, cols in enumerate(columns):
                    total = (sum_buf[way, hop - 1, index, :, cols].astype(F32) + staged(way, column)).astype(BF16)
                    if hop < hops:
                        sum_buf[way, hop - 1, index, :, cols] = total
                    else:
                        own_buf[way, index, :, cols] = (total.astype(F32) + hidden_buf[own_rows, cols].astype(F32)).astype(BF16)
            for way in range(2):
                if hop < hops:
                    send_sum(way, hop, index, sum_buf.at[way, hop - 1, index]).start()
                else:
                    send_out(way, 0, index, own_buf.at[way, index], me).start()
                    keep(way, index).start()
                    keep(way, index).wait()
            return carry

        lax.fori_loop(0, count, add, 0)

    for hop in range(1, tp_size):
        def forward(index, carry):
            for way in range(2):
                chunk = behind(way, hop)
                arrived = o_ref.at[rows(way, chunk, index)]
                send_out(way, hop - 1, index, arrived, chunk).wait_recv()
                if hop < hops:
                    send_out(way, hop, index, arrived, chunk).start()
            return carry

        lax.fori_loop(0, count, forward, 0)

    def drain(index, carry):
        for way in range(2):
            for hop in range(hops):
                send_sum(way, hop, index, sum_buf.at[way, hop, index]).wait_send()
                send_out(way, hop, index, own_buf.at[way, index], me).wait_send()
        return carry

    lax.fori_loop(0, count, drain, 0)


def finish(table, gates, outputs, hidden, tp_size, call_id):
    slots, width = outputs.shape
    own_tokens = hidden.shape[0]
    size = min(256, own_tokens // 2)
    count = own_tokens // (2 * size)
    hops = tp_size - 1
    pieces = (2, count, size, width)
    ring = DMA((2, hops, count))

    def vmem(*shape, dtype=BF16):
        return pltpu.VMEM(shape, dtype)

    return pl.pallas_call(
        functools.partial(finish_body, tp_size, count), out_shape=jax.ShapeDtypeStruct((tp_size * own_tokens, width), BF16),
        in_specs=[HBM_SPEC] * 4, out_specs=HBM_SPEC,
        scratch_shapes=[pltpu.SMEM(table.shape, jnp.int32), vmem(slots, 1, dtype=F32), vmem(slots, width), vmem(slots + 1, 8, 128, dtype=F32), vmem(2, size * 8, 128, dtype=F32), vmem(*pieces), vmem(own_tokens, width),
                        vmem(2, hops, *pieces[1:]), vmem(*pieces), DMA((5,)), DMA((4,)), ring, ring, ring, ring],
        compiler_params=settings(call_id), cost_estimate=cost(100), name='finish')(table, gates, outputs, hidden)


def solution(mesh):
    tp_size = mesh.shape['tp']
    ep_size = mesh.shape['ep']

    def local_fn(x, src_len, expert_idx, ln_gain, ln_bias, w_query, b_query, w_key, w_value, b_value, w_attn_out, b_attn_out, w_fc1, b_fc1, w_fc2, b_fc2, w_router, w_exp_in, b_exp_in, w_exp_out, b_exp_out):
        rows, seq, width = x.shape
        tokens = rows * seq
        num_experts = w_router.shape[1]
        capacity = 2 * (-(-tokens // num_experts))
        local_experts = w_exp_in.shape[0]
        own_experts = local_experts // tp_size
        _, _, local_heads, head_dim = w_query.shape
        head_cols = local_heads * head_dim

        def pack_attention(j):
            columns = [w[j].reshape(width, head_cols).T for w in (w_query, w_key, w_value)]
            return jnp.concatenate(columns + [w_attn_out[j].reshape(head_cols, width)], axis=0)

        def own_slice(value):
            size = value.shape[0] // ep_size
            return lax.dynamic_slice_in_dim(value, lax.axis_index('ep') * size, size, 0)

        own = jnp.stack([own_slice(value) for value in (pack_attention(0), w_fc1.T, w_fc2, pack_attention(1))])

        def piece(code):
            chunk, which, *part = map(int, code)
            size = width // 3 if part else width
            return chunk, which, sum(part) * size, size

        plan = ['210', '00', '01', '10', '11', '200', '201', '202'], ['211', '212', '30', '310', '311', '312']
        early, late = [[piece(code) for code in codes] for codes in plan]
        weights = w_exp_in, w_exp_out
        biases = b_query.transpose(1, 0, 2), b_value.transpose(1, 0, 2), b_fc1.reshape(-1, 128), b_exp_in
        table, dispatch, other, hidden, b_exp_in, *moved = front(
            src_len, expert_idx.transpose(0, 2, 1), ln_gain, ln_bias, b_attn_out, b_fc2.reshape(-1, 128), x, *weights, own, biases, num_experts, capacity, head_dim, tp_size, ep_size, early, 0)
        dispatch = dispatch.reshape(own_experts, ep_size, capacity, width)
        outputs, gates = experts(dispatch, moved, *weights, b_exp_in, b_exp_out, w_router, other, tp_size, ep_size, early, late, 1)
        return finish(table.reshape(-1), gates, outputs.reshape(-1, width), hidden.reshape(-1, width), tp_size, 2).reshape(rows, seq, width)

    axes = {'g': ('dp', 'ep'), 'e': 'ep', 't': 'tp', '.': None}

    def spec(code):
        return P(*[axes[letter] for letter in code])

    codes = ['g..', 'g', 'g..', '..', '..', '..t.', '.t.', '..t.', '..t.', '.t.', '.t..', '..', '.t', 't', 't.', '.', '..', 'e.t', 'et', 'et.', 'e.']
    in_specs = tuple(map(spec, codes))
    return jax.shard_map(local_fn, mesh=mesh, in_specs=in_specs, out_specs=spec('g..'), check_vma=False)
```

```python
import functools

import jax
import jax.numpy as jnp
from jax import lax
from jax.experimental import pallas as pl
from jax.experimental.pallas import tpu as pltpu
from jax.sharding import PartitionSpec as P

LN_EPS = 1e-5
BF16 = jnp.bfloat16
F32 = jnp.float32
LOG2E = 1.4426950408889634


MESH = pl.DeviceIdType.MESH
VMEM_SPEC = pl.BlockSpec(memory_space=pltpu.VMEM)
HBM_SPEC = pl.BlockSpec(memory_space=pltpu.HBM)
SMEM_SPEC = pl.BlockSpec(memory_space=pltpu.SMEM)
DMA = pltpu.SemaphoreType.DMA


def span(index, size):
    return pl.ds(pl.multiple_of(index * size, size), size)


def settings(call_id=None, mib=56, grid=None):
    return pltpu.CompilerParams(dimension_semantics=grid, collective_id=call_id, has_side_effects=call_id is not None, vmem_limit_bytes=mib << 20)


def cost(gflops):
    return pl.CostEstimate(flops=gflops * 10**9, transcendentals=0, bytes_accessed=10**7)


def dot_t(lhs, rhs_t):
    return lax.dot_general(lhs, rhs_t, (((1,), (1,)), ((), ())), preferred_element_type=F32)


def norm_rows(value, gain, shift):
    centered = value - jnp.mean(value, axis=-1, keepdims=True)
    variance = jnp.mean(centered * centered, axis=-1, keepdims=True)
    return centered * lax.rsqrt(variance + LN_EPS) * gain + shift


def away(axis, size, distance):
    return lax.rem(lax.axis_index(axis) + distance, size)


def enter(groups):
    barrier = pltpu.get_barrier_semaphore()
    count = 0
    for axis, size in groups:
        for distance in range(1, size):
            pl.semaphore_signal(barrier, device_id={axis: away(axis, size, distance)}, device_id_type=MESH)
            count += 1
    pl.semaphore_wait(barrier, count)


def exchange(tp_size, weights, piece, landing_ref, send_sem, recv_sem):
    chunk, which, start, cols = piece
    return [pltpu.make_async_remote_copy(
        src_ref=weights[which].at[chunk * tp_size + away('tp', tp_size, distance), :, pl.ds(start, cols)], dst_ref=landing_ref.at[distance - 1],
        send_sem=send_sem.at[distance - 1], recv_sem=recv_sem.at[distance - 1],
        device_id={'tp': away('tp', tp_size, distance)}, device_id_type=MESH)
        for distance in sorted(range(1, tp_size), key=lambda d: (min(d, tp_size - d), d))]


def exchange_all(tp_size, weights, pieces, landing_refs, send_sem, recv_sem):
    copies = []
    for index, piece in enumerate(pieces):
        copies += exchange(tp_size, weights, piece, landing_refs[index], send_sem.at[index], recv_sem.at[index])
    return copies


def landings(tp_size, weight, pieces):
    return [jax.ShapeDtypeStruct((tp_size - 1, weight.shape[1], cols), BF16) for _, _, _, cols in pieces]


def route_tables(own_experts, tp_size, ep_size, lens_ref, index_ref, table_ref, total_ref):
    rows, _, seq = index_ref.shape
    step = min(512, seq)
    per_row = seq // step
    wide, experts_count = total_ref.shape
    slots = wide // 3
    lanes = table_ref.shape[1]
    mine = lax.axis_index('tp')
    ids = lax.broadcasted_iota(jnp.int32, (experts_count, 1), 0)
    slot_ids = lax.broadcasted_iota(jnp.int32, (slots, 1), 0)
    before = (lax.broadcasted_iota(jnp.int32, (step, step), 0) < lax.broadcasted_iota(jnp.int32, (step, step), 1)).astype(BF16)
    total_ref[...] = jnp.zeros_like(total_ref)
    count = jnp.zeros((experts_count, 1), F32)
    for choice in range(2):
        def block(index, count):
            row = index // per_row
            start = pl.multiple_of((index % per_row) * step, step)
            cols = pl.ds(start, step)
            position = lax.broadcasted_iota(jnp.int32, (1, step), 1) + start
            chosen = jnp.where(position < lens_ref[row], index_ref[row, pl.ds(choice, 1), cols], -1)
            other = index_ref[row, pl.ds(1 - choice, 1), cols]
            token = position + row * seq
            hot = jnp.where(ids == chosen, 1.0, 0.0)
            rank = jnp.dot(hot.astype(BF16), before, preferred_element_type=F32) + count
            slot = jnp.sum(rank * hot, axis=0, keepdims=True).astype(jnp.int32)
            at_slot = slot_ids == slot
            parts = [jnp.where(at_slot, value.astype(F32), 0.0).astype(BF16) for value in (token & 255, (token >> 8) + 1, other)]
            values = jnp.concatenate(parts, axis=0)
            hot16 = hot.astype(BF16)
            total_ref[...] += dot_t(values, hot16)
            local = own_experts * tp_size
            own = (lax.rem(chosen, tp_size) == mine) & (slot < slots)
            line = (lax.div(lax.rem(chosen, local), tp_size) * ep_size + lax.div(chosen, local)) * slots + slot
            line = jnp.where(own, line, own_experts * ep_size * slots)
            for part in range(step // lanes):
                at = (choice * rows * per_row + index) * (step // lanes) + part
                table_ref[pl.ds(at, 1), :] = line[:, part * lanes:(part + 1) * lanes]
            return count + jnp.sum(hot, axis=1, keepdims=True)

        count = lax.fori_loop(0, rows * per_row, block, count)


def spread(ep_size, src_ref, view, sems, landed=False):
    cores = 2
    me = lax.axis_index('ep')
    count = ep_size // cores

    def send(src, dst, slot, device):
        return pltpu.make_async_remote_copy(src_ref=src, dst_ref=dst, send_sem=sems[0].at[slot], recv_sem=sems[1].at[slot], device_id={'ep': device}, device_id_type=MESH)

    along = [send(src_ref, view(me), step, away('ep', ep_size, cores * step)) for step in range(1, count)]
    across = []
    for step in range(count):
        part = view(away('ep', ep_size, ep_size - cores * step))
        across.append(send(part if step else src_ref, part, count + step, me + 1 - cores * lax.rem(me, cores)))
    kept = [] if landed else [pltpu.make_async_copy(src_ref, view(me), sems[0].at[0])]
    return along, across, kept


def by_kind(ref, ep_size):
    per = ep_size // ref.shape[0]
    return lambda index: ref.at[index // per, :, lax.rem(index, per)]


def front_body(tp_size, ep_size, pieces, own_experts, head_dim, lens_ref, index_ref, gain_ref, shift_ref, b_out_ref, b_fc2_ref, x_ref, w_in_ref, w_out_ref, own_ref, *refs):
    biases, refs = refs[:4], refs[4:]
    table_ref, o_ref, other_out, hidden_out, b_exp_ref, *refs = refs
    moved_refs, refs = refs[:len(pieces)], refs[len(pieces):]
    (other_ref, hidden_ref, b_query_ref, b_value_ref, b_fc1_ref, first_ref, second_ref, later_ref, fc1_ref, fc2_ref, source_ref, total_ref, bias_buf, qkv_ref, context_ref, all_buf,
     load_sem, move_send, move_recv, tp_send, tp_recv, spread_sem, ring_send, ring_recv) = refs
    mine = lax.axis_index('tp')
    me = lax.axis_index('ep')
    own_rows, seq, width = hidden_ref.shape
    _, ways, count, size, _ = all_buf.shape
    own_tokens = own_rows * seq

    view = by_kind(first_ref, ep_size)
    moves = exchange_all(tp_size, (w_in_ref, w_out_ref), pieces, moved_refs, move_send, move_recv)
    pairs = [(own_ref.at[0], view(me).at[mine])]
    pairs += [(bias, whole.at[mine]) for bias, whole in zip(biases, (b_query_ref, b_value_ref, b_fc1_ref, b_exp_ref))]
    pairs += [(own_ref.at[1 + index], later_ref.at[index, mine]) for index in range(later_ref.shape[0])]
    near = (1, tp_size - 1)
    gathers = []
    for index, (src, dst) in enumerate(pairs):
        far = range(2, tp_size - 1) if 0 < index <= len(biases) else ()
        gathers.append([pltpu.make_async_copy(src, dst, tp_send.at[index, 0])] + [pltpu.make_async_remote_copy(
            src_ref=src, dst_ref=dst, send_sem=tp_send.at[index, distance], recv_sem=tp_recv.at[index, distance],
            device_id={'tp': away('tp', tp_size, distance)}, device_id_type=MESH) for distance in (*near, *far)])

    def relay(index, where):
        half = own_ref.shape[1] // 2
        copies = []
        for way, distance in enumerate(near):
            piece = where(away('tp', tp_size, tp_size - distance)).at[pl.ds(way * half, half)]
            copies.append(pltpu.make_async_remote_copy(
                src_ref=piece, dst_ref=piece, send_sem=tp_send.at[index, 2 + 2 * way], recv_sem=tp_recv.at[index, 2 + 2 * way],
                device_id={'tp': away('tp', tp_size, distance)}, device_id_type=MESH))
        return copies

    load_x = pltpu.make_async_copy(x_ref.at[pl.ds(mine * own_rows, own_rows)], hidden_ref, load_sem.at[0])
    keep_other = pltpu.make_async_copy(other_ref, other_out, load_sem.at[1])
    keep_hidden = pltpu.make_async_copy(hidden_ref, hidden_out, load_sem.at[2])
    load_x.start()
    enter([('tp', tp_size), ('ep', ep_size)])
    for copies in gathers:
        for copy in copies:
            copy.start()
    one = tp_size - 1
    for copy in moves[:one]:
        copy.start()

    def sems(index):
        return spread_sem.at[0, index], spread_sem.at[1, index]

    along, across, _ = spread(ep_size, view(me), view, sems(0), True)
    for copy in gathers[0]:
        copy.wait()
    first_relay = relay(0, lambda part: view(me).at[part])
    for copy in first_relay:
        copy.start()
    for copies in gathers[1:]:
        for copy in copies:
            copy.wait()
    later_relays = [relay(1 + len(biases) + index, lambda part, index=index: later_ref.at[index, part]) for index in range(later_ref.shape[0])]
    for copies in later_relays:
        for copy in copies:
            copy.start()
    for copy in moves[one:-one]:
        copy.start()
    for copy in first_relay:
        copy.wait()
    for copy in [*along, across[0]]:
        copy.start()
    for copies in later_relays:
        for copy in copies:
            copy.wait()
    views = [lambda part: fc1_ref.at[:, part], lambda part: fc2_ref.at[:, part], by_kind(second_ref, ep_size)]
    spreads = [spread(ep_size, later_ref.at[index], where, sems(1 + index)) for index, where in enumerate(views)]
    for later_along, later_across, kept in spreads:
        for copy in [*later_along, later_across[0], *kept]:
            copy.start()

    route_tables(own_experts, tp_size, ep_size, lens_ref, index_ref, table_ref, total_ref)
    wide, experts_count = total_ref.shape
    slots = wide // 3
    lane = lax.broadcasted_iota(jnp.int32, (1, experts_count), 1)

    def take(index, carry):
        chunk = index // ep_size
        expert = (index % ep_size) * (own_experts * tp_size) + chunk * tp_size + mine
        column = jnp.sum(jnp.where(lane == expert, total_ref[...], 0.0), axis=1, keepdims=True).astype(jnp.int32)
        low, high, other = column[:slots], column[slots:2 * slots], column[2 * slots:]
        at = span(index, slots)
        source_ref[at, :] = jnp.where(high > 0, 256 * (high - 1) + low, -1)
        other_ref[at, :] = other
        return carry

    for copy, onward in zip(along, across[1:]):
        copy.wait()
        onward.start()
    lax.fori_loop(0, own_experts * ep_size, take, 0)
    for copy in across:
        copy.wait()
    load_x.wait()

    hops = tp_size - 1

    def behind(way, distance):
        return away('tp', tp_size, (tp_size - distance) % tp_size if way == 0 else distance % tp_size)

    def ring(way, hop, index, chunk):
        piece = all_buf.at[chunk, way, index]
        return pltpu.make_async_remote_copy(
            src_ref=piece, dst_ref=piece, send_sem=ring_send.at[way, hop, index], recv_sem=ring_recv.at[way, hop, index],
            device_id={'tp': away('tp', tp_size, 1 + way * (tp_size - 2))}, device_id_type=MESH)

    def norm(value, index):
        return norm_rows(value, gain_ref[pl.ds(index, 1), :], shift_ref[pl.ds(index, 1), :]).astype(BF16)

    pair = 2 * head_dim
    lane_head = lax.broadcasted_iota(jnp.int32, (1, pair), 1) // head_dim
    factor = (head_dim ** -0.5) * LOG2E
    blocks = seq // size

    def attention(layer, pack_ref):
        def pack_rows(start, number):
            return pack_ref[pl.ds(start, number)].reshape(number * width, width)

        bias_buf[...] = jnp.zeros_like(bias_buf)
        for ref, start in ((b_query_ref, 0), (b_value_ref, 2 * width)):
            parts = [ref[part, head, pl.ds(layer, 1), :] for part in range(tp_size) for head in range(ref.shape[1])]
            bias_buf[:, pl.ds(start, width)] = jnp.concatenate(parts, axis=1)
        def one_row(row, carry):
            key_ok = lax.broadcasted_iota(jnp.int32, (1, seq), 1) < lens_ref[mine * own_rows + row]

            def project(index, carry):
                rows = span(index, size)
                normed = norm(hidden_ref[row, rows, :].astype(F32), 2 * layer)
                qkv_ref[rows, :] = (dot_t(normed, pack_rows(0, 3)) + bias_buf[...]).astype(BF16)
                return carry

            lax.fori_loop(0, blocks, project, 0)

            def attend(block, carry):
                rows = span(block, size)

                def heads(index, carry):
                    lanes = pl.multiple_of(index * pair, pair)
                    query = qkv_ref[rows, pl.ds(lanes, pair)]
                    keys = qkv_ref[:, pl.ds(pl.multiple_of(lanes + width, pair), pair)]
                    values = qkv_ref[:, pl.ds(pl.multiple_of(lanes + 2 * width, pair), pair)]
                    result = None
                    for head in range(2):
                        scores = dot_t(jnp.where(lane_head == head, query, jnp.zeros_like(query)), keys)
                        scores = jnp.where(key_ok, scores, -1e30)
                        top = jnp.max(scores, axis=-1, keepdims=True)
                        weights = jnp.exp2((scores - top) * factor)
                        scale = 1.0 / jnp.sum(weights, axis=-1, keepdims=True)
                        part = jnp.dot((weights * scale).astype(BF16), values, preferred_element_type=F32)
                        result = part if result is None else jnp.where(lane_head == head, part, result)
                    context_ref[:, pl.ds(lanes, pair)] = result.astype(BF16)
                    return carry

                lax.fori_loop(0, width // pair, heads, 0)
                projected = jnp.dot(context_ref[...], pack_rows(3, 1), preferred_element_type=F32)
                hidden = (hidden_ref[row, rows, :].astype(F32) + projected + b_out_ref[pl.ds(layer, 1), :]).astype(BF16)
                hidden_ref[row, rows, :] = hidden
                if layer:
                    all_buf[mine, row, block] = norm(hidden.astype(F32), 2 * layer + 1)
                    ring(row, 0, block, mine).start()
                return carry

            lax.fori_loop(0, blocks, attend, 0)
            return carry

        lax.fori_loop(0, own_rows, one_row, 0)

    attention(0, first_ref)

    for later_along, later_across, kept in spreads:
        for copy, onward in zip(later_along, later_across[1:]):
            copy.wait()
            onward.start()
        for copy in kept:
            copy.wait()
    for _, later_across, _ in spreads[:2]:
        for copy in later_across:
            copy.wait()

    def as_row(ref):
        return jnp.concatenate([ref[pl.ds(part, 1), :] for part in range(ref.shape[0])], axis=1)

    def dense(index, carry):
        row, rows = index // blocks, span(index % blocks, size)
        value = hidden_ref[row, rows, :].astype(F32)
        normed = norm(value, 1)
        total = value + as_row(b_fc2_ref)
        for part in range(tp_size):
            cols = fc1_ref[part].reshape(-1, width)
            inner = jnp.maximum(dot_t(normed, cols) + as_row(b_fc1_ref.at[part]), 0.0).astype(BF16)
            total += jnp.dot(inner, fc2_ref[part].reshape(-1, width), preferred_element_type=F32)
        hidden_ref[row, rows, :] = total.astype(BF16)
        return carry

    lax.fori_loop(0, own_rows * blocks, dense, 0)
    for copy in spreads[2][1]:
        copy.wait()
    attention(1, second_ref)

    token = lax.broadcasted_iota(jnp.int32, (1, size), 1)
    slot_count, _ = o_ref.shape
    some = min(512, slot_count)

    def dispatch(index, chunks, fresh):
        def part(part, carry):
            at = span(part, some)
            total = None if fresh else o_ref[at, :].astype(F32)
            for way in range(ways):
                base = chunks[way] * own_tokens + (way * count + index) * size
                hot = jnp.where(source_ref[at, :] == token + base, 1.0, 0.0).astype(BF16)
                taken = jnp.dot(hot, all_buf[chunks[way], way, index], preferred_element_type=F32)
                total = taken if total is None else total + taken
            o_ref[at, :] = total.astype(BF16)
            return carry

        lax.fori_loop(0, slot_count // some, part, 0)

    dispatch(0, (mine, mine), True)

    def own(index, carry):
        dispatch(index, (mine, mine), False)
        return carry

    lax.fori_loop(1, count, own, 0)
    keep_hidden.start()
    keep_other.start()
    for hop in range(1, tp_size):
        def arrive(index, carry):
            chunks = [behind(way, hop) for way in range(ways)]
            for way in range(ways):
                ring(way, hop - 1, index, chunks[way]).wait_recv()
                if hop < hops:
                    ring(way, hop, index, chunks[way]).start()
            dispatch(index, chunks, False)
            return carry

        lax.fori_loop(0, count, arrive, 0)
        if hop == hops - 1:
            for copy in moves[-one:]:
                copy.start()

    def drain(index, carry):
        for way in range(ways):
            for hop in range(hops):
                ring(way, hop, index, mine).wait_send()
        return carry

    lax.fori_loop(0, count, drain, 0)
    for copy in [*moves, keep_hidden, keep_other]:
        copy.wait()


def front(lens, index, gain, shift, b_out, b_fc2, x, w_in, w_out, own, biases, num_experts, capacity, head_dim, tp_size, ep_size, pieces, call_id):
    own_experts = w_in.shape[0] // tp_size
    blocks = own_experts * ep_size
    packs, cut, width = own.shape
    rows, seq, _ = x.shape
    own_rows = rows // tp_size
    size = min(256, seq)
    count = seq // size
    slots = blocks * capacity
    per = ep_size // packs

    def vmem(*shape, dtype=BF16):
        return pltpu.VMEM(shape, dtype)

    moved = landings(tp_size, w_in, pieces)
    b_exp = jax.ShapeDtypeStruct((tp_size,) + biases[3].shape, F32)
    pack = vmem(packs, tp_size, per, cut, width)
    piece_dma, gather_dma, ring_dma = DMA((len(pieces), tp_size - 1)), DMA((packs + len(biases), tp_size + 1)), DMA((own_rows, tp_size - 1, count))
    return pl.pallas_call(
        functools.partial(front_body, tp_size, ep_size, pieces, own_experts, head_dim),
        out_shape=(jax.ShapeDtypeStruct((2 * rows * seq // 128, 128), jnp.int32), jax.ShapeDtypeStruct((slots, width), BF16), jax.ShapeDtypeStruct((slots, 1), jnp.int32),
                   jax.ShapeDtypeStruct((own_rows, seq, width), BF16), b_exp, *moved),
        in_specs=[SMEM_SPEC] + [VMEM_SPEC] * 5 + [HBM_SPEC] * (4 + len(biases)), out_specs=[VMEM_SPEC] * 2 + [HBM_SPEC] * (3 + len(pieces)),
        scratch_shapes=[vmem(slots, 1, dtype=jnp.int32), vmem(own_rows, seq, width), vmem(tp_size, *biases[0].shape, dtype=F32), vmem(tp_size, *biases[1].shape, dtype=F32), vmem(tp_size, *biases[2].shape, dtype=F32), pack, pack,
                        vmem(packs - 1, tp_size, cut, width), vmem(tp_size, ep_size, cut, width), vmem(tp_size, ep_size, cut, width), vmem(slots, 1, dtype=jnp.int32),
                        vmem(3 * capacity, num_experts, dtype=F32), vmem(1, 3 * width, dtype=F32), vmem(seq, 3 * width), vmem(size, width),
                        vmem(tp_size, own_rows, count, size, width), DMA((3,)), piece_dma, piece_dma, gather_dma, gather_dma, DMA((2, packs, ep_size)), ring_dma, ring_dma],
        compiler_params=settings(call_id, 62), cost_estimate=cost(100), name='front')(lens, index, gain, shift, b_out, b_fc2, x, w_in, w_out, own, *biases)


def experts_body(tp_size, ep_size, early, late, dispatch_ref, early_refs, w_in_ref, w_out_ref, b_in_ref, b_out_ref, w_router_ref, other_in, returned_ref, gates_out,
                 other_ref, gates_ref, sent_buf, arrived_ref, parts_buf, own_buf, out_buf, local_sem, send_sem, recv_sem, back_send, back_recv, move_send, move_recv):
    chunks, _, slots, width = arrived_ref.shape
    me = lax.axis_index('ep')
    mine = lax.axis_index('tp')
    weights = (w_in_ref, w_out_ref)
    units = [(chunk, which) for chunk in range(chunks) for which in range(2)]

    sends = {}
    for chunk in range(chunks):
        for distance in range(1, ep_size):
            peer = away('ep', ep_size, distance)
            sends[chunk, distance] = pltpu.make_async_remote_copy(
                src_ref=dispatch_ref.at[chunk, peer], dst_ref=arrived_ref.at[chunk, me], send_sem=send_sem.at[chunk, distance], recv_sem=recv_sem.at[chunk, distance],
                device_id={'ep': peer}, device_id_type=MESH)

    def landing(piece):
        chunk, which, start, cols = piece
        return parts_buf.at[units.index((chunk, which)), :, :, pl.ds(start, cols)]

    moves = {piece: exchange(tp_size, weights, piece, landing(piece), move_send.at[index], move_recv.at[index]) for index, piece in enumerate(late)}
    kept = [pltpu.make_async_copy(dispatch_ref.at[chunk, me], arrived_ref.at[chunk, me], local_sem.at[0, chunk]) for chunk in range(chunks)]
    owns = {unit: pltpu.make_async_copy(weights[unit[1]].at[unit[0] * tp_size + mine], own_buf.at[unit[0], unit[1]], local_sem.at[1 + unit[1], unit[0]]) for unit in units}
    earlies = {piece: pltpu.make_async_copy(early_refs[index], landing(piece), local_sem.at[3, index]) for index, piece in enumerate(early)}

    enter([('tp', tp_size), ('ep', ep_size)])
    for piece in late:
        for copy in moves[piece]:
            copy.start()
    for chunk in range(chunks):
        for distance in range(1, ep_size):
            sends[chunk, distance].start()
        kept[chunk].start()
    for unit in units:
        owns[unit].start()
        for piece in early:
            if piece[:2] == unit:
                earlies[piece].start()

    lane = lax.broadcasted_iota(jnp.int32, (1, w_router_ref.shape[1]), 1)
    group = lax.broadcasted_iota(jnp.int32, (ep_size * slots, 1), 0) // slots

    def load(chunk):
        return pltpu.make_async_copy(dispatch_ref.at[chunk], sent_buf.at[chunk % 2], local_sem.at[5, chunk % 2])

    load_other = pltpu.make_async_copy(other_in, other_ref, local_sem.at[5, 2])
    keep_gates = pltpu.make_async_copy(gates_ref, gates_out, local_sem.at[5, 3])
    load(0).start()
    load_other.start()
    load_other.wait()
    for chunk in range(chunks):
        if chunk + 1 < chunks:
            load(chunk + 1).start()
        load(chunk).wait()
        logits = jnp.dot(sent_buf[chunk % 2].reshape(ep_size * slots, width), w_router_ref[...].astype(BF16), preferred_element_type=F32)
        rows = pl.ds(chunk * ep_size * slots, ep_size * slots)
        own = jnp.sum(jnp.where(lane == group * (chunks * tp_size) + (chunk * tp_size + mine), logits, 0.0), axis=1, keepdims=True)
        other = jnp.sum(jnp.where(lane == other_ref[rows, :], logits, 0.0), axis=1, keepdims=True)
        gates_ref[rows, :] = jax.nn.sigmoid(own - other)

    def part_ref(unit, part):
        if part == 0:
            return own_buf.at[unit[0], unit[1]]
        return parts_buf.at[units.index(unit), part - 1]

    def give_back(chunk, slot, index, cols):
        for half in range(2):
            peer = 2 * index + half
            distance = lax.rem(peer - me + ep_size, ep_size)

            @pl.when(distance == 0)
            def _():
                pltpu.make_async_copy(out_buf.at[slot, peer, :, cols], returned_ref.at[chunk, me, :, cols], local_sem.at[4, chunk]).start()

            @pl.when(distance != 0)
            def _():
                pltpu.make_async_remote_copy(
                    src_ref=out_buf.at[slot, peer, :, cols], dst_ref=returned_ref.at[chunk, me, :, cols], send_sem=back_send.at[chunk, distance], recv_sem=back_recv.at[chunk, distance],
                    device_id={'ep': peer}, device_id_type=MESH).start()

    def weights_here(chunk, which, cols=None):
        unit = (chunk, which)
        if cols is None or cols.start == 0:
            owns[unit].wait()
            for piece in early:
                if piece[:2] == unit:
                    earlies[piece].wait()
        for piece in late:
            if piece[:2] == unit and (cols is None or piece[2] == cols.start):
                for copy in moves[piece]:
                    copy.wait_recv()

    def expert_row(chunk):
        return pl.ds(chunk * tp_size + mine, 1)

    def inner_part(chunk, index, part):
        tokens = arrived_ref[chunk, pl.ds(2 * index, 2)].reshape(2 * slots, width)
        inner = jnp.dot(tokens, part_ref((chunk, 0), part)[...], preferred_element_type=F32) + b_in_ref[away('tp', tp_size, tp_size - part), expert_row(chunk), :]
        return jnp.maximum(inner, 0.0).astype(BF16)

    backs = {}
    for chunk in range(chunks):
        last = chunk == chunks - 1
        slot = chunk % out_buf.shape[0]
        for distance in range(1, ep_size):
            sends[chunk, distance].wait_recv()
        kept[chunk].wait()
        weights_here(chunk, 0)
        before = chunk - out_buf.shape[0]
        if before >= 0:
            for copy in backs[before][:-1]:
                copy.wait_send()
            backs[before][-1].wait()

        held = [sent_buf.at[0], sent_buf.at[1], arrived_ref.at[0], arrived_ref.at[1]]
        if last:
            def first_product(index, carry):
                for part in range(tp_size):
                    held[part][pl.ds(2 * index, 2)] = inner_part(chunk, index, part).reshape(2, slots, width)
                return carry

            lax.fori_loop(0, ep_size // 2, first_product, 0)
        for cols in ([pl.ds(piece[2], piece[3]) for piece in late if piece[:2] == (chunk, 1)] if last else [pl.ds(0, width)]):
            weights_here(chunk, 1, cols if last else None)

            def rows(index, carry):
                total = jnp.zeros((2 * slots, cols.size), F32)
                for part in range(tp_size):
                    inner = held[part][pl.ds(2 * index, 2)].reshape(2 * slots, width) if last else inner_part(chunk, index, part)
                    total += jnp.dot(inner, part_ref((chunk, 1), part)[:, cols], preferred_element_type=F32)
                out_buf[slot, pl.ds(2 * index, 2), :, cols] = (total + b_out_ref[expert_row(chunk), cols]).astype(BF16).reshape(2, slots, cols.size)

                @pl.when(index > 0)
                def _():
                    give_back(chunk, slot, index - 1, cols)

                return carry

            lax.fori_loop(0, ep_size // 2, rows, 0)
            give_back(chunk, slot, ep_size // 2 - 1, cols)
        backs[chunk] = []
        for distance in range(1, ep_size):
            peer = away('ep', ep_size, distance)
            backs[chunk].append(pltpu.make_async_remote_copy(
                src_ref=out_buf.at[slot, peer], dst_ref=returned_ref.at[chunk, me], send_sem=back_send.at[chunk, distance], recv_sem=back_recv.at[chunk, distance],
                device_id={'ep': peer}, device_id_type=MESH))
        backs[chunk].append(pltpu.make_async_copy(out_buf.at[slot, me], returned_ref.at[chunk, me], local_sem.at[4, chunk]))

    keep_gates.start()
    for chunk in range(chunks):
        for distance in range(1, ep_size):
            sends[chunk, distance].wait_send()
        for copy in backs[chunk][:-1]:
            copy.wait_recv()
            if chunk + out_buf.shape[0] >= chunks:
                copy.wait_send()
        if chunk + out_buf.shape[0] >= chunks:
            backs[chunk][-1].wait()
    for piece in late:
        for copy in moves[piece]:
            copy.wait_send()
    keep_gates.wait()


def experts(dispatch, early_weights, w_in, w_out, b_in, b_out, w_router, other, tp_size, ep_size, early, late, call_id):
    chunks, _, slots, width = dispatch.shape
    hidden = w_in.shape[2]

    def body(dispatch_ref, *refs):
        experts_body(tp_size, ep_size, early, late, dispatch_ref, refs[:len(early)], *refs[len(early):])

    return pl.pallas_call(
        body, out_shape=(jax.ShapeDtypeStruct(dispatch.shape, BF16), jax.ShapeDtypeStruct(other.shape, F32)),
        in_specs=[HBM_SPEC] * (3 + len(early)) + [VMEM_SPEC] * 3 + [HBM_SPEC], out_specs=(HBM_SPEC, HBM_SPEC),
        scratch_shapes=[pltpu.VMEM(other.shape, jnp.int32), pltpu.VMEM(other.shape, F32), pltpu.VMEM((2,) + dispatch.shape[1:], BF16), pltpu.VMEM(dispatch.shape, BF16), pltpu.VMEM((2 * chunks, tp_size - 1, width, hidden), BF16),
                        pltpu.VMEM((chunks, 2, width, hidden), BF16), pltpu.VMEM((2, ep_size, slots, width), BF16),
                        DMA((6, max(chunks, len(early)))), DMA((chunks, ep_size)), DMA((chunks, ep_size)), DMA((chunks, ep_size)), DMA((chunks, ep_size)),
                        DMA((len(late), tp_size - 1)), DMA((len(late), tp_size - 1))],
        compiler_params=settings(call_id, 62),
        cost_estimate=cost(30),
        name='experts')(dispatch, *early_weights, w_in, w_out, b_in, b_out, w_router, other)


def finish_body(tp_size, count, table_in, gates_in, outputs_ref, hidden_ref, o_ref, table_ref, gates_ref, slots_buf, wide_ref, stage_ref, first_buf, hidden_buf, sum_buf, own_buf,
                load_sem, slots_sem, sum_send, sum_recv, out_send, out_recv):
    me = lax.axis_index('tp')
    own_tokens, width = hidden_ref.shape
    tokens = tp_size * own_tokens
    size = own_tokens // (2 * count)
    hops = tp_size - 1
    lanes = 128
    columns = [slice(start, start + lanes) for start in range(0, width, lanes)]

    def rows(way, chunk, index):
        return pl.ds(pl.multiple_of(chunk * own_tokens + (way * count + index) * size, size), size)

    def behind(way, distance):
        return away('tp', tp_size, (tp_size - distance) % tp_size if way == 0 else distance % tp_size)

    def ahead(way):
        return {'tp': away('tp', tp_size, 1 if way == 0 else tp_size - 1)}

    def send_sum(way, hop, index, src_ref):
        return pltpu.make_async_remote_copy(
            src_ref=src_ref, dst_ref=sum_buf.at[way, hop, index], send_sem=sum_send.at[way, hop, index], recv_sem=sum_recv.at[way, hop, index],
            device_id=ahead(way), device_id_type=MESH)

    def send_out(way, hop, index, src_ref, chunk):
        return pltpu.make_async_remote_copy(
            src_ref=src_ref, dst_ref=o_ref.at[rows(way, chunk, index)], send_sem=out_send.at[way, hop, index], recv_sem=out_recv.at[way, hop, index],
            device_id=ahead(way), device_id_type=MESH)

    slots = outputs_ref.shape[0]
    parts = slots_sem.shape[0]
    part_slots = slots // parts
    piece = min(128, part_slots)
    loads = [pltpu.make_async_copy(outputs_ref.at[span(part, part_slots)], slots_buf.at[span(part, part_slots)], slots_sem.at[part]) for part in range(parts)]
    load_hidden = pltpu.make_async_copy(hidden_ref, hidden_buf, load_sem.at[2])
    load_gates = pltpu.make_async_copy(gates_in, gates_ref, load_sem.at[3])
    load_table = pltpu.make_async_copy(table_in, table_ref, load_sem.at[4])
    for load in [load_gates, *loads, load_table, load_hidden]:
        load.start()
    enter([('tp', tp_size)])
    wide_ref[slots] = jnp.zeros(wide_ref.shape[1:], F32)
    flat_ref = wide_ref.reshape((slots + 1) * 8, lanes)

    def widen(index, carry):
        at = span(index, piece)
        for column, cols in enumerate(columns):
            flat_ref[pl.ds(index * (piece * 8) + column, piece, stride=8), :] = slots_buf[at, cols].astype(F32) * gates_ref[at, :]
        return carry

    load_gates.wait()
    for part, load in enumerate(loads):
        load.wait()
        lax.fori_loop(part * (part_slots // piece), (part + 1) * (part_slots // piece), widen, 0)

    def combine(way, chunk, index):
        base = chunk * own_tokens + (way * count + index) * size
        batch = 16

        def some(part, carry):
            first = part * batch
            for u in range(batch):
                slot_of = [table_ref[choice * tokens + base + first + u] for choice in range(2)]
                stage_ref[way, pl.ds(pl.multiple_of((first + u) * 8, 8), 8), :] = wide_ref[slot_of[0]] + wide_ref[slot_of[1]]
            return carry

        lax.fori_loop(0, size // batch, some, 0)

    def staged(way, column):
        return stage_ref[way, pl.ds(column, size, stride=8), :]

    def first(index, carry):
        for way in range(2):
            combine(way, behind(way, 1), index)
            for column, cols in enumerate(columns):
                first_buf[way, index, :, cols] = staged(way, column).astype(BF16)
            send_sum(way, 0, index, first_buf.at[way, index]).start()
        return carry

    load_table.wait()
    lax.fori_loop(0, count, first, 0)
    load_hidden.wait()

    def keep(way, index):
        return pltpu.make_async_copy(own_buf.at[way, index], o_ref.at[rows(way, me, index)], load_sem.at[way])

    for hop in range(1, tp_size):
        def add(index, carry):
            for way in range(2):
                combine(way, behind(way, hop + 1), index)
            for way in range(2):
                send_sum(way, hop - 1, index, sum_buf.at[way, hop - 1, index]).wait_recv()
                own_rows = pl.ds(pl.multiple_of((way * count + index) * size, size), size)
                for column, cols in enumerate(columns):
                    total = (sum_buf[way, hop - 1, index, :, cols].astype(F32) + staged(way, column)).astype(BF16)
                    if hop < hops:
                        sum_buf[way, hop - 1, index, :, cols] = total
                    else:
                        own_buf[way, index, :, cols] = (total.astype(F32) + hidden_buf[own_rows, cols].astype(F32)).astype(BF16)
            for way in range(2):
                if hop < hops:
                    send_sum(way, hop, index, sum_buf.at[way, hop - 1, index]).start()
                else:
                    send_out(way, 0, index, own_buf.at[way, index], me).start()
                    keep(way, index).start()
                    keep(way, index).wait()
            return carry

        lax.fori_loop(0, count, add, 0)

    for hop in range(1, tp_size):
        def forward(index, carry):
            for way in range(2):
                chunk = behind(way, hop)
                arrived = o_ref.at[rows(way, chunk, index)]
                send_out(way, hop - 1, index, arrived, chunk).wait_recv()
                if hop < hops:
                    send_out(way, hop, index, arrived, chunk).start()
            return carry

        lax.fori_loop(0, count, forward, 0)

    def drain(index, carry):
        for way in range(2):
            for hop in range(hops):
                send_sum(way, hop, index, sum_buf.at[way, hop, index]).wait_send()
                send_out(way, hop, index, own_buf.at[way, index], me).wait_send()
        return carry

    lax.fori_loop(0, count, drain, 0)


def finish(table, gates, outputs, hidden, tp_size, call_id):
    slots, width = outputs.shape
    own_tokens = hidden.shape[0]
    size = min(256, own_tokens // 2)
    count = own_tokens // (2 * size)
    hops = tp_size - 1
    pieces = (2, count, size, width)
    ring = DMA((2, hops, count))

    def vmem(*shape, dtype=BF16):
        return pltpu.VMEM(shape, dtype)

    return pl.pallas_call(
        functools.partial(finish_body, tp_size, count), out_shape=jax.ShapeDtypeStruct((tp_size * own_tokens, width), BF16),
        in_specs=[HBM_SPEC] * 4, out_specs=HBM_SPEC,
        scratch_shapes=[pltpu.SMEM(table.shape, jnp.int32), vmem(slots, 1, dtype=F32), vmem(slots, width), vmem(slots + 1, 8, 128, dtype=F32), vmem(2, size * 8, 128, dtype=F32), vmem(*pieces), vmem(own_tokens, width),
                        vmem(2, hops, *pieces[1:]), vmem(*pieces), DMA((5,)), DMA((4,)), ring, ring, ring, ring],
        compiler_params=settings(call_id), cost_estimate=cost(100), name='finish')(table, gates, outputs, hidden)


def solution(mesh):
    tp_size = mesh.shape['tp']
    ep_size = mesh.shape['ep']

    def local_fn(x, src_len, expert_idx, ln_gain, ln_bias, w_query, b_query, w_key, w_value, b_value, w_attn_out, b_attn_out, w_fc1, b_fc1, w_fc2, b_fc2, w_router, w_exp_in, b_exp_in, w_exp_out, b_exp_out):
        rows, seq, width = x.shape
        tokens = rows * seq
        num_experts = w_router.shape[1]
        capacity = 2 * (-(-tokens // num_experts))
        local_experts = w_exp_in.shape[0]
        own_experts = local_experts // tp_size
        _, _, local_heads, head_dim = w_query.shape
        head_cols = local_heads * head_dim

        def pack_attention(j):
            columns = [w[j].reshape(width, head_cols).T for w in (w_query, w_key, w_value)]
            return jnp.concatenate(columns + [w_attn_out[j].reshape(head_cols, width)], axis=0)

        def own_slice(value):
            size = value.shape[0] // ep_size
            return lax.dynamic_slice_in_dim(value, lax.axis_index('ep') * size, size, 0)

        own = jnp.stack([own_slice(value) for value in (pack_attention(0), w_fc1.T, w_fc2, pack_attention(1))])

        def piece(code):
            chunk, which, *part = map(int, code)
            size = width // 3 if part else width
            return chunk, which, sum(part) * size, size

        plan = ['210', '00', '01', '10', '11', '200', '201', '202'], ['211', '212', '30', '310', '311', '312']
        early, late = [[piece(code) for code in codes] for codes in plan]
        weights = w_exp_in, w_exp_out
        biases = b_query.transpose(1, 0, 2), b_value.transpose(1, 0, 2), b_fc1.reshape(-1, 128), b_exp_in
        table, dispatch, other, hidden, b_exp_in, *moved = front(
            src_len, expert_idx.transpose(0, 2, 1), ln_gain, ln_bias, b_attn_out, b_fc2.reshape(-1, 128), x, *weights, own, biases, num_experts, capacity, head_dim, tp_size, ep_size, early, 0)
        dispatch = dispatch.reshape(own_experts, ep_size, capacity, width)
        outputs, gates = experts(dispatch, moved, *weights, b_exp_in, b_exp_out, w_router, other, tp_size, ep_size, early, late, 1)
        return finish(table.reshape(-1), gates, outputs.reshape(-1, width), hidden.reshape(-1, width), tp_size, 2).reshape(rows, seq, width)

    axes = {'g': ('dp', 'ep'), 'e': 'ep', 't': 'tp', '.': None}

    def spec(code):
        return P(*[axes[letter] for letter in code])

    codes = ['g..', 'g', 'g..', '..', '..', '..t.', '.t.', '..t.', '..t.', '.t.', '.t..', '..', '.t', 't', 't.', '.', '..', 'e.t', 'et', 'et.', 'e.']
    in_specs = tuple(map(spec, codes))
    return jax.shard_map(local_fn, mesh=mesh, in_specs=in_specs, out_specs=spec('g..'), check_vma=False)
```

```python
import functools

import jax
import jax.numpy as jnp
from jax import lax
from jax.experimental import pallas as pl
from jax.experimental.pallas import tpu as pltpu
from jax.sharding import PartitionSpec as P

LN_EPS = 1e-5
BF16 = jnp.bfloat16
F32 = jnp.float32
LOG2E = 1.4426950408889634


MESH = pl.DeviceIdType.MESH
VMEM_SPEC = pl.BlockSpec(memory_space=pltpu.VMEM)
HBM_SPEC = pl.BlockSpec(memory_space=pltpu.HBM)
SMEM_SPEC = pl.BlockSpec(memory_space=pltpu.SMEM)
DMA = pltpu.SemaphoreType.DMA


def span(index, size):
    return pl.ds(pl.multiple_of(index * size, size), size)


def settings(call_id=None, mib=56, grid=None):
    return pltpu.CompilerParams(dimension_semantics=grid, collective_id=call_id, has_side_effects=call_id is not None, vmem_limit_bytes=mib << 20)


def cost(gflops):
    return pl.CostEstimate(flops=gflops * 10**9, transcendentals=0, bytes_accessed=10**7)


def dot_t(lhs, rhs_t):
    return lax.dot_general(lhs, rhs_t, (((1,), (1,)), ((), ())), preferred_element_type=F32)


def norm_rows(value, gain, shift):
    centered = value - jnp.mean(value, axis=-1, keepdims=True)
    variance = jnp.mean(centered * centered, axis=-1, keepdims=True)
    return centered * lax.rsqrt(variance + LN_EPS) * gain + shift


def away(axis, size, distance):
    return lax.rem(lax.axis_index(axis) + distance, size)


def enter(groups):
    barrier = pltpu.get_barrier_semaphore()
    count = 0
    for axis, size in groups:
        for distance in range(1, size):
            pl.semaphore_signal(barrier, device_id={axis: away(axis, size, distance)}, device_id_type=MESH)
            count += 1
    pl.semaphore_wait(barrier, count)


def exchange(tp_size, weights, piece, landing_ref, send_sem, recv_sem):
    chunk, which, start, cols = piece
    return [pltpu.make_async_remote_copy(
        src_ref=weights[which].at[chunk * tp_size + away('tp', tp_size, distance), :, pl.ds(start, cols)], dst_ref=landing_ref.at[distance - 1],
        send_sem=send_sem.at[distance - 1], recv_sem=recv_sem.at[distance - 1],
        device_id={'tp': away('tp', tp_size, distance)}, device_id_type=MESH)
        for distance in sorted(range(1, tp_size), key=lambda d: (min(d, tp_size - d), d))]


def exchange_all(tp_size, weights, pieces, landing_refs, send_sem, recv_sem):
    copies = []
    for index, piece in enumerate(pieces):
        copies += exchange(tp_size, weights, piece, landing_refs[index], send_sem.at[index], recv_sem.at[index])
    return copies


def landings(tp_size, weight, pieces):
    return [jax.ShapeDtypeStruct((tp_size - 1, weight.shape[1], cols), BF16) for _, _, _, cols in pieces]


def route_tables(own_experts, tp_size, ep_size, lens_ref, index_ref, table_ref, total_ref):
    rows, _, seq = index_ref.shape
    step = min(512, seq)
    per_row = seq // step
    wide, experts_count = total_ref.shape
    slots = wide // 3
    lanes = table_ref.shape[1]
    mine = lax.axis_index('tp')
    ids = lax.broadcasted_iota(jnp.int32, (experts_count, 1), 0)
    slot_ids = lax.broadcasted_iota(jnp.int32, (slots, 1), 0)
    before = (lax.broadcasted_iota(jnp.int32, (step, step), 0) < lax.broadcasted_iota(jnp.int32, (step, step), 1)).astype(BF16)
    total_ref[...] = jnp.zeros_like(total_ref)
    count = jnp.zeros((experts_count, 1), F32)
    for choice in range(2):
        def block(index, count):
            row = index // per_row
            start = pl.multiple_of((index % per_row) * step, step)
            cols = pl.ds(start, step)
            position = lax.broadcasted_iota(jnp.int32, (1, step), 1) + start
            chosen = jnp.where(position < lens_ref[row], index_ref[row, pl.ds(choice, 1), cols], -1)
            other = index_ref[row, pl.ds(1 - choice, 1), cols]
            token = position + row * seq
            hot = jnp.where(ids == chosen, 1.0, 0.0)
            rank = jnp.dot(hot.astype(BF16), before, preferred_element_type=F32) + count
            slot = jnp.sum(rank * hot, axis=0, keepdims=True).astype(jnp.int32)
            at_slot = slot_ids == slot
            parts = [jnp.where(at_slot, value.astype(F32), 0.0).astype(BF16) for value in (token & 255, (token >> 8) + 1, other)]
            values = jnp.concatenate(parts, axis=0)
            hot16 = hot.astype(BF16)
            total_ref[...] += dot_t(values, hot16)
            local = own_experts * tp_size
            own = (lax.rem(chosen, tp_size) == mine) & (slot < slots)
            line = (lax.div(lax.rem(chosen, local), tp_size) * ep_size + lax.div(chosen, local)) * slots + slot
            line = jnp.where(own, line, own_experts * ep_size * slots)
            for part in range(step // lanes):
                at = (choice * rows * per_row + index) * (step // lanes) + part
                table_ref[pl.ds(at, 1), :] = line[:, part * lanes:(part + 1) * lanes]
            return count + jnp.sum(hot, axis=1, keepdims=True)

        count = lax.fori_loop(0, rows * per_row, block, count)


def spread(ep_size, src_ref, view, sems, landed=False):
    cores = 2
    me = lax.axis_index('ep')
    count = ep_size // cores

    def send(src, dst, slot, device):
        return pltpu.make_async_remote_copy(src_ref=src, dst_ref=dst, send_sem=sems[0].at[slot], recv_sem=sems[1].at[slot], device_id={'ep': device}, device_id_type=MESH)

    along = [send(src_ref, view(me), step, away('ep', ep_size, cores * step)) for step in range(1, count)]
    across = []
    for step in range(count):
        part = view(away('ep', ep_size, ep_size - cores * step))
        across.append(send(part if step else src_ref, part, count + step, me + 1 - cores * lax.rem(me, cores)))
    kept = [] if landed else [pltpu.make_async_copy(src_ref, view(me), sems[0].at[0])]
    return along, across, kept


def by_kind(ref, ep_size):
    per = ep_size // ref.shape[0]
    return lambda index: ref.at[index // per, :, lax.rem(index, per)]


def front_body(tp_size, ep_size, pieces, own_experts, head_dim, lens_ref, index_ref, gain_ref, shift_ref, b_out_ref, b_fc2_ref, x_ref, w_in_ref, w_out_ref, own_ref, *refs):
    biases, refs = refs[:4], refs[4:]
    table_ref, o_out, other_out, hidden_out, b_exp_ref, *refs = refs
    moved_refs, refs = refs[:len(pieces)], refs[len(pieces):]
    (o_ref, other_ref, hidden_ref, b_query_ref, b_value_ref, b_fc1_ref, first_ref, second_ref, later_ref, fc1_ref, fc2_ref, source_ref, total_ref, bias_buf, qkv_ref, context_ref, all_buf,
     load_sem, move_send, move_recv, tp_send, tp_recv, spread_sem, ring_send, ring_recv) = refs
    mine = lax.axis_index('tp')
    me = lax.axis_index('ep')
    own_rows, seq, width = hidden_ref.shape
    _, ways, count, size, _ = all_buf.shape
    own_tokens = own_rows * seq

    view = by_kind(first_ref, ep_size)
    moves = exchange_all(tp_size, (w_in_ref, w_out_ref), pieces, moved_refs, move_send, move_recv)
    pairs = [(own_ref.at[0], view(me).at[mine])]
    pairs += [(bias, whole.at[mine]) for bias, whole in zip(biases, (b_query_ref, b_value_ref, b_fc1_ref, b_exp_ref))]
    pairs += [(own_ref.at[1 + index], later_ref.at[index, mine]) for index in range(later_ref.shape[0])]
    near = (1, tp_size - 1)
    gathers = []
    for index, (src, dst) in enumerate(pairs):
        far = range(2, tp_size - 1) if 0 < index <= len(biases) else ()
        gathers.append([pltpu.make_async_copy(src, dst, tp_send.at[index, 0])] + [pltpu.make_async_remote_copy(
            src_ref=src, dst_ref=dst, send_sem=tp_send.at[index, distance], recv_sem=tp_recv.at[index, distance],
            device_id={'tp': away('tp', tp_size, distance)}, device_id_type=MESH) for distance in (*near, *far)])

    def relay(index, where):
        half = own_ref.shape[1] // 2
        copies = []
        for way, distance in enumerate(near):
            piece = where(away('tp', tp_size, tp_size - distance)).at[pl.ds(way * half, half)]
            copies.append(pltpu.make_async_remote_copy(
                src_ref=piece, dst_ref=piece, send_sem=tp_send.at[index, 2 + 2 * way], recv_sem=tp_recv.at[index, 2 + 2 * way],
                device_id={'tp': away('tp', tp_size, distance)}, device_id_type=MESH))
        return copies

    load_x = pltpu.make_async_copy(x_ref.at[pl.ds(mine * own_rows, own_rows)], hidden_ref, load_sem.at[0])
    keep_other = pltpu.make_async_copy(other_ref, other_out, load_sem.at[1])
    keep_hidden = pltpu.make_async_copy(hidden_ref, hidden_out, load_sem.at[2])
    keep_rows = pltpu.make_async_copy(o_ref, o_out, load_sem.at[3])
    load_x.start()
    enter([('tp', tp_size), ('ep', ep_size)])
    for copies in gathers:
        for copy in copies:
            copy.start()
    one = tp_size - 1
    for copy in moves[:one]:
        copy.start()

    def sems(index):
        return spread_sem.at[0, index], spread_sem.at[1, index]

    along, across, _ = spread(ep_size, view(me), view, sems(0), True)
    for copy in gathers[0]:
        copy.wait()
    first_relay = relay(0, lambda part: view(me).at[part])
    for copy in first_relay:
        copy.start()
    for copies in gathers[1:]:
        for copy in copies:
            copy.wait()
    later_relays = [relay(1 + len(biases) + index, lambda part, index=index: later_ref.at[index, part]) for index in range(later_ref.shape[0])]
    for copies in later_relays:
        for copy in copies:
            copy.start()
    for copy in moves[one:-one]:
        copy.start()
    for copy in first_relay:
        copy.wait()
    for copy in [*along, across[0]]:
        copy.start()
    for copies in later_relays:
        for copy in copies:
            copy.wait()
    views = [lambda part: fc1_ref.at[:, part], lambda part: fc2_ref.at[:, part], by_kind(second_ref, ep_size)]
    spreads = [spread(ep_size, later_ref.at[index], where, sems(1 + index)) for index, where in enumerate(views)]
    for later_along, later_across, kept in spreads:
        for copy in [*later_along, later_across[0], *kept]:
            copy.start()

    route_tables(own_experts, tp_size, ep_size, lens_ref, index_ref, table_ref, total_ref)
    wide, experts_count = total_ref.shape
    slots = wide // 3
    lane = lax.broadcasted_iota(jnp.int32, (1, experts_count), 1)

    def take(index, carry):
        chunk = index // ep_size
        expert = (index % ep_size) * (own_experts * tp_size) + chunk * tp_size + mine
        column = jnp.sum(jnp.where(lane == expert, total_ref[...], 0.0), axis=1, keepdims=True).astype(jnp.int32)
        low, high, other = column[:slots], column[slots:2 * slots], column[2 * slots:]
        at = span(index, slots)
        source_ref[at, :] = jnp.where(high > 0, 256 * (high - 1) + low, -1)
        other_ref[at, :] = other
        return carry

    for copy, onward in zip(along, across[1:]):
        copy.wait()
        onward.start()
    lax.fori_loop(0, own_experts * ep_size, take, 0)
    for copy in across:
        copy.wait()
    load_x.wait()

    hops = tp_size - 1

    def behind(way, distance):
        return away('tp', tp_size, (tp_size - distance) % tp_size if way == 0 else distance % tp_size)

    def ring(way, hop, index, chunk):
        piece = all_buf.at[chunk, way, index]
        return pltpu.make_async_remote_copy(
            src_ref=piece, dst_ref=piece, send_sem=ring_send.at[way, hop, index], recv_sem=ring_recv.at[way, hop, index],
            device_id={'tp': away('tp', tp_size, 1 + way * (tp_size - 2))}, device_id_type=MESH)

    def norm(value, index):
        return norm_rows(value, gain_ref[pl.ds(index, 1), :], shift_ref[pl.ds(index, 1), :]).astype(BF16)

    pair = 2 * head_dim
    lane_head = lax.broadcasted_iota(jnp.int32, (1, pair), 1) // head_dim
    factor = (head_dim ** -0.5) * LOG2E
    blocks = seq // size

    def attention(layer, pack_ref):
        def pack_rows(start, number):
            return pack_ref[pl.ds(start, number)].reshape(number * width, width)

        bias_buf[...] = jnp.zeros_like(bias_buf)
        for ref, start in ((b_query_ref, 0), (b_value_ref, 2 * width)):
            parts = [ref[part, head, pl.ds(layer, 1), :] for part in range(tp_size) for head in range(ref.shape[1])]
            bias_buf[:, pl.ds(start, width)] = jnp.concatenate(parts, axis=1)
        def one_row(row, carry):
            key_ok = lax.broadcasted_iota(jnp.int32, (1, seq), 1) < lens_ref[mine * own_rows + row]

            def project(index, carry):
                rows = span(index, size)
                normed = norm(hidden_ref[row, rows, :].astype(F32), 2 * layer)
                qkv_ref[rows, :] = (dot_t(normed, pack_rows(0, 3)) + bias_buf[...]).astype(BF16)
                return carry

            lax.fori_loop(0, blocks, project, 0)

            def attend(block, carry):
                rows = span(block, size)

                def heads(index, carry):
                    lanes = pl.multiple_of(index * pair, pair)
                    query = qkv_ref[rows, pl.ds(lanes, pair)]
                    keys = qkv_ref[:, pl.ds(pl.multiple_of(lanes + width, pair), pair)]
                    values = qkv_ref[:, pl.ds(pl.multiple_of(lanes + 2 * width, pair), pair)]
                    result = None
                    for head in range(2):
                        scores = dot_t(jnp.where(lane_head == head, query, jnp.zeros_like(query)), keys)
                        scores = jnp.where(key_ok, scores, -1e30)
                        top = jnp.max(scores, axis=-1, keepdims=True)
                        weights = jnp.exp2((scores - top) * factor)
                        scale = 1.0 / jnp.sum(weights, axis=-1, keepdims=True)
                        part = jnp.dot((weights * scale).astype(BF16), values, preferred_element_type=F32)
                        result = part if result is None else jnp.where(lane_head == head, part, result)
                    context_ref[:, pl.ds(lanes, pair)] = result.astype(BF16)
                    return carry

                lax.fori_loop(0, width // pair, heads, 0)
                projected = jnp.dot(context_ref[...], pack_rows(3, 1), preferred_element_type=F32)
                hidden = (hidden_ref[row, rows, :].astype(F32) + projected + b_out_ref[pl.ds(layer, 1), :]).astype(BF16)
                hidden_ref[row, rows, :] = hidden
                if layer:
                    all_buf[mine, row, block] = norm(hidden.astype(F32), 2 * layer + 1)
                    ring(row, 0, block, mine).start()
                return carry

            lax.fori_loop(0, blocks, attend, 0)
            return carry

        lax.fori_loop(0, own_rows, one_row, 0)

    attention(0, first_ref)

    for later_along, later_across, kept in spreads:
        for copy, onward in zip(later_along, later_across[1:]):
            copy.wait()
            onward.start()
        for copy in kept:
            copy.wait()
    for _, later_across, _ in spreads[:2]:
        for copy in later_across:
            copy.wait()

    def as_row(ref):
        return jnp.concatenate([ref[pl.ds(part, 1), :] for part in range(ref.shape[0])], axis=1)

    def dense(index, carry):
        row, rows = index // blocks, span(index % blocks, size)
        value = hidden_ref[row, rows, :].astype(F32)
        normed = norm(value, 1)
        total = value + as_row(b_fc2_ref)
        for part in range(tp_size):
            cols = fc1_ref[part].reshape(-1, width)
            inner = jnp.maximum(dot_t(normed, cols) + as_row(b_fc1_ref.at[part]), 0.0).astype(BF16)
            total += jnp.dot(inner, fc2_ref[part].reshape(-1, width), preferred_element_type=F32)
        hidden_ref[row, rows, :] = total.astype(BF16)
        return carry

    lax.fori_loop(0, own_rows * blocks, dense, 0)
    for copy in spreads[2][1]:
        copy.wait()
    attention(1, second_ref)

    token = lax.broadcasted_iota(jnp.int32, (1, size), 1)
    slot_count, _ = o_ref.shape
    some = min(512, slot_count)

    def dispatch(index, chunks, fresh):
        def part(part, carry):
            at = span(part, some)
            total = None if fresh else o_ref[at, :].astype(F32)
            for way in range(ways):
                base = chunks[way] * own_tokens + (way * count + index) * size
                hot = jnp.where(source_ref[at, :] == token + base, 1.0, 0.0).astype(BF16)
                taken = jnp.dot(hot, all_buf[chunks[way], way, index], preferred_element_type=F32)
                total = taken if total is None else total + taken
            o_ref[at, :] = total.astype(BF16)
            return carry

        lax.fori_loop(0, slot_count // some, part, 0)

    dispatch(0, (mine, mine), True)

    def own(index, carry):
        dispatch(index, (mine, mine), False)
        return carry

    lax.fori_loop(1, count, own, 0)
    keep_hidden.start()
    keep_other.start()
    for hop in range(1, tp_size):
        def arrive(index, carry):
            chunks = [behind(way, hop) for way in range(ways)]
            for way in range(ways):
                ring(way, hop - 1, index, chunks[way]).wait_recv()
                if hop < hops:
                    ring(way, hop, index, chunks[way]).start()
            dispatch(index, chunks, False)
            return carry

        lax.fori_loop(0, count, arrive, 0)
        if hop == hops - 1:
            for copy in moves[-one:]:
                copy.start()

    def drain(index, carry):
        for way in range(ways):
            for hop in range(hops):
                ring(way, hop, index, mine).wait_send()
        return carry

    lax.fori_loop(0, count, drain, 0)
    keep_rows.start()
    for copy in [*moves, keep_hidden, keep_other, keep_rows]:
        copy.wait()


def front(lens, index, gain, shift, b_out, b_fc2, x, w_in, w_out, own, biases, num_experts, capacity, head_dim, tp_size, ep_size, pieces, call_id):
    own_experts = w_in.shape[0] // tp_size
    blocks = own_experts * ep_size
    packs, cut, width = own.shape
    rows, seq, _ = x.shape
    own_rows = rows // tp_size
    size = min(256, seq)
    count = seq // size
    slots = blocks * capacity
    per = ep_size // packs

    def vmem(*shape, dtype=BF16):
        return pltpu.VMEM(shape, dtype)

    moved = landings(tp_size, w_in, pieces)
    b_exp = jax.ShapeDtypeStruct((tp_size,) + biases[3].shape, F32)
    pack = vmem(packs, tp_size, per, cut, width)
    piece_dma, gather_dma, ring_dma = DMA((len(pieces), tp_size - 1)), DMA((packs + len(biases), tp_size + 1)), DMA((own_rows, tp_size - 1, count))
    return pl.pallas_call(
        functools.partial(front_body, tp_size, ep_size, pieces, own_experts, head_dim),
        out_shape=(jax.ShapeDtypeStruct((2 * rows * seq // 128, 128), jnp.int32), jax.ShapeDtypeStruct((slots, width), BF16), jax.ShapeDtypeStruct((slots, 1), jnp.int32),
                   jax.ShapeDtypeStruct((own_rows, seq, width), BF16), b_exp, *moved),
        in_specs=[SMEM_SPEC] + [VMEM_SPEC] * 5 + [HBM_SPEC] * (4 + len(biases)), out_specs=[VMEM_SPEC] + [HBM_SPEC] * (4 + len(pieces)),
        scratch_shapes=[vmem(slots, width), vmem(slots, 1, dtype=jnp.int32), vmem(own_rows, seq, width), vmem(tp_size, *biases[0].shape, dtype=F32), vmem(tp_size, *biases[1].shape, dtype=F32), vmem(tp_size, *biases[2].shape, dtype=F32), pack, pack,
                        vmem(packs - 1, tp_size, cut, width), vmem(tp_size, ep_size, cut, width), vmem(tp_size, ep_size, cut, width), vmem(slots, 1, dtype=jnp.int32),
                        vmem(3 * capacity, num_experts, dtype=F32), vmem(1, 3 * width, dtype=F32), vmem(seq, 3 * width), vmem(size, width),
                        vmem(tp_size, own_rows, count, size, width), DMA((4,)), piece_dma, piece_dma, gather_dma, gather_dma, DMA((2, packs, ep_size)), ring_dma, ring_dma],
        compiler_params=settings(call_id, 62), cost_estimate=cost(100), name='front')(lens, index, gain, shift, b_out, b_fc2, x, w_in, w_out, own, *biases)


def experts_body(tp_size, ep_size, early, late, dispatch_ref, early_refs, w_in_ref, w_out_ref, b_in_ref, b_out_ref, w_router_ref, other_in, returned_ref, gates_out,
                 other_ref, gates_ref, sent_buf, arrived_ref, parts_buf, own_buf, out_buf, local_sem, send_sem, recv_sem, back_send, back_recv, move_send, move_recv):
    chunks, _, slots, width = arrived_ref.shape
    me = lax.axis_index('ep')
    mine = lax.axis_index('tp')
    weights = (w_in_ref, w_out_ref)
    units = [(chunk, which) for chunk in range(chunks) for which in range(2)]

    sends = {}
    for chunk in range(chunks):
        for distance in range(1, ep_size):
            peer = away('ep', ep_size, distance)
            sends[chunk, distance] = pltpu.make_async_remote_copy(
                src_ref=dispatch_ref.at[chunk, peer], dst_ref=arrived_ref.at[chunk, me], send_sem=send_sem.at[chunk, distance], recv_sem=recv_sem.at[chunk, distance],
                device_id={'ep': peer}, device_id_type=MESH)

    def landing(piece):
        chunk, which, start, cols = piece
        return parts_buf.at[units.index((chunk, which)), :, :, pl.ds(start, cols)]

    moves = {piece: exchange(tp_size, weights, piece, landing(piece), move_send.at[index], move_recv.at[index]) for index, piece in enumerate(late)}
    kept = [pltpu.make_async_copy(dispatch_ref.at[chunk, me], arrived_ref.at[chunk, me], local_sem.at[0, chunk]) for chunk in range(chunks)]
    owns = {unit: pltpu.make_async_copy(weights[unit[1]].at[unit[0] * tp_size + mine], own_buf.at[unit[0], unit[1]], local_sem.at[1 + unit[1], unit[0]]) for unit in units}
    earlies = {piece: pltpu.make_async_copy(early_refs[index], landing(piece), local_sem.at[3, index]) for index, piece in enumerate(early)}

    enter([('tp', tp_size), ('ep', ep_size)])
    for piece in late:
        for copy in moves[piece]:
            copy.start()
    for chunk in range(chunks):
        for distance in range(1, ep_size):
            sends[chunk, distance].start()
        kept[chunk].start()
    for unit in units:
        owns[unit].start()
        for piece in early:
            if piece[:2] == unit:
                earlies[piece].start()

    lane = lax.broadcasted_iota(jnp.int32, (1, w_router_ref.shape[1]), 1)
    group = lax.broadcasted_iota(jnp.int32, (ep_size * slots, 1), 0) // slots

    def load(chunk):
        return pltpu.make_async_copy(dispatch_ref.at[chunk], sent_buf.at[chunk % 2], local_sem.at[5, chunk % 2])

    load_other = pltpu.make_async_copy(other_in, other_ref, local_sem.at[5, 2])
    keep_gates = pltpu.make_async_copy(gates_ref, gates_out, local_sem.at[5, 3])
    load(0).start()
    load_other.start()
    load_other.wait()
    for chunk in range(chunks):
        if chunk + 1 < chunks:
            load(chunk + 1).start()
        load(chunk).wait()
        logits = jnp.dot(sent_buf[chunk % 2].reshape(ep_size * slots, width), w_router_ref[...].astype(BF16), preferred_element_type=F32)
        rows = pl.ds(chunk * ep_size * slots, ep_size * slots)
        own = jnp.sum(jnp.where(lane == group * (chunks * tp_size) + (chunk * tp_size + mine), logits, 0.0), axis=1, keepdims=True)
        other = jnp.sum(jnp.where(lane == other_ref[rows, :], logits, 0.0), axis=1, keepdims=True)
        gates_ref[rows, :] = jax.nn.sigmoid(own - other)

    def part_ref(unit, part):
        if part == 0:
            return own_buf.at[unit[0], unit[1]]
        return parts_buf.at[units.index(unit), part - 1]

    def give_back(chunk, slot, index, cols):
        for half in range(2):
            peer = 2 * index + half
            distance = lax.rem(peer - me + ep_size, ep_size)

            @pl.when(distance == 0)
            def _():
                pltpu.make_async_copy(out_buf.at[slot, peer, :, cols], returned_ref.at[chunk, me, :, cols], local_sem.at[4, chunk]).start()

            @pl.when(distance != 0)
            def _():
                pltpu.make_async_remote_copy(
                    src_ref=out_buf.at[slot, peer, :, cols], dst_ref=returned_ref.at[chunk, me, :, cols], send_sem=back_send.at[chunk, distance], recv_sem=back_recv.at[chunk, distance],
                    device_id={'ep': peer}, device_id_type=MESH).start()

    def weights_here(chunk, which, cols=None):
        unit = (chunk, which)
        if cols is None or cols.start == 0:
            owns[unit].wait()
            for piece in early:
                if piece[:2] == unit:
                    earlies[piece].wait()
        for piece in late:
            if piece[:2] == unit and (cols is None or piece[2] == cols.start):
                for copy in moves[piece]:
                    copy.wait_recv()

    def expert_row(chunk):
        return pl.ds(chunk * tp_size + mine, 1)

    def inner_part(chunk, index, part):
        tokens = arrived_ref[chunk, pl.ds(2 * index, 2)].reshape(2 * slots, width)
        inner = jnp.dot(tokens, part_ref((chunk, 0), part)[...], preferred_element_type=F32) + b_in_ref[away('tp', tp_size, tp_size - part), expert_row(chunk), :]
        return jnp.maximum(inner, 0.0).astype(BF16)

    backs = {}
    for chunk in range(chunks):
        last = chunk == chunks - 1
        slot = chunk % out_buf.shape[0]
        for distance in range(1, ep_size):
            sends[chunk, distance].wait_recv()
        kept[chunk].wait()
        weights_here(chunk, 0)
        before = chunk - out_buf.shape[0]
        if before >= 0:
            for copy in backs[before][:-1]:
                copy.wait_send()
            backs[before][-1].wait()

        held = [sent_buf.at[0], sent_buf.at[1], arrived_ref.at[0], arrived_ref.at[1]]
        if last:
            def first_product(index, carry):
                for part in range(tp_size):
                    held[part][pl.ds(2 * index, 2)] = inner_part(chunk, index, part).reshape(2, slots, width)
                return carry

            lax.fori_loop(0, ep_size // 2, first_product, 0)
        for cols in ([pl.ds(piece[2], piece[3]) for piece in late if piece[:2] == (chunk, 1)] if last else [pl.ds(0, width)]):
            weights_here(chunk, 1, cols if last else None)

            def rows(index, carry):
                total = jnp.zeros((2 * slots, cols.size), F32)
                for part in range(tp_size):
                    inner = held[part][pl.ds(2 * index, 2)].reshape(2 * slots, width) if last else inner_part(chunk, index, part)
                    total += jnp.dot(inner, part_ref((chunk, 1), part)[:, cols], preferred_element_type=F32)
                out_buf[slot, pl.ds(2 * index, 2), :, cols] = (total + b_out_ref[expert_row(chunk), cols]).astype(BF16).reshape(2, slots, cols.size)

                @pl.when(index > 0)
                def _():
                    give_back(chunk, slot, index - 1, cols)

                return carry

            lax.fori_loop(0, ep_size // 2, rows, 0)
            give_back(chunk, slot, ep_size // 2 - 1, cols)
        backs[chunk] = []
        for distance in range(1, ep_size):
            peer = away('ep', ep_size, distance)
            backs[chunk].append(pltpu.make_async_remote_copy(
                src_ref=out_buf.at[slot, peer], dst_ref=returned_ref.at[chunk, me], send_sem=back_send.at[chunk, distance], recv_sem=back_recv.at[chunk, distance],
                device_id={'ep': peer}, device_id_type=MESH))
        backs[chunk].append(pltpu.make_async_copy(out_buf.at[slot, me], returned_ref.at[chunk, me], local_sem.at[4, chunk]))

    keep_gates.start()
    for chunk in range(chunks):
        for distance in range(1, ep_size):
            sends[chunk, distance].wait_send()
        for copy in backs[chunk][:-1]:
            copy.wait_recv()
            if chunk + out_buf.shape[0] >= chunks:
                copy.wait_send()
        if chunk + out_buf.shape[0] >= chunks:
            backs[chunk][-1].wait()
    for piece in late:
        for copy in moves[piece]:
            copy.wait_send()
    keep_gates.wait()


def experts(dispatch, early_weights, w_in, w_out, b_in, b_out, w_router, other, tp_size, ep_size, early, late, call_id):
    chunks, _, slots, width = dispatch.shape
    hidden = w_in.shape[2]

    def body(dispatch_ref, *refs):
        experts_body(tp_size, ep_size, early, late, dispatch_ref, refs[:len(early)], *refs[len(early):])

    return pl.pallas_call(
        body, out_shape=(jax.ShapeDtypeStruct(dispatch.shape, BF16), jax.ShapeDtypeStruct(other.shape, F32)),
        in_specs=[HBM_SPEC] * (3 + len(early)) + [VMEM_SPEC] * 3 + [HBM_SPEC], out_specs=(HBM_SPEC, HBM_SPEC),
        scratch_shapes=[pltpu.VMEM(other.shape, jnp.int32), pltpu.VMEM(other.shape, F32), pltpu.VMEM((2,) + dispatch.shape[1:], BF16), pltpu.VMEM(dispatch.shape, BF16), pltpu.VMEM((2 * chunks, tp_size - 1, width, hidden), BF16),
                        pltpu.VMEM((chunks, 2, width, hidden), BF16), pltpu.VMEM((2, ep_size, slots, width), BF16),
                        DMA((6, max(chunks, len(early)))), DMA((chunks, ep_size)), DMA((chunks, ep_size)), DMA((chunks, ep_size)), DMA((chunks, ep_size)),
                        DMA((len(late), tp_size - 1)), DMA((len(late), tp_size - 1))],
        compiler_params=settings(call_id, 62),
        cost_estimate=cost(30),
        name='experts')(dispatch, *early_weights, w_in, w_out, b_in, b_out, w_router, other)


def finish_body(tp_size, count, table_in, gates_in, outputs_ref, hidden_ref, o_ref, table_ref, gates_ref, slots_buf, wide_ref, stage_ref, first_buf, hidden_buf, sum_buf, own_buf,
                load_sem, slots_sem, sum_send, sum_recv, out_send, out_recv):
    me = lax.axis_index('tp')
    own_tokens, width = hidden_ref.shape
    tokens = tp_size * own_tokens
    size = own_tokens // (2 * count)
    hops = tp_size - 1
    lanes = 128
    columns = [slice(start, start + lanes) for start in range(0, width, lanes)]

    def rows(way, chunk, index):
        return pl.ds(pl.multiple_of(chunk * own_tokens + (way * count + index) * size, size), size)

    def behind(way, distance):
        return away('tp', tp_size, (tp_size - distance) % tp_size if way == 0 else distance % tp_size)

    def ahead(way):
        return {'tp': away('tp', tp_size, 1 if way == 0 else tp_size - 1)}

    def send_sum(way, hop, index, src_ref):
        return pltpu.make_async_remote_copy(
            src_ref=src_ref, dst_ref=sum_buf.at[way, hop, index], send_sem=sum_send.at[way, hop, index], recv_sem=sum_recv.at[way, hop, index],
            device_id=ahead(way), device_id_type=MESH)

    def send_out(way, hop, index, src_ref, chunk):
        return pltpu.make_async_remote_copy(
            src_ref=src_ref, dst_ref=o_ref.at[rows(way, chunk, index)], send_sem=out_send.at[way, hop, index], recv_sem=out_recv.at[way, hop, index],
            device_id=ahead(way), device_id_type=MESH)

    slots = outputs_ref.shape[0]
    parts = slots_sem.shape[0]
    part_slots = slots // parts
    piece = min(128, part_slots)
    loads = [pltpu.make_async_copy(outputs_ref.at[span(part, part_slots)], slots_buf.at[span(part, part_slots)], slots_sem.at[part]) for part in range(parts)]
    load_hidden = pltpu.make_async_copy(hidden_ref, hidden_buf, load_sem.at[2])
    load_gates = pltpu.make_async_copy(gates_in, gates_ref, load_sem.at[3])
    load_table = pltpu.make_async_copy(table_in, table_ref, load_sem.at[4])
    for load in [load_gates, *loads, load_table, load_hidden]:
        load.start()
    enter([('tp', tp_size)])
    wide_ref[slots] = jnp.zeros(wide_ref.shape[1:], F32)
    flat_ref = wide_ref.reshape((slots + 1) * 8, lanes)

    def widen(index, carry):
        at = span(index, piece)
        for column, cols in enumerate(columns):
            flat_ref[pl.ds(index * (piece * 8) + column, piece, stride=8), :] = slots_buf[at, cols].astype(F32) * gates_ref[at, :]
        return carry

    load_gates.wait()
    for part, load in enumerate(loads):
        load.wait()
        lax.fori_loop(part * (part_slots // piece), (part + 1) * (part_slots // piece), widen, 0)

    def combine(way, chunk, index):
        base = chunk * own_tokens + (way * count + index) * size
        batch = 16

        def some(part, carry):
            first = part * batch
            for u in range(batch):
                slot_of = [table_ref[choice * tokens + base + first + u] for choice in range(2)]
                stage_ref[way, pl.ds(pl.multiple_of((first + u) * 8, 8), 8), :] = wide_ref[slot_of[0]] + wide_ref[slot_of[1]]
            return carry

        lax.fori_loop(0, size // batch, some, 0)

    def staged(way, column):
        return stage_ref[way, pl.ds(column, size, stride=8), :]

    def first(index, carry):
        for way in range(2):
            combine(way, behind(way, 1), index)
            for column, cols in enumerate(columns):
                first_buf[way, index, :, cols] = staged(way, column).astype(BF16)
            send_sum(way, 0, index, first_buf.at[way, index]).start()
        return carry

    load_table.wait()
    lax.fori_loop(0, count, first, 0)
    load_hidden.wait()

    def keep(way, index):
        return pltpu.make_async_copy(own_buf.at[way, index], o_ref.at[rows(way, me, index)], load_sem.at[way])

    for hop in range(1, tp_size):
        def add(index, carry):
            for way in range(2):
                combine(way, behind(way, hop + 1), index)
            for way in range(2):
                send_sum(way, hop - 1, index, sum_buf.at[way, hop - 1, index]).wait_recv()
                own_rows = pl.ds(pl.multiple_of((way * count + index) * size, size), size)
                for column, cols in enumerate(columns):
                    total = (sum_buf[way, hop - 1, index, :, cols].astype(F32) + staged(way, column)).astype(BF16)
                    if hop < hops:
                        sum_buf[way, hop - 1, index, :, cols] = total
                    else:
                        own_buf[way, index, :, cols] = (total.astype(F32) + hidden_buf[own_rows, cols].astype(F32)).astype(BF16)
            for way in range(2):
                if hop < hops:
                    send_sum(way, hop, index, sum_buf.at[way, hop - 1, index]).start()
                else:
                    send_out(way, 0, index, own_buf.at[way, index], me).start()
                    keep(way, index).start()
                    keep(way, index).wait()
            return carry

        lax.fori_loop(0, count, add, 0)

    for hop in range(1, tp_size):
        def forward(index, carry):
            for way in range(2):
                chunk = behind(way, hop)
                arrived = o_ref.at[rows(way, chunk, index)]
                send_out(way, hop - 1, index, arrived, chunk).wait_recv()
                if hop < hops:
                    send_out(way, hop, index, arrived, chunk).start()
            return carry

        lax.fori_loop(0, count, forward, 0)

    def drain(index, carry):
        for way in range(2):
            for hop in range(hops):
                send_sum(way, hop, index, sum_buf.at[way, hop, index]).wait_send()
                send_out(way, hop, index, own_buf.at[way, index], me).wait_send()
        return carry

    lax.fori_loop(0, count, drain, 0)


def finish(table, gates, outputs, hidden, tp_size, call_id):
    slots, width = outputs.shape
    own_tokens = hidden.shape[0]
    size = min(256, own_tokens // 2)
    count = own_tokens // (2 * size)
    hops = tp_size - 1
    pieces = (2, count, size, width)
    ring = DMA((2, hops, count))

    def vmem(*shape, dtype=BF16):
        return pltpu.VMEM(shape, dtype)

    return pl.pallas_call(
        functools.partial(finish_body, tp_size, count), out_shape=jax.ShapeDtypeStruct((tp_size * own_tokens, width), BF16),
        in_specs=[HBM_SPEC] * 4, out_specs=HBM_SPEC,
        scratch_shapes=[pltpu.SMEM(table.shape, jnp.int32), vmem(slots, 1, dtype=F32), vmem(slots, width), vmem(slots + 1, 8, 128, dtype=F32), vmem(2, size * 8, 128, dtype=F32), vmem(*pieces), vmem(own_tokens, width),
                        vmem(2, hops, *pieces[1:]), vmem(*pieces), DMA((5,)), DMA((4,)), ring, ring, ring, ring],
        compiler_params=settings(call_id), cost_estimate=cost(100), name='finish')(table, gates, outputs, hidden)


def solution(mesh):
    tp_size = mesh.shape['tp']
    ep_size = mesh.shape['ep']

    def local_fn(x, src_len, expert_idx, ln_gain, ln_bias, w_query, b_query, w_key, w_value, b_value, w_attn_out, b_attn_out, w_fc1, b_fc1, w_fc2, b_fc2, w_router, w_exp_in, b_exp_in, w_exp_out, b_exp_out):
        rows, seq, width = x.shape
        tokens = rows * seq
        num_experts = w_router.shape[1]
        capacity = 2 * (-(-tokens // num_experts))
        local_experts = w_exp_in.shape[0]
        own_experts = local_experts // tp_size
        _, _, local_heads, head_dim = w_query.shape
        head_cols = local_heads * head_dim

        def pack_attention(j):
            columns = [w[j].reshape(width, head_cols).T for w in (w_query, w_key, w_value)]
            return jnp.concatenate(columns + [w_attn_out[j].reshape(head_cols, width)], axis=0)

        def own_slice(value):
            size = value.shape[0] // ep_size
            return lax.dynamic_slice_in_dim(value, lax.axis_index('ep') * size, size, 0)

        own = jnp.stack([own_slice(value) for value in (pack_attention(0), w_fc1.T, w_fc2, pack_attention(1))])

        def piece(code):
            chunk, which, *part = map(int, code)
            size = width // 3 if part else width
            return chunk, which, sum(part) * size, size

        plan = ['210', '00', '01', '10', '11', '200', '201', '202'], ['211', '212', '30', '310', '311', '312']
        early, late = [[piece(code) for code in codes] for codes in plan]
        weights = w_exp_in, w_exp_out
        biases = b_query.transpose(1, 0, 2), b_value.transpose(1, 0, 2), b_fc1.reshape(-1, 128), b_exp_in
        table, dispatch, other, hidden, b_exp_in, *moved = front(
            src_len, expert_idx.transpose(0, 2, 1), ln_gain, ln_bias, b_attn_out, b_fc2.reshape(-1, 128), x, *weights, own, biases, num_experts, capacity, head_dim, tp_size, ep_size, early, 0)
        dispatch = dispatch.reshape(own_experts, ep_size, capacity, width)
        outputs, gates = experts(dispatch, moved, *weights, b_exp_in, b_exp_out, w_router, other, tp_size, ep_size, early, late, 1)
        return finish(table.reshape(-1), gates, outputs.reshape(-1, width), hidden.reshape(-1, width), tp_size, 2).reshape(rows, seq, width)

    axes = {'g': ('dp', 'ep'), 'e': 'ep', 't': 'tp', '.': None}

    def spec(code):
        return P(*[axes[letter] for letter in code])

    codes = ['g..', 'g', 'g..', '..', '..', '..t.', '.t.', '..t.', '..t.', '.t.', '.t..', '..', '.t', 't', 't.', '.', '..', 'e.t', 'et', 'et.', 'e.']
    in_specs = tuple(map(spec, codes))
    return jax.shard_map(local_fn, mesh=mesh, in_specs=in_specs, out_specs=spec('g..'), check_vma=False)
```
